8 devices in a mesh: dp: 1 (over z), sp: 8 (over y, x, core).
Axes of the slice: x: 2, y: 2, z: 1, core: 2. Of those that a mesh axis runs over, the one named last changes fastest.
Arguments:
- hidden_in: bfloat16 [4, 1024, 4096], P('dp', 'sp')
- pos_ids: int32 [4, 1024], P('dp', 'sp')
- block_pos: int32 [4, 1024], P('dp', 'sp')
- prefix_len: int32 [4], P('dp')
- ln_gamma: bfloat16 [4096], replicated
- ln_beta: bfloat16 [4096], replicated
- w_qkv: bfloat16 [4096, 12288], replicated
- b_qkv: bfloat16 [12288], replicated
- w_o: bfloat16 [4096, 4096], replicated
- b_o: bfloat16 [4096], replicated
- grad_out: bfloat16 [4, 1024, 4096], P('dp', 'sp')
Outputs:
- output 1: bfloat16 [4, 1024, 4096], P('dp', 'sp')
- output 2: bfloat16 [4, 1024, 4096], P('dp', 'sp')
- output 3: float32 [4096], P('dp')
- output 4: float32 [4096], P('dp')
- output 5: float32 [4096, 12288], P('dp')
- output 6: float32 [12288], P('dp')
- output 7: float32 [4096, 4096], P('dp')
- output 8: float32 [4096], P('dp')
All inputs are finite; a program needn't handle non-finite values.
Results may differ from the reference program's by a relative error of at most 0.0110327.
Values are sent between devices in bfloat16 or wider.
A program may use at most 1.75 GiB of HBM per device.

```python
import math
import jax
import jax.numpy as jnp
from jax import lax

BATCH = 4
SEQ = 1024
HEADS = 32
HEAD = 128
HIDDEN = 4096
QUARTER = HEAD // 4
ALPHA = math.sqrt(56.0)
LN_EPS = 1e-5
ROT_BASE = 10000.0
SCALE = 1.0 / math.sqrt(HEAD)
MASK_FILL = -1e30


def query_block(n_query, row_count):
    blk_size = math.gcd(n_query, 512)
    while blk_size > 8 and blk_size * row_count * SEQ > 2 ** 24:
        blk_size = blk_size // 2
    return blk_size


def position_ids(prefix_len):
    tok_index = jnp.arange(SEQ, dtype=jnp.int32)[None, :]
    prefix_col = prefix_len[:, None]
    in_prefix = tok_index < prefix_col
    pos_ids = jnp.where(in_prefix, tok_index, prefix_col - 1)
    block_pos = jnp.where(in_prefix, 0, tok_index - prefix_col + 1)
    return pos_ids.astype(jnp.int32), block_pos.astype(jnp.int32)


def setup_inputs(seed: int = 0, part: int = 0) -> dict:
    part_keys = jax.random.split(jax.random.fold_in(jax.random.key(seed), part), 3)
    weight_keys = jax.random.split(jax.random.key(seed + 1), 6)
    prefix_len = jax.random.randint(part_keys[0], (BATCH,), SEQ // 4, 3 * SEQ // 4 + 1, dtype=jnp.int32)
    pos_ids, block_pos = position_ids(prefix_len)
    hidden_in = jax.random.normal(part_keys[1], (BATCH, SEQ, HIDDEN), jnp.float32)
    grad_out = jax.random.normal(part_keys[2], (BATCH, SEQ, HIDDEN), jnp.float32)
    ln_gamma = 1.0 + 0.3 * jax.random.normal(weight_keys[0], (HIDDEN,), jnp.float32)
    ln_beta = 0.3 * jax.random.normal(weight_keys[1], (HIDDEN,), jnp.float32)
    w_qkv = jax.random.normal(weight_keys[2], (HIDDEN, 3 * HIDDEN), jnp.float32) * HIDDEN ** -0.5
    slot_scale = jnp.array([0.5, 0.5, SEQ ** -0.5], jnp.float32)
    b_qkv = (jax.random.normal(weight_keys[3], (HEADS, 3, HEAD), jnp.float32) * slot_scale[:, None]).reshape(3 * HIDDEN)
    w_o = jax.random.normal(weight_keys[4], (HIDDEN, HIDDEN), jnp.float32) * (0.5 * ALPHA * math.sqrt(SEQ) * HIDDEN ** -0.5)
    b_o = 0.5 * ALPHA * jax.random.normal(weight_keys[5], (HIDDEN,), jnp.float32)
    return {
        'hidden_in': hidden_in.astype(jnp.bfloat16),
        'pos_ids': pos_ids,
        'block_pos': block_pos,
        'prefix_len': prefix_len,
        'ln_gamma': ln_gamma.astype(jnp.bfloat16),
        'ln_beta': ln_beta.astype(jnp.bfloat16),
        'w_qkv': w_qkv.astype(jnp.bfloat16),
        'b_qkv': b_qkv.astype(jnp.bfloat16),
        'w_o': w_o.astype(jnp.bfloat16),
        'b_o': b_o.astype(jnp.bfloat16),
        'grad_out': grad_out.astype(jnp.bfloat16),
    }


def layer_norm(x_val, ln_gain, ln_shift):
    row_mean = jnp.mean(x_val, axis=-1, keepdims=True)
    centered = x_val - row_mean
    row_var = jnp.mean(centered * centered, axis=-1, keepdims=True)
    return centered * lax.rsqrt(row_var + LN_EPS) * ln_gain + ln_shift


def rope_tables(pos_ids, block_pos):
    inv_freq = ROT_BASE ** (-jnp.arange(QUARTER, dtype=jnp.float32) / QUARTER)
    angles = jnp.stack([pos_ids, block_pos], axis=-1).astype(jnp.float32)[..., None] * inv_freq
    return jnp.cos(angles), jnp.sin(angles)


def rotate(vals, cos_tab, sin_tab, direction):
    shaped = vals.reshape(vals.shape[:3] + (2, 2, QUARTER))
    half_a = shaped[..., 0, :]
    half_b = shaped[..., 1, :]
    cos_b = cos_tab[:, :, None]
    sin_b = direction * sin_tab[:, :, None]
    rotated = jnp.stack([half_a * cos_b - half_b * sin_b, half_b * cos_b + half_a * sin_b], axis=-2)
    return rotated.reshape(vals.shape)


def block_probs(q_blk, key_rot, prefix_len, row_start):
    scores = jnp.einsum('bqhd,bkhd->bhqk', q_blk, key_rot) * SCALE
    query_idx = row_start + jnp.arange(q_blk.shape[1])
    key_idx = jnp.arange(key_rot.shape[1])
    allowed = (key_idx[None, None, :] < prefix_len[:, None, None]) | (key_idx[None, None, :] <= query_idx[None, :, None])
    scores = jnp.where(allowed[:, None], scores, MASK_FILL)
    row_max = jnp.max(scores, axis=-1, keepdims=True)
    exp_scores = jnp.exp(scores - row_max)
    return exp_scores / jnp.sum(exp_scores, axis=-1, keepdims=True)


def reference(hidden_in, pos_ids, block_pos, prefix_len, ln_gamma, ln_beta, w_qkv, b_qkv, w_o, b_o, grad_out):
    normed_f, norm_vjp = jax.vjp(layer_norm, hidden_in.astype(jnp.float32), ln_gamma.astype(jnp.float32), ln_beta.astype(jnp.float32))
    flat_n = normed_f.astype(jnp.bfloat16).reshape(BATCH * SEQ, HIDDEN)
    pre_qkv = jnp.dot(flat_n, w_qkv, preferred_element_type=jnp.float32) + b_qkv.astype(jnp.float32)
    pre_qkv = pre_qkv.reshape(BATCH, SEQ, HEADS, 3, HEAD)
    cos_tab, sin_tab = rope_tables(pos_ids, block_pos)
    q_rot = rotate(pre_qkv[:, :, :, 0], cos_tab, sin_tab, 1.0).astype(jnp.bfloat16).astype(jnp.float32)
    k_rot = rotate(pre_qkv[:, :, :, 1], cos_tab, sin_tab, 1.0).astype(jnp.bfloat16).astype(jnp.float32)
    v_val = pre_qkv[:, :, :, 2].astype(jnp.bfloat16).astype(jnp.float32)
    q_size = query_block(SEQ, BATCH * HEADS)
    n_blocks = SEQ // q_size

    def fwd_block(blk_index):
        row_start = blk_index * q_size
        q_blk = lax.dynamic_slice_in_dim(q_rot, row_start, q_size, axis=1)
        probs = block_probs(q_blk, k_rot, prefix_len, row_start)
        probs_b = probs.astype(jnp.bfloat16).astype(jnp.float32)
        return jnp.einsum('bhqk,bkhd->bqhd', probs_b, v_val).astype(jnp.bfloat16)

    ctx_blocks = lax.map(fwd_block, jnp.arange(n_blocks))
    ctx = jnp.moveaxis(ctx_blocks, 0, 1).reshape(BATCH * SEQ, HIDDEN)
    out_f = jnp.dot(ctx, w_o, preferred_element_type=jnp.float32) + b_o.astype(jnp.float32)
    hidden_out = (ALPHA * flat_n.astype(jnp.float32) + out_f).astype(jnp.bfloat16).reshape(BATCH, SEQ, HIDDEN)

    flat_dy = grad_out.reshape(BATCH * SEQ, HIDDEN)
    grad_bo = jnp.sum(flat_dy.astype(jnp.float32), axis=0)
    grad_wo = jnp.dot(ctx.T, flat_dy, preferred_element_type=jnp.float32)
    d_ctx = jnp.dot(flat_dy, w_o.T, preferred_element_type=jnp.float32).astype(jnp.bfloat16)
    d_ctx = d_ctx.astype(jnp.float32).reshape(BATCH, SEQ, HEADS, HEAD)
    ctx_f = ctx.astype(jnp.float32).reshape(BATCH, SEQ, HEADS, HEAD)

    def bwd_block(carry, blk_index):
        dk_acc, dv_acc = carry
        row_start = blk_index * q_size
        q_blk = lax.dynamic_slice_in_dim(q_rot, row_start, q_size, axis=1)
        ctx_blk = lax.dynamic_slice_in_dim(ctx_f, row_start, q_size, axis=1)
        grad_blk = lax.dynamic_slice_in_dim(d_ctx, row_start, q_size, axis=1)
        probs = block_probs(q_blk, k_rot, prefix_len, row_start)
        probs_b = probs.astype(jnp.bfloat16).astype(jnp.float32)
        dv_acc = dv_acc + jnp.einsum('bhqk,bqhd->bkhd', probs_b, grad_blk)
        d_prob = jnp.einsum('bqhd,bkhd->bhqk', grad_blk, v_val)
        row_delta = jnp.einsum('bqhd,bqhd->bhq', grad_blk, ctx_blk)
        d_score = (probs * (d_prob - row_delta[..., None]) * SCALE).astype(jnp.bfloat16).astype(jnp.float32)
        dq_blk = jnp.einsum('bhqk,bkhd->bqhd', d_score, k_rot)
        dk_acc = dk_acc + jnp.einsum('bhqk,bqhd->bkhd', d_score, q_blk)
        return (dk_acc, dv_acc), dq_blk.astype(jnp.bfloat16)

    zero_acc = jnp.zeros((BATCH, SEQ, HEADS, HEAD), jnp.float32)
    (dk_sum, dv_sum), dq_blocks = lax.scan(bwd_block, (zero_acc, zero_acc), jnp.arange(n_blocks))
    d_q = jnp.moveaxis(dq_blocks, 0, 1).reshape(BATCH, SEQ, HEADS, HEAD).astype(jnp.float32)
    d_k = dk_sum.astype(jnp.bfloat16).astype(jnp.float32)
    d_v = dv_sum.astype(jnp.bfloat16).astype(jnp.float32)
    g_pre = jnp.stack([rotate(d_q, cos_tab, sin_tab, -1.0), rotate(d_k, cos_tab, sin_tab, -1.0), d_v], axis=3)
    g_pre = g_pre.reshape(BATCH * SEQ, 3 * HIDDEN)
    grad_bqkv = jnp.sum(g_pre, axis=0)
    g_pre_b = g_pre.astype(jnp.bfloat16)
    grad_wqkv = jnp.dot(flat_n.T, g_pre_b, preferred_element_type=jnp.float32)
    d_norm = jnp.dot(g_pre_b, w_qkv.T, preferred_element_type=jnp.float32) + ALPHA * flat_dy.astype(jnp.float32)
    d_x, grad_gamma, grad_beta = norm_vjp(d_norm.reshape(BATCH, SEQ, HIDDEN))
    grad_in = d_x.astype(jnp.bfloat16)
    return (hidden_out, grad_in, grad_gamma, grad_beta, grad_wqkv, grad_bqkv, grad_wo, grad_bo)
```

```python
import functools
import math
import jax
import jax.numpy as jnp
from jax import lax
from jax.experimental import pallas as pl
from jax.experimental.pallas import tpu as pltpu
from jax.sharding import PartitionSpec as P

HEAD = 128
QUARTER = 32
ALPHA = math.sqrt(56.0)
LN_EPS = 1e-5
ROT_BASE = 10000.0
SCALE = 1.0 / math.sqrt(HEAD)
LOG2E = math.log2(math.e)
MASK_FILL = -1e30
BLK = 256
MIB = 1 << 20
F32 = jnp.float32
BF16 = jnp.bfloat16


def dot(lhs, rhs, lhs_dim, rhs_dim):
    return lax.dot_general(lhs, rhs, (((lhs_dim,), (rhs_dim,)), ((), ())), preferred_element_type=F32)


def cost(flops, nbytes, transcendentals=0):
    return pl.CostEstimate(flops=int(flops), bytes_accessed=int(nbytes), transcendentals=int(transcendentals))


def layer_norm(x_val, ln_gain, ln_shift):
    row_mean = jnp.mean(x_val, axis=-1, keepdims=True)
    centered = x_val - row_mean
    row_var = jnp.mean(centered * centered, axis=-1, keepdims=True)
    return centered * lax.rsqrt(row_var + LN_EPS) * ln_gain + ln_shift


def rope_tables(prefix_len, seq):
    tok = jnp.arange(seq, dtype=jnp.int32)[None, :]
    pre = prefix_len[:, None]
    inside = tok < pre
    pos = jnp.where(inside, tok, pre - 1)
    blk = jnp.where(inside, 0, tok - pre + 1)
    inv_freq = ROT_BASE ** (-jnp.arange(QUARTER, dtype=F32) / QUARTER)
    angles = jnp.stack([pos, blk], axis=-1).astype(F32)[..., None] * inv_freq
    cos, sin = jnp.cos(angles), jnp.sin(angles)
    shape = pos.shape + (HEAD,)
    return (jnp.stack([cos, cos], axis=-2).reshape(shape), jnp.stack([-sin, sin], axis=-2).reshape(shape))


def turn(x, cos, sin):
    lane = lax.broadcasted_iota(jnp.int32, x.shape, 1)
    other = jnp.where(lane % (2 * QUARTER) < QUARTER, pltpu.roll(x, HEAD - QUARTER, 1), pltpu.roll(x, QUARTER, 1))
    return x * cos + other * sin


def qkv_kernel(me_ref, n_ref, w_ref, b_ref, cos_ref, sin_ref, q_ref, k_ref, v_ref):
    rows = cos_ref.shape[1]
    x = n_ref[...].reshape(rows, n_ref.shape[-1])
    cos, sin = cos_ref[0], sin_ref[0]
    pre = dot(x, w_ref[...], 1, 0) + b_ref[...].astype(F32)
    for h in range(q_ref.shape[0]):
        base = 3 * h * HEAD
        q_ref[h, 0] = turn(pre[:, base:base + HEAD], cos, sin).astype(BF16)
        k_ref[h, 0] = turn(pre[:, base + HEAD:base + 2 * HEAD], cos, sin).astype(BF16)
        v_ref[h, 0] = pre[:, base + 2 * HEAD:base + 3 * HEAD].astype(BF16)


def project_qkv(me, n_all, w_qkv, b_qkv, cos, sin):
    n_dev, batch, local_len, hidden = n_all.shape
    seq = n_dev * local_len
    cols = w_qkv.shape[1] // n_dev
    own = cols // (3 * HEAD)
    per = 2
    rows = per * local_len
    out = jax.ShapeDtypeStruct((own, batch, seq, HEAD), BF16)
    out_spec = pl.BlockSpec((own, 1, rows, HEAD), lambda b, j, me: (0, b, j, 0))
    tab_spec = pl.BlockSpec((1, rows, HEAD), lambda b, j, me: (b, j, 0))
    return pl.pallas_call(
        qkv_kernel,
        grid_spec=pltpu.PrefetchScalarGridSpec(
            num_scalar_prefetch=1,
            grid=(batch, n_dev // per),
            in_specs=[
                pl.BlockSpec((per, 1, local_len, hidden), lambda b, j, me: (j, b, 0, 0)),
                pl.BlockSpec((hidden, cols), lambda b, j, me: (0, me[0])),
                pl.BlockSpec((1, cols), lambda b, j, me: (0, me[0])),
                tab_spec, tab_spec,
            ],
            out_specs=[out_spec] * 3,
        ),
        out_shape=[out] * 3,
        compiler_params=pltpu.CompilerParams(vmem_limit_bytes=56 * MIB),
        cost_estimate=cost(2 * batch * seq * hidden * cols, 2 * (batch * seq * hidden + hidden * cols + batch * seq * cols)),
        name='qkv',
    )(me, n_all, w_qkv, b_qkv.reshape(1, -1), cos, sin)


def forward_kernel(pre_ref, q_ref, k_ref, v_ref, ctx_ref, lse_ref):
    seq = q_ref.shape[2]
    local_len = ctx_ref.shape[2]
    per = BLK // local_len
    prefix = pre_ref[pl.program_id(1)]

    def block(r, n_key):
        q_blk = q_ref[0, 0, r * BLK:(r + 1) * BLK]
        query = lax.broadcasted_iota(jnp.int32, (1, BLK), 1) + r * BLK
        last = jnp.maximum(query, prefix - 1)
        parts = []
        for c in range(n_key):
            part = dot(k_ref[0, 0, c * BLK:(c + 1) * BLK], q_blk, 1, 1) * (SCALE * LOG2E)
            if c >= r:
                key = lax.broadcasted_iota(jnp.int32, (BLK, BLK), 0) + c * BLK
                part = jnp.where(key <= last, part, MASK_FILL)
            parts.append(part)
        top = functools.reduce(jnp.maximum, [jnp.max(p, axis=0, keepdims=True) for p in parts])
        parts = [jnp.exp2(p - top) for p in parts]
        total = functools.reduce(jnp.add, [jnp.sum(p, axis=0, keepdims=True) for p in parts])
        inv = 1.0 / total
        probs = jnp.concatenate([(p * inv).astype(BF16) for p in parts], axis=0)
        ctx_t = dot(v_ref[0, 0, :n_key * BLK], probs, 0, 0)
        ctx_ref[r * per:(r + 1) * per, 0] = ctx_t.T.astype(BF16).reshape(per, local_len, HEAD)
        lse_ref[0, 0, :, r * BLK:(r + 1) * BLK] = top + jnp.log2(total)

    n_blk = seq // BLK
    for r in range(n_blk):
        for n_key in range(r + 1, n_blk + 1):
            low = (n_key - 1) * BLK
            cond = prefix <= n_key * BLK if n_key == r + 1 else prefix > low
            if n_key < n_blk and n_key > r + 1:
                cond = jnp.logical_and(cond, prefix <= n_key * BLK)
            if n_key == n_blk and n_key == r + 1:
                block(r, n_key)
            else:
                pl.when(cond)(functools.partial(block, r, n_key))


def attention_forward(prefix_len, q, k, v, n_dev):
    own, batch, seq, _ = q.shape
    local_len = seq // n_dev
    qkv_spec = pl.BlockSpec((1, 1, seq, HEAD), lambda h, b, pre: (h, b, 0, 0))
    return pl.pallas_call(
        forward_kernel,
        grid_spec=pltpu.PrefetchScalarGridSpec(
            num_scalar_prefetch=1,
            grid=(own, batch),
            in_specs=[qkv_spec] * 3,
            out_specs=[
                pl.BlockSpec((n_dev, 1, local_len, HEAD), lambda h, b, pre: (0, b, 0, h)),
                pl.BlockSpec((1, 1, 1, seq), lambda h, b, pre: (h, b, 0, 0)),
            ],
        ),
        out_shape=[
            jax.ShapeDtypeStruct((n_dev, batch, local_len, own * HEAD), BF16),
            jax.ShapeDtypeStruct((own, batch, 1, seq), F32),
        ],
        compiler_params=pltpu.CompilerParams(vmem_limit_bytes=32 * MIB),
        cost_estimate=cost(8 * own * batch * seq * seq * HEAD, 8 * own * batch * seq * HEAD, own * batch * seq * seq),
        name='attn_fwd',
    )(prefix_len, q, k, v)


def backward_kernel(pre_ref, q_ref, k_ref, v_ref, ctx_ref, dctx_ref, lse_ref, cos_ref, sin_ref, g_ref, sum_ref, dq_acc, dk_acc, dv_acc):
    seq = q_ref.shape[2]
    n_dev, _, local_len, _ = g_ref.shape
    n_blk = seq // BLK
    prefix = pre_ref[pl.program_id(0)]
    d_ctx = dctx_ref[...].reshape(seq, HEAD)
    prod = d_ctx.astype(F32) * ctx_ref[...].reshape(seq, HEAD).astype(F32)
    delta = jnp.sum(prod.T, axis=0, keepdims=True)

    def block(c, first):
        keys = k_ref[0, 0, c * BLK:(c + 1) * BLK]
        vals = v_ref[0, 0, c * BLK:(c + 1) * BLK]
        start = first * BLK
        q_part = q_ref[0, 0, start:]
        g_part = d_ctx[start:]
        s_t = dot(keys, q_part, 1, 1)
        dp_t = dot(vals, g_part, 1, 1)
        probs, d_scores = [], []
        for r in range(first, n_blk):
            lo = r * BLK
            piece = s_t[:, lo - start:lo - start + BLK] * (SCALE * LOG2E)
            if r <= c:
                key = lax.broadcasted_iota(jnp.int32, (BLK, BLK), 0) + c * BLK
                query = lax.broadcasted_iota(jnp.int32, (1, BLK), 1) + lo
                piece = jnp.where(key <= jnp.maximum(query, prefix - 1), piece, MASK_FILL)
            p = jnp.exp2(piece - lse_ref[0, 0, :, lo:lo + BLK])
            probs.append(p.astype(BF16))
            d_p = dp_t[:, lo - start:lo - start + BLK] - delta[:, lo:lo + BLK]
            d_scores.append((p * d_p * SCALE).astype(BF16))
        probs = jnp.concatenate(probs, axis=1)
        d_scores = jnp.concatenate(d_scores, axis=1)
        dv_acc[c * BLK:(c + 1) * BLK] = dot(probs, g_part, 1, 0)
        dk_acc[c * BLK:(c + 1) * BLK] = dot(d_scores, q_part, 1, 0)
        dq_part = dot(keys, d_scores, 0, 0)
        if c == 0:
            dq_acc[...] = dq_part
        else:
            dq_acc[:, start:] += dq_part

    block(0, 0)
    for c in range(1, n_blk):
        pl.when(prefix > c * BLK)(functools.partial(block, c, 0))
        pl.when(prefix <= c * BLK)(functools.partial(block, c, c))

    cos, sin = cos_ref[0], sin_ref[0]
    g_q = turn(dq_acc[...].T.astype(BF16).astype(F32), cos, -sin)
    g_k = turn(dk_acc[...].astype(BF16).astype(F32), cos, -sin)
    g_v = dv_acc[...].astype(BF16).astype(F32)
    for i, g in enumerate((g_q, g_k, g_v)):
        g_ref[:, 0, :, i * HEAD:(i + 1) * HEAD] = g.astype(BF16).reshape(n_dev, local_len, HEAD)
        sum_ref[0, :, i * HEAD:(i + 1) * HEAD] = jnp.sum(g, axis=0, keepdims=True)


def attention_backward(head, prefix_len, q, k, v, ctx, d_ctx, lse, cos, sin):
    _, batch, seq, _ = q.shape
    n_dev, _, local_len, _ = ctx.shape
    qkv_spec = pl.BlockSpec((1, 1, seq, HEAD), lambda b, pre: (head, b, 0, 0))
    tok_spec = pl.BlockSpec((n_dev, 1, local_len, HEAD), lambda b, pre: (0, b, 0, head))
    tab_spec = pl.BlockSpec((1, seq, HEAD), lambda b, pre: (b, 0, 0))
    return pl.pallas_call(
        backward_kernel,
        grid_spec=pltpu.PrefetchScalarGridSpec(
            num_scalar_prefetch=1,
            grid=(batch,),
            in_specs=[qkv_spec] * 3 + [tok_spec, tok_spec, pl.BlockSpec((1, 1, 1, seq), lambda b, pre: (head, b, 0, 0)), tab_spec, tab_spec],
            out_specs=[
                pl.BlockSpec((n_dev, 1, local_len, 3 * HEAD), lambda b, pre: (0, b, 0, 0)),
                pl.BlockSpec((1, 1, 3 * HEAD), lambda b, pre: (b, 0, 0)),
            ],
            scratch_shapes=[pltpu.VMEM((HEAD, seq), F32), pltpu.VMEM((seq, HEAD), F32), pltpu.VMEM((seq, HEAD), F32)],
        ),
        out_shape=[
            jax.ShapeDtypeStruct((n_dev, batch, local_len, 3 * HEAD), BF16),
            jax.ShapeDtypeStruct((batch, 1, 3 * HEAD), F32),
        ],
        compiler_params=pltpu.CompilerParams(vmem_limit_bytes=40 * MIB),
        cost_estimate=cost(20 * batch * seq * seq * HEAD, 20 * batch * seq * HEAD, batch * seq * seq),
        name='attn_bwd',
    )(prefix_len, q, k, v, ctx, d_ctx, lse, cos, sin)


def wo_grad_kernel(ctx_ref, dy_ref, out_ref):
    out_ref[...] = dot(ctx_ref[0], dy_ref[...], 0, 0)


def weight_grad_o(ctx_all, dy_all):
    n_dev, tokens, cols = ctx_all.shape
    hidden = dy_all.shape[1]
    wide = hidden // 4
    return pl.pallas_call(
        wo_grad_kernel,
        grid=(hidden // wide, n_dev),
        in_specs=[
            pl.BlockSpec((1, tokens, cols), lambda n, d: (d, 0, 0)),
            pl.BlockSpec((tokens, wide), lambda n, d: (0, n)),
        ],
        out_specs=pl.BlockSpec((cols, wide), lambda n, d: (d, n)),
        out_shape=jax.ShapeDtypeStruct((n_dev * cols, hidden), F32),
        compiler_params=pltpu.CompilerParams(vmem_limit_bytes=56 * MIB),
        cost_estimate=cost(2 * tokens * n_dev * cols * hidden, 2 * 4 * tokens * n_dev * cols + 2 * tokens * hidden + 4 * hidden * n_dev * cols),
        name='wo_grad',
    )(ctx_all, dy_all)


def wqkv_grad_kernel(head, wide, n_ref, g_ref, *rest):
    out_ref, rhs, buf, sems = rest[-4:]
    half, m = pl.program_id(0), pl.program_id(1)
    n_m = pl.num_programs(1)
    group, _, cols = g_ref.shape
    rows = n_ref.shape[1]
    step = half * n_m + m
    slot = lax.rem(step, 2)

    def copies(at_step, at_slot):
        h, r = at_step // n_m, lax.rem(at_step, n_m)
        for d in range(group):
            col = (h * group + d) * wide + head * cols
            yield pltpu.make_async_copy(
                buf.at[at_slot, :, pl.ds(d * cols, cols)],
                out_ref.at[pl.ds(pl.multiple_of(r * rows, rows), rows), pl.ds(pl.multiple_of(col, HEAD), cols)],
                sems.at[at_slot, d])

    @pl.when(m == 0)
    def _():
        for d in range(group):
            rhs[:, d * cols:(d + 1) * cols] = g_ref[d]

    @pl.when(step >= 2)
    def _():
        for c in copies(step - 2, slot):
            c.wait()

    buf[slot] = dot(n_ref[...], rhs[...], 0, 0)
    for c in copies(step, slot):
        c.start()

    @pl.when(step == 2 * n_m - 1)
    def _():
        for c in copies(step - 1, 1 - slot):
            c.wait()
        for c in copies(step, slot):
            c.wait()


def weight_grad_qkv(head, own, n_flat, g_all, partial):
    tokens, hidden = n_flat.shape
    n_dev, _, cols = g_all.shape
    group = n_dev // 2
    wide = own * cols
    rows = BLK
    any_spec = pl.BlockSpec(memory_space=pl.ANY)
    args, specs, alias = [n_flat, g_all], [
        pl.BlockSpec((tokens, rows), lambda s, m: (0, m)),
        pl.BlockSpec((group, tokens, cols), lambda s, m: (s, 0, 0)),
    ], {}
    if partial is not None:
        args.append(partial)
        specs.append(any_spec)
        alias = {2: 0}
    return pl.pallas_call(
        functools.partial(wqkv_grad_kernel, head, wide),
        grid=(2, hidden // rows),
        in_specs=specs,
        out_specs=any_spec,
        out_shape=jax.ShapeDtypeStruct((hidden, n_dev * wide), F32),
        scratch_shapes=[
            pltpu.VMEM((tokens, group * cols), BF16),
            pltpu.VMEM((2, rows, group * cols), F32),
            pltpu.SemaphoreType.DMA((2, group)),
        ],
        input_output_aliases=alias,
        compiler_params=pltpu.CompilerParams(vmem_limit_bytes=60 * MIB),
        cost_estimate=cost(2 * tokens * hidden * n_dev * cols, 4 * tokens * hidden + 2 * n_dev * tokens * cols + 4 * hidden * n_dev * cols),
        name='wqkv_grad',
    )(*args)


def solution(mesh):
    n_dev = mesh.shape['sp']
    tok_spec = P('dp', 'sp', None)
    pos_spec = P('dp', 'sp')
    in_specs = (tok_spec, pos_spec, pos_spec, P('dp'), P(), P(), P(), P(), P(), P(), tok_spec)
    out_specs = (tok_spec, tok_spec, P('dp'), P('dp'), P('dp', None), P('dp'), P('dp', None), P('dp'))

    def device_step(hidden_in, pos_ids, block_pos, prefix_len, ln_gamma, ln_beta, w_qkv, b_qkv, w_o, b_o, grad_out):
        batch, local_len, hidden = hidden_in.shape
        own = hidden // HEAD // n_dev
        rows = batch * local_len
        tokens = n_dev * rows
        rank = lax.axis_index('sp')
        me = rank.reshape(1).astype(jnp.int32)
        normed_f, norm_vjp = jax.vjp(layer_norm, hidden_in.astype(F32), ln_gamma.astype(F32), ln_beta.astype(F32))
        normed = normed_f.astype(BF16)
        n_all = lax.all_gather(normed, 'sp')
        dy_all = lax.all_gather(grad_out, 'sp')
        cos, sin = rope_tables(prefix_len, n_dev * local_len)

        q, k, v = project_qkv(me, n_all, w_qkv, b_qkv, cos, sin)
        ctx, lse = attention_forward(prefix_len, q, k, v, n_dev)
        ctx_all = lax.all_gather(ctx.reshape(tokens, own * HEAD), 'sp')

        w_o_own = lax.dynamic_slice_in_dim(w_o, rank * (own * HEAD), own * HEAD, axis=0)
        d_ctx = jnp.einsum('dbtc,hc->dbth', dy_all, w_o_own, preferred_element_type=F32).astype(BF16)
        g_parts, g_sums = [], []
        for head in range(own):
            g, g_sum = attention_backward(head, prefix_len, q, k, v, ctx, d_ctx, lse, cos, sin)
            g_parts.append(lax.all_gather(g.reshape(tokens, 3 * HEAD), 'sp'))
            g_sums.append(jnp.sum(g_sum, axis=(0, 1)))
        grad_bqkv = lax.all_gather(jnp.concatenate(g_sums), 'sp').reshape(-1)

        dy_flat = dy_all.reshape(tokens, hidden)
        grad_bo = jnp.sum(dy_flat.astype(F32), axis=0)
        grad_wo = weight_grad_o(ctx_all, dy_flat)
        ctx_tok = lax.dynamic_slice_in_dim(ctx_all, rank * rows, rows, axis=1)
        ctx_tok = jnp.transpose(ctx_tok, (1, 0, 2)).reshape(batch, local_len, hidden)
        out_f = jnp.einsum('bsh,hc->bsc', ctx_tok, w_o, preferred_element_type=F32) + b_o.astype(F32)
        hidden_out = (ALPHA * normed.astype(F32) + out_f).astype(BF16)

        n_flat = n_all.reshape(tokens, hidden)
        grad_wqkv = None
        for head in range(own):
            grad_wqkv = weight_grad_qkv(head, own, n_flat, g_parts[head], grad_wqkv)

        g_tok = [lax.dynamic_slice_in_dim(g, rank * rows, rows, axis=1) for g in g_parts]
        g_tok = jnp.transpose(jnp.stack(g_tok, axis=1), (2, 0, 1, 3)).reshape(batch, local_len, 3 * hidden)
        d_norm = jnp.einsum('bsc,hc->bsh', g_tok, w_qkv, preferred_element_type=F32) + ALPHA * grad_out.astype(F32)
        d_x, grad_gamma, grad_beta = norm_vjp(d_norm)
        grad_gamma, grad_beta = lax.psum((grad_gamma, grad_beta), 'sp')
        return (hidden_out, d_x.astype(BF16), grad_gamma, grad_beta, grad_wqkv, grad_bqkv, grad_wo, grad_bo)

    return jax.shard_map(device_step, mesh=mesh, in_specs=in_specs, out_specs=out_specs, check_vma=False)
```

```python
import functools
import math
import jax
import jax.numpy as jnp
from jax import lax
from jax.experimental import pallas as pl
from jax.experimental.pallas import tpu as pltpu
from jax.sharding import PartitionSpec as P

HEAD = 128
QUARTER = 32
ALPHA = math.sqrt(56.0)
LN_EPS = 1e-5
ROT_BASE = 10000.0
SCALE = 1.0 / math.sqrt(HEAD)
LOG2E = math.log2(math.e)
MASK_FILL = -1e30
BLK = 256
MIB = 1 << 20
F32 = jnp.float32
BF16 = jnp.bfloat16


def dot(lhs, rhs, lhs_dim, rhs_dim):
    return lax.dot_general(lhs, rhs, (((lhs_dim,), (rhs_dim,)), ((), ())), preferred_element_type=F32)


def cost(flops, nbytes, transcendentals=0):
    return pl.CostEstimate(flops=int(flops), bytes_accessed=int(nbytes), transcendentals=int(transcendentals))


def layer_norm(x_val, ln_gain, ln_shift):
    row_mean = jnp.mean(x_val, axis=-1, keepdims=True)
    centered = x_val - row_mean
    row_var = jnp.mean(centered * centered, axis=-1, keepdims=True)
    return centered * lax.rsqrt(row_var + LN_EPS) * ln_gain + ln_shift


def rope_tables(prefix_len, seq):
    tok = jnp.arange(seq, dtype=jnp.int32)[None, :]
    pre = prefix_len[:, None]
    inside = tok < pre
    pos = jnp.where(inside, tok, pre - 1)
    blk = jnp.where(inside, 0, tok - pre + 1)
    inv_freq = ROT_BASE ** (-jnp.arange(QUARTER, dtype=F32) / QUARTER)
    angles = jnp.stack([pos, blk], axis=-1).astype(F32)[..., None] * inv_freq
    cos, sin = jnp.cos(angles), jnp.sin(angles)
    shape = pos.shape + (HEAD,)
    return (jnp.stack([cos, cos], axis=-2).reshape(shape), jnp.stack([-sin, sin], axis=-2).reshape(shape))


def turn(x, cos, sin):
    lane = lax.broadcasted_iota(jnp.int32, x.shape, 1)
    other = jnp.where(lane % (2 * QUARTER) < QUARTER, pltpu.roll(x, HEAD - QUARTER, 1), pltpu.roll(x, QUARTER, 1))
    return x * cos + other * sin


def qkv_kernel(me_ref, n_ref, w_ref, b_ref, cos_ref, sin_ref, q_ref, k_ref, v_ref):
    rows = cos_ref.shape[1]
    x = n_ref[...].reshape(rows, n_ref.shape[-1])
    cos, sin = cos_ref[0], sin_ref[0]
    pre = dot(x, w_ref[...], 1, 0) + b_ref[...].astype(F32)
    for h in range(q_ref.shape[0]):
        base = 3 * h * HEAD
        q_ref[h, 0] = turn(pre[:, base:base + HEAD], cos, sin).astype(BF16)
        k_ref[h, 0] = turn(pre[:, base + HEAD:base + 2 * HEAD], cos, sin).astype(BF16)
        v_ref[h, 0] = pre[:, base + 2 * HEAD:base + 3 * HEAD].astype(BF16)


def project_qkv(me, n_all, w_qkv, b_qkv, cos, sin):
    n_dev, batch, local_len, hidden = n_all.shape
    seq = n_dev * local_len
    cols = w_qkv.shape[1] // n_dev
    own = cols // (3 * HEAD)
    per = 2
    rows = per * local_len
    out = jax.ShapeDtypeStruct((own, batch, seq, HEAD), BF16)
    out_spec = pl.BlockSpec((own, 1, rows, HEAD), lambda b, j, me: (0, b, j, 0))
    tab_spec = pl.BlockSpec((1, rows, HEAD), lambda b, j, me: (b, j, 0))
    return pl.pallas_call(
        qkv_kernel,
        grid_spec=pltpu.PrefetchScalarGridSpec(
            num_scalar_prefetch=1,
            grid=(batch, n_dev // per),
            in_specs=[
                pl.BlockSpec((per, 1, local_len, hidden), lambda b, j, me: (j, b, 0, 0)),
                pl.BlockSpec((hidden, cols), lambda b, j, me: (0, me[0])),
                pl.BlockSpec((1, cols), lambda b, j, me: (0, me[0])),
                tab_spec, tab_spec,
            ],
            out_specs=[out_spec] * 3,
        ),
        out_shape=[out] * 3,
        compiler_params=pltpu.CompilerParams(vmem_limit_bytes=56 * MIB),
        cost_estimate=cost(2 * batch * seq * hidden * cols, 2 * (batch * seq * hidden + hidden * cols + batch * seq * cols)),
        name='qkv',
    )(me, n_all, w_qkv, b_qkv.reshape(1, -1), cos, sin)


def forward_kernel(pre_ref, q_ref, k_ref, v_ref, ctx_ref, lse_ref):
    seq = q_ref.shape[2]
    local_len = ctx_ref.shape[2]
    per = BLK // local_len
    prefix = pre_ref[pl.program_id(1)]

    def block(r, n_key):
        q_blk = q_ref[0, 0, r * BLK:(r + 1) * BLK]
        query = lax.broadcasted_iota(jnp.int32, (1, BLK), 1) + r * BLK
        last = jnp.maximum(query, prefix - 1)
        parts = []
        for c in range(n_key):
            part = dot(k_ref[0, 0, c * BLK:(c + 1) * BLK], q_blk, 1, 1) * (SCALE * LOG2E)
            if c >= r:
                key = lax.broadcasted_iota(jnp.int32, (BLK, BLK), 0) + c * BLK
                part = jnp.where(key <= last, part, MASK_FILL)
            parts.append(part)
        top = functools.reduce(jnp.maximum, [jnp.max(p, axis=0, keepdims=True) for p in parts])
        parts = [jnp.exp2(p - top) for p in parts]
        total = functools.reduce(jnp.add, [jnp.sum(p, axis=0, keepdims=True) for p in parts])
        inv = 1.0 / total
        probs = jnp.concatenate([(p * inv).astype(BF16) for p in parts], axis=0)
        ctx_t = dot(v_ref[0, 0, :n_key * BLK], probs, 0, 0)
        ctx_ref[r * per:(r + 1) * per, 0] = ctx_t.T.astype(BF16).reshape(per, local_len, HEAD)
        lse_ref[0, 0, :, r * BLK:(r + 1) * BLK] = top + jnp.log2(total)

    n_blk = seq // BLK
    for r in range(n_blk):
        for n_key in range(r + 1, n_blk + 1):
            low = (n_key - 1) * BLK
            cond = prefix <= n_key * BLK if n_key == r + 1 else prefix > low
            if n_key < n_blk and n_key > r + 1:
                cond = jnp.logical_and(cond, prefix <= n_key * BLK)
            if n_key == n_blk and n_key == r + 1:
                block(r, n_key)
            else:
                pl.when(cond)(functools.partial(block, r, n_key))


def attention_forward(prefix_len, q, k, v, n_dev):
    own, batch, seq, _ = q.shape
    local_len = seq // n_dev
    qkv_spec = pl.BlockSpec((1, 1, seq, HEAD), lambda h, b, pre: (h, b, 0, 0))
    return pl.pallas_call(
        forward_kernel,
        grid_spec=pltpu.PrefetchScalarGridSpec(
            num_scalar_prefetch=1,
            grid=(own, batch),
            in_specs=[qkv_spec] * 3,
            out_specs=[
                pl.BlockSpec((n_dev, 1, local_len, HEAD), lambda h, b, pre: (0, b, 0, h)),
                pl.BlockSpec((1, 1, 1, seq), lambda h, b, pre: (h, b, 0, 0)),
            ],
        ),
        out_shape=[
            jax.ShapeDtypeStruct((n_dev, batch, local_len, own * HEAD), BF16),
            jax.ShapeDtypeStruct((own, batch, 1, seq), F32),
        ],
        compiler_params=pltpu.CompilerParams(vmem_limit_bytes=32 * MIB),
        cost_estimate=cost(8 * own * batch * seq * seq * HEAD, 8 * own * batch * seq * HEAD, own * batch * seq * seq),
        name='attn_fwd',
    )(prefix_len, q, k, v)


def backward_kernel(pre_ref, q_ref, k_ref, v_ref, ctx_ref, dctx_ref, lse_ref, cos_ref, sin_ref, g_ref, sum_ref, dq_acc, dk_acc, dv_acc):
    seq = q_ref.shape[2]
    n_dev, _, local_len, _ = g_ref.shape
    n_blk = seq // BLK
    prefix = pre_ref[pl.program_id(0)]
    d_ctx = dctx_ref[...].reshape(seq, HEAD)
    prod = d_ctx.astype(F32) * ctx_ref[...].reshape(seq, HEAD).astype(F32)
    delta = jnp.sum(prod.T, axis=0, keepdims=True)

    def block(c, first):
        keys = k_ref[0, 0, c * BLK:(c + 1) * BLK]
        vals = v_ref[0, 0, c * BLK:(c + 1) * BLK]
        start = first * BLK
        q_part = q_ref[0, 0, start:]
        g_part = d_ctx[start:]
        s_t = dot(keys, q_part, 1, 1)
        dp_t = dot(vals, g_part, 1, 1)
        probs, d_scores = [], []
        for r in range(first, n_blk):
            lo = r * BLK
            piece = s_t[:, lo - start:lo - start + BLK] * (SCALE * LOG2E)
            if r <= c:
                key = lax.broadcasted_iota(jnp.int32, (BLK, BLK), 0) + c * BLK
                query = lax.broadcasted_iota(jnp.int32, (1, BLK), 1) + lo
                piece = jnp.where(key <= jnp.maximum(query, prefix - 1), piece, MASK_FILL)
            p = jnp.exp2(piece - lse_ref[0, 0, :, lo:lo + BLK])
            probs.append(p.astype(BF16))
            d_p = dp_t[:, lo - start:lo - start + BLK] - delta[:, lo:lo + BLK]
            d_scores.append((p * d_p * SCALE).astype(BF16))
        probs = jnp.concatenate(probs, axis=1)
        d_scores = jnp.concatenate(d_scores, axis=1)
        dv_acc[c * BLK:(c + 1) * BLK] = dot(probs, g_part, 1, 0)
        dk_acc[c * BLK:(c + 1) * BLK] = dot(d_scores, q_part, 1, 0)
        dq_part = dot(keys, d_scores, 0, 0)
        if c == 0:
            dq_acc[...] = dq_part
        else:
            dq_acc[:, start:] += dq_part

    block(0, 0)
    for c in range(1, n_blk):
        pl.when(prefix > c * BLK)(functools.partial(block, c, 0))
        pl.when(prefix <= c * BLK)(functools.partial(block, c, c))

    cos, sin = cos_ref[0], sin_ref[0]
    g_q = turn(dq_acc[...].T.astype(BF16).astype(F32), cos, -sin)
    g_k = turn(dk_acc[...].astype(BF16).astype(F32), cos, -sin)
    g_v = dv_acc[...].astype(BF16).astype(F32)
    for i, g in enumerate((g_q, g_k, g_v)):
        g_ref[:, 0, :, i * HEAD:(i + 1) * HEAD] = g.astype(BF16).reshape(n_dev, local_len, HEAD)
        sum_ref[0, :, i * HEAD:(i + 1) * HEAD] = jnp.sum(g, axis=0, keepdims=True)


def attention_backward(head, prefix_len, q, k, v, ctx, d_ctx, lse, cos, sin):
    _, batch, seq, _ = q.shape
    n_dev, _, local_len, _ = ctx.shape
    qkv_spec = pl.BlockSpec((1, 1, seq, HEAD), lambda b, pre: (head, b, 0, 0))
    tok_spec = pl.BlockSpec((n_dev, 1, local_len, HEAD), lambda b, pre: (0, b, 0, head))
    tab_spec = pl.BlockSpec((1, seq, HEAD), lambda b, pre: (b, 0, 0))
    return pl.pallas_call(
        backward_kernel,
        grid_spec=pltpu.PrefetchScalarGridSpec(
            num_scalar_prefetch=1,
            grid=(batch,),
            in_specs=[qkv_spec] * 3 + [tok_spec, tok_spec, pl.BlockSpec((1, 1, 1, seq), lambda b, pre: (head, b, 0, 0)), tab_spec, tab_spec],
            out_specs=[
                pl.BlockSpec((n_dev, 1, local_len, 3 * HEAD), lambda b, pre: (0, b, 0, 0)),
                pl.BlockSpec((1, 1, 3 * HEAD), lambda b, pre: (b, 0, 0)),
            ],
            scratch_shapes=[pltpu.VMEM((HEAD, seq), F32), pltpu.VMEM((seq, HEAD), F32), pltpu.VMEM((seq, HEAD), F32)],
        ),
        out_shape=[
            jax.ShapeDtypeStruct((n_dev, batch, local_len, 3 * HEAD), BF16),
            jax.ShapeDtypeStruct((batch, 1, 3 * HEAD), F32),
        ],
        compiler_params=pltpu.CompilerParams(vmem_limit_bytes=40 * MIB),
        cost_estimate=cost(20 * batch * seq * seq * HEAD, 20 * batch * seq * HEAD, batch * seq * seq),
        name='attn_bwd',
    )(prefix_len, q, k, v, ctx, d_ctx, lse, cos, sin)


def wo_grad_kernel(core_ref, ctx_ref, dy_ref, out_ref, copy_ref):
    res = dot(ctx_ref[0], dy_ref[...], 0, 0)
    out_ref[...] = res
    copy_ref[...] = res


def weight_grad_o(core, ctx_par, dy_all):
    n_grp, tokens, cols = ctx_par.shape
    hidden = dy_all.shape[1]
    wide = hidden // 4
    return pl.pallas_call(
        wo_grad_kernel,
        grid_spec=pltpu.PrefetchScalarGridSpec(
            num_scalar_prefetch=1,
            grid=(hidden // wide, n_grp),
            in_specs=[
                pl.BlockSpec((1, tokens, cols), lambda n, c, core: (c, 0, 0)),
                pl.BlockSpec((tokens, wide), lambda n, c, core: (0, n)),
            ],
            out_specs=[
                pl.BlockSpec((cols, wide), lambda n, c, core: (2 * c + core[0], n)),
                pl.BlockSpec((cols, wide), lambda n, c, core: (c, n)),
            ],
        ),
        out_shape=[
            jax.ShapeDtypeStruct((2 * n_grp * cols, hidden), F32),
            jax.ShapeDtypeStruct((n_grp * cols, hidden), F32),
        ],
        compiler_params=pltpu.CompilerParams(vmem_limit_bytes=56 * MIB),
        cost_estimate=cost(2 * tokens * n_grp * cols * hidden, 8 * tokens * n_grp * cols + 2 * tokens * hidden + 8 * hidden * n_grp * cols),
        name='wo_grad',
    )(core, ctx_par, dy_all)


def paste_kernel(core_ref, new_ref, old_ref, out_ref):
    out_ref[...] = new_ref[...]


def paste_rows(core, block, whole):
    rows, hidden = block.shape
    n_grp = 4
    cols = rows // n_grp
    return pl.pallas_call(
        paste_kernel,
        grid_spec=pltpu.PrefetchScalarGridSpec(
            num_scalar_prefetch=1,
            grid=(n_grp,),
            in_specs=[pl.BlockSpec((cols, hidden), lambda c, core: (c, 0)), pl.BlockSpec(memory_space=pl.ANY)],
            out_specs=pl.BlockSpec((cols, hidden), lambda c, core: (2 * c + 1 - core[0], 0)),
        ),
        out_shape=jax.ShapeDtypeStruct(whole.shape, F32),
        input_output_aliases={2: 0},
        compiler_params=pltpu.CompilerParams(vmem_limit_bytes=48 * MIB),
        cost_estimate=cost(rows * hidden, 8 * rows * hidden),
        name='paste_wo',
    )(core, block, whole)


def column_copies(src, out_ref, sem_of, row, rows, parity, wide, head, cols, n_grp):
    for c in range(n_grp):
        col = pl.multiple_of((2 * c + parity) * wide + head * cols, HEAD)
        yield pltpu.make_async_copy(
            src.at[:, pl.ds(c * cols, cols)],
            out_ref.at[pl.ds(pl.multiple_of(row, BLK), rows), pl.ds(col, cols)],
            sem_of(c))


def wqkv_grad_kernel(head, wide, has_old, core_ref, n_ref, g_ref, *rest):
    recv_ref = rest[0] if has_old else None
    out_ref, copy_ref, rhs, buf, g_sems, out_sems, copy_sems, paste_sems = rest[-8:]
    m = pl.program_id(0)
    n_m = pl.num_programs(0)
    core = core_ref[0]
    n_grp, _, cols = g_ref.shape
    rows = n_ref.shape[1]
    slot = lax.rem(m, 2)

    def loads():
        for c in range(n_grp):
            yield pltpu.make_async_copy(g_ref.at[c], rhs.at[:, pl.ds(c * cols, cols)], g_sems.at[c])

    def stores(step, at):
        yield from column_copies(buf.at[at], out_ref, lambda c: out_sems.at[at, c], step * rows, rows, core, wide, head, cols, n_grp)
        yield pltpu.make_async_copy(buf.at[at], copy_ref.at[pl.ds(pl.multiple_of(step * rows, BLK), rows)], copy_sems.at[at])

    def pastes():
        return column_copies(recv_ref, out_ref, lambda c: paste_sems.at[c], m * rows, rows, 1 - core, wide, head - 1, cols, n_grp)

    @pl.when(m == 0)
    def _():
        for c in loads():
            c.start()
        for c in loads():
            c.wait()

    if has_old:
        for c in pastes():
            c.start()

    @pl.when(m >= 2)
    def _():
        for c in stores(m - 2, slot):
            c.wait()

    buf[slot] = dot(n_ref[...], rhs[...], 0, 0)
    for c in stores(m, slot):
        c.start()
    if has_old:
        for c in pastes():
            c.wait()

    @pl.when(m == n_m - 1)
    def _():
        for c in stores(m - 1, 1 - slot):
            c.wait()
        for c in stores(m, slot):
            c.wait()


def weight_grad_qkv(core, head, own, n_flat, g_par, recv, whole):
    tokens, hidden = n_flat.shape
    n_grp, _, cols = g_par.shape
    wide = own * cols
    rows = BLK
    any_spec = pl.BlockSpec(memory_space=pl.ANY)
    args, specs, alias = [core, n_flat, g_par], [pl.BlockSpec((tokens, rows), lambda m, core: (0, m)), any_spec], {}
    if recv is not None:
        args += [recv, whole]
        specs += [pl.BlockSpec((rows, n_grp * cols), lambda m, core: (m, 0)), any_spec]
        alias = {4: 0}
    dma = pltpu.SemaphoreType.DMA
    return pl.pallas_call(
        functools.partial(wqkv_grad_kernel, head, wide, recv is not None),
        grid_spec=pltpu.PrefetchScalarGridSpec(
            num_scalar_prefetch=1,
            grid=(hidden // rows,),
            in_specs=specs,
            out_specs=[any_spec, any_spec],
            scratch_shapes=[
                pltpu.VMEM((tokens, n_grp * cols), BF16),
                pltpu.VMEM((2, rows, n_grp * cols), F32),
                dma((n_grp,)), dma((2, n_grp)), dma((2,)), dma((n_grp,)),
            ],
        ),
        out_shape=[
            jax.ShapeDtypeStruct((hidden, 2 * n_grp * wide), F32),
            jax.ShapeDtypeStruct((hidden, n_grp * cols), F32),
        ],
        input_output_aliases=alias,
        compiler_params=pltpu.CompilerParams(vmem_limit_bytes=56 * MIB),
        cost_estimate=cost(2 * tokens * hidden * n_grp * cols, 2 * tokens * hidden + 2 * n_grp * tokens * cols + 16 * hidden * n_grp * cols),
        name='wqkv_grad',
    )(*args)


def paste_columns_kernel(head, wide, n_grp, core_ref, recv_ref, old_ref, out_ref, sems):
    rows, cols = recv_ref.shape[0], recv_ref.shape[1] // n_grp
    row = pl.program_id(0) * rows
    for c in column_copies(recv_ref, out_ref, lambda c: sems.at[c], row, rows, 1 - core_ref[0], wide, head, cols, n_grp):
        c.start()
    for c in column_copies(recv_ref, out_ref, lambda c: sems.at[c], row, rows, 1 - core_ref[0], wide, head, cols, n_grp):
        c.wait()


def paste_columns(core, head, own, recv, whole):
    n_grp = 4
    hidden, block = recv.shape
    rows = 4 * BLK
    any_spec = pl.BlockSpec(memory_space=pl.ANY)
    return pl.pallas_call(
        functools.partial(paste_columns_kernel, head, own * block // n_grp, n_grp),
        grid_spec=pltpu.PrefetchScalarGridSpec(
            num_scalar_prefetch=1,
            grid=(hidden // rows,),
            in_specs=[pl.BlockSpec((rows, block), lambda m, core: (m, 0)), any_spec],
            out_specs=any_spec,
            scratch_shapes=[pltpu.SemaphoreType.DMA((n_grp,))],
        ),
        out_shape=jax.ShapeDtypeStruct(whole.shape, F32),
        input_output_aliases={2: 0},
        compiler_params=pltpu.CompilerParams(vmem_limit_bytes=48 * MIB),
        cost_estimate=cost(hidden * block, 8 * hidden * block),
        name='paste_wqkv',
    )(core, recv, whole)


def normed_grad_kernel(first, core_ref, g_ref, w_ref, init_ref, out_ref):
    j = pl.program_id(1)

    @pl.when(j == 0)
    def _():
        out_ref[...] = init_ref[...].astype(F32) * ALPHA if first else init_ref[...]

    out_ref[...] += dot(g_ref[j], w_ref[...], 1, 1)


def normed_grad(core, part, g_tok, w_qkv, init):
    n_dev, rows, cols = g_tok.shape
    hidden, width = w_qkv.shape
    n_part = width // (n_dev * cols)
    wide = hidden // 4

    def w_index(n, j, core):
        dev = jnp.where(j < n_dev // 2, 2 * j + core[0], 2 * (j - n_dev // 2) + 1 - core[0])
        return n, dev * n_part + part

    return pl.pallas_call(
        functools.partial(normed_grad_kernel, part == 0),
        grid_spec=pltpu.PrefetchScalarGridSpec(
            num_scalar_prefetch=1,
            grid=(hidden // wide, n_dev),
            in_specs=[
                pl.BlockSpec((n_dev, rows, cols), lambda n, j, core: (0, 0, 0)),
                pl.BlockSpec((wide, cols), w_index),
                pl.BlockSpec((rows, wide), lambda n, j, core: (0, n)),
            ],
            out_specs=pl.BlockSpec((rows, wide), lambda n, j, core: (0, n)),
        ),
        out_shape=jax.ShapeDtypeStruct((rows, hidden), F32),
        compiler_params=pltpu.CompilerParams(vmem_limit_bytes=48 * MIB),
        cost_estimate=cost(2 * rows * n_dev * cols * hidden, 2 * n_dev * cols * (rows + hidden) + 8 * rows * hidden),
        name='dn',
    )(core, g_tok, w_qkv, init)


def output_kernel(core_ref, ctx_ref, w_ref, n_ref, b_ref, out_ref, acc):
    j = pl.program_id(1)
    part = dot(ctx_ref[j], w_ref[...], 1, 0)

    @pl.when(j == 0)
    def _():
        acc[...] = part

    @pl.when(j > 0)
    def _():
        acc[...] += part

    @pl.when(j == pl.num_programs(1) - 1)
    def _():
        out_ref[...] = (ALPHA * n_ref[...].astype(F32) + (acc[...] + b_ref[...].astype(F32))).astype(BF16)


def project_out(core, ctx_tok, w_o, normed, b_o):
    n_dev, rows, cols = ctx_tok.shape
    hidden = w_o.shape[1]
    wide = hidden // 4

    def w_index(n, j, core):
        return jnp.where(j < n_dev // 2, 2 * j + core[0], 2 * (j - n_dev // 2) + 1 - core[0]), n

    return pl.pallas_call(
        output_kernel,
        grid_spec=pltpu.PrefetchScalarGridSpec(
            num_scalar_prefetch=1,
            grid=(hidden // wide, n_dev),
            in_specs=[
                pl.BlockSpec((n_dev, rows, cols), lambda n, j, core: (0, 0, 0)),
                pl.BlockSpec((cols, wide), w_index),
                pl.BlockSpec((rows, wide), lambda n, j, core: (0, n)),
                pl.BlockSpec((1, wide), lambda n, j, core: (0, n)),
            ],
            out_specs=pl.BlockSpec((rows, wide), lambda n, j, core: (0, n)),
            scratch_shapes=[pltpu.VMEM((rows, wide), F32)],
        ),
        out_shape=jax.ShapeDtypeStruct((rows, hidden), BF16),
        compiler_params=pltpu.CompilerParams(vmem_limit_bytes=40 * MIB),
        cost_estimate=cost(2 * rows * hidden * hidden, 2 * hidden * hidden + 6 * rows * hidden),
        name='out_proj',
    )(core, ctx_tok, w_o, normed, b_o.reshape(1, -1))


def together(*values):
    return lax.optimization_barrier(values)


def solution(mesh):
    n_dev = mesh.shape['sp']
    tok_spec = P('dp', 'sp', None)
    pos_spec = P('dp', 'sp')
    in_specs = (tok_spec, pos_spec, pos_spec, P('dp'), P(), P(), P(), P(), P(), P(), tok_spec)
    out_specs = (tok_spec, tok_spec, P('dp'), P('dp'), P('dp', None), P('dp'), P('dp', None), P('dp'))

    same_core = [list(range(core, n_dev, 2)) for core in range(2)]
    partners = [(dev, dev ^ 1) for dev in range(n_dev)]

    def device_step(hidden_in, pos_ids, block_pos, prefix_len, ln_gamma, ln_beta, w_qkv, b_qkv, w_o, b_o, grad_out):
        batch, local_len, hidden = hidden_in.shape
        own = hidden // HEAD // n_dev
        rows = batch * local_len
        tokens = n_dev * rows
        rank = lax.axis_index('sp')
        me = rank.reshape(1).astype(jnp.int32)
        core = lax.rem(me, 2)
        gather_core = functools.partial(lax.all_gather, axis_name='sp', axis_index_groups=same_core)
        to_partner = functools.partial(lax.ppermute, axis_name='sp', perm=partners)
        pair = rank + 1 - 2 * lax.rem(rank, 2)

        def token_rows(par):
            mine = lax.dynamic_slice_in_dim(par, rank * rows, rows, axis=1)
            theirs = lax.dynamic_slice_in_dim(par, pair * rows, rows, axis=1)
            return mine, to_partner(theirs)

        normed_f, norm_vjp = jax.vjp(layer_norm, hidden_in.astype(F32), ln_gamma.astype(F32), ln_beta.astype(F32))
        normed = normed_f.astype(BF16)
        n_send, dy_send = together(normed, grad_out)
        n_all = lax.all_gather(n_send, 'sp')
        dy_all = lax.all_gather(dy_send, 'sp')
        cos, sin = rope_tables(prefix_len, n_dev * local_len)

        q, k, v = project_qkv(me, n_all, w_qkv, b_qkv, cos, sin)
        ctx, lse = attention_forward(prefix_len, q, k, v, n_dev)
        ctx_par = gather_core(ctx.reshape(tokens, own * HEAD))

        w_o_own = lax.dynamic_slice_in_dim(w_o, rank * (own * HEAD), own * HEAD, axis=0)
        d_ctx = jnp.einsum('dbtc,hc->dbth', dy_all, w_o_own, preferred_element_type=F32).astype(BF16)
        g_own, g_sums = [], []
        for head in range(own):
            g, g_sum = attention_backward(head, prefix_len, q, k, v, ctx, d_ctx, lse, cos, sin)
            g_own.append(g.reshape(tokens, 3 * HEAD))
            g_sums.append(jnp.sum(g_sum, axis=(0, 1)))
        ctx_par, *g_own = together(ctx_par, *g_own)
        g_par = [gather_core(g) for g in g_own]

        dy_flat = dy_all.reshape(tokens, hidden)
        n_flat = n_all.reshape(tokens, hidden)
        ctx_mine, ctx_theirs = token_rows(ctx_par)
        grad_wo, wo_block = weight_grad_o(core, ctx_par, dy_flat)
        ctx_tok, wo_block = together(jnp.concatenate([ctx_mine, ctx_theirs], axis=0), wo_block)
        wo_recv = to_partner(wo_block)
        hidden_out = project_out(core, ctx_tok, w_o, normed.reshape(rows, hidden), b_o)

        g_tok = [token_rows(g) for g in g_par]

        def token_part(first):
            half = [jnp.concatenate([g_tok[first][side], g_tok[first + 1][side]], axis=2) for side in range(2)]
            return jnp.concatenate(half, axis=0)

        n_flat, hidden_out = together(n_flat, hidden_out)
        grad_wqkv, block = weight_grad_qkv(core, 0, own, n_flat, g_par[0], None, None)
        wo_recv, block = together(wo_recv, block)
        recv = to_partner(block)
        grad_wo = paste_rows(core, wo_recv, grad_wo)
        n_flat, grad_wo = together(n_flat, grad_wo)
        grad_wqkv, block = weight_grad_qkv(core, 1, own, n_flat, g_par[1], recv, grad_wqkv)
        g_first, block = together(token_part(0), block)
        recv = to_partner(block)
        d_norm = normed_grad(core, 0, g_first, w_qkv, grad_out.reshape(rows, hidden))
        n_flat, d_norm = together(n_flat, d_norm)
        grad_wqkv, block = weight_grad_qkv(core, 2, own, n_flat, g_par[2], recv, grad_wqkv)
        recv = to_partner(block)
        grad_wqkv, block = weight_grad_qkv(core, 3, own, n_flat, g_par[3], recv, grad_wqkv)
        g_last, block = together(token_part(2), block)
        recv = to_partner(block)
        d_norm = normed_grad(core, 1, g_last, w_qkv, d_norm)
        d_x, grad_gamma, grad_beta = norm_vjp(d_norm.reshape(batch, local_len, hidden))
        grad_in = d_x.astype(BF16)
        grad_bo = jnp.sum(grad_out.astype(F32), axis=(0, 1))
        small = lax.all_gather(jnp.concatenate(g_sums + [grad_gamma, grad_beta, grad_bo]), 'sp')
        recv, small = together(recv, small)
        grad_bqkv = small[:, :3 * own * HEAD].reshape(-1)
        grad_gamma, grad_beta, grad_bo = jnp.sum(small[:, 3 * own * HEAD:], axis=0).reshape(3, hidden)
        grad_wqkv = paste_columns(core, 3, own, recv, grad_wqkv)
        return (hidden_out.reshape(batch, local_len, hidden), grad_in, grad_gamma, grad_beta, grad_wqkv, grad_bqkv, grad_wo, grad_bo)

    return jax.shard_map(device_step, mesh=mesh, in_specs=in_specs, out_specs=out_specs, check_vma=False)
```

```python
import functools
import math
import jax
import jax.numpy as jnp
from jax import lax
from jax.experimental import pallas as pl
from jax.experimental.pallas import tpu as pltpu
from jax.sharding import PartitionSpec as P

HEAD = 128
QUARTER = 32
ALPHA = math.sqrt(56.0)
LN_EPS = 1e-5
ROT_BASE = 10000.0
SCALE = 1.0 / math.sqrt(HEAD)
LOG2E = math.log2(math.e)
MASK_FILL = -1e30
BLK = 256
MIB = 1 << 20
SHARED = 8
WIDTH = 3 * HEAD
F32 = jnp.float32
BF16 = jnp.bfloat16


def dot(lhs, rhs, lhs_dim, rhs_dim):
    return lax.dot_general(lhs, rhs, (((lhs_dim,), (rhs_dim,)), ((), ())), preferred_element_type=F32)


def cost(flops, nbytes, transcendentals=0):
    return pl.CostEstimate(flops=int(flops), bytes_accessed=int(nbytes), transcendentals=int(transcendentals))


def layer_norm(x_val, ln_gain, ln_shift):
    row_mean = jnp.mean(x_val, axis=-1, keepdims=True)
    centered = x_val - row_mean
    row_var = jnp.mean(centered * centered, axis=-1, keepdims=True)
    return centered * lax.rsqrt(row_var + LN_EPS) * ln_gain + ln_shift


def rope_tables(prefix_len, seq):
    tok = jnp.arange(seq, dtype=jnp.int32)[None, :]
    pre = prefix_len[:, None]
    inside = tok < pre
    pos = jnp.where(inside, tok, pre - 1)
    blk = jnp.where(inside, 0, tok - pre + 1)
    inv_freq = ROT_BASE ** (-jnp.arange(QUARTER, dtype=F32) / QUARTER)
    angles = jnp.stack([pos, blk], axis=-1).astype(F32)[..., None] * inv_freq
    cos, sin = jnp.cos(angles), jnp.sin(angles)
    shape = pos.shape + (HEAD,)
    return (jnp.stack([cos, cos], axis=-2).reshape(shape), jnp.stack([-sin, sin], axis=-2).reshape(shape))


def turn(x, cos, sin):
    lane = lax.broadcasted_iota(jnp.int32, x.shape, 1)
    other = jnp.where(lane % (2 * QUARTER) < QUARTER, pltpu.roll(x, HEAD - QUARTER, 1), pltpu.roll(x, QUARTER, 1))
    return x * cos + other * sin


def dma_sems(*shape):
    return pltpu.SemaphoreType.DMA(shape)


def qkv_kernel(n_dist, me_ref, n_ref, w_ref, b_ref, cos_ref, sin_ref, qd_ref, kd_ref, vd_ref, qr_ref, kr_ref, vr_ref, w_buf, sems):
    rows = cos_ref.shape[1]
    hidden = n_ref.shape[-1]
    dist = n_dist * WIDTH
    first = jnp.logical_and(pl.program_id(0) == 0, pl.program_id(1) == 0)
    n_piece = sems.shape[0]
    piece = hidden // n_piece
    starts = (me_ref[0], me_ref[1])

    def loads(i):
        span = pl.ds(i * piece, piece)
        yield pltpu.make_async_copy(w_ref.at[span, pl.ds(pl.multiple_of(starts[0], HEAD), dist)], w_buf.at[span, pl.ds(0, dist)], sems.at[i, 0])
        shared = w_buf.shape[1] - dist
        yield pltpu.make_async_copy(w_ref.at[span, pl.ds(pl.multiple_of(starts[1], HEAD), shared)], w_buf.at[span, pl.ds(dist, shared)], sems.at[i, 1])

    @pl.when(first)
    def _():
        for i in range(n_piece):
            for c in loads(i):
                c.start()
        for i in range(n_piece):
            for c in loads(i):
                c.wait()

    x = n_ref[...].reshape(rows, hidden)
    cos, sin = cos_ref[0], sin_ref[0]
    pre = dot(x, w_buf[...], 1, 0) + b_ref[...]
    n_shared = qr_ref.shape[0]
    for h in range(n_dist + n_shared):
        q_ref, k_ref, v_ref, at = (qd_ref, kd_ref, vd_ref, h) if h < n_dist else (qr_ref, kr_ref, vr_ref, h - n_dist)
        base = h * WIDTH
        q_ref[at, 0] = turn(pre[:, base:base + HEAD], cos, sin).astype(BF16)
        k_ref[at, 0] = turn(pre[:, base + HEAD:base + 2 * HEAD], cos, sin).astype(BF16)
        v_ref[at, 0] = pre[:, base + 2 * HEAD:base + 3 * HEAD].astype(BF16)


def project_qkv(starts, n_dist, n_shared, n_all, w_qkv, bias, cos, sin):
    n_dev, batch, local_len, hidden = n_all.shape
    seq = n_dev * local_len
    cols = (n_dist + n_shared) * WIDTH
    per = 4
    rows = per * local_len
    outs, out_specs = [], []
    for n_head in (n_dist, n_shared):
        outs += [jax.ShapeDtypeStruct((n_head, batch, seq, HEAD), BF16)] * 3
        out_specs += [pl.BlockSpec((n_head, 1, rows, HEAD), lambda b, j, me: (0, b, j, 0))] * 3
    tab_spec = pl.BlockSpec((1, rows, HEAD), lambda b, j, me: (b, j, 0))
    return pl.pallas_call(
        functools.partial(qkv_kernel, n_dist),
        grid_spec=pltpu.PrefetchScalarGridSpec(
            num_scalar_prefetch=1,
            grid=(batch, n_dev // per),
            in_specs=[
                pl.BlockSpec((per, 1, local_len, hidden), lambda b, j, me: (j, b, 0, 0)),
                pl.BlockSpec(memory_space=pl.ANY),
                pl.BlockSpec((1, cols), lambda b, j, me: (0, 0)),
                tab_spec, tab_spec,
            ],
            out_specs=out_specs,
            scratch_shapes=[pltpu.VMEM((hidden, cols), BF16), dma_sems(2, 2)],
        ),
        out_shape=outs,
        compiler_params=pltpu.CompilerParams(vmem_limit_bytes=60 * MIB),
        cost_estimate=cost(2 * batch * seq * hidden * cols, 2 * (batch * seq * hidden + hidden * cols + batch * seq * cols)),
        name='qkv',
    )(starts, n_all, w_qkv, bias, cos, sin)


def forward_kernel(pre_ref, q_ref, k_ref, v_ref, ctx_ref, lse_ref):
    n_head, _, seq, _ = q_ref.shape
    local_len = ctx_ref.shape[2]
    per = BLK // local_len
    prefix = pre_ref[pl.program_id(1)]

    def block(r, n_key):
        query = lax.broadcasted_iota(jnp.int32, (1, BLK), 1) + r * BLK
        last = jnp.maximum(query, prefix - 1) - (n_key - 1) * BLK
        scores = []
        for h in range(n_head):
            q_blk = q_ref[h, 0, r * BLK:(r + 1) * BLK]
            parts = [dot(k_ref[h, 0, c * BLK:(c + 1) * BLK], q_blk, 1, 1) * (SCALE * LOG2E) for c in range(n_key)]
            key = lax.broadcasted_iota(jnp.int32, (BLK, BLK), 0)
            parts[-1] = jnp.where(key <= last, parts[-1], MASK_FILL)
            scores.append(parts)
        for h, parts in enumerate(scores):
            top = functools.reduce(jnp.maximum, [jnp.max(p, axis=0, keepdims=True) for p in parts])
            parts = [jnp.exp2(p - top) for p in parts]
            total = functools.reduce(jnp.add, [jnp.sum(p, axis=0, keepdims=True) for p in parts])
            inv = 1.0 / total
            probs = jnp.concatenate([(p * inv).astype(BF16) for p in parts], axis=0)
            ctx_t = dot(v_ref[h, 0, :n_key * BLK], probs, 0, 0)
            ctx = ctx_t.T.astype(BF16).reshape(per, local_len, HEAD)
            ctx_ref[r * per:(r + 1) * per, 0, :, h * HEAD:(h + 1) * HEAD] = ctx
            lse_ref[h, 0, :, r * BLK:(r + 1) * BLK] = top + jnp.log2(total)

    n_blk = seq // BLK
    for r in range(n_blk):
        for n_key in range(r + 1, n_blk + 1):
            low = (n_key - 1) * BLK
            cond = prefix <= n_key * BLK if n_key == r + 1 else prefix > low
            if n_key < n_blk and n_key > r + 1:
                cond = jnp.logical_and(cond, prefix <= n_key * BLK)
            if n_key == n_blk and n_key == r + 1:
                block(r, n_key)
            else:
                pl.when(cond)(functools.partial(block, r, n_key))


def attention_forward(prefix_len, q, k, v, n_dev):
    own, batch, seq, _ = q.shape
    local_len = seq // n_dev
    qkv_spec = pl.BlockSpec((own, 1, seq, HEAD), lambda h, b, pre: (h, b, 0, 0))
    return pl.pallas_call(
        forward_kernel,
        grid_spec=pltpu.PrefetchScalarGridSpec(
            num_scalar_prefetch=1,
            grid=(1, batch),
            in_specs=[qkv_spec] * 3,
            out_specs=[
                pl.BlockSpec((n_dev, 1, local_len, own * HEAD), lambda h, b, pre: (0, b, 0, h)),
                pl.BlockSpec((own, 1, 1, seq), lambda h, b, pre: (h, b, 0, 0)),
            ],
        ),
        out_shape=[
            jax.ShapeDtypeStruct((n_dev, batch, local_len, own * HEAD), BF16),
            jax.ShapeDtypeStruct((own, batch, 1, seq), F32),
        ],
        compiler_params=pltpu.CompilerParams(vmem_limit_bytes=40 * MIB),
        cost_estimate=cost(4 * own * batch * seq * seq * HEAD, 8 * own * batch * seq * HEAD, own * batch * seq * seq),
        name='attn_fwd',
    )(prefix_len, q, k, v)


def backward_kernel(pre_ref, q_ref, k_ref, v_ref, ctx_ref, dctx_ref, lse_ref, cos_ref, sin_ref, g_ref, sum_ref, dq_acc, dk_acc, dv_acc):
    seq = q_ref.shape[2]
    n_dev, _, local_len, _ = g_ref.shape
    n_blk = seq // BLK
    prefix = pre_ref[pl.program_id(1)]
    d_ctx = dctx_ref[...].reshape(seq, HEAD)
    prod = d_ctx.astype(F32) * ctx_ref[...].reshape(seq, HEAD).astype(F32)
    delta = jnp.sum(prod.T, axis=0, keepdims=True)

    def block(c, first):
        keys = k_ref[0, 0, c * BLK:(c + 1) * BLK]
        vals = v_ref[0, 0, c * BLK:(c + 1) * BLK]
        start = first * BLK
        q_part = q_ref[0, 0, start:]
        g_part = d_ctx[start:]
        s_t = dot(keys, q_part, 1, 1)
        dp_t = dot(vals, g_part, 1, 1)
        probs, d_scores = [], []
        for r in range(first, n_blk):
            lo = r * BLK
            piece = s_t[:, lo - start:lo - start + BLK] * (SCALE * LOG2E)
            if r <= c:
                key = lax.broadcasted_iota(jnp.int32, (BLK, BLK), 0)
                query = lax.broadcasted_iota(jnp.int32, (1, BLK), 1) + lo
                piece = jnp.where(key <= jnp.maximum(query, prefix - 1) - c * BLK, piece, MASK_FILL)
            p = jnp.exp2(piece - lse_ref[0, 0, :, lo:lo + BLK])
            probs.append(p.astype(BF16))
            d_p = dp_t[:, lo - start:lo - start + BLK] - delta[:, lo:lo + BLK]
            d_scores.append((p * d_p * SCALE).astype(BF16))
        probs = jnp.concatenate(probs, axis=1)
        d_scores = jnp.concatenate(d_scores, axis=1)
        dv_acc[c * BLK:(c + 1) * BLK] = dot(probs, g_part, 1, 0)
        dk_acc[c * BLK:(c + 1) * BLK] = dot(d_scores, q_part, 1, 0)
        dq_part = dot(keys, d_scores, 0, 0)
        if c == 0:
            dq_acc[...] = dq_part
        else:
            dq_acc[:, start:] += dq_part

    block(0, 0)
    for c in range(1, n_blk):
        pl.when(prefix > c * BLK)(functools.partial(block, c, 0))
        pl.when(prefix <= c * BLK)(functools.partial(block, c, c))

    cos, sin = cos_ref[0], sin_ref[0]
    g_q = turn(dq_acc[...].T.astype(BF16).astype(F32), cos, -sin)
    g_k = turn(dk_acc[...].astype(BF16).astype(F32), cos, -sin)
    g_v = dv_acc[...].astype(BF16).astype(F32)
    for i, g in enumerate((g_q, g_k, g_v)):
        g_ref[:, 0, :, i * HEAD:(i + 1) * HEAD] = g.astype(BF16).reshape(n_dev, local_len, HEAD)
        sum_ref[0, :, i * HEAD:(i + 1) * HEAD] = jnp.sum(g, axis=0, keepdims=True)


def attention_backward(head, n_head, d_col, prefix_len, q, k, v, ctx, d_ctx, lse, cos, sin):
    _, batch, seq, _ = q.shape
    n_dev, _, local_len, _ = ctx.shape
    qkv_spec = pl.BlockSpec((1, 1, seq, HEAD), lambda h, b, pre: (head + h, b, 0, 0))

    def tok_spec(at):
        return pl.BlockSpec((n_dev, 1, local_len, HEAD), lambda h, b, pre: (0, b, 0, at + h))

    tab_spec = pl.BlockSpec((1, seq, HEAD), lambda h, b, pre: (b, 0, 0))
    return pl.pallas_call(
        backward_kernel,
        grid_spec=pltpu.PrefetchScalarGridSpec(
            num_scalar_prefetch=1,
            grid=(n_head, batch),
            in_specs=[qkv_spec] * 3 + [
                tok_spec(head), tok_spec(d_col), pl.BlockSpec((1, 1, 1, seq), lambda h, b, pre: (head + h, b, 0, 0)), tab_spec, tab_spec],
            out_specs=[
                pl.BlockSpec((n_dev, 1, local_len, WIDTH), lambda h, b, pre: (0, b, 0, h)),
                pl.BlockSpec((1, 1, WIDTH), lambda h, b, pre: (b, 0, h)),
            ],
            scratch_shapes=[pltpu.VMEM((HEAD, seq), F32), pltpu.VMEM((seq, HEAD), F32), pltpu.VMEM((seq, HEAD), F32)],
        ),
        out_shape=[
            jax.ShapeDtypeStruct((n_dev, batch, local_len, n_head * WIDTH), BF16),
            jax.ShapeDtypeStruct((batch, 1, n_head * WIDTH), F32),
        ],
        compiler_params=pltpu.CompilerParams(vmem_limit_bytes=40 * MIB),
        cost_estimate=cost(10 * n_head * batch * seq * seq * HEAD, 20 * n_head * batch * seq * HEAD, n_head * batch * seq * seq),
        name='attn_bwd',
    )(prefix_len, q, k, v, ctx, d_ctx, lse, cos, sin)


def wo_grad_kernel(row_of, block_row_of, core_ref, ctx_ref, dy_ref, *rest):
    out_ref, copy_ref, buf, sems = rest[-4:]
    n, c = pl.program_id(0), pl.program_id(1)
    n_grp = pl.num_programs(1)
    last = pl.num_programs(0) * n_grp - 1
    step = n * n_grp + c
    slot = lax.rem(step, 2)
    _, rows, wide = buf.shape
    core = core_ref[0]

    def stores(at_step, at):
        n_at, c_at = at_step // n_grp, lax.rem(at_step, n_grp)
        cols = pl.ds(pl.multiple_of(n_at * wide, HEAD), wide)
        for i, (ref, row) in enumerate(((out_ref, row_of(c_at, core)), (copy_ref, block_row_of(c_at)))):
            yield pltpu.make_async_copy(buf.at[at], ref.at[pl.ds(pl.multiple_of(row, HEAD), rows), cols], sems.at[at, i])

    @pl.when(step >= 2)
    def _():
        for copy in stores(step - 2, slot):
            copy.wait()

    buf[slot] = dot(ctx_ref[0], dy_ref[...], 0, 0)
    for copy in stores(step, slot):
        copy.start()

    @pl.when(step == last)
    def _():
        for copy in stores(step - 1, 1 - slot):
            copy.wait()
        for copy in stores(step, slot):
            copy.wait()


def weight_grad_o(core, ctx_par, dy_all, row_of, block_row_of, block_rows, wide, earlier):
    n_grp, tokens, cols = ctx_par.shape
    hidden = dy_all.shape[1]
    any_spec = pl.BlockSpec(memory_space=pl.ANY)
    return pl.pallas_call(
        functools.partial(wo_grad_kernel, row_of, block_row_of),
        grid_spec=pltpu.PrefetchScalarGridSpec(
            num_scalar_prefetch=1,
            grid=(hidden // wide, n_grp),
            in_specs=[
                pl.BlockSpec((1, tokens, cols), lambda n, c, core: (c, 0, 0)),
                pl.BlockSpec((tokens, wide), lambda n, c, core: (0, n)),
            ] + [any_spec] * len(earlier),
            out_specs=[any_spec, any_spec],
            scratch_shapes=[pltpu.VMEM((2, cols, wide), F32), dma_sems(2, 2)],
        ),
        out_shape=[jax.ShapeDtypeStruct((hidden, hidden), F32), jax.ShapeDtypeStruct((block_rows, hidden), F32)],
        input_output_aliases={3: 0, 4: 1} if earlier else {},
        compiler_params=pltpu.CompilerParams(vmem_limit_bytes=60 * MIB),
        cost_estimate=cost(2 * tokens * n_grp * cols * hidden, 2 * tokens * n_grp * cols + 2 * tokens * hidden + 8 * hidden * n_grp * cols),
        name='wo_grad',
    )(core, ctx_par, dy_all, *earlier)


def paste_kernel(core_ref, new_ref, old_ref, out_ref):
    out_ref[...] = new_ref[...]


def paste_rows(core, block, whole, tile_of):
    rows, hidden = block.shape
    return pl.pallas_call(
        paste_kernel,
        grid_spec=pltpu.PrefetchScalarGridSpec(
            num_scalar_prefetch=1,
            grid=(rows // HEAD,),
            in_specs=[pl.BlockSpec((HEAD, hidden), lambda t, core: (t, 0)), pl.BlockSpec(memory_space=pl.ANY)],
            out_specs=pl.BlockSpec((HEAD, hidden), lambda t, core: (tile_of(t, 1 - core[0]), 0)),
        ),
        out_shape=jax.ShapeDtypeStruct(whole.shape, F32),
        input_output_aliases={2: 0},
        compiler_params=pltpu.CompilerParams(vmem_limit_bytes=32 * MIB),
        cost_estimate=cost(rows * hidden, 8 * rows * hidden),
        name='paste_wo',
    )(core, block, whole)


def column_copies(src, out_ref, sem_of, row, rows, places):
    width = src.shape[-1] // len(places)
    for i, col in enumerate(places):
        yield pltpu.make_async_copy(
            src.at[:, pl.ds(i * width, width)],
            out_ref.at[pl.ds(pl.multiple_of(row, BLK), rows), pl.ds(pl.multiple_of(col, HEAD), width)],
            sem_of(i))


def wqkv_grad_kernel(places_of, old_places_of, core_ref, n_ref, g_ref, *rest):
    recv_ref = rest[0] if old_places_of else None
    out_ref, copy_ref, rhs, buf, g_sems, out_sems, copy_sems, paste_sems = rest[-8:]
    m = pl.program_id(0)
    n_m = pl.num_programs(0)
    core = core_ref[0]
    n_grp, _, cols = g_ref.shape
    rows = n_ref.shape[1]
    slot = lax.rem(m, 2)

    def loads():
        for c in range(n_grp):
            yield pltpu.make_async_copy(g_ref.at[c], rhs.at[:, pl.ds(c * cols, cols)], g_sems.at[c])

    def stores(step, at):
        yield from column_copies(buf.at[at], out_ref, lambda i: out_sems.at[at, i], step * rows, rows, places_of(core))
        yield pltpu.make_async_copy(buf.at[at], copy_ref.at[pl.ds(pl.multiple_of(step * rows, BLK), rows)], copy_sems.at[at])

    def pastes():
        return column_copies(recv_ref, out_ref, lambda i: paste_sems.at[i], m * rows, rows, old_places_of(1 - core))

    @pl.when(m == 0)
    def _():
        for copy in loads():
            copy.start()
        for copy in loads():
            copy.wait()

    if old_places_of:
        for copy in pastes():
            copy.start()

    @pl.when(m >= 2)
    def _():
        for copy in stores(m - 2, slot):
            copy.wait()

    buf[slot] = dot(n_ref[...], rhs[...], 0, 0)
    for copy in stores(m, slot):
        copy.start()
    if old_places_of:
        for copy in pastes():
            copy.wait()

    @pl.when(m == n_m - 1)
    def _():
        for copy in stores(m - 1, 1 - slot):
            copy.wait()
        for copy in stores(m, slot):
            copy.wait()


def weight_grad_qkv(core, places_of, n_flat, g_par, width, earlier):
    tokens, hidden = n_flat.shape
    n_grp, _, cols = g_par.shape
    rows = 2 * BLK
    any_spec = pl.BlockSpec(memory_space=pl.ANY)
    args, specs, alias, old_places_of = [core, n_flat, g_par], [pl.BlockSpec((tokens, rows), lambda m, core: (0, m)), any_spec], {}, None
    if earlier:
        recv, old_places_of, whole = earlier
        args += [recv, whole]
        specs += [pl.BlockSpec((rows, recv.shape[1]), lambda m, core: (m, 0)), any_spec]
        alias = {4: 0}
    return pl.pallas_call(
        functools.partial(wqkv_grad_kernel, places_of, old_places_of),
        grid_spec=pltpu.PrefetchScalarGridSpec(
            num_scalar_prefetch=1,
            grid=(hidden // rows,),
            in_specs=specs,
            out_specs=[any_spec, any_spec],
            scratch_shapes=[
                pltpu.VMEM((tokens, n_grp * cols), BF16),
                pltpu.VMEM((2, rows, n_grp * cols), F32),
                dma_sems(n_grp), dma_sems(2, 8), dma_sems(2), dma_sems(8),
            ],
        ),
        out_shape=[jax.ShapeDtypeStruct((hidden, width), F32), jax.ShapeDtypeStruct((hidden, n_grp * cols), F32)],
        input_output_aliases=alias,
        compiler_params=pltpu.CompilerParams(vmem_limit_bytes=60 * MIB),
        cost_estimate=cost(2 * tokens * hidden * n_grp * cols, 2 * tokens * hidden + 2 * n_grp * tokens * cols + 16 * hidden * n_grp * cols),
        name='wqkv_grad',
    )(*args)


def paste_columns_kernel(places_of, core_ref, recv_ref, old_ref, out_ref, sems):
    rows = recv_ref.shape[0]
    row = pl.program_id(0) * rows
    copies = list(column_copies(recv_ref, out_ref, lambda i: sems.at[i], row, rows, places_of(1 - core_ref[0])))
    for copy in copies:
        copy.start()
    for copy in copies:
        copy.wait()


def paste_columns(core, places_of, recv, whole):
    hidden, block = recv.shape
    rows = 2 * BLK
    any_spec = pl.BlockSpec(memory_space=pl.ANY)
    return pl.pallas_call(
        functools.partial(paste_columns_kernel, places_of),
        grid_spec=pltpu.PrefetchScalarGridSpec(
            num_scalar_prefetch=1,
            grid=(hidden // rows,),
            in_specs=[pl.BlockSpec((rows, block), lambda m, core: (m, 0)), any_spec],
            out_specs=any_spec,
            scratch_shapes=[dma_sems(8)],
        ),
        out_shape=jax.ShapeDtypeStruct(whole.shape, F32),
        input_output_aliases={2: 0},
        compiler_params=pltpu.CompilerParams(vmem_limit_bytes=48 * MIB),
        cost_estimate=cost(hidden * block, 8 * hidden * block),
        name='paste_wqkv',
    )(core, recv, whole)


def normed_grad_kernel(scale, cols_ref, g_ref, w_ref, init_ref, out_ref, w_buf, sems):
    j = pl.program_id(0)
    slot = lax.rem(j, 2)
    half = w_buf.shape[2] // 2

    def loads(step, at):
        for i in range(2):
            col = pl.multiple_of(cols_ref[2 * step + i], HEAD)
            yield pltpu.make_async_copy(w_ref.at[:, pl.ds(col, half)], w_buf.at[at, :, pl.ds(i * half, half)], sems.at[at, i])

    @pl.when(j == 0)
    def _():
        for copy in loads(0, 0):
            copy.start()
        out_ref[...] = init_ref[...].astype(F32) * scale if scale else init_ref[...]

    @pl.when(j + 1 < pl.num_programs(0))
    def _():
        for copy in loads(j + 1, 1 - slot):
            copy.start()

    for copy in loads(j, slot):
        copy.wait()
    out_ref[...] += dot(g_ref[0], w_buf[slot], 1, 1)


def normed_grad(cols, g_tok, w_qkv, init, scale):
    steps, rows, width = g_tok.shape
    hidden = w_qkv.shape[0]
    whole = pl.BlockSpec((rows, hidden), lambda j, cols: (0, 0))
    return pl.pallas_call(
        functools.partial(normed_grad_kernel, scale),
        grid_spec=pltpu.PrefetchScalarGridSpec(
            num_scalar_prefetch=1,
            grid=(steps,),
            in_specs=[pl.BlockSpec((1, rows, width), lambda j, cols: (j, 0, 0)), pl.BlockSpec(memory_space=pl.ANY), whole],
            out_specs=whole,
            scratch_shapes=[pltpu.VMEM((2, hidden, width), BF16), dma_sems(2, 2)],
        ),
        out_shape=jax.ShapeDtypeStruct((rows, hidden), F32),
        compiler_params=pltpu.CompilerParams(vmem_limit_bytes=60 * MIB),
        cost_estimate=cost(2 * rows * steps * width * hidden, 2 * steps * width * (rows + hidden) + 8 * rows * hidden),
        name='dn',
    )(cols, g_tok, w_qkv, init)


def output_kernel(n_dist, core_ref, ctx_ref, shared_ref, w_ref, w_shared_ref, n_ref, b_ref, out_ref, acc):
    j = pl.program_id(0)

    @pl.when(j == 0)
    def _():
        acc[...] = dot(ctx_ref[0], w_ref[...], 1, 0)

    @pl.when(jnp.logical_and(j > 0, j < n_dist))
    def _():
        acc[...] += dot(ctx_ref[0], w_ref[...], 1, 0)

    @pl.when(j >= n_dist)
    def _():
        acc[...] += dot(shared_ref[0], w_shared_ref[...], 1, 0)

    @pl.when(j == pl.num_programs(0) - 1)
    def _():
        out_ref[...] = (ALPHA * n_ref[...].astype(F32) + (acc[...] + b_ref[...].astype(F32))).astype(BF16)


def project_out(core, ctx_tok, shared_tok, w_o, normed, b_o):
    n_dev, rows, cols = ctx_tok.shape
    n_core, _, shared = shared_tok.shape
    hidden = w_o.shape[1]
    base = n_dev * cols // shared

    def dist_index(j, core):
        at = jnp.minimum(j, n_dev - 1)
        return jnp.where(at < n_dev // 2, 2 * at + core[0], 2 * (at - n_dev // 2) + 1 - core[0])

    def shared_index(j, core):
        return jnp.where(j <= n_dev, core[0], 1 - core[0])

    whole = pl.BlockSpec((rows, hidden), lambda j, core: (0, 0))
    return pl.pallas_call(
        functools.partial(output_kernel, n_dev),
        grid_spec=pltpu.PrefetchScalarGridSpec(
            num_scalar_prefetch=1,
            grid=(n_dev + n_core,),
            in_specs=[
                pl.BlockSpec((1, rows, cols), lambda j, core: (jnp.minimum(j, n_dev - 1), 0, 0)),
                pl.BlockSpec((1, rows, shared), lambda j, core: (jnp.maximum(j - n_dev, 0), 0, 0)),
                pl.BlockSpec((cols, hidden), lambda j, core: (dist_index(j, core), 0)),
                pl.BlockSpec((shared, hidden), lambda j, core: (base + shared_index(j, core), 0)),
                whole,
                pl.BlockSpec((1, hidden), lambda j, core: (0, 0)),
            ],
            out_specs=whole,
            scratch_shapes=[pltpu.VMEM((rows, hidden), F32)],
        ),
        out_shape=jax.ShapeDtypeStruct((rows, hidden), BF16),
        compiler_params=pltpu.CompilerParams(vmem_limit_bytes=56 * MIB),
        cost_estimate=cost(2 * rows * hidden * hidden, 2 * hidden * hidden + 6 * rows * hidden),
        name='out_proj',
    )(core, ctx_tok, shared_tok, w_o, w_o, normed, b_o.reshape(1, -1))


def together(*values):
    return lax.optimization_barrier(values)


def solution(mesh):
    n_dev = mesh.shape['sp']
    tok_spec = P('dp', 'sp', None)
    pos_spec = P('dp', 'sp')
    in_specs = (tok_spec, pos_spec, pos_spec, P('dp'), P(), P(), P(), P(), P(), P(), tok_spec)
    out_specs = (tok_spec, tok_spec, P('dp'), P('dp'), P('dp', None), P('dp'), P('dp', None), P('dp'))
    same_core = [list(range(core, n_dev, 2)) for core in range(2)]
    partners = [(dev, dev ^ 1) for dev in range(n_dev)]
    n_chip = n_dev // 2

    def device_step(hidden_in, pos_ids, block_pos, prefix_len, ln_gamma, ln_beta, w_qkv, b_qkv, w_o, b_o, grad_out):
        batch, local_len, hidden = hidden_in.shape
        heads = hidden // HEAD
        n_dist, n_half = (heads - SHARED) // n_dev, SHARED // 2
        shared_at = n_dev * n_dist
        rows = batch * local_len
        tokens = n_dev * rows
        rank = lax.axis_index('sp')
        parity = lax.rem(rank, 2)
        core = parity.reshape(1).astype(jnp.int32)
        gather_core = functools.partial(lax.all_gather, axis_name='sp', axis_index_groups=same_core)
        to_partner = functools.partial(lax.ppermute, axis_name='sp', perm=partners)
        pair = rank + 1 - 2 * parity

        def token_rows(par):
            axis = par.ndim - 2
            mine = lax.dynamic_slice_in_dim(par, rank * rows, rows, axis=axis)
            theirs = lax.dynamic_slice_in_dim(par, pair * rows, rows, axis=axis)
            return mine, to_partner(theirs)

        def heads_of(weight, axis, width):
            spread = lax.dynamic_slice_in_dim(weight, rank * (n_dist * width), n_dist * width, axis=axis)
            shared = lax.dynamic_slice_in_dim(weight, (shared_at + parity * n_half) * width, n_half * width, axis=axis)
            return jnp.concatenate([spread, shared], axis=axis)

        def places(head):
            return lambda par: [((2 * c + par) * n_dist + head) * WIDTH for c in range(n_chip)]

        def shared_places(par):
            return [(shared_at + par * n_half) * WIDTH]

        normed_f, norm_vjp = jax.vjp(layer_norm, hidden_in.astype(F32), ln_gamma.astype(F32), ln_beta.astype(F32))
        normed = normed_f.astype(BF16)
        n_send, dy_send = together(normed, grad_out)
        n_all = lax.all_gather(n_send, 'sp')
        dy_all = lax.all_gather(dy_send, 'sp')
        cos, sin = rope_tables(prefix_len, n_dev * local_len)

        starts = jnp.stack([rank * n_dist, shared_at + parity * n_half]).astype(jnp.int32) * WIDTH
        bias = heads_of(b_qkv, 0, WIDTH).astype(F32).reshape(1, -1)
        qd, kd, vd, qr, kr, vr = project_qkv(starts, n_dist, n_half, n_all, w_qkv, bias, cos, sin)
        ctx_d, lse_d = attention_forward(prefix_len, qd, kd, vd, n_dev)
        ctx_d, qr = together(ctx_d, qr)
        ctx_par = gather_core(ctx_d.reshape(tokens, n_dist * HEAD))
        ctx_r, lse_r = attention_forward(prefix_len, qr, kr, vr, n_dev)

        w_o_own, ctx_r = together(heads_of(w_o, 0, HEAD), ctx_r)
        d_ctx = jnp.einsum('dbtc,hc->dbth', dy_all, w_o_own, preferred_element_type=F32).astype(BF16)
        g_own, g_sums = [], []
        for head in range(n_dist):
            g, g_sum = attention_backward(head, 1, head, prefix_len, qd, kd, vd, ctx_d, d_ctx, lse_d, cos, sin)
            g_own.append(g.reshape(tokens, WIDTH))
            g_sums.append(jnp.sum(g_sum, axis=(0, 1)))
        d_ctx, *g_own = together(d_ctx, *g_own)
        g_par = [gather_core(g) for g in g_own]
        g_r, g_sum = attention_backward(0, n_half, n_dist, prefix_len, qr, kr, vr, ctx_r, d_ctx, lse_r, cos, sin)
        g_sums.append(jnp.sum(g_sum, axis=(0, 1)))
        g_r = g_r.reshape(tokens, n_half * WIDTH)

        dy_flat = dy_all.reshape(tokens, hidden)
        n_flat = n_all.reshape(tokens, hidden)
        block_rows = hidden // 2
        ctx_rf, g_r = together(ctx_r.reshape(tokens, n_half * HEAD), g_r)
        wo_parts = weight_grad_o(
            core, ctx_rf[None], dy_flat, lambda c, par: (shared_at + par * n_half) * HEAD, lambda c: 0, block_rows, hidden // 4, ())
        n_flat, wo_block = together(n_flat, wo_parts[1])
        grad_wqkv, block = weight_grad_qkv(core, shared_places, n_flat, g_r[None], 3 * hidden, None)
        ctx_par, block = together(ctx_par, block)
        recv = to_partner(block)
        grad_wo, wo_block = weight_grad_o(
            core, ctx_par, dy_flat, lambda c, par: (2 * c + par) * (n_dist * HEAD), lambda c: n_half * HEAD + c * (n_dist * HEAD),
            block_rows, hidden // 2, (wo_parts[0], wo_block))
        ctx_tok = jnp.concatenate(token_rows(ctx_par), axis=0)
        shared_tok = jnp.stack(token_rows(ctx_rf))
        ctx_tok, wo_block = together(ctx_tok, wo_block)
        wo_recv = to_partner(wo_block)
        hidden_out = project_out(core, ctx_tok, shared_tok, w_o, normed.reshape(rows, hidden), b_o)
        n_flat, hidden_out = together(n_flat, hidden_out)

        grad_wqkv, block = weight_grad_qkv(core, places(0), n_flat, g_par[0], 3 * hidden, (recv, shared_places, grad_wqkv))
        wo_recv, block = together(wo_recv, block)
        recv = to_partner(block)

        def wo_tile(t, par):
            spread = t - n_half
            return jnp.where(t < n_half, shared_at + par * n_half + t, (2 * (spread // n_dist) + par) * n_dist + lax.rem(spread, n_dist))

        grad_wo = paste_rows(core, wo_recv, grad_wo, wo_tile)
        n_flat, grad_wo = together(n_flat, grad_wo)
        grad_wqkv, block = weight_grad_qkv(core, places(1), n_flat, g_par[1], 3 * hidden, (recv, places(0), grad_wqkv))

        g_tok = [token_rows(g) for g in g_par[:2]]
        r_tok = token_rows(g_r)
        wide = 2 * WIDTH
        g_first = [part[:, i * wide:(i + 1) * wide] for part in r_tok for i in range(n_half // 2)]
        cols = [(shared_at + par * n_half + 2 * i) * WIDTH + half * WIDTH for par in (parity, 1 - parity) for i in range(n_half // 2) for half in range(2)]
        for side, par in ((0, parity), (1, 1 - parity)):
            for c in range(n_chip):
                g_first.append(jnp.concatenate([g_tok[0][side][c], g_tok[1][side][c]], axis=1))
                cols += [((2 * c + par) * n_dist + head) * WIDTH for head in (0, 1)]
        g_first, block = together(jnp.stack(g_first), block)
        recv = to_partner(block)
        d_norm = normed_grad(jnp.stack(cols).astype(jnp.int32), g_first, w_qkv, grad_out.reshape(rows, hidden), ALPHA)
        n_flat, d_norm, g_par[2] = together(n_flat, d_norm, g_par[2])
        grad_wqkv, block = weight_grad_qkv(core, places(2), n_flat, g_par[2], 3 * hidden, (recv, places(1), grad_wqkv))
        cols = jnp.stack([((2 * c + par) * n_dist + 2) * WIDTH for c in range(n_chip) for par in (parity, 1 - parity)])
        g_last, block = together(jnp.concatenate(token_rows(g_par[2]), axis=2), block)
        recv = to_partner(block)
        d_norm = normed_grad(cols.astype(jnp.int32), g_last, w_qkv, d_norm, None)
        d_x, grad_gamma, grad_beta = norm_vjp(d_norm.reshape(batch, local_len, hidden))
        grad_in = d_x.astype(BF16)
        grad_bo = jnp.sum(grad_out.astype(F32), axis=(0, 1))
        small = lax.all_gather(jnp.concatenate(g_sums + [grad_gamma, grad_beta, grad_bo]), 'sp')
        recv, small = together(recv, small)
        spread, shared = small[:, :n_dist * WIDTH], small[:2, n_dist * WIDTH:(n_dist + n_half) * WIDTH]
        grad_bqkv = jnp.concatenate([spread.reshape(-1), shared.reshape(-1)])
        grad_gamma, grad_beta, grad_bo = jnp.sum(small[:, (n_dist + n_half) * WIDTH:], axis=0).reshape(3, hidden)
        grad_wqkv = paste_columns(core, places(2), recv, grad_wqkv)
        return (hidden_out.reshape(batch, local_len, hidden), grad_in, grad_gamma, grad_beta, grad_wqkv, grad_bqkv, grad_wo, grad_bo)

    return jax.shard_map(device_step, mesh=mesh, in_specs=in_specs, out_specs=out_specs, check_vma=False)
```

```python
import functools
import math
import jax
import jax.numpy as jnp
import numpy as np
from jax import lax
from jax.experimental import pallas as pl
from jax.experimental.pallas import tpu as pltpu
from jax.sharding import PartitionSpec as P

HEAD = 128
QUARTER = 32
ALPHA = math.sqrt(56.0)
LN_EPS = 1e-5
ROT_BASE = 10000.0
SCALE = 1.0 / math.sqrt(HEAD)
LOG2E = math.log2(math.e)
MASK_FILL = -1e30
BLK = 256
MIB = 1 << 20
SHARED = 8
WIDTH = 3 * HEAD
F32 = jnp.float32
BF16 = jnp.bfloat16


def dot(lhs, rhs, lhs_dim, rhs_dim):
    return lax.dot_general(lhs, rhs, (((lhs_dim,), (rhs_dim,)), ((), ())), preferred_element_type=F32)


def cost(flops, nbytes, transcendentals=0):
    return pl.CostEstimate(flops=int(flops), bytes_accessed=int(nbytes), transcendentals=int(transcendentals))


def layer_norm(x_val, ln_gain, ln_shift):
    row_mean = jnp.mean(x_val, axis=-1, keepdims=True)
    centered = x_val - row_mean
    row_var = jnp.mean(centered * centered, axis=-1, keepdims=True)
    return centered * lax.rsqrt(row_var + LN_EPS) * ln_gain + ln_shift


def rope_tables(prefix_len, seq):
    tok = jnp.arange(seq, dtype=jnp.int32)[None, :]
    pre = prefix_len[:, None]
    inside = tok < pre
    pos = jnp.where(inside, tok, pre - 1)
    blk = jnp.where(inside, 0, tok - pre + 1)
    inv_freq = ROT_BASE ** (-jnp.arange(QUARTER, dtype=F32) / QUARTER)
    angles = jnp.stack([pos, blk], axis=-1).astype(F32)[..., None] * inv_freq
    cos, sin = jnp.cos(angles), jnp.sin(angles)
    shape = pos.shape + (HEAD,)
    return (jnp.stack([cos, cos], axis=-2).reshape(shape), jnp.stack([-sin, sin], axis=-2).reshape(shape))


def turn(x, cos, sin):
    lane = lax.broadcasted_iota(jnp.int32, x.shape, 1)
    other = jnp.where(lane % (2 * QUARTER) < QUARTER, pltpu.roll(x, HEAD - QUARTER, 1), pltpu.roll(x, QUARTER, 1))
    return x * cos + other * sin


def dma_sems(*shape):
    return pltpu.SemaphoreType.DMA(shape)


def dma_sems(*shape):
    return pltpu.SemaphoreType.DMA(shape)


def start_all(copies):
    for copy in copies:
        copy.start()


def wait_all(copies):
    for copy in copies:
        copy.wait()


ANY = pl.BlockSpec(memory_space=pl.ANY)
PIECES = 4


def qkv_kernel(n_dist, start_ref, n_ref, w_ref, b_ref, cos_ref, sin_ref, qd_ref, kd_ref, vd_ref, qr_ref, kr_ref, vr_ref, w_buf, x_buf, acc, sems):
    rows = cos_ref.shape[1]
    hidden = n_ref.shape[-1]
    dist = n_dist * WIDTH
    shared = w_buf.shape[1] - dist
    first = jnp.logical_and(pl.program_id(0) == 0, pl.program_id(1) == 0)
    piece = hidden // PIECES

    def loads(i):
        span = pl.ds(pl.multiple_of(i * piece, piece), piece)
        for part, (at, width) in enumerate(((0, dist), (dist, shared))):
            col = pl.multiple_of(start_ref[part] * WIDTH, HEAD)
            yield pltpu.make_async_copy(w_ref.at[span, pl.ds(col, width)], w_buf.at[span, pl.ds(at, width)], sems.at[i, part])

    x_buf[...] = n_ref[...].reshape(rows, hidden)

    @pl.when(first)
    def _():
        for i in range(PIECES):
            start_all(loads(i))
        acc[...] = jnp.broadcast_to(b_ref[...], acc.shape)

        @pl.loop(0, PIECES)
        def _(i):
            wait_all(loads(i))
            span = pl.ds(pl.multiple_of(i * piece, piece), piece)
            acc[...] += dot(x_buf[:, span], w_buf[span], 1, 0)

    @pl.when(jnp.logical_not(first))
    def _():
        acc[...] = dot(x_buf[...], w_buf[...], 1, 0) + b_ref[...]

    cos, sin = cos_ref[0], sin_ref[0]
    n_shared = qr_ref.shape[0]
    for h in range(n_dist + n_shared):
        q_ref, k_ref, v_ref, at = (qd_ref, kd_ref, vd_ref, h) if h < n_dist else (qr_ref, kr_ref, vr_ref, h - n_dist)
        base = h * WIDTH
        q_ref[at, 0] = turn(acc[:, base:base + HEAD], cos, sin).astype(BF16)
        k_ref[at, 0] = turn(acc[:, base + HEAD:base + 2 * HEAD], cos, sin).astype(BF16)
        v_ref[at, 0] = acc[:, base + 2 * HEAD:base + 3 * HEAD].astype(BF16)


def project_qkv(half, starts, n_dist, n_shared, n_half, w_qkv, bias, cos, sin):
    n_dev, batch, local_len, hidden = n_half.shape
    seq = n_dev * local_len
    cols = (n_dist + n_shared) * WIDTH
    per = 4
    rows = per * local_len
    outs, out_specs = [], []
    for n_head in (n_dist, n_shared):
        outs += [jax.ShapeDtypeStruct((n_head, batch, seq, HEAD), BF16)] * 3
        out_specs += [pl.BlockSpec((n_head, 1, rows, HEAD), lambda b, j, at: (0, b, j, 0))] * 3
    tab_spec = pl.BlockSpec((1, rows, HEAD), lambda b, j, at: (half * batch + b, j, 0))
    return pl.pallas_call(
        functools.partial(qkv_kernel, n_dist),
        grid_spec=pltpu.PrefetchScalarGridSpec(
            num_scalar_prefetch=1,
            grid=(batch, n_dev // per),
            in_specs=[
                pl.BlockSpec((per, 1, local_len, hidden), lambda b, j, at: (j, b, 0, 0)),
                ANY,
                pl.BlockSpec((1, cols), lambda b, j, at: (0, 0)),
                tab_spec, tab_spec,
            ],
            out_specs=out_specs,
            scratch_shapes=[
                pltpu.VMEM((hidden, cols), BF16), pltpu.VMEM((rows, hidden), BF16), pltpu.VMEM((rows, cols), F32), dma_sems(PIECES, 2)],
        ),
        out_shape=outs,
        compiler_params=pltpu.CompilerParams(vmem_limit_bytes=62 * MIB),
        cost_estimate=cost(2 * batch * seq * hidden * cols, 2 * (batch * seq * hidden + hidden * cols + batch * seq * cols)),
        name='qkv',
    )(starts, n_half, w_qkv, bias, cos, sin)


def forward_kernel(pre_ref, q_ref, k_ref, v_ref, *rest):
    ctx_ref, lse_ref = rest[-2:]
    n_head, _, seq, _ = q_ref.shape
    local_len = ctx_ref.shape[3]
    per = BLK // local_len
    prefix = pre_ref[pl.program_id(0)]

    def block(r, n_key):
        query = lax.broadcasted_iota(jnp.int32, (1, BLK), 1) + r * BLK
        last = jnp.maximum(query, prefix - 1) - (n_key - 1) * BLK
        scores = []
        for h in range(n_head):
            q_blk = q_ref[h, 0, r * BLK:(r + 1) * BLK]
            parts = [dot(k_ref[h, 0, c * BLK:(c + 1) * BLK], q_blk, 1, 1) * (SCALE * LOG2E) for c in range(n_key)]
            key = lax.broadcasted_iota(jnp.int32, (BLK, BLK), 0)
            parts[-1] = jnp.where(key <= last, parts[-1], MASK_FILL)
            scores.append(parts)
        for h, parts in enumerate(scores):
            top = functools.reduce(jnp.maximum, [jnp.max(p, axis=0, keepdims=True) for p in parts])
            parts = [jnp.exp2(p - top) for p in parts]
            total = functools.reduce(jnp.add, [jnp.sum(p, axis=0, keepdims=True) for p in parts])
            inv = 1.0 / total
            probs = jnp.concatenate([(p * inv).astype(BF16) for p in parts], axis=0)
            ctx_t = dot(v_ref[h, 0, :n_key * BLK], probs, 0, 0)
            ctx = ctx_t.T.astype(BF16).reshape(per, local_len, HEAD)
            ctx_ref[0, r * per:(r + 1) * per, 0, :, h * HEAD:(h + 1) * HEAD] = ctx
            lse_ref[h, 0, :, r * BLK:(r + 1) * BLK] = top + jnp.log2(total)

    n_blk = seq // BLK
    for r in range(n_blk):
        for n_key in range(r + 1, n_blk + 1):
            low = (n_key - 1) * BLK
            cond = prefix <= n_key * BLK if n_key == r + 1 else prefix > low
            if n_key < n_blk and n_key > r + 1:
                cond = jnp.logical_and(cond, prefix <= n_key * BLK)
            if n_key == n_blk and n_key == r + 1:
                block(r, n_key)
            else:
                pl.when(cond)(functools.partial(block, r, n_key))


def attention_forward(half, prefix_half, q, k, v, n_dev, ctx):
    own, batch, seq, _ = q.shape
    local_len = seq // n_dev
    qkv_spec = pl.BlockSpec((own, 1, seq, HEAD), lambda b, pre: (0, b, 0, 0))
    earlier = [] if ctx is None else [ctx]
    return pl.pallas_call(
        forward_kernel,
        grid_spec=pltpu.PrefetchScalarGridSpec(
            num_scalar_prefetch=1,
            grid=(batch,),
            in_specs=[qkv_spec] * 3 + [ANY] * len(earlier),
            out_specs=[
                pl.BlockSpec((1, n_dev, 1, local_len, own * HEAD), lambda b, pre: (half, 0, b, 0, 0)),
                pl.BlockSpec((own, 1, 1, seq), lambda b, pre: (0, b, 0, 0)),
            ],
        ),
        out_shape=[
            jax.ShapeDtypeStruct((2, n_dev, batch, local_len, own * HEAD), BF16),
            jax.ShapeDtypeStruct((own, batch, 1, seq), F32),
        ],
        input_output_aliases={4: 0} if earlier else {},
        compiler_params=pltpu.CompilerParams(vmem_limit_bytes=40 * MIB),
        cost_estimate=cost(4 * own * batch * seq * seq * HEAD, 8 * own * batch * seq * HEAD, own * batch * seq * seq),
        name='attn_fwd',
    )(prefix_half, q, k, v, *earlier)


def d_ctx_kernel(start_ref, dy_ref, w_ref, out_ref, w_buf, sems):
    per, _, local_len, hidden = dy_ref.shape
    first = jnp.logical_and(pl.program_id(0) == 0, pl.program_id(1) == 0)
    widths = (out_ref.shape[-1] - SHARED // 2 * HEAD, SHARED // 2 * HEAD)

    def loads():
        at = 0
        for part, width in enumerate(widths):
            row = pl.multiple_of(start_ref[part] * HEAD, HEAD)
            yield pltpu.make_async_copy(w_ref.at[pl.ds(row, width)], w_buf.at[pl.ds(at, width)], sems.at[part])
            at += width

    @pl.when(first)
    def _():
        start_all(loads())
        wait_all(loads())

    res = dot(dy_ref[...].reshape(per * local_len, hidden), w_buf[...], 1, 1)
    out_ref[...] = res.astype(BF16).reshape(per, 1, local_len, w_buf.shape[0])


def context_grad(starts, n_own, dy_half, w_o):
    n_dev, batch, local_len, hidden = dy_half.shape
    cols = n_own * HEAD
    per = 4
    return pl.pallas_call(
        d_ctx_kernel,
        grid_spec=pltpu.PrefetchScalarGridSpec(
            num_scalar_prefetch=1,
            grid=(batch, n_dev // per),
            in_specs=[pl.BlockSpec((per, 1, local_len, hidden), lambda b, j, at: (j, b, 0, 0)), ANY],
            out_specs=pl.BlockSpec((per, 1, local_len, cols), lambda b, j, at: (j, b, 0, 0)),
            scratch_shapes=[pltpu.VMEM((cols, hidden), BF16), dma_sems(2)],
        ),
        out_shape=jax.ShapeDtypeStruct((n_dev, batch, local_len, cols), BF16),
        compiler_params=pltpu.CompilerParams(vmem_limit_bytes=40 * MIB),
        cost_estimate=cost(2 * n_dev * batch * local_len * hidden * cols, 2 * n_dev * batch * local_len * (hidden + cols) + 2 * cols * hidden),
        name='dctx',
    )(starts, dy_half, w_o)


def backward_kernel(pre_ref, q_ref, k_ref, v_ref, ctx_ref, dctx_ref, lse_ref, cos_ref, sin_ref, *rest):
    g_ref, sum_ref, dq_acc, dk_acc, dv_acc = rest[-5:]
    seq = q_ref.shape[2]
    n_dev, local_len = g_ref.shape[2], g_ref.shape[4]
    n_blk = seq // BLK
    prefix = pre_ref[pl.program_id(1)]
    d_ctx = dctx_ref[...].reshape(seq, HEAD)
    prod = d_ctx.astype(F32) * ctx_ref[...].reshape(seq, HEAD).astype(F32)
    delta = jnp.sum(prod.T, axis=0, keepdims=True)

    def block(c, first):
        keys = k_ref[0, 0, c * BLK:(c + 1) * BLK]
        vals = v_ref[0, 0, c * BLK:(c + 1) * BLK]
        start = first * BLK
        q_part = q_ref[0, 0, start:]
        g_part = d_ctx[start:]
        s_t = dot(keys, q_part, 1, 1)
        dp_t = dot(vals, g_part, 1, 1)
        probs, d_scores = [], []
        for r in range(first, n_blk):
            lo = r * BLK
            piece = s_t[:, lo - start:lo - start + BLK] * (SCALE * LOG2E)
            if r <= c:
                key = lax.broadcasted_iota(jnp.int32, (BLK, BLK), 0)
                query = lax.broadcasted_iota(jnp.int32, (1, BLK), 1) + lo
                piece = jnp.where(key <= jnp.maximum(query, prefix - 1) - c * BLK, piece, MASK_FILL)
            p = jnp.exp2(piece - lse_ref[0, 0, :, lo:lo + BLK])
            probs.append(p.astype(BF16))
            d_p = dp_t[:, lo - start:lo - start + BLK] - delta[:, lo:lo + BLK]
            d_scores.append((p * d_p * SCALE).astype(BF16))
        probs = jnp.concatenate(probs, axis=1)
        d_scores = jnp.concatenate(d_scores, axis=1)
        dv_acc[c * BLK:(c + 1) * BLK] = dot(probs, g_part, 1, 0)
        dk_acc[c * BLK:(c + 1) * BLK] = dot(d_scores, q_part, 1, 0)
        dq_part = dot(keys, d_scores, 0, 0)
        if c == 0:
            dq_acc[...] = dq_part
        else:
            dq_acc[:, start:] += dq_part

    block(0, 0)
    for c in range(1, n_blk):
        pl.when(prefix > c * BLK)(functools.partial(block, c, 0))
        pl.when(prefix <= c * BLK)(functools.partial(block, c, c))

    cos, sin = cos_ref[0], sin_ref[0]
    g_q = turn(dq_acc[...].T.astype(BF16).astype(F32), cos, -sin)
    g_k = turn(dk_acc[...].astype(BF16).astype(F32), cos, -sin)
    g_v = dv_acc[...].astype(BF16).astype(F32)
    for i, g in enumerate((g_q, g_k, g_v)):
        g_ref[0, 0, :, 0, :, i * HEAD:(i + 1) * HEAD] = g.astype(BF16).reshape(n_dev, local_len, HEAD)
        sum_ref[0, :, i * HEAD:(i + 1) * HEAD] = jnp.sum(g, axis=0, keepdims=True)


def attention_backward(half, d_col, prefix_half, q, k, v, ctx, d_ctx, lse, cos, sin, g_all):
    n_head, batch, seq, _ = q.shape
    _, n_dev, _, local_len, _ = ctx.shape
    qkv_spec = pl.BlockSpec((1, 1, seq, HEAD), lambda h, b, pre: (h, b, 0, 0))
    tab_spec = pl.BlockSpec((1, seq, HEAD), lambda h, b, pre: (half * batch + b, 0, 0))
    earlier = [] if g_all is None else [g_all]
    return pl.pallas_call(
        backward_kernel,
        grid_spec=pltpu.PrefetchScalarGridSpec(
            num_scalar_prefetch=1,
            grid=(n_head, batch),
            in_specs=[qkv_spec] * 3 + [
                pl.BlockSpec((1, n_dev, 1, local_len, HEAD), lambda h, b, pre: (half, 0, b, 0, h)),
                pl.BlockSpec((n_dev, 1, local_len, HEAD), lambda h, b, pre: (0, b, 0, d_col + h)),
                pl.BlockSpec((1, 1, 1, seq), lambda h, b, pre: (h, b, 0, 0)), tab_spec, tab_spec] + [ANY] * len(earlier),
            out_specs=[
                pl.BlockSpec((1, 1, n_dev, 1, local_len, WIDTH), lambda h, b, pre: (h, half, 0, b, 0, 0)),
                pl.BlockSpec((1, 1, WIDTH), lambda h, b, pre: (b, 0, h)),
            ],
            scratch_shapes=[pltpu.VMEM((HEAD, seq), F32), pltpu.VMEM((seq, HEAD), F32), pltpu.VMEM((seq, HEAD), F32)],
        ),
        out_shape=[
            jax.ShapeDtypeStruct((n_head, 2, n_dev, batch, local_len, WIDTH), BF16),
            jax.ShapeDtypeStruct((batch, 1, n_head * WIDTH), F32),
        ],
        input_output_aliases={9: 0} if earlier else {},
        compiler_params=pltpu.CompilerParams(vmem_limit_bytes=40 * MIB),
        cost_estimate=cost(10 * n_head * batch * seq * seq * HEAD, 20 * n_head * batch * seq * HEAD, n_head * batch * seq * seq),
        name='attn_bwd',
    )(prefix_half, q, k, v, ctx, d_ctx, lse, cos, sin, *earlier)


def wo_grad_kernel(row_of, block_row_of, core_ref, ctx_ref, dya_ref, dyb_ref, *rest):
    out_ref, copy_ref, rhs, buf, rhs_sems, sems = rest[-6:]
    n, c = pl.program_id(0), pl.program_id(1)
    n_col, n_grp = pl.num_programs(0), pl.num_programs(1)
    step = n * n_grp + c
    slot, n_slot = lax.rem(step, 2), lax.rem(n, 2)
    _, rows, wide = buf.shape
    half = dya_ref.shape[0]
    core = core_ref[0]

    def loads(n_at, at):
        cols = pl.ds(pl.multiple_of(n_at * wide, HEAD), wide)
        for i, ref in enumerate((dya_ref, dyb_ref)):
            yield pltpu.make_async_copy(ref.at[:, cols], rhs.at[at, pl.ds(i * half, half)], rhs_sems.at[at, i])

    def stores(at_step, at):
        n_at, c_at = at_step // n_grp, lax.rem(at_step, n_grp)
        cols = pl.ds(pl.multiple_of(n_at * wide, HEAD), wide)
        for i, (ref, row) in enumerate(((out_ref, row_of(c_at, core)), (copy_ref, block_row_of(c_at)))):
            yield pltpu.make_async_copy(buf.at[at], ref.at[pl.ds(pl.multiple_of(row, HEAD), rows), cols], sems.at[at, i])

    @pl.when(step == 0)
    def _():
        start_all(loads(0, 0))

    @pl.when(c == 0)
    def _():
        @pl.when(n + 1 < n_col)
        def _():
            start_all(loads(n + 1, 1 - n_slot))

        wait_all(loads(n, n_slot))

    @pl.when(step >= 2)
    def _():
        wait_all(stores(step - 2, slot))

    buf[slot] = dot(ctx_ref[0], rhs[n_slot], 0, 0)
    start_all(stores(step, slot))

    @pl.when(step == n_col * n_grp - 1)
    def _():
        wait_all(stores(step - 1, 1 - slot))
        wait_all(stores(step, slot))


def weight_grad_o(core, ctx_par, dy_a, dy_b, row_of, block_row_of, block_rows, earlier):
    n_grp, tokens, cols = ctx_par.shape
    hidden = dy_a.shape[1]
    wide = hidden // 4
    return pl.pallas_call(
        functools.partial(wo_grad_kernel, row_of, block_row_of),
        grid_spec=pltpu.PrefetchScalarGridSpec(
            num_scalar_prefetch=1,
            grid=(hidden // wide, n_grp),
            in_specs=[pl.BlockSpec((1, tokens, cols), lambda n, c, core: (c, 0, 0)), ANY, ANY] + [ANY] * len(earlier),
            out_specs=[ANY, ANY],
            scratch_shapes=[pltpu.VMEM((2, tokens, wide), BF16), pltpu.VMEM((2, cols, wide), F32), dma_sems(2, 2), dma_sems(2, 2)],
        ),
        out_shape=[jax.ShapeDtypeStruct((hidden, hidden), F32), jax.ShapeDtypeStruct((block_rows, hidden), F32)],
        input_output_aliases={4: 0, 5: 1} if earlier else {},
        compiler_params=pltpu.CompilerParams(vmem_limit_bytes=48 * MIB),
        cost_estimate=cost(2 * tokens * n_grp * cols * hidden, 2 * tokens * n_grp * cols + 2 * tokens * hidden + 8 * hidden * n_grp * cols),
        name='wo_grad',
    )(core, ctx_par, dy_a, dy_b, *earlier)


def column_copies(src, out_ref, sem_of, row, places):
    rows, width = src.shape[0], src.shape[1] // len(places)
    for i, col in enumerate(places):
        yield pltpu.make_async_copy(
            src.at[:, pl.ds(i * width, width)],
            out_ref.at[pl.ds(pl.multiple_of(row, BLK), rows), pl.ds(pl.multiple_of(col, HEAD), width)],
            sem_of(i))


def wqkv_grad_kernel(places_of, old_places_of, wo_tile, core_ref, na_ref, nb_ref, g_ref, *rest):
    rest = list(rest)
    recv_ref = rest.pop(0) if old_places_of else None
    wo_recv_ref = rest.pop(0) if wo_tile else None
    n_buf, rhs, buf, n_sems, g_sems, out_sems, copy_sems, paste_sems, wo_sems = rest[-9:]
    outs = rest[:-9][-3 if wo_tile else -2:]
    out_ref, copy_ref = outs[:2]
    m = pl.program_id(0)
    n_m = pl.num_programs(0)
    core = core_ref[0]
    n_grp, tokens, cols = g_ref.shape
    half, rows = tokens // 2, n_buf.shape[2]
    piece = tokens // PIECES
    slot = lax.rem(m, 2)

    def n_loads(step, at):
        span = pl.ds(pl.multiple_of(step * rows, BLK), rows)
        for i, ref in enumerate((na_ref, nb_ref)):
            yield pltpu.make_async_copy(ref.at[:, span], n_buf.at[at, pl.ds(i * half, half)], n_sems.at[at, i])

    def g_loads(i):
        span = pl.ds(pl.multiple_of(i * piece, piece), piece)
        for c in range(n_grp):
            yield pltpu.make_async_copy(g_ref.at[c, span], rhs.at[span, pl.ds(c * cols, cols)], g_sems.at[i, c])

    def stores(step, at):
        yield from column_copies(buf.at[at], out_ref, lambda i: out_sems.at[at, i], step * rows, places_of(core))
        yield pltpu.make_async_copy(buf.at[at], copy_ref.at[pl.ds(pl.multiple_of(step * rows, BLK), rows)], copy_sems.at[at])

    def pastes():
        if old_places_of:
            yield from column_copies(recv_ref, out_ref, lambda i: paste_sems.at[i], m * rows, old_places_of(1 - core))
        if wo_tile:
            tiles = wo_recv_ref.shape[0] // HEAD
            for t in range(tiles):
                row = pl.multiple_of(wo_tile(m * tiles + t, 1 - core) * HEAD, HEAD)
                yield pltpu.make_async_copy(wo_recv_ref.at[pl.ds(t * HEAD, HEAD)], outs[2].at[pl.ds(row, HEAD)], wo_sems.at[t])

    @pl.when(m == 0)
    def _():
        start_all(n_loads(0, 0))
        for i in range(PIECES):
            start_all(g_loads(i))

    @pl.when(m + 1 < n_m)
    def _():
        start_all(n_loads(m + 1, 1 - slot))

    start_all(pastes())

    @pl.when(m >= 2)
    def _():
        wait_all(stores(m - 2, slot))

    wait_all(n_loads(m, slot))

    @pl.when(m == 0)
    def _():
        buf[0] = jnp.zeros(buf.shape[1:], F32)

        @pl.loop(0, PIECES)
        def _(i):
            wait_all(g_loads(i))
            span = pl.ds(pl.multiple_of(i * piece, piece), piece)
            buf[0] += dot(n_buf[0, span], rhs[span], 0, 0)

    @pl.when(m > 0)
    def _():
        buf[slot] = dot(n_buf[slot], rhs[...], 0, 0)

    start_all(stores(m, slot))
    wait_all(pastes())

    @pl.when(m == n_m - 1)
    def _():
        wait_all(stores(m - 1, 1 - slot))
        wait_all(stores(m, slot))


def weight_grad_qkv(core, places_of, n_a, n_b, g_par, whole, recv=None, old_places_of=None, wo=None):
    hidden = n_a.shape[1]
    n_grp, tokens, cols = g_par.shape
    width = n_grp * cols
    rows = 2 * BLK
    steps = hidden // rows
    args, specs, alias = [core, n_a, n_b, g_par], [ANY, ANY, ANY], {}
    outs = [jax.ShapeDtypeStruct((hidden, 3 * hidden), F32), jax.ShapeDtypeStruct((hidden, width), F32)]
    wo_tile = None
    if recv is not None:
        args.append(recv)
        specs.append(pl.BlockSpec((rows, recv.shape[1]), lambda m, core: (m, 0)))
    if wo is not None:
        wo_recv, wo_whole, wo_tile = wo
        args.append(wo_recv)
        specs.append(pl.BlockSpec((wo_recv.shape[0] // steps, hidden), lambda m, core: (m, 0)))
        outs.append(jax.ShapeDtypeStruct(wo_whole.shape, F32))
    if whole is not None:
        alias[len(args)] = 0
        args.append(whole)
        specs.append(ANY)
    if wo is not None:
        alias[len(args)] = 2
        args.append(wo_whole)
        specs.append(ANY)
    return pl.pallas_call(
        functools.partial(wqkv_grad_kernel, places_of, old_places_of, wo_tile),
        grid_spec=pltpu.PrefetchScalarGridSpec(
            num_scalar_prefetch=1,
            grid=(steps,),
            in_specs=specs,
            out_specs=[ANY] * len(outs),
            scratch_shapes=[
                pltpu.VMEM((2, tokens, rows), BF16),
                pltpu.VMEM((tokens, width), BF16),
                pltpu.VMEM((2, rows, width), F32),
                dma_sems(2, 2), dma_sems(PIECES, n_grp), dma_sems(2, n_grp), dma_sems(2), dma_sems(n_grp), dma_sems(4),
            ],
        ),
        out_shape=outs,
        input_output_aliases=alias,
        compiler_params=pltpu.CompilerParams(vmem_limit_bytes=60 * MIB),
        cost_estimate=cost(2 * tokens * hidden * width, 2 * tokens * (hidden + width) + 16 * hidden * width),
        name='wqkv_grad',
    )(*args)


def normed_grad_kernel(places_of, n_paste, final, cols_ref, g_ref, w_ref, init_ref, recv_ref, *rest):
    if final:
        x_ref, gain_ref, _, whole_ref, dx_ref, sum_ref, acc, w_buf, sems, paste_sems, init_sem, sum_acc = rest
    else:
        _, whole_ref, acc, w_buf, sems, paste_sems = rest
    j = pl.program_id(0)
    slot = lax.rem(j, 2)
    width = w_buf.shape[2] // 2
    other = cols_ref[2 * pl.num_programs(0)]

    def loads(step, at):
        for i in range(2):
            col = pl.multiple_of(cols_ref[2 * step + i], HEAD)
            yield pltpu.make_async_copy(w_ref.at[:, pl.ds(col, width)], w_buf.at[at, :, pl.ds(i * width, width)], sems.at[at, i])

    def pastes():
        return column_copies(recv_ref, whole_ref, lambda i: paste_sems.at[i], j * recv_ref.shape[0], places_of(other))

    @pl.when(j == 0)
    def _():
        start_all(loads(0, 0))
        if final:
            init = pltpu.make_async_copy(init_ref, acc, init_sem)
            init.start()
            init.wait()
        else:
            acc[...] = init_ref[...].astype(F32) * ALPHA

    @pl.when(j + 1 < pl.num_programs(0))
    def _():
        start_all(loads(j + 1, 1 - slot))

    @pl.when(j < n_paste)
    def _():
        start_all(pastes())

    wait_all(loads(j, slot))
    acc[...] += dot(g_ref[0], w_buf[slot], 1, 1)

    if final:
        @pl.when(j == pl.num_programs(0) - 1)
        def _():
            sum_acc[...] = jnp.zeros_like(sum_acc)
            gain = gain_ref[...].astype(F32)
            rows = 16

            @pl.loop(0, acc.shape[0] // rows)
            def _(i):
                span = pl.ds(pl.multiple_of(i * rows, rows), rows)
                d_n = acc[span]
                x = x_ref[span].astype(F32)
                x = x - jnp.mean(x, axis=-1, keepdims=True)
                inv = lax.rsqrt(jnp.mean(x * x, axis=-1, keepdims=True) + LN_EPS)
                x = x * inv
                d_x = d_n * gain
                mean = jnp.mean(d_x, axis=-1, keepdims=True)
                slope = jnp.mean(d_x * x, axis=-1, keepdims=True)
                dx_ref[span] = (inv * (d_x - mean - x * slope)).astype(BF16)
                prod = d_n * x
                sum_acc[0] += prod[:8] + prod[8:]
                sum_acc[1] += d_n[:8] + d_n[8:]

            sum_ref[...] = jnp.sum(sum_acc[...], axis=1)

    @pl.when(j < n_paste)
    def _():
        wait_all(pastes())


def normed_grad(cols, g_tok, w_qkv, init, recv, places_of, n_paste, whole, norm=None):
    steps, rows, width = g_tok.shape
    hidden = w_qkv.shape[0]
    flat = pl.BlockSpec((rows, hidden), lambda j, cols: (0, 0))
    block = pl.BlockSpec((hidden // n_paste, recv.shape[1]), lambda j, cols: (jnp.minimum(j, n_paste - 1), 0))
    args = [cols, g_tok, w_qkv, init, recv]
    specs = [pl.BlockSpec((1, rows, width), lambda j, cols: (j, 0, 0)), ANY, ANY if norm else flat, block]
    outs, out_specs = [jax.ShapeDtypeStruct(whole.shape, F32)], [ANY]
    scratch = [pltpu.VMEM((2, hidden, width), BF16), dma_sems(2, 2), dma_sems(8)]
    if norm:
        args += list(norm)
        specs += [flat, pl.BlockSpec((1, hidden), lambda j, cols: (0, 0))]
        outs += [jax.ShapeDtypeStruct((rows, hidden), BF16), jax.ShapeDtypeStruct((2, hidden), F32)]
        out_specs += [flat, pl.BlockSpec((2, hidden), lambda j, cols: (0, 0))]
        scratch = [pltpu.VMEM((rows, hidden), F32)] + scratch + [pltpu.SemaphoreType.DMA, pltpu.VMEM((2, 8, hidden), F32)]
    else:
        outs.append(jax.ShapeDtypeStruct((rows, hidden), F32))
        out_specs.append(flat)
    return pl.pallas_call(
        functools.partial(normed_grad_kernel, places_of, n_paste, norm is not None),
        grid_spec=pltpu.PrefetchScalarGridSpec(
            num_scalar_prefetch=1,
            grid=(steps,),
            in_specs=specs + [ANY],
            out_specs=out_specs,
            scratch_shapes=scratch,
        ),
        out_shape=outs,
        input_output_aliases={len(args): 0},
        compiler_params=pltpu.CompilerParams(vmem_limit_bytes=62 * MIB),
        cost_estimate=cost(2 * rows * steps * width * hidden, 2 * steps * width * (rows + hidden) + 8 * rows * hidden + 8 * recv.size),
        name='dn',
    )(*args, whole)


def output_kernel(n_dist, core_ref, ctx_ref, shared_ref, w_ref, w_shared_ref, n_ref, b_ref, out_ref, acc):
    j = pl.program_id(0)

    @pl.when(j == 0)
    def _():
        acc[...] = dot(ctx_ref[0], w_ref[...], 1, 0)

    @pl.when(jnp.logical_and(j > 0, j < n_dist))
    def _():
        acc[...] += dot(ctx_ref[0], w_ref[...], 1, 0)

    @pl.when(j >= n_dist)
    def _():
        acc[...] += dot(shared_ref[0], w_shared_ref[...], 1, 0)

    @pl.when(j == pl.num_programs(0) - 1)
    def _():
        out_ref[...] = (ALPHA * n_ref[...].astype(F32) + (acc[...] + b_ref[...].astype(F32))).astype(BF16)


def project_out(core, ctx_tok, shared_tok, w_o, normed, b_o):
    n_dev, rows, cols = ctx_tok.shape
    n_core, _, shared = shared_tok.shape
    hidden = w_o.shape[1]
    base = n_dev * cols // shared

    def dist_index(j, core):
        at = jnp.minimum(j, n_dev - 1)
        return jnp.where(at < n_dev // 2, 2 * at + core[0], 2 * (at - n_dev // 2) + 1 - core[0])

    def shared_index(j, core):
        return jnp.where(j <= n_dev, core[0], 1 - core[0])

    whole = pl.BlockSpec((rows, hidden), lambda j, core: (0, 0))
    return pl.pallas_call(
        functools.partial(output_kernel, n_dev),
        grid_spec=pltpu.PrefetchScalarGridSpec(
            num_scalar_prefetch=1,
            grid=(n_dev + n_core,),
            in_specs=[
                pl.BlockSpec((1, rows, cols), lambda j, core: (jnp.minimum(j, n_dev - 1), 0, 0)),
                pl.BlockSpec((1, rows, shared), lambda j, core: (jnp.maximum(j - n_dev, 0), 0, 0)),
                pl.BlockSpec((cols, hidden), lambda j, core: (dist_index(j, core), 0)),
                pl.BlockSpec((shared, hidden), lambda j, core: (base + shared_index(j, core), 0)),
                whole,
                pl.BlockSpec((1, hidden), lambda j, core: (0, 0)),
            ],
            out_specs=whole,
            scratch_shapes=[pltpu.VMEM((rows, hidden), F32)],
        ),
        out_shape=jax.ShapeDtypeStruct((rows, hidden), BF16),
        compiler_params=pltpu.CompilerParams(vmem_limit_bytes=56 * MIB),
        cost_estimate=cost(2 * rows * hidden * hidden, 2 * hidden * hidden + 6 * rows * hidden),
        name='out_proj',
    )(core, ctx_tok, shared_tok, w_o, w_o, normed, b_o.reshape(1, -1))


def together(*values):
    return lax.optimization_barrier(values)


def solution(mesh):
    n_dev = mesh.shape['sp']
    tok_spec = P('dp', 'sp', None)
    pos_spec = P('dp', 'sp')
    in_specs = (tok_spec, pos_spec, pos_spec, P('dp'), P(), P(), P(), P(), P(), P(), tok_spec)
    out_specs = (tok_spec, tok_spec, P('dp'), P('dp'), P('dp', None), P('dp'), P('dp', None), P('dp'))
    same_core = [list(range(core, n_dev, 2)) for core in range(2)]
    partners = [(dev, dev ^ 1) for dev in range(n_dev)]
    n_chip = n_dev // 2

    def device_step(hidden_in, pos_ids, block_pos, prefix_len, ln_gamma, ln_beta, w_qkv, b_qkv, w_o, b_o, grad_out):
        batch, local_len, hidden = hidden_in.shape
        per_half = batch // 2
        heads = hidden // HEAD
        n_dist, n_shared = (heads - SHARED) // n_dev, SHARED // 2
        shared_at = n_dev * n_dist
        rows = batch * local_len
        tokens = n_dev * rows
        rank = lax.axis_index('sp')
        parity = lax.rem(rank, 2)
        pair = rank + 1 - 2 * parity
        core = parity.reshape(1).astype(jnp.int32)
        gather = functools.partial(lax.all_gather, axis_name='sp')
        gather_core = functools.partial(lax.all_gather, axis_name='sp', axis_index_groups=same_core)
        to_partner = functools.partial(lax.ppermute, axis_name='sp', perm=partners)

        def token_rows(arr, dev):
            split = arr.reshape(arr.shape[:-2] + (2, n_dev, rows // 2, arr.shape[-1]))
            return lax.dynamic_index_in_dim(split, dev, axis=split.ndim - 3, keepdims=False).reshape(arr.shape[:-2] + (rows, arr.shape[-1]))

        def places(head):
            return lambda par: [((2 * c + par) * n_dist + head) * WIDTH for c in range(n_chip)]

        def shared_places(par):
            return [(shared_at + par * n_shared + i) * WIDTH for i in range(n_shared)]

        def wo_tile(t, par):
            spread = t - n_shared
            return jnp.where(t < n_shared, shared_at + par * n_shared + t, (2 * (spread // n_dist) + par) * n_dist + lax.rem(spread, n_dist))

        halves = range(2)
        normed = layer_norm(hidden_in.astype(F32), ln_gamma.astype(F32), ln_beta.astype(F32)).astype(BF16)
        sends = [arr[half * per_half:(half + 1) * per_half] for arr in (normed, grad_out) for half in halves]
        n_a, n_b, dy_a, dy_b = [gather(part) for part in together(*sends)]
        cos, sin = rope_tables(prefix_len, n_dev * local_len)
        prefix = [prefix_len[half * per_half:(half + 1) * per_half] for half in halves]
        starts = jnp.stack([rank * n_dist, shared_at + parity * n_shared]).astype(jnp.int32)
        bias = jnp.concatenate([
            lax.dynamic_slice_in_dim(b_qkv, starts[0] * WIDTH, n_dist * WIDTH),
            lax.dynamic_slice_in_dim(b_qkv, starts[1] * WIDTH, n_shared * WIDTH)]).astype(F32).reshape(1, -1)
        grad_bo = jnp.sum(grad_out.astype(F32), axis=(0, 1))
        n_a, grad_bo = together(n_a, grad_bo)

        ctx_d = ctx_r = None
        qkv, lses = [], []
        for half in halves:
            if half:
                n_b, ctx_r = together(n_b, ctx_r)
            qd, kd, vd, qr, kr, vr = project_qkv(half, starts, n_dist, n_shared, n_b if half else n_a, w_qkv, bias, cos, sin)
            ctx_d, lse_d = attention_forward(half, prefix[half], qd, kd, vd, n_dev, ctx_d)
            qr, ctx_d = together(qr, ctx_d)
            ctx_r, lse_r = attention_forward(half, prefix[half], qr, kr, vr, n_dev, ctx_r)
            qkv.append((qd, kd, vd, qr, kr, vr))
            lses.append((lse_d, lse_r))
        ctx_par = gather_core(ctx_d.reshape(tokens, n_dist * HEAD))

        dy_a, ctx_r = together(dy_a, ctx_r)
        g_d = g_r = None
        sum_d, sum_r = [], []
        for half in halves:
            if half:
                dy_b, g_r = together(dy_b, g_r)
            qd, kd, vd, qr, kr, vr = qkv[half]
            d_ctx = context_grad(starts, n_dist + n_shared, dy_b if half else dy_a, w_o)
            g_d, sums = attention_backward(half, 0, prefix[half], qd, kd, vd, ctx_d, d_ctx, lses[half][0], cos, sin, g_d)
            sum_d.append(sums)
            qr, g_d = together(qr, g_d)
            g_r, sums = attention_backward(half, n_dist, prefix[half], qr, kr, vr, ctx_r, d_ctx, lses[half][1], cos, sin, g_r)
            sum_r.append(sums)
        g_d = g_d.reshape(n_dist, tokens, WIDTH)
        g_r = g_r.reshape(n_shared, tokens, WIDTH)
        g_par = [gather_core(g_d[head]) for head in range(n_dist)]
        sums = [jnp.sum(jnp.concatenate(part), axis=(0, 1)) for part in (sum_d, sum_r)]

        n_a, n_b, dy_a, dy_b = [part.reshape(tokens // 2, hidden) for part in (n_a, n_b, dy_a, dy_b)]
        ctx_r = ctx_r.reshape(tokens, n_shared * HEAD)
        r_recv, shared_recv = to_partner(token_rows(g_r, pair)), to_partner(token_rows(ctx_r, pair))
        ctx_r, g_r = together(ctx_r, g_r)
        grad_wo, wo_block = weight_grad_o(
            core, ctx_r[None], dy_a, dy_b, lambda c, par: (shared_at + par * n_shared) * HEAD, lambda c: 0, hidden // 2, ())
        r_recv, shared_recv, wo_block, n_a = together(r_recv, shared_recv, wo_block, n_a)
        grad_wqkv, block = weight_grad_qkv(core, shared_places, n_a, n_b, g_r, None)
        ctx_recv = to_partner(token_rows(ctx_par, pair))
        ctx_par, ctx_recv, block = together(ctx_par, ctx_recv, block)
        recv_r = to_partner(block)
        grad_wo, wo_block = weight_grad_o(
            core, ctx_par, dy_a, dy_b, lambda c, par: (2 * c + par) * (n_dist * HEAD), lambda c: (n_shared + c * n_dist) * HEAD,
            hidden // 2, (grad_wo, wo_block))
        ctx_tok = jnp.concatenate([token_rows(ctx_par, rank), ctx_recv])
        ctx_tok, wo_block = together(ctx_tok, wo_block)
        wo_recv = to_partner(wo_block)
        shared_tok = jnp.stack([token_rows(ctx_r, rank), shared_recv])
        hidden_out = project_out(core, ctx_tok, shared_tok, w_o, normed.reshape(rows, hidden), b_o)
        n_a, hidden_out, g_par[0] = together(n_a, hidden_out, g_par[0])

        recvs, tok = [recv_r], []
        for head in range(n_dist):
            extra = [dict(recv=recv_r, old_places_of=shared_places), dict(wo=(wo_recv, grad_wo, wo_tile)), dict(recv=recvs[1] if head > 1 else None, old_places_of=places(0))][head]
            res = weight_grad_qkv(core, places(head), n_a, n_b, g_par[head], grad_wqkv, **extra)
            grad_wqkv, block = res[:2]
            if head == 1:
                grad_wo = res[2]
            tok_recv = to_partner(token_rows(g_par[head], pair))
            tok_recv, block = together(tok_recv, block)
            if head + 1 < n_dist:
                g_par[head + 1], block = together(g_par[head + 1], block)
            tok.append((token_rows(g_par[head], rank), tok_recv))
            recvs.append(to_partner(block))

        g_first = [jnp.concatenate([part[0::2], part[1::2]], axis=2) for part in (token_rows(g_r, rank), r_recv)]
        g_first += [jnp.concatenate([tok[0][side], tok[1][side]], axis=2) for side in range(2)]

        def columns(table):
            at = [np.array([h * WIDTH for h in table(par)] + [1 - par], np.int32) for par in range(2)]
            return jnp.asarray(at[0]) + parity.astype(jnp.int32) * jnp.asarray(at[1] - at[0])

        cols = columns(lambda mine: [shared_at + par * n_shared + i for par in (mine, 1 - mine) for i in range(n_shared)] + [
            (2 * c + par) * n_dist + head for par in (mine, 1 - mine) for c in range(n_chip) for head in (0, 1)])
        grad_wqkv, d_norm = normed_grad(cols, jnp.concatenate(g_first), w_qkv, grad_out.reshape(rows, hidden), recvs[2], places(1), 8, grad_wqkv)
        cols = columns(lambda mine: [(2 * c + par) * n_dist + 2 for c in range(n_chip) for par in (mine, 1 - mine)])
        grad_wqkv, grad_in, norm_sums = normed_grad(
            cols, jnp.concatenate(tok[2], axis=2), w_qkv, d_norm, recvs[3], places(2), 4, grad_wqkv,
            (hidden_in.reshape(rows, hidden), ln_gamma.reshape(1, hidden)))
        small = gather(jnp.concatenate(sums + [norm_sums.reshape(-1), grad_bo]))
        spread, shared = small[:, :n_dist * WIDTH], small[:2, n_dist * WIDTH:(n_dist + n_shared) * WIDTH]
        grad_bqkv = jnp.concatenate([spread.reshape(-1), shared.reshape(-1)])
        grad_gamma, grad_beta, grad_bo = jnp.sum(small[:, (n_dist + n_shared) * WIDTH:], axis=0).reshape(3, hidden)
        shape = (batch, local_len, hidden)
        return (hidden_out.reshape(shape), grad_in.reshape(shape), grad_gamma, grad_beta, grad_wqkv, grad_bqkv, grad_wo, grad_bo)

    return jax.shard_map(device_step, mesh=mesh, in_specs=in_specs, out_specs=out_specs, check_vma=False)
```

```python
import functools
import math
import jax
import jax.numpy as jnp
import numpy as np
from jax import lax
from jax.experimental import pallas as pl
from jax.experimental.pallas import tpu as pltpu
from jax.sharding import PartitionSpec as P

HEAD = 128
QUARTER = 32
ALPHA = math.sqrt(56.0)
LN_EPS = 1e-5
ROT_BASE = 10000.0
SCALE = 1.0 / math.sqrt(HEAD)
LOG2E = math.log2(math.e)
MASK_FILL = -1e30
BLK = 256
VMEM_BIG = pltpu.CompilerParams(vmem_limit_bytes=62 << 20)
SHARED = 8
Z = 0
SLOTS = 2
WIDTH = 3 * HEAD
F32 = jnp.float32
BF16 = jnp.bfloat16


def dot(lhs, rhs, lhs_dim, rhs_dim):
    return lax.dot_general(lhs, rhs, (((lhs_dim,), (rhs_dim,)), ((), ())), preferred_element_type=F32)


def dot_nn(lhs, rhs):
    return dot(lhs, rhs, 1, 0)


def dot_nt(lhs, rhs):
    return dot(lhs, rhs, 1, 1)


def dot_tn(lhs, rhs):
    return dot(lhs, rhs, 0, 0)


def matmul_cost(rows, depth, cols, extra=0):
    return pl.CostEstimate(
        flops=2 * rows * depth * cols, bytes_accessed=2 * (rows * depth + depth * cols + rows * cols) + extra, transcendentals=0)


def attention_cost(n_head, batch, seq, products):
    pairs = n_head * batch * seq * seq
    return pl.CostEstimate(flops=2 * products * pairs * HEAD, bytes_accessed=8 * products * n_head * batch * seq * HEAD, transcendentals=pairs)


def run(index, size):
    return pl.ds(pl.multiple_of(index * size, size), size)


def part(index, size):
    return slice(index * size, (index + 1) * size)


def rope_tables(prefix_len, seq):
    tok = jnp.arange(seq, dtype=jnp.int32)[None, :]
    pre = prefix_len[:, None]
    inside = tok < pre
    pos = jnp.where(inside, tok, pre - 1)
    blk = jnp.where(inside, 0, tok - pre + 1)
    inv_freq = ROT_BASE ** (-jnp.arange(QUARTER, dtype=F32) / QUARTER)
    angles = jnp.stack([pos, blk], axis=-1).astype(F32)[..., None] * inv_freq
    cos, sin = jnp.cos(angles), jnp.sin(angles)
    shape = pos.shape + (HEAD,)
    return (jnp.stack([cos, cos], axis=-2).reshape(shape), jnp.stack([-sin, sin], axis=-2).reshape(shape))


def turn(x, cos, sin):
    lane = lax.broadcasted_iota(jnp.int32, x.shape, 1)
    other = jnp.where(lane % (2 * QUARTER) < QUARTER, pltpu.roll(x, HEAD - QUARTER, 1), pltpu.roll(x, QUARTER, 1))
    return x * cos + other * sin


def dma_sems(*shape):
    return pltpu.SemaphoreType.DMA(shape)


def dma_sems(*shape):
    return pltpu.SemaphoreType.DMA(shape)


def start_all(copies):
    for copy in copies:
        copy.start()


def wait_all(copies):
    for copy in copies:
        copy.wait()


ANY = pl.BlockSpec(memory_space=pl.ANY)
PIECES = 4


NORM_ROWS = 16


def centred(x):
    x = x.astype(F32)
    x = x - jnp.mean(x, axis=-1, keepdims=True)
    return x, lax.rsqrt(jnp.mean(x * x, axis=-1, keepdims=True) + LN_EPS)


def norm_kernel(x_ref, gain_ref, shift_ref, out_ref):
    gain, shift = gain_ref[...].astype(F32), shift_ref[...].astype(F32)

    @pl.loop(0, x_ref.shape[0] // NORM_ROWS)
    def _(i):
        rows = run(i, NORM_ROWS)
        x, inv = centred(x_ref[rows])
        out_ref[rows] = (x * inv * gain + shift).astype(BF16)


def normalize(half, x, gain, shift):
    rows, hidden = x.shape
    block = rows // 4
    vec = pl.BlockSpec((1, hidden), lambda i: (Z, Z))
    return pl.pallas_call(
        norm_kernel,
        grid=(2,),
        in_specs=[pl.BlockSpec((block, hidden), lambda i: (2 * half + i, Z)), vec, vec],
        out_specs=pl.BlockSpec((block, hidden), lambda i: (i, Z)),
        out_shape=jax.ShapeDtypeStruct((2 * block, hidden), BF16),
        compiler_params=VMEM_BIG,
        name='norm',
    )(x, gain, shift)


def qkv_kernel(n_dist, start_ref, n_ref, w_ref, b_ref, cos_ref, sin_ref, qd_ref, kd_ref, vd_ref, qr_ref, kr_ref, vr_ref, w_buf, acc, sems):
    rows = cos_ref.shape[1]
    hidden = n_ref.shape[-1]
    dist = n_dist * WIDTH
    shared = w_buf.shape[1] - dist
    first = jnp.logical_and(pl.program_id(0) == 0, pl.program_id(1) == 0)
    piece = hidden // PIECES

    def loads(i):
        span = run(i, piece)
        for kind, (at, width) in enumerate(((0, dist), (dist, shared))):
            col = pl.multiple_of(start_ref[kind] * WIDTH, HEAD)
            yield pltpu.make_async_copy(w_ref.at[span, pl.ds(col, width)], w_buf.at[span, pl.ds(at, width)], sems.at[i, kind])

    @pl.when(first)
    def _():
        for i in range(PIECES):
            start_all(loads(i))
        acc[...] = jnp.broadcast_to(b_ref[...], acc.shape)

        @pl.loop(0, PIECES)
        def _(i):
            wait_all(loads(i))
            span = run(i, piece)
            acc[...] += dot_nn(n_ref[:, :, :, span].reshape(rows, piece), w_buf[span])

    @pl.when(jnp.logical_not(first))
    def _():
        acc[...] = dot_nn(n_ref[...].reshape(rows, hidden), w_buf[...]) + b_ref[...]

    cos, sin = cos_ref[0], sin_ref[0]
    n_shared = qr_ref.shape[0]
    for h in range(n_dist + n_shared):
        q_ref, k_ref, v_ref, at = (qd_ref, kd_ref, vd_ref, h) if h < n_dist else (qr_ref, kr_ref, vr_ref, h - n_dist)
        pre_q, pre_k, pre_v = [acc[:, part(3 * h + i, HEAD)] for i in range(3)]
        q_ref[at, 0] = turn(pre_q, cos, sin).astype(BF16)
        k_ref[at, 0] = turn(pre_k, cos, sin).astype(BF16)
        v_ref[at, 0] = pre_v.astype(BF16)


def project_qkv(half, starts, n_dist, n_shared, n_half, w_qkv, bias, cos, sin):
    n_dev, batch, local_len, hidden = n_half.shape
    seq = n_dev * local_len
    cols = (n_dist + n_shared) * WIDTH
    per = 4
    rows = per * local_len
    outs, out_specs = [], []
    for n_head in (n_dist, n_shared):
        outs += [jax.ShapeDtypeStruct((n_head, batch, seq, HEAD), BF16)] * 3
        out_specs += [pl.BlockSpec((n_head, 1, rows, HEAD), lambda b, j, at: (Z, b, j, Z))] * 3
    tab_spec = pl.BlockSpec((1, rows, HEAD), lambda b, j, at: (half * batch + b, j, Z))
    return pl.pallas_call(
        functools.partial(qkv_kernel, n_dist),
        grid_spec=pltpu.PrefetchScalarGridSpec(
            num_scalar_prefetch=1,
            grid=(batch, n_dev // per),
            in_specs=[
                pl.BlockSpec((per, 1, local_len, hidden), lambda b, j, at: (j, b, Z, Z)),
                ANY,
                pl.BlockSpec((1, cols), lambda b, j, at: (Z, Z)),
                tab_spec, tab_spec,
            ],
            out_specs=out_specs,
            scratch_shapes=[
                pltpu.VMEM((hidden, cols), BF16), pltpu.VMEM((rows, cols), F32), dma_sems(PIECES, SLOTS)],
        ),
        out_shape=outs,
        compiler_params=VMEM_BIG,
        cost_estimate=matmul_cost(batch * seq, hidden, cols),
        name='qkv',
    )(starts, n_half, w_qkv, bias, cos, sin)


def forward_kernel(pre_ref, q_ref, k_ref, v_ref, *rest):
    ctx_ref, lse_ref = rest[-2:]
    n_head, _, seq, _ = q_ref.shape
    local_len = ctx_ref.shape[3]
    per = BLK // local_len
    prefix = pre_ref[pl.program_id(0)]

    def block(r, n_key):
        query = lax.broadcasted_iota(jnp.int32, (1, BLK), 1) + r * BLK
        last = jnp.maximum(query, prefix - 1) - (n_key - 1) * BLK
        scores = []
        for h in range(n_head):
            q_blk = q_ref[h, 0, part(r, BLK)]
            parts = [dot_nt(k_ref[h, 0, part(c, BLK)], q_blk) * (SCALE * LOG2E) for c in range(n_key)]
            key = lax.broadcasted_iota(jnp.int32, (BLK, BLK), 0)
            parts[-1] = jnp.where(key <= last, parts[-1], MASK_FILL)
            scores.append(parts)
        for h, parts in enumerate(scores):
            top = functools.reduce(jnp.maximum, [jnp.max(p, axis=0, keepdims=True) for p in parts])
            parts = [jnp.exp2(p - top) for p in parts]
            total = functools.reduce(jnp.add, [jnp.sum(p, axis=0, keepdims=True) for p in parts])
            inv = 1.0 / total
            probs = jnp.concatenate([(p * inv).astype(BF16) for p in parts], axis=0)
            ctx_t = dot_tn(v_ref[h, 0, :n_key * BLK], probs)
            ctx = ctx_t.T.astype(BF16).reshape(per, local_len, HEAD)
            ctx_ref[0, part(r, per), 0, :, part(h, HEAD)] = ctx
            lse_ref[h, 0, :, part(r, BLK)] = top + jnp.log2(total)

    n_blk = seq // BLK
    for r in range(n_blk):
        for n_key in range(r + 1, n_blk + 1):
            low = (n_key - 1) * BLK
            cond = prefix <= n_key * BLK if n_key == r + 1 else prefix > low
            if n_key < n_blk and n_key > r + 1:
                cond = jnp.logical_and(cond, prefix <= n_key * BLK)
            if n_key == n_blk and n_key == r + 1:
                block(r, n_key)
            else:
                pl.when(cond)(functools.partial(block, r, n_key))


def attention_forward(half, prefix_half, q, k, v, n_dev, ctx):
    own, batch, seq, _ = q.shape
    local_len = seq // n_dev
    qkv_spec = pl.BlockSpec((own, 1, seq, HEAD), lambda b, pre: (Z, b, Z, Z))
    earlier = [] if ctx is None else [ctx]
    return pl.pallas_call(
        forward_kernel,
        grid_spec=pltpu.PrefetchScalarGridSpec(
            num_scalar_prefetch=1,
            grid=(batch,),
            in_specs=[qkv_spec] * 3 + [ANY] * len(earlier),
            out_specs=[
                pl.BlockSpec((1, n_dev, 1, local_len, own * HEAD), lambda b, pre: (half, Z, b, Z, Z)),
                pl.BlockSpec((own, 1, 1, seq), lambda b, pre: (Z, b, Z, Z)),
            ],
        ),
        out_shape=[
            jax.ShapeDtypeStruct((2, n_dev, batch, local_len, own * HEAD), BF16),
            jax.ShapeDtypeStruct((own, batch, 1, seq), F32),
        ],
        input_output_aliases={4: 0} if earlier else {},
        compiler_params=VMEM_BIG,
        cost_estimate=attention_cost(own, batch, seq, 2),
        name='attn_fwd',
    )(prefix_half, q, k, v, *earlier)


def d_ctx_kernel(start_ref, dy_ref, w_ref, out_ref, w_buf, sems):
    per, _, local_len, hidden = dy_ref.shape
    first = jnp.logical_and(pl.program_id(0) == 0, pl.program_id(1) == 0)
    shared = SHARED // 2 * HEAD
    widths = (shared, out_ref.shape[-1] - shared)

    def loads():
        at = 0
        for kind, width in enumerate(widths):
            row = pl.multiple_of(start_ref[1 - kind] * HEAD, HEAD)
            yield pltpu.make_async_copy(w_ref.at[pl.ds(row, width)], w_buf.at[pl.ds(at, width)], sems.at[kind])
            at += width

    @pl.when(first)
    def _():
        start_all(loads())
        wait_all(loads())

    res = dot_nt(dy_ref[...].reshape(per * local_len, hidden), w_buf[...])
    out_ref[...] = res.astype(BF16).reshape(per, 1, local_len, w_buf.shape[0])


def context_grad(starts, n_own, dy_half, w_o):
    n_dev, batch, local_len, hidden = dy_half.shape
    cols = n_own * HEAD
    per = 4
    return pl.pallas_call(
        d_ctx_kernel,
        grid_spec=pltpu.PrefetchScalarGridSpec(
            num_scalar_prefetch=1,
            grid=(batch, n_dev // per),
            in_specs=[pl.BlockSpec((per, 1, local_len, hidden), lambda b, j, at: (j, b, Z, Z)), ANY],
            out_specs=pl.BlockSpec((per, 1, local_len, cols), lambda b, j, at: (j, b, Z, Z)),
            scratch_shapes=[pltpu.VMEM((cols, hidden), BF16), dma_sems(2)],
        ),
        out_shape=jax.ShapeDtypeStruct((n_dev, batch, local_len, cols), BF16),
        compiler_params=VMEM_BIG,
        cost_estimate=matmul_cost(n_dev * batch * local_len, hidden, cols),
        name='dctx',
    )(starts, dy_half, w_o)


def backward_kernel(pre_ref, q_ref, k_ref, v_ref, ctx_ref, dctx_ref, lse_ref, cos_ref, sin_ref, *rest):
    g_ref, sum_ref, dq_acc, dk_acc, dv_acc = rest[-5:]
    n_head, _, seq, _ = q_ref.shape
    n_dev, local_len = g_ref.shape[2], g_ref.shape[4]
    n_blk = seq // BLK
    prefix = pre_ref[pl.program_id(1)]
    d_ctx, delta = [], []
    for h in range(n_head):
        lanes = part(h, HEAD)
        grad = dctx_ref[:, :, :, lanes].reshape(seq, HEAD)
        prod = grad.astype(F32) * ctx_ref[0, :, :, :, lanes].reshape(seq, HEAD).astype(F32)
        d_ctx.append(grad)
        delta.append(jnp.sum(prod.T, axis=0, keepdims=True))

    def block(c, first):
        span = part(c, BLK)
        start = first * BLK
        products = []
        for h in range(n_head):
            s_t = dot_nt(k_ref[h, 0, span], q_ref[h, 0, start:])
            dp_t = dot_nt(v_ref[h, 0, span], d_ctx[h][start:])
            products.append((s_t, dp_t))
        for h, (s_t, dp_t) in enumerate(products):
            probs, d_scores = [], []
            for r in range(first, n_blk):
                cols, here = part(r, BLK), part(r - first, BLK)
                piece = s_t[:, here] * (SCALE * LOG2E)
                if r <= c:
                    key = lax.broadcasted_iota(jnp.int32, (BLK, BLK), 0)
                    query = lax.broadcasted_iota(jnp.int32, (1, BLK), 1) + r * BLK
                    piece = jnp.where(key <= jnp.maximum(query, prefix - 1) - c * BLK, piece, MASK_FILL)
                p = jnp.exp2(piece - lse_ref[h, 0, :, cols])
                probs.append(p.astype(BF16))
                d_scores.append((p * (dp_t[:, here] - delta[h][:, cols]) * SCALE).astype(BF16))
            probs = jnp.concatenate(probs, axis=1)
            d_scores = jnp.concatenate(d_scores, axis=1)
            dv_acc[h, span] = dot_nn(probs, d_ctx[h][start:])
            dk_acc[h, span] = dot_nn(d_scores, q_ref[h, 0, start:])
            dq_part = dot_tn(k_ref[h, 0, span], d_scores)
            if c:
                dq_acc[h, :, start:] += dq_part
            else:
                dq_acc[h] = dq_part

    block(0, 0)
    for c in range(1, n_blk):
        pl.when(prefix > c * BLK)(functools.partial(block, c, 0))
        pl.when(prefix <= c * BLK)(functools.partial(block, c, c))

    cos, sin = cos_ref[0], sin_ref[0]
    for h in range(n_head):
        g_q = turn(dq_acc[h].T.astype(BF16).astype(F32), cos, -sin)
        g_k = turn(dk_acc[h].astype(BF16).astype(F32), cos, -sin)
        g_v = dv_acc[h].astype(BF16).astype(F32)
        for i, g in enumerate((g_q, g_k, g_v)):
            lanes = part(i, HEAD)
            g_ref[h, 0, :, 0, :, lanes] = g.astype(BF16).reshape(n_dev, local_len, HEAD)
            sum_ref[h, 0, :, lanes] = jnp.sum(g, axis=0, keepdims=True)


def attention_backward(half, d_col, prefix_half, q, k, v, ctx, d_ctx, lse, cos, sin, g_all, group=1):
    n_head, batch, seq, _ = q.shape
    _, n_dev, _, local_len, _ = ctx.shape
    qkv_spec = pl.BlockSpec((group, 1, seq, HEAD), lambda h, b, pre: (h, b, Z, Z))
    tab_spec = pl.BlockSpec((1, seq, HEAD), lambda h, b, pre: (half * batch + b, Z, Z))
    earlier = [] if g_all is None else [g_all]
    stat = functools.partial(pltpu.VMEM, dtype=F32)
    return pl.pallas_call(
        backward_kernel,
        grid_spec=pltpu.PrefetchScalarGridSpec(
            num_scalar_prefetch=1,
            grid=(n_head // group, batch),
            in_specs=[qkv_spec] * 3 + [
                pl.BlockSpec((1, n_dev, 1, local_len, group * HEAD), lambda h, b, pre: (half, Z, b, Z, h)),
                pl.BlockSpec((n_dev, 1, local_len, group * HEAD), lambda h, b, pre: (Z, b, Z, d_col // group + h)),
                pl.BlockSpec((group, 1, 1, seq), lambda h, b, pre: (h, b, Z, Z)), tab_spec, tab_spec] + [ANY] * len(earlier),
            out_specs=[
                pl.BlockSpec((group, 1, n_dev, 1, local_len, WIDTH), lambda h, b, pre: (h, half, Z, b, Z, Z)),
                pl.BlockSpec((group, 1, 1, WIDTH), lambda h, b, pre: (h, b, Z, Z)),
            ],
            scratch_shapes=[stat((group, HEAD, seq)), stat((group, seq, HEAD)), stat((group, seq, HEAD))],
        ),
        out_shape=[
            jax.ShapeDtypeStruct((n_head, 2, n_dev, batch, local_len, WIDTH), BF16),
            jax.ShapeDtypeStruct((n_head, batch, 1, WIDTH), F32),
        ],
        input_output_aliases={9: 0} if earlier else {},
        compiler_params=VMEM_BIG,
        cost_estimate=attention_cost(n_head, batch, seq, 5),
        name='attn_bwd',
    )(prefix_half, q, k, v, ctx, d_ctx, lse, cos, sin, *earlier)


def wo_grad_kernel(row_of, block_row_of, core_ref, ctx_ref, dya_ref, dyb_ref, *rest):
    out_ref, copy_ref, rhs, buf, rhs_sems, sems = rest[-6:]
    n, c = pl.program_id(0), pl.program_id(1)
    n_col, n_grp = pl.num_programs(0), pl.num_programs(1)
    step = n * n_grp + c
    slot, n_slot = lax.rem(step, SLOTS), lax.rem(n, SLOTS)
    _, rows, wide = buf.shape
    half = dya_ref.shape[0]
    core = core_ref[0]

    def loads(n_at, at):
        for i, ref in enumerate((dya_ref, dyb_ref)):
            yield pltpu.make_async_copy(ref.at[:, run(n_at, wide)], rhs.at[at, run(i, half)], rhs_sems.at[at, i])

    def stores(at_step, at):
        n_at, c_at = at_step // n_grp, lax.rem(at_step, n_grp)
        for i, (ref, row) in enumerate(((out_ref, row_of(c_at, core)), (copy_ref, block_row_of(c_at)))):
            yield pltpu.make_async_copy(buf.at[at], ref.at[pl.ds(pl.multiple_of(row, HEAD), rows), run(n_at, wide)], sems.at[at, i])

    @pl.when(step == 0)
    def _():
        start_all(loads(0, 0))

    @pl.when(c == 0)
    def _():
        @pl.when(n + 1 < n_col)
        def _():
            start_all(loads(n + 1, 1 - n_slot))

        wait_all(loads(n, n_slot))

    @pl.when(step >= 2)
    def _():
        wait_all(stores(step - 2, slot))

    buf[slot] = dot_tn(ctx_ref[0], rhs[n_slot])
    start_all(stores(step, slot))

    @pl.when(step == n_col * n_grp - 1)
    def _():
        wait_all(stores(step - 1, 1 - slot))
        wait_all(stores(step, slot))


def weight_grad_o(core, ctx_par, dy_a, dy_b, row_of, block_row_of, block_rows, earlier):
    n_grp, tokens, cols = ctx_par.shape
    hidden = dy_a.shape[1]
    wide = hidden // 4
    return pl.pallas_call(
        functools.partial(wo_grad_kernel, row_of, block_row_of),
        grid_spec=pltpu.PrefetchScalarGridSpec(
            num_scalar_prefetch=1,
            grid=(hidden // wide, n_grp),
            in_specs=[pl.BlockSpec((1, tokens, cols), lambda n, c, core: (c, Z, Z)), ANY, ANY] + [ANY] * len(earlier),
            out_specs=[ANY, ANY],
            scratch_shapes=[pltpu.VMEM((SLOTS, tokens, wide), BF16), pltpu.VMEM((SLOTS, cols, wide), F32), dma_sems(SLOTS, SLOTS), dma_sems(SLOTS, SLOTS)],
        ),
        out_shape=[jax.ShapeDtypeStruct((hidden, hidden), F32), jax.ShapeDtypeStruct((block_rows, hidden), F32)],
        input_output_aliases={4: 0, 5: 1} if earlier else {},
        compiler_params=VMEM_BIG,
        cost_estimate=matmul_cost(n_grp * cols, tokens, hidden, 8 * hidden * n_grp * cols),
        name='wo_grad',
    )(core, ctx_par, dy_a, dy_b, *earlier)


def column_copies(src, out_ref, sem_of, row, places):
    rows, width = src.shape[0], src.shape[1] // len(places)
    for i, col in enumerate(places):
        yield pltpu.make_async_copy(
            src.at[:, run(i, width)],
            out_ref.at[pl.ds(pl.multiple_of(row, BLK), rows), pl.ds(pl.multiple_of(col, HEAD), width)],
            sem_of(i))


def wqkv_grad_kernel(places_of, old_places_of, wo_tile, core_ref, na_ref, nb_ref, g_ref, *rest):
    rest = list(rest)
    recv_ref = rest.pop(0) if old_places_of else None
    wo_recv_ref = rest.pop(0) if wo_tile else None
    n_buf, rhs, buf, n_sems, g_sems, out_sems, copy_sems, paste_sems, wo_sems = rest[-9:]
    outs = rest[:-9][-3 if wo_tile else -2:]
    out_ref, copy_ref = outs[:2]
    m = pl.program_id(0)
    n_m = pl.num_programs(0)
    core = core_ref[0]
    n_grp, tokens, cols = g_ref.shape
    half, rows = tokens // 2, n_buf.shape[2]
    piece = tokens // PIECES
    slot = lax.rem(m, SLOTS)

    def n_loads(step, at):
        for i, ref in enumerate((na_ref, nb_ref)):
            yield pltpu.make_async_copy(ref.at[:, run(step, rows)], n_buf.at[at, run(i, half)], n_sems.at[at, i])

    def g_loads(i):
        for c in range(n_grp):
            yield pltpu.make_async_copy(g_ref.at[c, run(i, piece)], rhs.at[run(i, piece), run(c, cols)], g_sems.at[i, c])

    def stores(step, at):
        yield from column_copies(buf.at[at], out_ref, lambda i: out_sems.at[at, i], step * rows, places_of(core))
        yield pltpu.make_async_copy(buf.at[at], copy_ref.at[run(step, rows)], copy_sems.at[at])

    def pastes():
        if old_places_of:
            yield from column_copies(recv_ref, out_ref, lambda i: paste_sems.at[i], m * rows, old_places_of(1 - core))
        if wo_tile:
            tiles = wo_recv_ref.shape[0] // HEAD
            for t in range(tiles):
                tile = wo_tile(m * tiles + t, 1 - core)
                yield pltpu.make_async_copy(wo_recv_ref.at[run(t, HEAD)], outs[2].at[run(tile, HEAD)], wo_sems.at[t])

    @pl.when(m == 0)
    def _():
        start_all(n_loads(0, 0))
        for i in range(PIECES):
            start_all(g_loads(i))

    @pl.when(m + 1 < n_m)
    def _():
        start_all(n_loads(m + 1, 1 - slot))

    start_all(pastes())

    @pl.when(m >= 2)
    def _():
        wait_all(stores(m - 2, slot))

    wait_all(n_loads(m, slot))

    @pl.when(m == 0)
    def _():
        buf[slot] = jnp.zeros((rows, n_grp * cols), F32)

        @pl.loop(0, PIECES)
        def _(i):
            wait_all(g_loads(i))
            buf[slot] += dot_tn(n_buf[slot, run(i, piece)], rhs[run(i, piece)])

    @pl.when(m > 0)
    def _():
        buf[slot] = dot_tn(n_buf[slot], rhs[...])

    start_all(stores(m, slot))
    wait_all(pastes())

    @pl.when(m == n_m - 1)
    def _():
        wait_all(stores(m - 1, 1 - slot))
        wait_all(stores(m, slot))


def weight_grad_qkv(core, places_of, n_a, n_b, g_par, whole, recv=None, old_places_of=None, wo=None):
    hidden = n_a.shape[1]
    n_grp, tokens, cols = g_par.shape
    width = n_grp * cols
    rows = 2 * BLK
    steps = hidden // rows
    args, specs, alias = [core, n_a, n_b, g_par], [ANY, ANY, ANY], {}
    outs = [jax.ShapeDtypeStruct((hidden, 3 * hidden), F32), jax.ShapeDtypeStruct((hidden, width), F32)]
    wo_tile = None
    if recv is not None:
        args.append(recv)
        specs.append(pl.BlockSpec((rows, recv.shape[1]), lambda m, core: (m, Z)))
    if wo is not None:
        wo_recv, wo_whole, wo_tile = wo
        args.append(wo_recv)
        specs.append(pl.BlockSpec((wo_recv.shape[0] // steps, hidden), lambda m, core: (m, Z)))
        outs.append(jax.ShapeDtypeStruct(wo_whole.shape, F32))
    if whole is not None:
        alias[len(args)] = 0
        args.append(whole)
        specs.append(ANY)
    if wo is not None:
        alias[len(args)] = 2
        args.append(wo_whole)
        specs.append(ANY)
    return pl.pallas_call(
        functools.partial(wqkv_grad_kernel, places_of, old_places_of, wo_tile),
        grid_spec=pltpu.PrefetchScalarGridSpec(
            num_scalar_prefetch=1,
            grid=(steps,),
            in_specs=specs,
            out_specs=[ANY] * len(outs),
            scratch_shapes=[
                pltpu.VMEM((SLOTS, tokens, rows), BF16),
                pltpu.VMEM((tokens, width), BF16),
                pltpu.VMEM((SLOTS, rows, width), F32),
                dma_sems(SLOTS, SLOTS), dma_sems(PIECES, n_grp), dma_sems(SLOTS, n_grp), dma_sems(SLOTS), dma_sems(n_grp), dma_sems(4),
            ],
        ),
        out_shape=outs,
        input_output_aliases=alias,
        compiler_params=VMEM_BIG,
        cost_estimate=matmul_cost(hidden, tokens, width, 16 * hidden * width),
        name='wqkv_grad',
    )(*args)


def normed_grad_kernel(runs, n_src, places_of, n_paste, final, cols_ref, *rest):
    srcs, (w_ref, init_ref, recv_ref, *rest) = rest[:n_src], rest[n_src:]
    if final:
        x_ref, gain_ref, _, whole_ref, dx_ref, sum_ref, acc, w_buf, g_buf, sems, g_sems, paste_sems, init_sem, sum_acc = rest
    else:
        _, whole_ref, acc, w_buf, g_buf, sems, g_sems, paste_sems = rest
    j, steps = pl.program_id(0), pl.num_programs(0)
    slot = lax.rem(j, SLOTS)
    rows, width = g_buf.shape[1], g_buf.shape[2] // 2
    other, rank = cols_ref[2 * steps], cols_ref[2 * steps + 1]

    def w_loads(step, at):
        for i in range(2):
            col = pl.multiple_of(cols_ref[2 * step + i], HEAD)
            yield pltpu.make_async_copy(w_ref.at[:, pl.ds(col, width)], w_buf.at[at, :, run(i, width)], sems.at[at, i])

    def g_loads(step):
        at = step % 2
        for i, (src, grp) in enumerate(runs[part(step, 2)]):
            ref, dst = srcs[src].at[grp], g_buf.at[at, :, run(i, width)]
            tokens = ref.shape[0]
            pairs = [(ref, dst)] if tokens == rows else [
                (ref.at[pl.ds(pl.multiple_of(h * (tokens // 2) + rank * (rows // 2), BLK), rows // 2)], dst.at[run(h, rows // 2)]) for h in range(2)]
            for pair in pairs:
                yield pltpu.make_async_copy(*pair, g_sems.at[at, i])

    def g_waits(at):
        for i in range(2):
            block = g_buf.at[at, :, run(i, width)]
            yield pltpu.make_async_copy(block, block, g_sems.at[at, i])

    def pastes():
        return column_copies(recv_ref, whole_ref, lambda i: paste_sems.at[i], j * recv_ref.shape[0], places_of(other))

    @pl.when(j == 0)
    def _():
        start_all(w_loads(0, 0))
        start_all(g_loads(0))
        if final:
            init = pltpu.make_async_copy(init_ref, acc, init_sem)
            init.start()
            init.wait()
        else:
            acc[...] = init_ref[...].astype(F32) * ALPHA

    @pl.when(j + 1 < steps)
    def _():
        start_all(w_loads(j + 1, 1 - slot))

    for step in range(1, len(runs) // 2):
        @pl.when(j + 1 == step)
        def _():
            start_all(g_loads(step))

    @pl.when(j < n_paste)
    def _():
        start_all(pastes())

    wait_all(w_loads(j, slot))
    wait_all(g_waits(slot))
    acc[...] += dot_nt(g_buf[slot], w_buf[slot])

    if final:
        @pl.when(j == steps - 1)
        def _():
            sum_acc[...] = jnp.zeros_like(sum_acc)
            gain = gain_ref[...].astype(F32)

            @pl.loop(0, rows // NORM_ROWS)
            def _(i):
                at = run(i, NORM_ROWS)
                d_n = acc[at]
                x, inv = centred(x_ref[at])
                x = x * inv
                d_x = d_n * gain
                mean = jnp.mean(d_x, axis=-1, keepdims=True)
                slope = jnp.mean(d_x * x, axis=-1, keepdims=True)
                dx_ref[at] = (inv * (d_x - mean - x * slope)).astype(BF16)
                for kind, term in enumerate((d_n * x, d_n)):
                    sum_acc[kind] += jnp.sum(term.reshape((2,) + sum_acc.shape[1:]), axis=0)

            sum_ref[...] = jnp.sum(sum_acc[...], axis=1)

    @pl.when(j < n_paste)
    def _():
        wait_all(pastes())


def normed_grad(cols, runs, srcs, w_qkv, init, recv, places_of, n_paste, whole, norm=None):
    rows, hidden = init.shape
    steps, width = len(runs) // 2, 2 * srcs[0].shape[-1]
    flat = pl.BlockSpec((rows, hidden), lambda j, cols: (Z, Z))
    block = pl.BlockSpec((hidden // n_paste, recv.shape[1]), lambda j, cols: (jnp.minimum(j, n_paste - 1), Z))
    args = [cols, *srcs, w_qkv, init, recv]
    specs = [ANY] * (len(srcs) + 1) + [ANY if norm else flat, block]
    outs, out_specs = [jax.ShapeDtypeStruct(whole.shape, F32)], [ANY]
    scratch = [pltpu.VMEM((SLOTS, hidden, width), BF16), pltpu.VMEM((SLOTS, rows, width), BF16), dma_sems(SLOTS, SLOTS), dma_sems(SLOTS, SLOTS), dma_sems(8)]
    if norm:
        args += list(norm)
        specs += [flat, pl.BlockSpec((1, hidden), lambda j, cols: (Z, Z))]
        outs += [jax.ShapeDtypeStruct((rows, hidden), BF16), jax.ShapeDtypeStruct((2, hidden), F32)]
        out_specs += [flat, pl.BlockSpec((2, hidden), lambda j, cols: (Z, Z))]
        scratch = [pltpu.VMEM((rows, hidden), F32)] + scratch + [pltpu.SemaphoreType.DMA, pltpu.VMEM((2, 8, hidden), F32)]
    else:
        outs.append(jax.ShapeDtypeStruct((rows, hidden), F32))
        out_specs.append(flat)
    return pl.pallas_call(
        functools.partial(normed_grad_kernel, runs, len(srcs), places_of, n_paste, norm is not None),
        grid_spec=pltpu.PrefetchScalarGridSpec(
            num_scalar_prefetch=1,
            grid=(steps,),
            in_specs=specs + [ANY],
            out_specs=out_specs,
            scratch_shapes=scratch,
        ),
        out_shape=outs,
        input_output_aliases={len(args): 0},
        compiler_params=VMEM_BIG,
        cost_estimate=matmul_cost(rows, steps * width, hidden, 8 * recv.size),
        name='dn',
    )(*args, whole)


def output_kernel(n_dist, core_ref, ctx_ref, shared_ref, w_ref, w_shared_ref, na_ref, nb_ref, b_ref, out_ref, acc):
    j = pl.program_id(0)

    @pl.when(j == 0)
    def _():
        acc[...] = dot_nn(ctx_ref[0], w_ref[...])

    @pl.when(jnp.logical_and(j > 0, j < n_dist))
    def _():
        acc[...] += dot_nn(ctx_ref[0], w_ref[...])

    @pl.when(j >= n_dist)
    def _():
        acc[...] += dot_nn(shared_ref[0], w_shared_ref[...])

    @pl.when(j == pl.num_programs(0) - 1)
    def _():
        for half, n_ref in enumerate((na_ref, nb_ref)):
            rows = part(half, n_ref.shape[0])
            out_ref[rows] = (ALPHA * n_ref[...].astype(F32) + (acc[rows] + b_ref[...].astype(F32))).astype(BF16)


def project_out(core, ctx_tok, shared_tok, w_o, n_halves, b_o):
    n_dev, rows, cols = ctx_tok.shape
    n_core, _, shared = shared_tok.shape
    hidden = w_o.shape[1]
    base = n_dev * cols // shared

    def dist_index(j, core):
        at = jnp.minimum(j, n_dev - 1)
        return jnp.where(at < n_dev // 2, 2 * at + core[0], 2 * (at - n_dev // 2) + 1 - core[0])

    def shared_index(j, core):
        return jnp.where(j <= n_dev, core[0], 1 - core[0])

    whole, half = [pl.BlockSpec((size, hidden), lambda j, core: (Z, Z)) for size in (rows, rows // 2)]
    return pl.pallas_call(
        functools.partial(output_kernel, n_dev),
        grid_spec=pltpu.PrefetchScalarGridSpec(
            num_scalar_prefetch=1,
            grid=(n_dev + n_core,),
            in_specs=[
                pl.BlockSpec((1, rows, cols), lambda j, core: (jnp.minimum(j, n_dev - 1), Z, Z)),
                pl.BlockSpec((1, rows, shared), lambda j, core: (jnp.maximum(j - n_dev, Z), Z, Z)),
                pl.BlockSpec((cols, hidden), lambda j, core: (dist_index(j, core), Z)),
                pl.BlockSpec((shared, hidden), lambda j, core: (base + shared_index(j, core), Z)),
                half, half,
                pl.BlockSpec((1, hidden), lambda j, core: (Z, Z)),
            ],
            out_specs=whole,
            scratch_shapes=[pltpu.VMEM((rows, hidden), F32)],
        ),
        out_shape=jax.ShapeDtypeStruct((rows, hidden), BF16),
        compiler_params=VMEM_BIG,
        cost_estimate=matmul_cost(rows, hidden, hidden),
        name='out_proj',
    )(core, ctx_tok, shared_tok, w_o, w_o, *n_halves, b_o.reshape(1, -1))


def together(*values):
    return lax.optimization_barrier(values)


def solution(mesh):
    n_dev = mesh.shape['sp']
    tok_spec = P('dp', 'sp', None)
    pos_spec = P('dp', 'sp')
    in_specs = (tok_spec, pos_spec, pos_spec, P('dp'), P(), P(), P(), P(), P(), P(), tok_spec)
    out_specs = (tok_spec, tok_spec, P('dp'), P('dp'), P('dp', None), P('dp'), P('dp', None), P('dp'))
    same_core = [list(range(core, n_dev, 2)) for core in range(2)]
    partners = [(dev, dev ^ 1) for dev in range(n_dev)]
    n_chip = n_dev // 2

    def device_step(hidden_in, pos_ids, block_pos, prefix_len, ln_gamma, ln_beta, w_qkv, b_qkv, w_o, b_o, grad_out):
        batch, local_len, hidden = hidden_in.shape
        per_half = batch // 2
        heads = hidden // HEAD
        n_dist, n_shared = (heads - SHARED) // n_dev, SHARED // 2
        shared_at = n_dev * n_dist
        rows = batch * local_len
        tokens = n_dev * rows
        rank = lax.axis_index('sp')
        parity = lax.rem(rank, SLOTS)
        pair = rank + 1 - 2 * parity
        core = parity.reshape(1).astype(jnp.int32)
        gather = functools.partial(lax.all_gather, axis_name='sp')
        gather_core = functools.partial(lax.all_gather, axis_name='sp', axis_index_groups=same_core)
        to_partner = functools.partial(lax.ppermute, axis_name='sp', perm=partners)

        def token_rows(arr, dev):
            split = arr.reshape(arr.shape[:-2] + (2, n_dev, rows // 2, arr.shape[-1]))
            return lax.dynamic_index_in_dim(split, dev, axis=split.ndim - 3, keepdims=False).reshape(arr.shape[:-2] + (rows, arr.shape[-1]))

        def places(head):
            return lambda par: [((2 * c + par) * n_dist + head) * WIDTH for c in range(n_chip)]

        def shared_places(par):
            return [(shared_at + par * n_shared + i) * WIDTH for i in range(n_shared)]

        def wo_tile(t, par):
            spread = t - n_shared
            return jnp.where(t < n_shared, shared_at + par * n_shared + t, (2 * (spread // n_dist) + par) * n_dist + lax.rem(spread, n_dist))

        halves = range(2)
        x_flat, gain = hidden_in.reshape(rows, hidden), ln_gamma.reshape(1, hidden)
        n_own = [normalize(half, x_flat, gain, ln_beta.reshape(1, hidden)) for half in halves]
        dy_own = [grad_out[part(half, per_half)] for half in halves]
        n_own[1], *dy_own = together(n_own[1], *dy_own)
        n_a, n_b, dy_a, dy_b = [gather(send.reshape(per_half, local_len, hidden)) for send in n_own + dy_own]
        cos, sin = rope_tables(prefix_len, n_dev * local_len)
        prefix = [prefix_len[part(half, per_half)] for half in halves]
        starts = jnp.stack([rank * n_dist, shared_at + parity * n_shared]).astype(jnp.int32)
        bias = jnp.concatenate([
            lax.dynamic_slice_in_dim(b_qkv, starts[0] * WIDTH, n_dist * WIDTH),
            lax.dynamic_slice_in_dim(b_qkv, starts[1] * WIDTH, n_shared * WIDTH)]).astype(F32).reshape(1, -1)
        grad_bo = jnp.sum(grad_out.astype(F32), axis=(0, 1))
        n_a, grad_bo = together(n_a, grad_bo)

        ctx_d = ctx_r = None
        qkv, lses = [], []
        for half in halves:
            if half:
                n_b, ctx_r = together(n_b, ctx_r)
            qd, kd, vd, qr, kr, vr = project_qkv(half, starts, n_dist, n_shared, n_b if half else n_a, w_qkv, bias, cos, sin)
            ctx_d, lse_d = attention_forward(half, prefix[half], qd, kd, vd, n_dev, ctx_d)
            qr, ctx_d = together(qr, ctx_d)
            ctx_r, lse_r = attention_forward(half, prefix[half], qr, kr, vr, n_dev, ctx_r)
            qkv.append((qd, kd, vd, qr, kr, vr))
            lses.append((lse_d, lse_r))
        ctx_par = gather_core(ctx_d.reshape(tokens, n_dist * HEAD))

        dy_a, ctx_r = together(dy_a, ctx_r)
        g_d = g_r = None
        sum_d, sum_r = [], []
        for half in halves:
            if half:
                dy_b, g_r = together(dy_b, g_r)
            qd, kd, vd, qr, kr, vr = qkv[half]
            d_ctx = context_grad(starts, n_dist + n_shared, dy_b if half else dy_a, w_o)
            g_d, sums = attention_backward(half, n_shared, prefix[half], qd, kd, vd, ctx_d, d_ctx, lses[half][0], cos, sin, g_d)
            sum_d.append(sums)
            qr, g_d = together(qr, g_d)
            g_r, sums = attention_backward(half, 0, prefix[half], qr, kr, vr, ctx_r, d_ctx, lses[half][1], cos, sin, g_r, 2)
            sum_r.append(sums)
        g_d = g_d.reshape(n_dist, tokens, WIDTH)
        g_r = g_r.reshape(n_shared, tokens, WIDTH)
        g_par = [gather_core(g_d[head]) for head in range(n_dist)]
        sums = [jnp.sum(jnp.concatenate(part, axis=1), axis=(1, 2)).reshape(-1) for part in (sum_d, sum_r)]

        n_a, n_b, dy_a, dy_b = [part.reshape(tokens // 2, hidden) for part in (n_a, n_b, dy_a, dy_b)]
        ctx_r = ctx_r.reshape(tokens, n_shared * HEAD)
        r_recv, shared_recv = to_partner(token_rows(g_r, pair)), to_partner(token_rows(ctx_r, pair))
        ctx_r, g_r = together(ctx_r, g_r)
        grad_wo, wo_block = weight_grad_o(
            core, ctx_r[None], dy_a, dy_b, lambda c, par: (shared_at + par * n_shared) * HEAD, lambda c: Z, hidden // 2, ())
        r_recv, shared_recv, wo_block, n_a = together(r_recv, shared_recv, wo_block, n_a)
        grad_wqkv, block = weight_grad_qkv(core, shared_places, n_a, n_b, g_r, None)
        ctx_recv = to_partner(token_rows(ctx_par, pair))
        ctx_par, ctx_recv, block = together(ctx_par, ctx_recv, block)
        recv_r = to_partner(block)
        grad_wo, wo_block = weight_grad_o(
            core, ctx_par, dy_a, dy_b, lambda c, par: (2 * c + par) * (n_dist * HEAD), lambda c: (n_shared + c * n_dist) * HEAD,
            hidden // 2, (grad_wo, wo_block))
        ctx_tok = jnp.concatenate([token_rows(ctx_par, rank), ctx_recv])
        ctx_tok, wo_block = together(ctx_tok, wo_block)
        wo_recv = to_partner(wo_block)
        shared_tok = jnp.stack([token_rows(ctx_r, rank), shared_recv])
        hidden_out = project_out(core, ctx_tok, shared_tok, w_o, n_own, b_o)
        n_a, hidden_out, g_par[0] = together(n_a, hidden_out, g_par[0])

        recvs, tok = [recv_r], []
        for head in range(n_dist):
            extra = [dict(recv=recv_r, old_places_of=shared_places), dict(wo=(wo_recv, grad_wo, wo_tile)), dict(recv=recvs[1] if head > 1 else None, old_places_of=places(0))][head]
            res = weight_grad_qkv(core, places(head), n_a, n_b, g_par[head], grad_wqkv, **extra)
            grad_wqkv, block = res[:2]
            if head == 1:
                grad_wo = res[2]
            tok_recv = to_partner(token_rows(g_par[head], pair))
            tok_recv, block = together(tok_recv, block)
            if head + 1 < n_dist:
                g_par[head + 1], block = together(g_par[head + 1], block)
            tok.append(tok_recv)
            recvs.append(to_partner(block))

        def columns(table):
            at = [np.array([h * WIDTH for h in table(par)] + [1 - par, 0], np.int32) for par in range(2)]
            last = np.arange(at[0].size) == at[0].size - 1
            return jnp.asarray(at[0]) + parity.astype(jnp.int32) * jnp.asarray(at[1] - at[0]) + rank.astype(jnp.int32) * jnp.asarray(last.astype(np.int32))

        cols = columns(lambda mine: [shared_at + par * n_shared + i for par in (mine, 1 - mine) for i in range(n_shared)] + [
            (2 * c + par) * n_dist + head for par in (mine, 1 - mine) for c in range(n_chip) for head in (0, 1)])
        srcs = [g_r, r_recv, g_par[0], g_par[1], *tok[:2]]
        runs = [(src, i) for src in (0, 1) for i in range(n_shared)] + [(src, c) for pair in ((2, 3), (4, 5)) for c in range(n_chip) for src in pair]
        grad_wqkv, d_norm = normed_grad(cols, runs, srcs, w_qkv, grad_out.reshape(rows, hidden), recvs[2], places(1), 8, grad_wqkv)
        cols = columns(lambda mine: [(2 * c + par) * n_dist + 2 for c in range(n_chip) for par in (mine, 1 - mine)])
        grad_wqkv, grad_in, norm_sums = normed_grad(
            cols, [(src, c) for c in range(n_chip) for src in range(2)], [g_par[2], tok[2]], w_qkv, d_norm, recvs[3], places(2), 4, grad_wqkv,
            (x_flat, gain))
        small = gather(jnp.concatenate(sums + [norm_sums.reshape(-1), grad_bo]))
        spread, shared = small[:, :n_dist * WIDTH], small[:2, n_dist * WIDTH:(n_dist + n_shared) * WIDTH]
        grad_bqkv = jnp.concatenate([spread.reshape(-1), shared.reshape(-1)])
        grad_gamma, grad_beta, grad_bo = jnp.sum(small[:, (n_dist + n_shared) * WIDTH:], axis=0).reshape(3, hidden)
        shape = (batch, local_len, hidden)
        return (hidden_out.reshape(shape), grad_in.reshape(shape), grad_gamma, grad_beta, grad_wqkv, grad_bqkv, grad_wo, grad_bo)

    return jax.shard_map(device_step, mesh=mesh, in_specs=in_specs, out_specs=out_specs, check_vma=False)
```

```python
import functools
import math
import jax
import jax.numpy as jnp
import numpy as np
from jax import lax
from jax.experimental import pallas as pl
from jax.experimental.pallas import tpu as pltpu
from jax.sharding import PartitionSpec as P

HEAD = 128
QUARTER = 32
ALPHA = math.sqrt(56.0)
LN_EPS = 1e-5
ROT_BASE = 10000.0
SCALE = 1.0 / math.sqrt(HEAD)
LOG2E = math.log2(math.e)
MASK_FILL = -1e30
BLK = 256
VMEM_BIG = pltpu.CompilerParams(vmem_limit_bytes=62 << 20)
SHARED = 8
FWD = ((3, 4), (1, 2))
BWD = (2, 4)
Z = 0
SLOTS = 2
WIDTH = 3 * HEAD
F32 = jnp.float32
BF16 = jnp.bfloat16


def dot(lhs, rhs, lhs_dim, rhs_dim):
    return lax.dot_general(lhs, rhs, (((lhs_dim,), (rhs_dim,)), ((), ())), preferred_element_type=F32)


def dot_nn(lhs, rhs):
    return dot(lhs, rhs, 1, 0)


def dot_nt(lhs, rhs):
    return dot(lhs, rhs, 1, 1)


def dot_tn(lhs, rhs):
    return dot(lhs, rhs, 0, 0)


def matmul_cost(rows, depth, cols, extra=0):
    return pl.CostEstimate(
        flops=2 * rows * depth * cols, bytes_accessed=2 * (rows * depth + depth * cols + rows * cols) + extra, transcendentals=0)


def attention_cost(n_head, batch, seq, products):
    pairs = n_head * batch * seq * seq
    return pl.CostEstimate(flops=2 * products * pairs * HEAD, bytes_accessed=8 * products * n_head * batch * seq * HEAD, transcendentals=pairs)


def run(index, size):
    return pl.ds(pl.multiple_of(index * size, size), size)


def part(index, size):
    return slice(index * size, (index + 1) * size)


def rope_tables(prefix_len, seq):
    tok = jnp.arange(seq, dtype=jnp.int32)[None, :]
    pre = prefix_len[:, None]
    inside = tok < pre
    pos = jnp.where(inside, tok, pre - 1)
    blk = jnp.where(inside, 0, tok - pre + 1)
    inv_freq = ROT_BASE ** (-jnp.arange(QUARTER, dtype=F32) / QUARTER)
    angles = jnp.stack([pos, blk], axis=-1).astype(F32)[..., None] * inv_freq
    cos, sin = jnp.cos(angles), jnp.sin(angles)
    shape = pos.shape + (HEAD,)
    return (jnp.stack([cos, cos], axis=-2).reshape(shape), jnp.stack([-sin, sin], axis=-2).reshape(shape))


def turn(x, cos, sin):
    lane = lax.broadcasted_iota(jnp.int32, x.shape, 1)
    other = jnp.where(lane % (2 * QUARTER) < QUARTER, pltpu.roll(x, HEAD - QUARTER, 1), pltpu.roll(x, QUARTER, 1))
    return x * cos + other * sin


def dma_sems(*shape):
    return pltpu.SemaphoreType.DMA(shape)


def dma_sems(*shape):
    return pltpu.SemaphoreType.DMA(shape)


def start_all(copies):
    for copy in copies:
        copy.start()


def wait_all(copies):
    for copy in copies:
        copy.wait()


ANY = pl.BlockSpec(memory_space=pl.ANY)
PIECES = 4


NORM_ROWS = 16


def centred(x):
    x = x.astype(F32)
    x = x - jnp.mean(x, axis=-1, keepdims=True)
    return x, lax.rsqrt(jnp.mean(x * x, axis=-1, keepdims=True) + LN_EPS)


def norm_kernel(x_ref, gain_ref, shift_ref, out_ref):
    gain, shift = gain_ref[...].astype(F32), shift_ref[...].astype(F32)

    @pl.loop(0, x_ref.shape[0] // NORM_ROWS)
    def _(i):
        rows = run(i, NORM_ROWS)
        x, inv = centred(x_ref[rows])
        out_ref[rows] = (x * inv * gain + shift).astype(BF16)


def normalize(half, x, gain, shift):
    rows, hidden = x.shape
    block = rows // 4
    vec = pl.BlockSpec((1, hidden), lambda i: (Z, Z))
    return pl.pallas_call(
        norm_kernel,
        grid=(2,),
        in_specs=[pl.BlockSpec((block, hidden), lambda i: (2 * half + i, Z)), vec, vec],
        out_specs=pl.BlockSpec((block, hidden), lambda i: (i, Z)),
        out_shape=jax.ShapeDtypeStruct((2 * block, hidden), BF16),
        compiler_params=VMEM_BIG,
        name='norm',
    )(x, gain, shift)


def qkv_kernel(n_dist, start_ref, n_ref, w_ref, b_ref, cos_ref, sin_ref, qd_ref, kd_ref, vd_ref, qr_ref, kr_ref, vr_ref, w_buf, acc, sems):
    rows = cos_ref.shape[1]
    hidden = n_ref.shape[-1]
    dist = n_dist * WIDTH
    shared = w_buf.shape[1] - dist
    step, last = pl.program_id(0), pl.num_programs(0) - 1
    slot = lax.rem(step, SLOTS)
    piece = hidden // PIECES

    def loads(i):
        span = run(i, piece)
        for kind, (at, width) in enumerate(((0, dist), (dist, shared))):
            col = pl.multiple_of(start_ref[kind] * WIDTH, HEAD)
            yield pltpu.make_async_copy(w_ref.at[span, pl.ds(col, width)], w_buf.at[span, pl.ds(at, width)], sems.at[i, kind])

    def finish():
        cos, sin = cos_ref[0], sin_ref[0]
        n_shared = qr_ref.shape[0]
        for h in range(n_dist + n_shared):
            q_ref, k_ref, v_ref, at = (qd_ref, kd_ref, vd_ref, h) if h < n_dist else (qr_ref, kr_ref, vr_ref, h - n_dist)
            pre_q, pre_k, pre_v = [acc[1 - slot, :, part(3 * h + i, HEAD)] + b_ref[:, part(3 * h + i, HEAD)] for i in range(3)]
            q_ref[at, 0] = turn(pre_q, cos, sin).astype(BF16)
            k_ref[at, 0] = turn(pre_k, cos, sin).astype(BF16)
            v_ref[at, 0] = pre_v.astype(BF16)

    @pl.when(step == 0)
    def _():
        for i in range(PIECES):
            start_all(loads(i))
        acc[slot] = jnp.zeros((rows, dist + shared), F32)

        @pl.loop(0, PIECES)
        def _(i):
            wait_all(loads(i))
            span = run(i, piece)
            acc[slot] += dot_nn(n_ref[:, :, :, span].reshape(rows, piece), w_buf[span])

    @pl.when(jnp.logical_and(step > 0, step < last))
    def _():
        finish()
        acc[slot] = dot_nn(n_ref[...].reshape(rows, hidden), w_buf[...])

    pl.when(step == last)(finish)


def project_qkv(half, starts, n_dist, n_shared, n_half, w_qkv, bias, cos, sin):
    n_dev, batch, local_len, hidden = n_half.shape
    seq = n_dev * local_len
    cols = (n_dist + n_shared) * WIDTH
    per = 4
    rows = per * local_len
    outs, out_specs = [], []
    for n_head in (n_dist, n_shared):
        outs += [jax.ShapeDtypeStruct((n_head, batch, seq, HEAD), BF16)] * 3
        out_specs += [pl.BlockSpec((n_head, 1, rows, HEAD), lambda step, at: (Z, *behind(step), Z))] * 3
    steps = n_dev // per

    def behind(step):
        at = jnp.maximum(step - 1, 0)
        return at // steps, lax.rem(at, steps)

    def ahead(step):
        at = jnp.minimum(step, batch * steps - 1)
        return lax.rem(at, steps), at // steps

    def tab_index(step, at):
        b, j = behind(step)
        return half * batch + b, j, Z

    tab_spec = pl.BlockSpec((1, rows, HEAD), tab_index)
    return pl.pallas_call(
        functools.partial(qkv_kernel, n_dist),
        grid_spec=pltpu.PrefetchScalarGridSpec(
            num_scalar_prefetch=1,
            grid=(batch * steps + 1,),
            in_specs=[
                pl.BlockSpec((per, 1, local_len, hidden), lambda step, at: (*ahead(step), Z, Z)),
                ANY,
                pl.BlockSpec((1, cols), lambda step, at: (Z, Z)),
                tab_spec, tab_spec,
            ],
            out_specs=out_specs,
            scratch_shapes=[
                pltpu.VMEM((hidden, cols), BF16), pltpu.VMEM((SLOTS, rows, cols), F32), dma_sems(PIECES, SLOTS)],
        ),
        out_shape=outs,
        compiler_params=VMEM_BIG,
        cost_estimate=matmul_cost(batch * seq, hidden, cols),
        name='qkv',
    )(starts, n_half, w_qkv, bias, cos, sin)


def forward_kernel(pre_ref, q_ref, k_ref, v_ref, *rest):
    ctx_ref, lse_ref = rest[-2:]
    n_head, _, seq, _ = q_ref.shape
    local_len = ctx_ref.shape[3]
    per = BLK // local_len
    prefix = pre_ref[pl.program_id(1)]

    def block(r, n_key):
        query = lax.broadcasted_iota(jnp.int32, (1, BLK), 1) + r * BLK
        last = jnp.maximum(query, prefix - 1) - (n_key - 1) * BLK
        scores = []
        for h in range(n_head):
            q_blk = q_ref[h, 0, part(r, BLK)]
            parts = [dot_nt(k_ref[h, 0, part(c, BLK)], q_blk) * (SCALE * LOG2E) for c in range(n_key)]
            key = lax.broadcasted_iota(jnp.int32, (BLK, BLK), 0)
            parts[-1] = jnp.where(key <= last, parts[-1], MASK_FILL)
            scores.append(parts)
        for h, parts in enumerate(scores):
            top = functools.reduce(jnp.maximum, [jnp.max(p, axis=0, keepdims=True) for p in parts])
            parts = [jnp.exp2(p - top) for p in parts]
            total = functools.reduce(jnp.add, [jnp.sum(p, axis=0, keepdims=True) for p in parts])
            inv = 1.0 / total
            probs = jnp.concatenate([(p * inv).astype(BF16) for p in parts], axis=0)
            ctx_t = dot_tn(v_ref[h, 0, :n_key * BLK], probs)
            ctx = ctx_t.T.astype(BF16).reshape(per, local_len, HEAD)
            ctx_ref[0, part(r, per), 0, :, part(h, HEAD)] = ctx
            lse_ref[h, 0, :, part(r, BLK)] = top + jnp.log2(total)

    n_blk = seq // BLK
    for r in range(n_blk):
        for n_key in range(r + 1, n_blk + 1):
            low = (n_key - 1) * BLK
            cond = prefix <= n_key * BLK if n_key == r + 1 else prefix > low
            if n_key < n_blk and n_key > r + 1:
                cond = jnp.logical_and(cond, prefix <= n_key * BLK)
            if n_key == n_blk and n_key == r + 1:
                block(r, n_key)
            else:
                pl.when(cond)(functools.partial(block, r, n_key))


def attention_forward(half, prefix_half, q, k, v, n_dev, ctx, group):
    own, batch, seq, _ = q.shape
    local_len = seq // n_dev
    qkv_spec = pl.BlockSpec((group, 1, seq, HEAD), lambda h, b, pre: (h, b, Z, Z))
    earlier = [] if ctx is None else [ctx]
    return pl.pallas_call(
        forward_kernel,
        grid_spec=pltpu.PrefetchScalarGridSpec(
            num_scalar_prefetch=1,
            grid=(own // group, batch),
            in_specs=[qkv_spec] * 3 + [ANY] * len(earlier),
            out_specs=[
                pl.BlockSpec((1, n_dev, 1, local_len, group * HEAD), lambda h, b, pre: (half, Z, b, Z, h)),
                pl.BlockSpec((group, 1, 1, seq), lambda h, b, pre: (h, b, Z, Z)),
            ],
        ),
        out_shape=[
            jax.ShapeDtypeStruct((2, n_dev, batch, local_len, own * HEAD), BF16),
            jax.ShapeDtypeStruct((own, batch, 1, seq), F32),
        ],
        input_output_aliases={4: 0} if earlier else {},
        compiler_params=VMEM_BIG,
        cost_estimate=attention_cost(own, batch, seq, 2),
        name='attn_fwd',
    )(prefix_half, q, k, v, *earlier)


def d_ctx_kernel(start_ref, dy_ref, w_ref, out_ref, w_buf, sems):
    per, _, local_len, hidden = dy_ref.shape
    first = jnp.logical_and(pl.program_id(0) == 0, pl.program_id(1) == 0)
    shared = SHARED // 2 * HEAD
    widths = (shared, out_ref.shape[-1] - shared)

    def loads():
        at = 0
        for kind, width in enumerate(widths):
            row = pl.multiple_of(start_ref[1 - kind] * HEAD, HEAD)
            yield pltpu.make_async_copy(w_ref.at[pl.ds(row, width)], w_buf.at[pl.ds(at, width)], sems.at[kind])
            at += width

    @pl.when(first)
    def _():
        start_all(loads())
        wait_all(loads())

    res = dot_nt(dy_ref[...].reshape(per * local_len, hidden), w_buf[...])
    out_ref[...] = res.astype(BF16).reshape(per, 1, local_len, w_buf.shape[0])


def context_grad(starts, n_own, dy_half, w_o):
    n_dev, batch, local_len, hidden = dy_half.shape
    cols = n_own * HEAD
    per = 4
    return pl.pallas_call(
        d_ctx_kernel,
        grid_spec=pltpu.PrefetchScalarGridSpec(
            num_scalar_prefetch=1,
            grid=(batch, n_dev // per),
            in_specs=[pl.BlockSpec((per, 1, local_len, hidden), lambda b, j, at: (j, b, Z, Z)), ANY],
            out_specs=pl.BlockSpec((per, 1, local_len, cols), lambda b, j, at: (j, b, Z, Z)),
            scratch_shapes=[pltpu.VMEM((cols, hidden), BF16), dma_sems(2)],
        ),
        out_shape=jax.ShapeDtypeStruct((n_dev, batch, local_len, cols), BF16),
        compiler_params=VMEM_BIG,
        cost_estimate=matmul_cost(n_dev * batch * local_len, hidden, cols),
        name='dctx',
    )(starts, dy_half, w_o)


def backward_kernel(pre_ref, q_ref, k_ref, v_ref, ctx_ref, dctx_ref, lse_ref, cos_ref, sin_ref, *rest):
    g_ref, sum_ref, dq_acc, dk_acc, dv_acc = rest[-5:]
    n_head, _, seq, _ = q_ref.shape
    n_dev, local_len = g_ref.shape[2], g_ref.shape[4]
    n_blk = seq // BLK
    prefix = pre_ref[pl.program_id(1)]
    d_ctx, delta = [], []
    for h in range(n_head):
        lanes = part(h, HEAD)
        grad = dctx_ref[:, :, :, lanes].reshape(seq, HEAD)
        prod = grad.astype(F32) * ctx_ref[0, :, :, :, lanes].reshape(seq, HEAD).astype(F32)
        d_ctx.append(grad)
        delta.append(jnp.sum(prod.T, axis=0, keepdims=True))

    def block(c, first):
        span = part(c, BLK)
        start = first * BLK
        products = []
        for h in range(n_head):
            s_t = dot_nt(k_ref[h, 0, span], q_ref[h, 0, start:])
            dp_t = dot_nt(v_ref[h, 0, span], d_ctx[h][start:])
            products.append((s_t, dp_t))
        for h, (s_t, dp_t) in enumerate(products):
            probs, d_scores = [], []
            for r in range(first, n_blk):
                cols, here = part(r, BLK), part(r - first, BLK)
                piece = s_t[:, here] * (SCALE * LOG2E)
                if r <= c:
                    key = lax.broadcasted_iota(jnp.int32, (BLK, BLK), 0)
                    query = lax.broadcasted_iota(jnp.int32, (1, BLK), 1) + r * BLK
                    piece = jnp.where(key <= jnp.maximum(query, prefix - 1) - c * BLK, piece, MASK_FILL)
                p = jnp.exp2(piece - lse_ref[h, 0, :, cols])
                probs.append(p.astype(BF16))
                d_scores.append((p * (dp_t[:, here] - delta[h][:, cols]) * SCALE).astype(BF16))
            probs = jnp.concatenate(probs, axis=1)
            d_scores = jnp.concatenate(d_scores, axis=1)
            dv_acc[h, span] = dot_nn(probs, d_ctx[h][start:])
            dk_acc[h, span] = dot_nn(d_scores, q_ref[h, 0, start:])
            dq_part = dot_tn(k_ref[h, 0, span], d_scores)
            if c:
                dq_acc[h, :, start:] += dq_part
            else:
                dq_acc[h] = dq_part

    block(0, 0)
    for c in range(1, n_blk):
        pl.when(prefix > c * BLK)(functools.partial(block, c, 0))
        pl.when(prefix <= c * BLK)(functools.partial(block, c, c))

    cos, sin = cos_ref[0], sin_ref[0]
    for h in range(n_head):
        g_q = turn(dq_acc[h].T.astype(BF16).astype(F32), cos, -sin)
        g_k = turn(dk_acc[h].astype(BF16).astype(F32), cos, -sin)
        g_v = dv_acc[h].astype(BF16).astype(F32)
        for i, g in enumerate((g_q, g_k, g_v)):
            lanes = part(i, HEAD)
            g_ref[h, 0, :, 0, :, lanes] = g.astype(BF16).reshape(n_dev, local_len, HEAD)
            sum_ref[h, 0, :, lanes] = jnp.sum(g, axis=0, keepdims=True)


def attention_backward(half, d_col, prefix_half, q, k, v, ctx, d_ctx, lse, cos, sin, g_all, group=1):
    n_head, batch, seq, _ = q.shape
    _, n_dev, _, local_len, _ = ctx.shape
    qkv_spec = pl.BlockSpec((group, 1, seq, HEAD), lambda h, b, pre: (h, b, Z, Z))
    tab_spec = pl.BlockSpec((1, seq, HEAD), lambda h, b, pre: (half * batch + b, Z, Z))
    earlier = [] if g_all is None else [g_all]
    stat = functools.partial(pltpu.VMEM, dtype=F32)
    return pl.pallas_call(
        backward_kernel,
        grid_spec=pltpu.PrefetchScalarGridSpec(
            num_scalar_prefetch=1,
            grid=(n_head // group, batch),
            in_specs=[qkv_spec] * 3 + [
                pl.BlockSpec((1, n_dev, 1, local_len, group * HEAD), lambda h, b, pre: (half, Z, b, Z, h)),
                pl.BlockSpec((n_dev, 1, local_len, group * HEAD), lambda h, b, pre: (Z, b, Z, d_col // group + h)),
                pl.BlockSpec((group, 1, 1, seq), lambda h, b, pre: (h, b, Z, Z)), tab_spec, tab_spec] + [ANY] * len(earlier),
            out_specs=[
                pl.BlockSpec((group, 1, n_dev, 1, local_len, WIDTH), lambda h, b, pre: (h, half, Z, b, Z, Z)),
                pl.BlockSpec((group, 1, 1, WIDTH), lambda h, b, pre: (h, b, Z, Z)),
            ],
            scratch_shapes=[stat((group, HEAD, seq)), stat((group, seq, HEAD)), stat((group, seq, HEAD))],
        ),
        out_shape=[
            jax.ShapeDtypeStruct((n_head, 2, n_dev, batch, local_len, WIDTH), BF16),
            jax.ShapeDtypeStruct((n_head, batch, 1, WIDTH), F32),
        ],
        input_output_aliases={9: 0} if earlier else {},
        compiler_params=VMEM_BIG,
        cost_estimate=attention_cost(n_head, batch, seq, 5),
        name='attn_bwd',
    )(prefix_half, q, k, v, ctx, d_ctx, lse, cos, sin, *earlier)


def wo_grad_kernel(row_of, block_row_of, core_ref, ctx_ref, dya_ref, dyb_ref, *rest):
    out_ref, copy_ref, rhs, buf, rhs_sems, sems = rest[-6:]
    n, c = pl.program_id(0), pl.program_id(1)
    n_col, n_grp = pl.num_programs(0), pl.num_programs(1)
    step = n * n_grp + c
    slot, n_slot = lax.rem(step, SLOTS), lax.rem(n, SLOTS)
    _, rows, wide = buf.shape
    half = dya_ref.shape[0]
    core = core_ref[0]

    def loads(n_at, at):
        for i, ref in enumerate((dya_ref, dyb_ref)):
            yield pltpu.make_async_copy(ref.at[:, run(n_at, wide)], rhs.at[at, run(i, half)], rhs_sems.at[at, i])

    def stores(at_step, at):
        n_at, c_at = at_step // n_grp, lax.rem(at_step, n_grp)
        for i, (ref, row) in enumerate(((out_ref, row_of(c_at, core)), (copy_ref, block_row_of(c_at)))):
            yield pltpu.make_async_copy(buf.at[at], ref.at[pl.ds(pl.multiple_of(row, HEAD), rows), run(n_at, wide)], sems.at[at, i])

    @pl.when(step == 0)
    def _():
        start_all(loads(0, 0))

    @pl.when(c == 0)
    def _():
        @pl.when(n + 1 < n_col)
        def _():
            start_all(loads(n + 1, 1 - n_slot))

        wait_all(loads(n, n_slot))

    @pl.when(step >= 2)
    def _():
        wait_all(stores(step - 2, slot))

    buf[slot] = dot_tn(ctx_ref[0], rhs[n_slot])
    start_all(stores(step, slot))

    @pl.when(step == n_col * n_grp - 1)
    def _():
        wait_all(stores(step - 1, 1 - slot))
        wait_all(stores(step, slot))


def weight_grad_o(core, ctx_par, dy_a, dy_b, row_of, block_row_of, block_rows, earlier):
    n_grp, tokens, cols = ctx_par.shape
    hidden = dy_a.shape[1]
    wide = hidden // 4
    return pl.pallas_call(
        functools.partial(wo_grad_kernel, row_of, block_row_of),
        grid_spec=pltpu.PrefetchScalarGridSpec(
            num_scalar_prefetch=1,
            grid=(hidden // wide, n_grp),
            in_specs=[pl.BlockSpec((1, tokens, cols), lambda n, c, core: (c, Z, Z)), ANY, ANY] + [ANY] * len(earlier),
            out_specs=[ANY, ANY],
            scratch_shapes=[pltpu.VMEM((SLOTS, tokens, wide), BF16), pltpu.VMEM((SLOTS, cols, wide), F32), dma_sems(SLOTS, SLOTS), dma_sems(SLOTS, SLOTS)],
        ),
        out_shape=[jax.ShapeDtypeStruct((hidden, hidden), F32), jax.ShapeDtypeStruct((block_rows, hidden), F32)],
        input_output_aliases={4: 0, 5: 1} if earlier else {},
        compiler_params=VMEM_BIG,
        cost_estimate=matmul_cost(n_grp * cols, tokens, hidden, 8 * hidden * n_grp * cols),
        name='wo_grad',
    )(core, ctx_par, dy_a, dy_b, *earlier)


def column_copies(src, out_ref, sem_of, row, places):
    rows, width = src.shape[0], src.shape[1] // len(places)
    for i, col in enumerate(places):
        yield pltpu.make_async_copy(
            src.at[:, run(i, width)],
            out_ref.at[pl.ds(pl.multiple_of(row, BLK), rows), pl.ds(pl.multiple_of(col, HEAD), width)],
            sem_of(i))


def wqkv_grad_kernel(places_of, old_places_of, wo_tile, core_ref, na_ref, nb_ref, g_ref, *rest):
    rest = list(rest)
    recv_ref = rest.pop(0) if old_places_of else None
    wo_recv_ref = rest.pop(0) if wo_tile else None
    n_buf, rhs, buf, n_sems, g_sems, out_sems, copy_sems, paste_sems, wo_sems = rest[-9:]
    outs = rest[:-9][-3 if wo_tile else -2:]
    out_ref, copy_ref = outs[:2]
    m = pl.program_id(0)
    n_m = pl.num_programs(0)
    core = core_ref[0]
    n_grp, tokens, cols = g_ref.shape
    half, rows = tokens // 2, n_buf.shape[2]
    piece = tokens // PIECES
    slot = lax.rem(m, SLOTS)

    def n_loads(step, at):
        for i, ref in enumerate((na_ref, nb_ref)):
            yield pltpu.make_async_copy(ref.at[:, run(step, rows)], n_buf.at[at, run(i, half)], n_sems.at[at, i])

    def g_loads(i):
        for c in range(n_grp):
            yield pltpu.make_async_copy(g_ref.at[c, run(i, piece)], rhs.at[run(i, piece), run(c, cols)], g_sems.at[i, c])

    def stores(step, at):
        yield from column_copies(buf.at[at], out_ref, lambda i: out_sems.at[at, i], step * rows, places_of(core))
        yield pltpu.make_async_copy(buf.at[at], copy_ref.at[run(step, rows)], copy_sems.at[at])

    def pastes():
        if old_places_of:
            yield from column_copies(recv_ref, out_ref, lambda i: paste_sems.at[i], m * rows, old_places_of(1 - core))
        if wo_tile:
            tiles = wo_recv_ref.shape[0] // HEAD
            for t in range(tiles):
                tile = wo_tile(m * tiles + t, 1 - core)
                yield pltpu.make_async_copy(wo_recv_ref.at[run(t, HEAD)], outs[2].at[run(tile, HEAD)], wo_sems.at[t])

    @pl.when(m == 0)
    def _():
        start_all(n_loads(0, 0))
        for i in range(PIECES):
            start_all(g_loads(i))

    @pl.when(m + 1 < n_m)
    def _():
        start_all(n_loads(m + 1, 1 - slot))

    start_all(pastes())

    @pl.when(m >= 2)
    def _():
        wait_all(stores(m - 2, slot))

    wait_all(n_loads(m, slot))

    @pl.when(m == 0)
    def _():
        buf[slot] = jnp.zeros((rows, n_grp * cols), F32)

        @pl.loop(0, PIECES)
        def _(i):
            wait_all(g_loads(i))
            buf[slot] += dot_tn(n_buf[slot, run(i, piece)], rhs[run(i, piece)])

    @pl.when(m > 0)
    def _():
        buf[slot] = dot_tn(n_buf[slot], rhs[...])

    start_all(stores(m, slot))
    wait_all(pastes())

    @pl.when(m == n_m - 1)
    def _():
        wait_all(stores(m - 1, 1 - slot))
        wait_all(stores(m, slot))


def weight_grad_qkv(core, places_of, n_a, n_b, g_par, whole, recv=None, old_places_of=None, wo=None):
    hidden = n_a.shape[1]
    n_grp, tokens, cols = g_par.shape
    width = n_grp * cols
    rows = 2 * BLK
    steps = hidden // rows
    args, specs, alias = [core, n_a, n_b, g_par], [ANY, ANY, ANY], {}
    outs = [jax.ShapeDtypeStruct((hidden, 3 * hidden), F32), jax.ShapeDtypeStruct((hidden, width), F32)]
    wo_tile = None
    if recv is not None:
        args.append(recv)
        specs.append(pl.BlockSpec((rows, recv.shape[1]), lambda m, core: (m, Z)))
    if wo is not None:
        wo_recv, wo_whole, wo_tile = wo
        args.append(wo_recv)
        specs.append(pl.BlockSpec((wo_recv.shape[0] // steps, hidden), lambda m, core: (m, Z)))
        outs.append(jax.ShapeDtypeStruct(wo_whole.shape, F32))
    if whole is not None:
        alias[len(args)] = 0
        args.append(whole)
        specs.append(ANY)
    if wo is not None:
        alias[len(args)] = 2
        args.append(wo_whole)
        specs.append(ANY)
    return pl.pallas_call(
        functools.partial(wqkv_grad_kernel, places_of, old_places_of, wo_tile),
        grid_spec=pltpu.PrefetchScalarGridSpec(
            num_scalar_prefetch=1,
            grid=(steps,),
            in_specs=specs,
            out_specs=[ANY] * len(outs),
            scratch_shapes=[
                pltpu.VMEM((SLOTS, tokens, rows), BF16),
                pltpu.VMEM((tokens, width), BF16),
                pltpu.VMEM((SLOTS, rows, width), F32),
                dma_sems(SLOTS, SLOTS), dma_sems(PIECES, n_grp), dma_sems(SLOTS, n_grp), dma_sems(SLOTS), dma_sems(n_grp), dma_sems(4),
            ],
        ),
        out_shape=outs,
        input_output_aliases=alias,
        compiler_params=VMEM_BIG,
        cost_estimate=matmul_cost(hidden, tokens, width, 16 * hidden * width),
        name='wqkv_grad',
    )(*args)


def normed_grad_kernel(runs, n_src, final, places_of, cols_ref, *rest):
    srcs, (w_ref, init_ref, *rest) = rest[:n_src], rest[n_src:]
    if final:
        x_ref, gain_ref, dx_ref, sum_ref, acc, w_buf, g_buf, sems, g_sems, init_sem, sum_acc = rest
    else:
        recv_ref, _, acc, whole_ref, w_buf, g_buf, sems, g_sems, paste_sems = rest
    j, steps = pl.program_id(0), pl.num_programs(0)
    slot = lax.rem(j, SLOTS)
    rows, width = g_buf.shape[1], g_buf.shape[2] // 2
    other, rank = cols_ref[2 * steps], cols_ref[2 * steps + 1]
    n_paste = 0 if final else w_ref.shape[0] // recv_ref.shape[0]

    def w_loads(step, at):
        for i in range(2):
            col = pl.multiple_of(cols_ref[2 * step + i], HEAD)
            yield pltpu.make_async_copy(w_ref.at[:, pl.ds(col, width)], w_buf.at[at, :, run(i, width)], sems.at[at, i])

    def g_loads(step):
        at = step % 2
        for i, (src, grp) in enumerate(runs[part(step, 2)]):
            ref, dst = srcs[src].at[grp], g_buf.at[at, :, run(i, width)]
            tokens = ref.shape[0]
            pairs = [(ref, dst)] if tokens == rows else [
                (ref.at[pl.ds(pl.multiple_of(h * (tokens // 2) + rank * (rows // 2), BLK), rows // 2)], dst.at[run(h, rows // 2)]) for h in range(2)]
            for pair in pairs:
                yield pltpu.make_async_copy(*pair, g_sems.at[at, i])

    def g_waits(at):
        for i in range(2):
            block = g_buf.at[at, :, run(i, width)]
            yield pltpu.make_async_copy(block, block, g_sems.at[at, i])

    def pastes():
        return column_copies(recv_ref, whole_ref, lambda i: paste_sems.at[i], j * recv_ref.shape[0], places_of(other))

    @pl.when(j == 0)
    def _():
        start_all(w_loads(0, 0))
        start_all(g_loads(0))
        if final:
            init = pltpu.make_async_copy(init_ref, acc, init_sem)
            init.start()
            init.wait()
        else:
            acc[...] = init_ref[...].astype(F32) * ALPHA

    @pl.when(j + 1 < steps)
    def _():
        start_all(w_loads(j + 1, 1 - slot))

    for step in range(1, len(runs) // 2):
        @pl.when(j + 1 == step)
        def _():
            start_all(g_loads(step))

    @pl.when(j < n_paste)
    def _():
        start_all([] if final else pastes())

    wait_all(w_loads(j, slot))
    wait_all(g_waits(slot))
    acc[...] += dot_nt(g_buf[slot], w_buf[slot])

    if final:
        @pl.when(j == steps - 1)
        def _():
            sum_acc[...] = jnp.zeros_like(sum_acc)
            gain = gain_ref[...].astype(F32)

            @pl.loop(0, rows // NORM_ROWS)
            def _(i):
                at = run(i, NORM_ROWS)
                d_n = acc[at]
                x, inv = centred(x_ref[at])
                x = x * inv
                d_x = d_n * gain
                mean = jnp.mean(d_x, axis=-1, keepdims=True)
                slope = jnp.mean(d_x * x, axis=-1, keepdims=True)
                dx_ref[at] = (inv * (d_x - mean - x * slope)).astype(BF16)
                for kind, term in enumerate((d_n * x, d_n)):
                    sum_acc[kind] += jnp.sum(term.reshape((2,) + sum_acc.shape[1:]), axis=0)

            sum_ref[...] = jnp.sum(sum_acc[...], axis=1)

    @pl.when(j < n_paste)
    def _():
        wait_all([] if final else pastes())


def normed_grad(cols, runs, srcs, w_qkv, init, paste=None, norm=None):
    rows, hidden = init.shape
    steps, width = len(runs) // 2, 2 * srcs[0].shape[-1]
    flat = pl.BlockSpec((rows, hidden), lambda j, cols: (Z, Z))
    args = [cols, *srcs, w_qkv, init]
    specs = [ANY] * (len(srcs) + 1) + [ANY if norm else flat]
    scratch = [pltpu.VMEM((SLOTS, hidden, width), BF16), pltpu.VMEM((SLOTS, rows, width), BF16), dma_sems(SLOTS, SLOTS), dma_sems(SLOTS, SLOTS)]
    alias, places_of = {}, None
    if norm:
        args += list(norm)
        specs += [flat, pl.BlockSpec((1, hidden), lambda j, cols: (Z, Z))]
        outs = [jax.ShapeDtypeStruct((rows, hidden), BF16), jax.ShapeDtypeStruct((2, hidden), F32)]
        out_specs = [flat, pl.BlockSpec((2, hidden), lambda j, cols: (Z, Z))]
        scratch = [pltpu.VMEM((rows, hidden), F32)] + scratch + [pltpu.SemaphoreType.DMA, pltpu.VMEM((2, 8, hidden), F32)]
    else:
        recv, places_of, whole = paste
        n_paste = 8
        alias = {len(args) + 1: 1}
        args += [recv, whole]
        specs += [pl.BlockSpec((hidden // n_paste, recv.shape[1]), lambda j, cols: (jnp.minimum(j, n_paste - 1), Z)), ANY]
        outs = [jax.ShapeDtypeStruct((rows, hidden), F32), jax.ShapeDtypeStruct(whole.shape, F32)]
        out_specs = [flat, ANY]
        scratch.append(dma_sems(8))
    return pl.pallas_call(
        functools.partial(normed_grad_kernel, runs, len(srcs), norm is not None, places_of),
        grid_spec=pltpu.PrefetchScalarGridSpec(
            num_scalar_prefetch=1,
            grid=(steps,),
            in_specs=specs,
            out_specs=out_specs,
            scratch_shapes=scratch,
        ),
        out_shape=outs,
        input_output_aliases=alias,
        compiler_params=VMEM_BIG,
        cost_estimate=matmul_cost(rows, steps * width, hidden),
        name='dn',
    )(*args)


def paste_kernel(places_of, core_ref, recv_ref, _, out_ref, sems):
    row = pl.program_id(0) * recv_ref.shape[0]
    copies = list(column_copies(recv_ref, out_ref, lambda i: sems.at[i], row, places_of(1 - core_ref[0])))
    start_all(copies)
    wait_all(copies)


def paste_columns(core, places_of, recv, whole):
    hidden, block = recv.shape
    rows = 2 * BLK
    return pl.pallas_call(
        functools.partial(paste_kernel, places_of),
        grid_spec=pltpu.PrefetchScalarGridSpec(
            num_scalar_prefetch=1,
            grid=(hidden // rows,),
            in_specs=[pl.BlockSpec((rows, block), lambda m, core: (m, Z)), ANY],
            out_specs=ANY,
            scratch_shapes=[dma_sems(8)],
        ),
        out_shape=jax.ShapeDtypeStruct(whole.shape, F32),
        input_output_aliases={2: 0},
        compiler_params=VMEM_BIG,
        name='paste',
    )(core, recv, whole)


def output_kernel(n_dist, core_ref, ctx_ref, shared_ref, w_ref, w_shared_ref, na_ref, nb_ref, b_ref, out_ref, acc):
    j = pl.program_id(0)

    @pl.when(j == 0)
    def _():
        acc[...] = dot_nn(ctx_ref[0], w_ref[...])

    @pl.when(jnp.logical_and(j > 0, j < n_dist))
    def _():
        acc[...] += dot_nn(ctx_ref[0], w_ref[...])

    @pl.when(j >= n_dist)
    def _():
        acc[...] += dot_nn(shared_ref[0], w_shared_ref[...])

    @pl.when(j == pl.num_programs(0) - 1)
    def _():
        for half, n_ref in enumerate((na_ref, nb_ref)):
            rows = part(half, n_ref.shape[0])
            out_ref[rows] = (ALPHA * n_ref[...].astype(F32) + (acc[rows] + b_ref[...].astype(F32))).astype(BF16)


def project_out(core, ctx_tok, shared_tok, w_o, n_halves, b_o):
    n_dev, rows, cols = ctx_tok.shape
    n_core, _, shared = shared_tok.shape
    hidden = w_o.shape[1]
    base = n_dev * cols // shared

    def dist_index(j, core):
        at = jnp.minimum(j, n_dev - 1)
        return jnp.where(at < n_dev // 2, 2 * at + core[0], 2 * (at - n_dev // 2) + 1 - core[0])

    def shared_index(j, core):
        return jnp.where(j <= n_dev, core[0], 1 - core[0])

    whole, half = [pl.BlockSpec((size, hidden), lambda j, core: (Z, Z)) for size in (rows, rows // 2)]
    return pl.pallas_call(
        functools.partial(output_kernel, n_dev),
        grid_spec=pltpu.PrefetchScalarGridSpec(
            num_scalar_prefetch=1,
            grid=(n_dev + n_core,),
            in_specs=[
                pl.BlockSpec((1, rows, cols), lambda j, core: (jnp.minimum(j, n_dev - 1), Z, Z)),
                pl.BlockSpec((1, rows, shared), lambda j, core: (jnp.maximum(j - n_dev, Z), Z, Z)),
                pl.BlockSpec((cols, hidden), lambda j, core: (dist_index(j, core), Z)),
                pl.BlockSpec((shared, hidden), lambda j, core: (base + shared_index(j, core), Z)),
                half, half,
                pl.BlockSpec((1, hidden), lambda j, core: (Z, Z)),
            ],
            out_specs=whole,
            scratch_shapes=[pltpu.VMEM((rows, hidden), F32)],
        ),
        out_shape=jax.ShapeDtypeStruct((rows, hidden), BF16),
        compiler_params=VMEM_BIG,
        cost_estimate=matmul_cost(rows, hidden, hidden),
        name='out_proj',
    )(core, ctx_tok, shared_tok, w_o, w_o, *n_halves, b_o.reshape(1, -1))


def together(*values):
    return lax.optimization_barrier(values)


def solution(mesh):
    n_dev = mesh.shape['sp']
    tok_spec = P('dp', 'sp', None)
    pos_spec = P('dp', 'sp')
    in_specs = (tok_spec, pos_spec, pos_spec, P('dp'), P(), P(), P(), P(), P(), P(), tok_spec)
    out_specs = (tok_spec, tok_spec, P('dp'), P('dp'), P('dp', None), P('dp'), P('dp', None), P('dp'))
    same_core = [list(range(core, n_dev, 2)) for core in range(2)]
    partners = [(dev, dev ^ 1) for dev in range(n_dev)]
    n_chip = n_dev // 2

    def device_step(hidden_in, pos_ids, block_pos, prefix_len, ln_gamma, ln_beta, w_qkv, b_qkv, w_o, b_o, grad_out):
        batch, local_len, hidden = hidden_in.shape
        per_half = batch // 2
        heads = hidden // HEAD
        n_dist, n_shared = (heads - SHARED) // n_dev, SHARED // 2
        shared_at = n_dev * n_dist
        rows = batch * local_len
        tokens = n_dev * rows
        rank = lax.axis_index('sp')
        parity = lax.rem(rank, SLOTS)
        pair = rank + 1 - 2 * parity
        core = parity.reshape(1).astype(jnp.int32)
        gather = functools.partial(lax.all_gather, axis_name='sp')
        gather_core = functools.partial(lax.all_gather, axis_name='sp', axis_index_groups=same_core)
        to_partner = functools.partial(lax.ppermute, axis_name='sp', perm=partners)

        def token_rows(arr, dev):
            split = arr.reshape(arr.shape[:-2] + (2, n_dev, rows // 2, arr.shape[-1]))
            return lax.dynamic_index_in_dim(split, dev, axis=split.ndim - 3, keepdims=False).reshape(arr.shape[:-2] + (rows, arr.shape[-1]))

        def places(head):
            return lambda par: [((2 * c + par) * n_dist + head) * WIDTH for c in range(n_chip)]

        def shared_places(par):
            return [(shared_at + par * n_shared + i) * WIDTH for i in range(n_shared)]

        def wo_tile(t, par):
            spread = t - n_shared
            return jnp.where(t < n_shared, shared_at + par * n_shared + t, (2 * (spread // n_dist) + par) * n_dist + lax.rem(spread, n_dist))

        halves = range(2)
        x_flat, gain = hidden_in.reshape(rows, hidden), ln_gamma.reshape(1, hidden)
        n_own = [normalize(half, x_flat, gain, ln_beta.reshape(1, hidden)) for half in halves]
        dy_own = [grad_out[part(half, per_half)] for half in halves]
        n_own[1], *dy_own = together(n_own[1], *dy_own)
        n_a, n_b, dy_a, dy_b = [gather(send.reshape(per_half, local_len, hidden)) for send in n_own + dy_own]
        cos, sin = rope_tables(prefix_len, n_dev * local_len)
        prefix = [prefix_len[part(half, per_half)] for half in halves]
        starts = jnp.stack([rank * n_dist, shared_at + parity * n_shared]).astype(jnp.int32)
        bias = jnp.concatenate([
            lax.dynamic_slice_in_dim(b_qkv, starts[0] * WIDTH, n_dist * WIDTH),
            lax.dynamic_slice_in_dim(b_qkv, starts[1] * WIDTH, n_shared * WIDTH)]).astype(F32).reshape(1, -1)
        grad_bo = jnp.sum(grad_out.astype(F32), axis=(0, 1))
        n_a, grad_bo = together(n_a, grad_bo)

        ctx_d = ctx_r = None
        qkv, lses = [], []
        for half in halves:
            if half:
                n_b, ctx_r = together(n_b, ctx_r)
            qd, kd, vd, qr, kr, vr = project_qkv(half, starts, n_dist, n_shared, n_b if half else n_a, w_qkv, bias, cos, sin)
            ctx_d, lse_d = attention_forward(half, prefix[half], qd, kd, vd, n_dev, ctx_d, FWD[half][0])
            qr, ctx_d = together(qr, ctx_d)
            ctx_r, lse_r = attention_forward(half, prefix[half], qr, kr, vr, n_dev, ctx_r, FWD[half][1])
            qkv.append((qd, kd, vd, qr, kr, vr))
            lses.append((lse_d, lse_r))
        ctx_par = gather_core(ctx_d.reshape(tokens, n_dist * HEAD))

        dy_a, ctx_r = together(dy_a, ctx_r)
        g_d = g_r = None
        sum_d, sum_r = [], []
        for half in halves:
            if half:
                dy_b, g_r = together(dy_b, g_r)
            qd, kd, vd, qr, kr, vr = qkv[half]
            d_ctx = context_grad(starts, n_dist + n_shared, dy_b if half else dy_a, w_o)
            g_d, sums = attention_backward(half, n_shared, prefix[half], qd, kd, vd, ctx_d, d_ctx, lses[half][0], cos, sin, g_d)
            sum_d.append(sums)
            qr, g_d = together(qr, g_d)
            g_r, sums = attention_backward(half, 0, prefix[half], qr, kr, vr, ctx_r, d_ctx, lses[half][1], cos, sin, g_r, BWD[half])
            sum_r.append(sums)
        g_d = g_d.reshape(n_dist, tokens, WIDTH)
        g_r = g_r.reshape(n_shared, tokens, WIDTH)
        g_par = [gather_core(g_d[head]) for head in range(n_dist)]
        sums = [jnp.sum(jnp.concatenate(part, axis=1), axis=(1, 2)).reshape(-1) for part in (sum_d, sum_r)]

        n_a, n_b, dy_a, dy_b = [part.reshape(tokens // 2, hidden) for part in (n_a, n_b, dy_a, dy_b)]
        ctx_r = ctx_r.reshape(tokens, n_shared * HEAD)
        r_recv, shared_recv = to_partner(token_rows(g_r, pair)), to_partner(token_rows(ctx_r, pair))
        ctx_r, g_r = together(ctx_r, g_r)
        grad_wo, wo_block = weight_grad_o(
            core, ctx_r[None], dy_a, dy_b, lambda c, par: (shared_at + par * n_shared) * HEAD, lambda c: Z, hidden // 2, ())
        r_recv, shared_recv, wo_block, n_a = together(r_recv, shared_recv, wo_block, n_a)
        grad_wqkv, block = weight_grad_qkv(core, shared_places, n_a, n_b, g_r, None)
        ctx_recv = to_partner(token_rows(ctx_par, pair))
        ctx_par, ctx_recv, block = together(ctx_par, ctx_recv, block)
        recv_r = to_partner(block)
        grad_wo, wo_block = weight_grad_o(
            core, ctx_par, dy_a, dy_b, lambda c, par: (2 * c + par) * (n_dist * HEAD), lambda c: (n_shared + c * n_dist) * HEAD,
            hidden // 2, (grad_wo, wo_block))
        ctx_tok = jnp.concatenate([token_rows(ctx_par, rank), ctx_recv])
        ctx_tok, wo_block, recv_r = together(ctx_tok, wo_block, recv_r)
        wo_recv = to_partner(wo_block)
        shared_tok = jnp.stack([token_rows(ctx_r, rank), shared_recv])
        hidden_out = project_out(core, ctx_tok, shared_tok, w_o, n_own, b_o)
        n_a, hidden_out, g_par[0] = together(n_a, hidden_out, g_par[0])

        def columns(table):
            at = [np.array([h * WIDTH for h in table(par)] + [1 - par, 0], np.int32) for par in range(2)]
            last = (np.arange(at[0].size) == at[0].size - 1).astype(np.int32)
            return jnp.asarray(at[0]) + parity.astype(jnp.int32) * jnp.asarray(at[1] - at[0]) + rank.astype(jnp.int32) * jnp.asarray(last)

        def spread_grad(head, whole, **extra):
            whole, block, *rest = weight_grad_qkv(core, places(head), n_a, n_b, g_par[head], whole, **extra)
            tok = to_partner(token_rows(g_par[head], pair))
            tok, block = together(tok, block)
            return whole, tok, to_partner(block), rest

        grad_wqkv, tok_0, recv_0, _ = spread_grad(0, grad_wqkv, recv=recv_r, old_places_of=shared_places)
        g_par[1], grad_wqkv = together(g_par[1], grad_wqkv)
        grad_wqkv, tok_1, recv_1, (grad_wo,) = spread_grad(1, grad_wqkv, wo=(wo_recv, grad_wo, wo_tile))
        cols = columns(lambda mine: [shared_at + par * n_shared + i for par in (mine, 1 - mine) for i in range(n_shared)] + [
            (2 * c + par) * n_dist + head for par in (mine, 1 - mine) for c in range(n_chip) for head in (0, 1)])
        runs = [(src, i) for src in (0, 1) for i in range(n_shared)] + [(src, c) for pair in ((2, 3), (4, 5)) for c in range(n_chip) for src in pair]
        d_norm, grad_wqkv = normed_grad(
            cols, runs, [g_r, r_recv, g_par[0], g_par[1], tok_0, tok_1], w_qkv, grad_out.reshape(rows, hidden), (recv_0, places(0), grad_wqkv))
        n_a, d_norm, g_par[2] = together(n_a, d_norm, g_par[2])
        grad_wqkv, tok_2, recv_2, _ = spread_grad(2, grad_wqkv, recv=recv_1, old_places_of=places(1))
        cols = columns(lambda mine: [(2 * c + par) * n_dist + 2 for c in range(n_chip) for par in (mine, 1 - mine)])
        grad_in, norm_sums = normed_grad(
            cols, [(src, c) for c in range(n_chip) for src in range(2)], [g_par[2], tok_2], w_qkv, d_norm, norm=(x_flat, gain))
        small = gather(jnp.concatenate(sums + [norm_sums.reshape(-1), grad_bo]))
        recv_2, small = together(recv_2, small)
        grad_wqkv = paste_columns(core, places(2), recv_2, grad_wqkv)
        spread, shared = small[:, :n_dist * WIDTH], small[:2, n_dist * WIDTH:(n_dist + n_shared) * WIDTH]
        grad_bqkv = jnp.concatenate([spread.reshape(-1), shared.reshape(-1)])
        grad_gamma, grad_beta, grad_bo = jnp.sum(small[:, (n_dist + n_shared) * WIDTH:], axis=0).reshape(3, hidden)
        shape = (batch, local_len, hidden)
        return (hidden_out.reshape(shape), grad_in.reshape(shape), grad_gamma, grad_beta, grad_wqkv, grad_bqkv, grad_wo, grad_bo)

    return jax.shard_map(device_step, mesh=mesh, in_specs=in_specs, out_specs=out_specs, check_vma=False)
```

```python
import functools
import math
import jax
import jax.numpy as jnp
import numpy as np
from jax import lax
from jax.experimental import pallas as pl
from jax.experimental.pallas import tpu as pltpu
from jax.sharding import PartitionSpec as P

HEAD = 128
QUARTER = 32
ALPHA = math.sqrt(56.0)
LN_EPS = 1e-5
ROT_BASE = 10000.0
SCALE = 1.0 / math.sqrt(HEAD)
LOG2E = math.log2(math.e)
MASK_FILL = -1e30
BLK = 256
VMEM_BIG = pltpu.CompilerParams(vmem_limit_bytes=62 << 20)
SHARED = 8
Z = 0
SLOTS = CORES = 2
WIDTH = 3 * HEAD
F32 = jnp.float32
BF16 = jnp.bfloat16


def dot(lhs, rhs, lhs_dim, rhs_dim):
    return lax.dot_general(lhs, rhs, (((lhs_dim,), (rhs_dim,)), ((), ())), preferred_element_type=F32)


def dot_nn(lhs, rhs):
    return dot(lhs, rhs, 1, 0)


def dot_nt(lhs, rhs):
    return dot(lhs, rhs, 1, 1)


def dot_tn(lhs, rhs):
    return dot(lhs, rhs, 0, 0)


def matmul_cost(rows, depth, cols, extra=0):
    return pl.CostEstimate(
        flops=2 * rows * depth * cols, bytes_accessed=2 * (rows * depth + depth * cols + rows * cols) + extra, transcendentals=0)


def attention_cost(n_head, batch, seq, products):
    pairs = n_head * batch * seq * seq
    return pl.CostEstimate(flops=2 * products * pairs * HEAD, bytes_accessed=8 * products * n_head * batch * seq * HEAD, transcendentals=pairs)


def run(index, size):
    return pl.ds(pl.multiple_of(index * size, size), size)


def part(index, size):
    return slice(index * size, (index + 1) * size)


def rope_tables(prefix_len, seq):
    tok = jnp.arange(seq, dtype=jnp.int32)[None, :]
    pre = prefix_len[:, None]
    inside = tok < pre
    pos = jnp.where(inside, tok, pre - 1)
    blk = jnp.where(inside, 0, tok - pre + 1)
    inv_freq = ROT_BASE ** (-jnp.arange(QUARTER, dtype=F32) / QUARTER)
    angles = jnp.stack([pos, blk], axis=-1).astype(F32)[..., None] * inv_freq
    cos, sin = jnp.cos(angles), jnp.sin(angles)
    shape = pos.shape + (HEAD,)
    return (jnp.stack([cos, cos], axis=-2).reshape(shape), jnp.stack([-sin, sin], axis=-2).reshape(shape))


def turn(x, cos, sin):
    lane = lax.broadcasted_iota(jnp.int32, x.shape, 1)
    other = jnp.where(lane % (2 * QUARTER) < QUARTER, pltpu.roll(x, HEAD - QUARTER, 1), pltpu.roll(x, QUARTER, 1))
    return x * cos + other * sin


def dma_sems(*shape):
    return pltpu.SemaphoreType.DMA(shape)


def dma_sems(*shape):
    return pltpu.SemaphoreType.DMA(shape)


def start_all(copies):
    for copy in copies:
        copy.start()


def wait_all(copies):
    for copy in copies:
        copy.wait()


ANY = pl.BlockSpec(memory_space=pl.ANY)
PIECES = 4
QKV_IN = 6


NORM_ROWS = 16


def centred(x):
    x = x.astype(F32)
    x = x - jnp.mean(x, axis=-1, keepdims=True)
    return x, lax.rsqrt(jnp.mean(x * x, axis=-1, keepdims=True) + LN_EPS)


def norm_kernel(x_ref, gain_ref, shift_ref, out_ref):
    gain, shift = gain_ref[...].astype(F32), shift_ref[...].astype(F32)

    @pl.loop(0, x_ref.shape[0] // NORM_ROWS)
    def _(i):
        rows = run(i, NORM_ROWS)
        x, inv = centred(x_ref[rows])
        out_ref[rows] = (x * inv * gain + shift).astype(BF16)


def normalize(half, x, gain, shift):
    rows, hidden = x.shape
    block = rows // 4
    vec = pl.BlockSpec((1, hidden), lambda i: (Z, Z))
    return pl.pallas_call(
        norm_kernel,
        grid=(2,),
        in_specs=[pl.BlockSpec((block, hidden), lambda i: (2 * half + i, Z)), vec, vec],
        out_specs=pl.BlockSpec((block, hidden), lambda i: (i, Z)),
        out_shape=jax.ShapeDtypeStruct((2 * block, hidden), BF16),
        compiler_params=VMEM_BIG,
        name='norm',
    )(x, gain, shift)


def qkv_kernel(n_dist, n_tile, start_ref, n_ref, w_ref, b_ref, cos_ref, sin_ref, *rest):
    outs, (w_buf, acc, sems) = rest[:-3], rest[-3:]
    _, rows, cols = acc.shape
    hidden = n_ref.shape[-1]
    dist = n_dist * WIDTH
    step, last = pl.program_id(0), pl.num_programs(0) - 1
    slot = lax.rem(step, SLOTS)
    piece = hidden // PIECES
    tile = n_ref.shape[-2]

    def loads(i):
        span = run(i, piece)
        for kind, (at, width) in enumerate(((0, dist), (dist, cols - dist))):
            col = pl.multiple_of(start_ref[kind] * WIDTH, HEAD)
            yield pltpu.make_async_copy(w_ref.at[span, pl.ds(col, width)], w_buf.at[span, pl.ds(at, width)], sems.at[i, kind])

    def finish():
        for i in range(rows // tile):
            group, batch, at, table = n_tile(i)
            cos, sin = cos_ref[table, part(at, tile)], sin_ref[table, part(at, tile)]
            for h in range(cols // WIDTH):
                kind, head = (0, h) if h < n_dist else (1, h - n_dist)
                refs = outs[part(CORES * group + kind, 3)]
                pre = [acc[1 - slot, part(i, tile), part(3 * h + j, HEAD)] + b_ref[:, part(3 * h + j, HEAD)] for j in range(3)]
                for ref, val in zip(refs, (turn(pre[0], cos, sin), turn(pre[1], cos, sin), pre[2])):
                    ref[head, batch, part(at, tile)] = val.astype(BF16)

    @pl.when(step == 0)
    def _():
        for i in range(PIECES):
            start_all(loads(i))
        acc[slot] = jnp.zeros((rows, cols), F32)

        @pl.loop(0, PIECES)
        def _(i):
            wait_all(loads(i))
            span = run(i, piece)
            acc[slot] += dot_nn(n_ref[:, :, :, span].reshape(rows, piece), w_buf[span])

    @pl.when(jnp.logical_and(step > 0, step < last))
    def _():
        finish()
        acc[slot] = dot_nn(n_ref[...].reshape(rows, hidden), w_buf[...])

    pl.when(step == last)(finish)


def project_qkv(starts, n_dist, n_shared, n_rows, w_qkv, bias, cos, sin, half=None, earlier=None):
    _, batch, local_len, hidden = n_rows.shape
    _, seq, _ = cos.shape
    cols = (n_dist + n_shared) * WIDTH
    own = earlier is None
    per_half = batch // CORES if own else batch
    steps = CORES if own else seq // local_len // CORES - 1
    n_chip = seq // local_len // CORES
    width = local_len if own else CORES * local_len

    def place(step, at):
        return at[CORES + step] if own else lax.rem(at[CORES] // CORES + 1 + step, n_chip)

    def ahead(step, at):
        step = jnp.minimum(step, steps - 1)
        return step if own else place(step, at)

    def behind(step, at):
        return place(jnp.maximum(step - 1, 0), at)

    shapes = [jax.ShapeDtypeStruct((n_head, per_half, seq, HEAD), BF16) for n_head in (n_dist, n_shared) for _ in range(3)]
    shapes = shapes * CORES if own else shapes
    tab_spec = pl.BlockSpec((batch, width, HEAD), lambda step, at: (Z if own else half, behind(step, at), Z))
    arrays = [] if own else list(earlier)

    def own_tile(i):
        return i // per_half, i % per_half, 0, i

    def other_tile(i):
        return 0, i % per_half, i // per_half, i % per_half

    return pl.pallas_call(
        functools.partial(without, len(arrays), functools.partial(qkv_kernel, n_dist, own_tile if own else other_tile)),
        grid_spec=pltpu.PrefetchScalarGridSpec(
            num_scalar_prefetch=1,
            grid=(steps + 1,),
            in_specs=[
                pl.BlockSpec((1 if own else CORES, batch, local_len, hidden), lambda step, at: (ahead(step, at), Z, Z, Z)),
                ANY,
                pl.BlockSpec((1, cols), lambda step, at: (Z, Z)),
                tab_spec, tab_spec,
            ] + [ANY] * len(arrays),
            out_specs=[pl.BlockSpec(shape.shape[:CORES] + (width, HEAD), lambda step, at: (Z, Z, behind(step, at), Z)) for shape in shapes],
            scratch_shapes=[
                pltpu.VMEM((hidden, cols), BF16), pltpu.VMEM((SLOTS, CORES * CORES * local_len, cols), F32), dma_sems(PIECES, SLOTS)],
        ),
        out_shape=shapes,
        input_output_aliases={QKV_IN + i: i for i in range(len(arrays))},
        compiler_params=VMEM_BIG,
        cost_estimate=matmul_cost(steps * CORES * batch * local_len, hidden, cols),
        name='qkv',
    )(starts, n_rows, w_qkv, bias, cos, sin, *arrays)


def without(count, kernel, *refs):
    kernel(*refs[:QKV_IN], *refs[QKV_IN + count:])


def forward_kernel(pre_ref, q_ref, k_ref, v_ref, *rest):
    ctx_ref, lse_ref = rest[-2:]
    n_head, _, seq, _ = q_ref.shape
    local_len = ctx_ref.shape[3]
    per = BLK // local_len
    prefix = pre_ref[pl.program_id(1)]

    def block(r, n_key):
        query = lax.broadcasted_iota(jnp.int32, (1, BLK), 1) + r * BLK
        last = jnp.maximum(query, prefix - 1) - (n_key - 1) * BLK
        scores = []
        for h in range(n_head):
            q_blk = q_ref[h, 0, part(r, BLK)]
            parts = [dot_nt(k_ref[h, 0, part(c, BLK)], q_blk) * (SCALE * LOG2E) for c in range(n_key)]
            key = lax.broadcasted_iota(jnp.int32, (BLK, BLK), 0)
            parts[-1] = jnp.where(key <= last, parts[-1], MASK_FILL)
            scores.append(parts)
        for h, parts in enumerate(scores):
            top = functools.reduce(jnp.maximum, [jnp.max(p, axis=0, keepdims=True) for p in parts])
            parts = [jnp.exp2(p - top) for p in parts]
            total = functools.reduce(jnp.add, [jnp.sum(p, axis=0, keepdims=True) for p in parts])
            inv = 1.0 / total
            probs = jnp.concatenate([(p * inv).astype(BF16) for p in parts], axis=0)
            ctx_t = dot_tn(v_ref[h, 0, :n_key * BLK], probs)
            ctx = ctx_t.T.astype(BF16).reshape(per, local_len, HEAD)
            ctx_ref[0, part(r, per), 0, :, part(h, HEAD)] = ctx
            lse_ref[h, 0, :, part(r, BLK)] = top + jnp.log2(total)

    n_blk = seq // BLK
    for r in range(n_blk):
        for n_key in range(r + 1, n_blk + 1):
            low = (n_key - 1) * BLK
            cond = prefix <= n_key * BLK if n_key == r + 1 else prefix > low
            if n_key < n_blk and n_key > r + 1:
                cond = jnp.logical_and(cond, prefix <= n_key * BLK)
            if n_key == n_blk and n_key == r + 1:
                block(r, n_key)
            else:
                pl.when(cond)(functools.partial(block, r, n_key))


def attention_forward(half, prefix_half, q, k, v, n_dev, ctx):
    own, batch, seq, _ = q.shape
    local_len = seq // n_dev
    group = own
    qkv_spec = pl.BlockSpec((group, 1, seq, HEAD), lambda h, b, pre: (h, b, Z, Z))
    earlier = [] if ctx is None else [ctx]
    return pl.pallas_call(
        forward_kernel,
        grid_spec=pltpu.PrefetchScalarGridSpec(
            num_scalar_prefetch=1,
            grid=(own // group, batch),
            in_specs=[qkv_spec] * 3 + [ANY] * len(earlier),
            out_specs=[
                pl.BlockSpec((1, n_dev, 1, local_len, group * HEAD), lambda h, b, pre: (half, Z, b, Z, h)),
                pl.BlockSpec((group, 1, 1, seq), lambda h, b, pre: (h, b, Z, Z)),
            ],
        ),
        out_shape=[
            jax.ShapeDtypeStruct((2, n_dev, batch, local_len, own * HEAD), BF16),
            jax.ShapeDtypeStruct((own, batch, 1, seq), F32),
        ],
        input_output_aliases={4: 0} if earlier else {},
        compiler_params=VMEM_BIG,
        cost_estimate=attention_cost(own, batch, seq, 2),
        name='attn_fwd',
    )(prefix_half, q, k, v, *earlier)


def d_ctx_kernel(start_ref, dy_ref, w_ref, *rest):
    outs, (w_buf, sems) = rest[:-2], rest[-2:]
    hidden = dy_ref.shape[-1]
    shared = SHARED // 2 * HEAD

    def loads():
        for kind, (at, width) in enumerate(((shared, w_buf.shape[0] - shared), (0, shared))):
            row = pl.multiple_of(start_ref[kind] * HEAD, HEAD)
            yield pltpu.make_async_copy(w_ref.at[pl.ds(row, width)], w_buf.at[pl.ds(at, width)], sems.at[kind])

    @pl.when(pl.program_id(0) == 0)
    def _():
        start_all(loads())
        wait_all(loads())

    res = dot_nt(dy_ref[...].reshape(-1, hidden), w_buf[...]).astype(BF16)
    rows = res.shape[0] // len(outs)
    for i, out_ref in enumerate(outs):
        out_ref[...] = res[part(i, rows)].reshape(out_ref.shape)


def context_grad(starts, n_own, dy_rows, w_o, n_dev, earlier=None):
    _, batch, local_len, hidden = dy_rows.shape
    cols = n_own * HEAD
    own = earlier is None
    n_chip = n_dev // CORES
    per_half, devs = (batch // CORES, 1) if own else (batch, CORES)

    def place(step, at):
        return at[CORES + step] if own else lax.rem(at[CORES] // CORES + 1 + step, n_chip)

    def block(step, at):
        return (place(step, at), Z, Z, Z)

    arrays = [] if own else [earlier]
    return pl.pallas_call(
        d_ctx_kernel if own else (lambda start, dy, w, _, *rest: d_ctx_kernel(start, dy, w, *rest)),
        grid_spec=pltpu.PrefetchScalarGridSpec(
            num_scalar_prefetch=1,
            grid=(CORES if own else n_chip - 1,),
            in_specs=[pl.BlockSpec((devs, batch, local_len, hidden), (lambda step, at: (step, Z, Z, Z)) if own else block), ANY] + [ANY] * len(arrays),
            out_specs=[pl.BlockSpec((devs, per_half, local_len, cols), block)] * (CORES if own else 1),
            scratch_shapes=[pltpu.VMEM((cols, hidden), BF16), dma_sems(CORES)],
        ),
        out_shape=[jax.ShapeDtypeStruct((n_dev, per_half, local_len, cols), BF16)] * (CORES if own else 1),
        input_output_aliases={} if own else {3: 0},
        compiler_params=VMEM_BIG,
        cost_estimate=matmul_cost(n_dev * batch * local_len, hidden, cols),
        name='dctx',
    )(starts, dy_rows, w_o, *arrays)


def backward_kernel(pre_ref, q_ref, k_ref, v_ref, ctx_ref, dctx_ref, lse_ref, cos_ref, sin_ref, *rest):
    g_ref, sum_ref, dq_acc, dk_acc, dv_acc = rest[-5:]
    n_head, _, seq, _ = q_ref.shape
    n_dev, local_len = g_ref.shape[2], g_ref.shape[4]
    n_blk = seq // BLK
    prefix = pre_ref[pl.program_id(1)]
    d_ctx, delta = [], []
    for h in range(n_head):
        lanes = part(h, HEAD)
        grad = dctx_ref[:, :, :, lanes].reshape(seq, HEAD)
        prod = grad.astype(F32) * ctx_ref[0, :, :, :, lanes].reshape(seq, HEAD).astype(F32)
        d_ctx.append(grad)
        delta.append(jnp.sum(prod.T, axis=0, keepdims=True))

    def block(c, first):
        span = part(c, BLK)
        start = first * BLK
        products = []
        for h in range(n_head):
            s_t = dot_nt(k_ref[h, 0, span], q_ref[h, 0, start:])
            dp_t = dot_nt(v_ref[h, 0, span], d_ctx[h][start:])
            products.append((s_t, dp_t))
        for h, (s_t, dp_t) in enumerate(products):
            probs, d_scores = [], []
            for r in range(first, n_blk):
                cols, here = part(r, BLK), part(r - first, BLK)
                piece = s_t[:, here] * (SCALE * LOG2E)
                if r <= c:
                    key = lax.broadcasted_iota(jnp.int32, (BLK, BLK), 0)
                    query = lax.broadcasted_iota(jnp.int32, (1, BLK), 1) + r * BLK
                    piece = jnp.where(key <= jnp.maximum(query, prefix - 1) - c * BLK, piece, MASK_FILL)
                p = jnp.exp2(piece - lse_ref[h, 0, :, cols])
                probs.append(p.astype(BF16))
                d_scores.append((p * (dp_t[:, here] - delta[h][:, cols]) * SCALE).astype(BF16))
            probs = jnp.concatenate(probs, axis=1)
            d_scores = jnp.concatenate(d_scores, axis=1)
            dv_acc[h, span] = dot_nn(probs, d_ctx[h][start:])
            dk_acc[h, span] = dot_nn(d_scores, q_ref[h, 0, start:])
            dq_part = dot_tn(k_ref[h, 0, span], d_scores)
            if c:
                dq_acc[h, :, start:] += dq_part
            else:
                dq_acc[h] = dq_part

    block(0, 0)
    for c in range(1, n_blk):
        pl.when(prefix > c * BLK)(functools.partial(block, c, 0))
        pl.when(prefix <= c * BLK)(functools.partial(block, c, c))

    cos, sin = cos_ref[0], sin_ref[0]
    for h in range(n_head):
        g_q = turn(dq_acc[h].T.astype(BF16).astype(F32), cos, -sin)
        g_k = turn(dk_acc[h].astype(BF16).astype(F32), cos, -sin)
        g_v = dv_acc[h].astype(BF16).astype(F32)
        for i, g in enumerate((g_q, g_k, g_v)):
            lanes = part(i, HEAD)
            g_ref[h, 0, :, 0, :, lanes] = g.astype(BF16).reshape(n_dev, local_len, HEAD)
            sum_ref[h, 0, :, lanes] = jnp.sum(g, axis=0, keepdims=True)


def attention_backward(half, d_col, prefix_half, q, k, v, ctx, d_ctx, lse, cos, sin, g_all, group=1):
    n_head, batch, seq, _ = q.shape
    _, n_dev, _, local_len, _ = ctx.shape
    qkv_spec = pl.BlockSpec((group, 1, seq, HEAD), lambda h, b, pre: (h, b, Z, Z))
    tab_spec = pl.BlockSpec((1, seq, HEAD), lambda h, b, pre: (half * batch + b, Z, Z))
    earlier = [] if g_all is None else [g_all]
    stat = functools.partial(pltpu.VMEM, dtype=F32)
    return pl.pallas_call(
        backward_kernel,
        grid_spec=pltpu.PrefetchScalarGridSpec(
            num_scalar_prefetch=1,
            grid=(n_head // group, batch),
            in_specs=[qkv_spec] * 3 + [
                pl.BlockSpec((1, n_dev, 1, local_len, group * HEAD), lambda h, b, pre: (half, Z, b, Z, h)),
                pl.BlockSpec((n_dev, 1, local_len, group * HEAD), lambda h, b, pre: (Z, b, Z, d_col // group + h)),
                pl.BlockSpec((group, 1, 1, seq), lambda h, b, pre: (h, b, Z, Z)), tab_spec, tab_spec] + [ANY] * len(earlier),
            out_specs=[
                pl.BlockSpec((group, 1, n_dev, 1, local_len, WIDTH), lambda h, b, pre: (h, half, Z, b, Z, Z)),
                pl.BlockSpec((group, 1, 1, WIDTH), lambda h, b, pre: (h, b, Z, Z)),
            ],
            scratch_shapes=[stat((group, HEAD, seq)), stat((group, seq, HEAD)), stat((group, seq, HEAD))],
        ),
        out_shape=[
            jax.ShapeDtypeStruct((n_head, 2, n_dev, batch, local_len, WIDTH), BF16),
            jax.ShapeDtypeStruct((n_head, batch, 1, WIDTH), F32),
        ],
        input_output_aliases={9: 0} if earlier else {},
        compiler_params=VMEM_BIG,
        cost_estimate=attention_cost(n_head, batch, seq, 5),
        name='attn_bwd',
    )(prefix_half, q, k, v, ctx, d_ctx, lse, cos, sin, *earlier)


def wo_grad_kernel(row_of, block_row_of, core_ref, ctx_ref, dya_ref, dyb_ref, *rest):
    out_ref, copy_ref, rhs, buf, rhs_sems, sems = rest[-6:]
    n, c = pl.program_id(0), pl.program_id(1)
    n_col, n_grp = pl.num_programs(0), pl.num_programs(1)
    step = n * n_grp + c
    slot, n_slot = lax.rem(step, SLOTS), lax.rem(n, SLOTS)
    _, rows, wide = buf.shape
    half = dya_ref.shape[0]
    core = core_ref[0]

    def loads(n_at, at):
        for i, ref in enumerate((dya_ref, dyb_ref)):
            yield pltpu.make_async_copy(ref.at[:, run(n_at, wide)], rhs.at[at, run(i, half)], rhs_sems.at[at, i])

    def stores(at_step, at):
        n_at, c_at = at_step // n_grp, lax.rem(at_step, n_grp)
        for i, (ref, row) in enumerate(((out_ref, row_of(c_at, core)), (copy_ref, block_row_of(c_at)))):
            yield pltpu.make_async_copy(buf.at[at], ref.at[pl.ds(pl.multiple_of(row, HEAD), rows), run(n_at, wide)], sems.at[at, i])

    @pl.when(step == 0)
    def _():
        start_all(loads(0, 0))

    @pl.when(c == 0)
    def _():
        @pl.when(n + 1 < n_col)
        def _():
            start_all(loads(n + 1, 1 - n_slot))

        wait_all(loads(n, n_slot))

    @pl.when(step >= 2)
    def _():
        wait_all(stores(step - 2, slot))

    buf[slot] = dot_tn(ctx_ref[0], rhs[n_slot])
    start_all(stores(step, slot))

    @pl.when(step == n_col * n_grp - 1)
    def _():
        wait_all(stores(step - 1, 1 - slot))
        wait_all(stores(step, slot))


def weight_grad_o(core, ctx_par, dy_a, dy_b, row_of, block_row_of, block_rows, earlier):
    n_grp, tokens, cols = ctx_par.shape
    hidden = dy_a.shape[1]
    wide = hidden // 4
    return pl.pallas_call(
        functools.partial(wo_grad_kernel, row_of, block_row_of),
        grid_spec=pltpu.PrefetchScalarGridSpec(
            num_scalar_prefetch=1,
            grid=(hidden // wide, n_grp),
            in_specs=[pl.BlockSpec((1, tokens, cols), lambda n, c, core: (c, Z, Z)), ANY, ANY] + [ANY] * len(earlier),
            out_specs=[ANY, ANY],
            scratch_shapes=[pltpu.VMEM((SLOTS, tokens, wide), BF16), pltpu.VMEM((SLOTS, cols, wide), F32), dma_sems(SLOTS, SLOTS), dma_sems(SLOTS, SLOTS)],
        ),
        out_shape=[jax.ShapeDtypeStruct((hidden, hidden), F32), jax.ShapeDtypeStruct((block_rows, hidden), F32)],
        input_output_aliases={4: 0, 5: 1} if earlier else {},
        compiler_params=VMEM_BIG,
        cost_estimate=matmul_cost(n_grp * cols, tokens, hidden, 8 * hidden * n_grp * cols),
        name='wo_grad',
    )(core, ctx_par, dy_a, dy_b, *earlier)


def column_copies(src, out_ref, sem_of, row, places):
    rows, width = src.shape[0], src.shape[1] // len(places)
    for i, col in enumerate(places):
        yield pltpu.make_async_copy(
            src.at[:, run(i, width)],
            out_ref.at[pl.ds(pl.multiple_of(row, BLK), rows), pl.ds(pl.multiple_of(col, HEAD), width)],
            sem_of(i))


def wqkv_grad_kernel(places_of, old_places_of, wo_tile, core_ref, na_ref, nb_ref, g_ref, *rest):
    rest = list(rest)
    recv_ref = rest.pop(0) if old_places_of else None
    wo_recv_ref = rest.pop(0) if wo_tile else None
    n_buf, rhs, buf, n_sems, g_sems, out_sems, copy_sems, paste_sems, wo_sems = rest[-9:]
    outs = rest[:-9][-3 if wo_tile else -2:]
    out_ref, copy_ref = outs[:2]
    m = pl.program_id(0)
    n_m = pl.num_programs(0)
    core = core_ref[0]
    n_grp, tokens, cols = g_ref.shape
    half, rows = tokens // 2, n_buf.shape[2]
    piece = tokens // PIECES
    slot = lax.rem(m, SLOTS)

    def n_loads(step, at):
        for i, ref in enumerate((na_ref, nb_ref)):
            yield pltpu.make_async_copy(ref.at[:, run(step, rows)], n_buf.at[at, run(i, half)], n_sems.at[at, i])

    def g_loads(i):
        for c in range(n_grp):
            yield pltpu.make_async_copy(g_ref.at[c, run(i, piece)], rhs.at[run(i, piece), run(c, cols)], g_sems.at[i, c])

    def stores(step, at):
        yield from column_copies(buf.at[at], out_ref, lambda i: out_sems.at[at, i], step * rows, places_of(core))
        yield pltpu.make_async_copy(buf.at[at], copy_ref.at[run(step, rows)], copy_sems.at[at])

    def pastes():
        if old_places_of:
            yield from column_copies(recv_ref, out_ref, lambda i: paste_sems.at[i], m * rows, old_places_of(1 - core))
        if wo_tile:
            tiles = wo_recv_ref.shape[0] // HEAD
            for t in range(tiles):
                tile = wo_tile(m * tiles + t, 1 - core)
                yield pltpu.make_async_copy(wo_recv_ref.at[run(t, HEAD)], outs[2].at[run(tile, HEAD)], wo_sems.at[t])

    @pl.when(m == 0)
    def _():
        start_all(n_loads(0, 0))
        for i in range(PIECES):
            start_all(g_loads(i))

    @pl.when(m + 1 < n_m)
    def _():
        start_all(n_loads(m + 1, 1 - slot))

    start_all(pastes())

    @pl.when(m >= 2)
    def _():
        wait_all(stores(m - 2, slot))

    wait_all(n_loads(m, slot))

    @pl.when(m == 0)
    def _():
        buf[slot] = jnp.zeros((rows, n_grp * cols), F32)

        @pl.loop(0, PIECES)
        def _(i):
            wait_all(g_loads(i))
            buf[slot] += dot_tn(n_buf[slot, run(i, piece)], rhs[run(i, piece)])

    @pl.when(m > 0)
    def _():
        buf[slot] = dot_tn(n_buf[slot], rhs[...])

    start_all(stores(m, slot))
    wait_all(pastes())

    @pl.when(m == n_m - 1)
    def _():
        wait_all(stores(m - 1, 1 - slot))
        wait_all(stores(m, slot))


def weight_grad_qkv(core, places_of, n_a, n_b, g_par, whole, recv=None, old_places_of=None, wo=None):
    hidden = n_a.shape[1]
    n_grp, tokens, cols = g_par.shape
    width = n_grp * cols
    rows = 2 * BLK
    steps = hidden // rows
    args, specs, alias = [core, n_a, n_b, g_par], [ANY, ANY, ANY], {}
    outs = [jax.ShapeDtypeStruct((hidden, 3 * hidden), F32), jax.ShapeDtypeStruct((hidden, width), F32)]
    wo_tile = None
    if recv is not None:
        args.append(recv)
        specs.append(pl.BlockSpec((rows, recv.shape[1]), lambda m, core: (m, Z)))
    if wo is not None:
        wo_recv, wo_whole, wo_tile = wo
        args.append(wo_recv)
        specs.append(pl.BlockSpec((wo_recv.shape[0] // steps, hidden), lambda m, core: (m, Z)))
        outs.append(jax.ShapeDtypeStruct(wo_whole.shape, F32))
    if whole is not None:
        alias[len(args)] = 0
        args.append(whole)
        specs.append(ANY)
    if wo is not None:
        alias[len(args)] = 2
        args.append(wo_whole)
        specs.append(ANY)
    return pl.pallas_call(
        functools.partial(wqkv_grad_kernel, places_of, old_places_of, wo_tile),
        grid_spec=pltpu.PrefetchScalarGridSpec(
            num_scalar_prefetch=1,
            grid=(steps,),
            in_specs=specs,
            out_specs=[ANY] * len(outs),
            scratch_shapes=[
                pltpu.VMEM((SLOTS, tokens, rows), BF16),
                pltpu.VMEM((tokens, width), BF16),
                pltpu.VMEM((SLOTS, rows, width), F32),
                dma_sems(SLOTS, SLOTS), dma_sems(PIECES, n_grp), dma_sems(SLOTS, n_grp), dma_sems(SLOTS), dma_sems(n_grp), dma_sems(4),
            ],
        ),
        out_shape=outs,
        input_output_aliases=alias,
        compiler_params=VMEM_BIG,
        cost_estimate=matmul_cost(hidden, tokens, width, 16 * hidden * width),
        name='wqkv_grad',
    )(*args)


def normed_grad_kernel(runs, n_src, final, places_of, cols_ref, *rest):
    srcs, (w_ref, init_ref, *rest) = rest[:n_src], rest[n_src:]
    if final:
        x_ref, gain_ref, dx_ref, sum_ref, acc, w_buf, g_buf, sems, g_sems, init_sem, sum_acc = rest
    else:
        recv_ref, _, acc, whole_ref, w_buf, g_buf, sems, g_sems, paste_sems = rest
    j, steps = pl.program_id(0), pl.num_programs(0)
    slot = lax.rem(j, SLOTS)
    rows, width = g_buf.shape[1], g_buf.shape[2] // 2
    other, rank = cols_ref[2 * steps], cols_ref[2 * steps + 1]
    n_paste = 0 if final else w_ref.shape[0] // recv_ref.shape[0]

    def w_loads(step, at):
        for i in range(2):
            col = pl.multiple_of(cols_ref[2 * step + i], HEAD)
            yield pltpu.make_async_copy(w_ref.at[:, pl.ds(col, width)], w_buf.at[at, :, run(i, width)], sems.at[at, i])

    def g_loads(step):
        at = step % 2
        for i, (src, grp) in enumerate(runs[part(step, 2)]):
            ref, dst = srcs[src].at[grp], g_buf.at[at, :, run(i, width)]
            tokens = ref.shape[0]
            pairs = [(ref, dst)] if tokens == rows else [
                (ref.at[pl.ds(pl.multiple_of(h * (tokens // 2) + rank * (rows // 2), BLK), rows // 2)], dst.at[run(h, rows // 2)]) for h in range(2)]
            for pair in pairs:
                yield pltpu.make_async_copy(*pair, g_sems.at[at, i])

    def g_waits(at):
        for i in range(2):
            block = g_buf.at[at, :, run(i, width)]
            yield pltpu.make_async_copy(block, block, g_sems.at[at, i])

    def pastes():
        return column_copies(recv_ref, whole_ref, lambda i: paste_sems.at[i], j * recv_ref.shape[0], places_of(other))

    @pl.when(j == 0)
    def _():
        start_all(w_loads(0, 0))
        start_all(g_loads(0))
        if final:
            init = pltpu.make_async_copy(init_ref, acc, init_sem)
            init.start()
            init.wait()
        else:
            acc[...] = init_ref[...].astype(F32) * ALPHA

    @pl.when(j + 1 < steps)
    def _():
        start_all(w_loads(j + 1, 1 - slot))

    for step in range(1, len(runs) // 2):
        @pl.when(j + 1 == step)
        def _():
            start_all(g_loads(step))

    @pl.when(j < n_paste)
    def _():
        start_all([] if final else pastes())

    wait_all(w_loads(j, slot))
    wait_all(g_waits(slot))
    acc[...] += dot_nt(g_buf[slot], w_buf[slot])

    if final:
        @pl.when(j == steps - 1)
        def _():
            sum_acc[...] = jnp.zeros_like(sum_acc)
            gain = gain_ref[...].astype(F32)

            @pl.loop(0, rows // NORM_ROWS)
            def _(i):
                at = run(i, NORM_ROWS)
                d_n = acc[at]
                x, inv = centred(x_ref[at])
                x = x * inv
                d_x = d_n * gain
                mean = jnp.mean(d_x, axis=-1, keepdims=True)
                slope = jnp.mean(d_x * x, axis=-1, keepdims=True)
                dx_ref[at] = (inv * (d_x - mean - x * slope)).astype(BF16)
                for kind, term in enumerate((d_n * x, d_n)):
                    sum_acc[kind] += jnp.sum(term.reshape((2,) + sum_acc.shape[1:]), axis=0)

            sum_ref[...] = jnp.sum(sum_acc[...], axis=1)

    @pl.when(j < n_paste)
    def _():
        wait_all([] if final else pastes())


def normed_grad(cols, runs, srcs, w_qkv, init, paste=None, norm=None):
    rows, hidden = init.shape
    steps, width = len(runs) // 2, 2 * srcs[0].shape[-1]
    flat = pl.BlockSpec((rows, hidden), lambda j, cols: (Z, Z))
    args = [cols, *srcs, w_qkv, init]
    specs = [ANY] * (len(srcs) + 1) + [ANY if norm else flat]
    scratch = [pltpu.VMEM((SLOTS, hidden, width), BF16), pltpu.VMEM((SLOTS, rows, width), BF16), dma_sems(SLOTS, SLOTS), dma_sems(SLOTS, SLOTS)]
    alias, places_of = {}, None
    if norm:
        args += list(norm)
        specs += [flat, pl.BlockSpec((1, hidden), lambda j, cols: (Z, Z))]
        outs = [jax.ShapeDtypeStruct((rows, hidden), BF16), jax.ShapeDtypeStruct((2, hidden), F32)]
        out_specs = [flat, pl.BlockSpec((2, hidden), lambda j, cols: (Z, Z))]
        scratch = [pltpu.VMEM((rows, hidden), F32)] + scratch + [pltpu.SemaphoreType.DMA, pltpu.VMEM((2, 8, hidden), F32)]
    else:
        recv, places_of, whole = paste
        n_paste = 8
        alias = {len(args) + 1: 1}
        args += [recv, whole]
        specs += [pl.BlockSpec((hidden // n_paste, recv.shape[1]), lambda j, cols: (jnp.minimum(j, n_paste - 1), Z)), ANY]
        outs = [jax.ShapeDtypeStruct((rows, hidden), F32), jax.ShapeDtypeStruct(whole.shape, F32)]
        out_specs = [flat, ANY]
        scratch.append(dma_sems(8))
    return pl.pallas_call(
        functools.partial(normed_grad_kernel, runs, len(srcs), norm is not None, places_of),
        grid_spec=pltpu.PrefetchScalarGridSpec(
            num_scalar_prefetch=1,
            grid=(steps,),
            in_specs=specs,
            out_specs=out_specs,
            scratch_shapes=scratch,
        ),
        out_shape=outs,
        input_output_aliases=alias,
        compiler_params=VMEM_BIG,
        cost_estimate=matmul_cost(rows, steps * width, hidden),
        name='dn',
    )(*args)


def paste_kernel(places_of, core_ref, recv_ref, _, out_ref, sems):
    row = pl.program_id(0) * recv_ref.shape[0]
    copies = list(column_copies(recv_ref, out_ref, lambda i: sems.at[i], row, places_of(1 - core_ref[0])))
    start_all(copies)
    wait_all(copies)


def paste_columns(core, places_of, recv, whole):
    hidden, block = recv.shape
    rows = 2 * BLK
    return pl.pallas_call(
        functools.partial(paste_kernel, places_of),
        grid_spec=pltpu.PrefetchScalarGridSpec(
            num_scalar_prefetch=1,
            grid=(hidden // rows,),
            in_specs=[pl.BlockSpec((rows, block), lambda m, core: (m, Z)), ANY],
            out_specs=ANY,
            scratch_shapes=[dma_sems(8)],
        ),
        out_shape=jax.ShapeDtypeStruct(whole.shape, F32),
        input_output_aliases={2: 0},
        compiler_params=VMEM_BIG,
        name='paste',
    )(core, recv, whole)


def output_kernel(n_dist, core_ref, ctx_ref, shared_ref, w_ref, w_shared_ref, na_ref, nb_ref, b_ref, out_ref, acc):
    j = pl.program_id(0)

    @pl.when(j == 0)
    def _():
        acc[...] = dot_nn(ctx_ref[0], w_ref[...])

    @pl.when(jnp.logical_and(j > 0, j < n_dist))
    def _():
        acc[...] += dot_nn(ctx_ref[0], w_ref[...])

    @pl.when(j >= n_dist)
    def _():
        acc[...] += dot_nn(shared_ref[0], w_shared_ref[...])

    @pl.when(j == pl.num_programs(0) - 1)
    def _():
        for half, n_ref in enumerate((na_ref, nb_ref)):
            rows = part(half, n_ref.shape[0])
            out_ref[rows] = (ALPHA * n_ref[...].astype(F32) + (acc[rows] + b_ref[...].astype(F32))).astype(BF16)


def project_out(core, ctx_tok, shared_tok, w_o, n_halves, b_o):
    n_dev, rows, cols = ctx_tok.shape
    n_core, _, shared = shared_tok.shape
    hidden = w_o.shape[1]
    base = n_dev * cols // shared

    def dist_index(j, core):
        at = jnp.minimum(j, n_dev - 1)
        return jnp.where(at < n_dev // 2, 2 * at + core[0], 2 * (at - n_dev // 2) + 1 - core[0])

    def shared_index(j, core):
        return jnp.where(j <= n_dev, core[0], 1 - core[0])

    whole, half = [pl.BlockSpec((size, hidden), lambda j, core: (Z, Z)) for size in (rows, rows // 2)]
    return pl.pallas_call(
        functools.partial(output_kernel, n_dev),
        grid_spec=pltpu.PrefetchScalarGridSpec(
            num_scalar_prefetch=1,
            grid=(n_dev + n_core,),
            in_specs=[
                pl.BlockSpec((1, rows, cols), lambda j, core: (jnp.minimum(j, n_dev - 1), Z, Z)),
                pl.BlockSpec((1, rows, shared), lambda j, core: (jnp.maximum(j - n_dev, Z), Z, Z)),
                pl.BlockSpec((cols, hidden), lambda j, core: (dist_index(j, core), Z)),
                pl.BlockSpec((shared, hidden), lambda j, core: (base + shared_index(j, core), Z)),
                half, half,
                pl.BlockSpec((1, hidden), lambda j, core: (Z, Z)),
            ],
            out_specs=whole,
            scratch_shapes=[pltpu.VMEM((rows, hidden), F32)],
        ),
        out_shape=jax.ShapeDtypeStruct((rows, hidden), BF16),
        compiler_params=VMEM_BIG,
        cost_estimate=matmul_cost(rows, hidden, hidden),
        name='out_proj',
    )(core, ctx_tok, shared_tok, w_o, w_o, *n_halves, b_o.reshape(1, -1))


def together(*values):
    return lax.optimization_barrier(values)


def solution(mesh):
    n_dev = mesh.shape['sp']
    tok_spec = P('dp', 'sp', None)
    pos_spec = P('dp', 'sp')
    in_specs = (tok_spec, pos_spec, pos_spec, P('dp'), P(), P(), P(), P(), P(), P(), tok_spec)
    out_specs = (tok_spec, tok_spec, P('dp'), P('dp'), P('dp', None), P('dp'), P('dp', None), P('dp'))
    same_core = [list(range(core, n_dev, 2)) for core in range(2)]
    partners = [(dev, dev ^ 1) for dev in range(n_dev)]
    n_chip = n_dev // 2

    def device_step(hidden_in, pos_ids, block_pos, prefix_len, ln_gamma, ln_beta, w_qkv, b_qkv, w_o, b_o, grad_out):
        batch, local_len, hidden = hidden_in.shape
        per_half = batch // 2
        heads = hidden // HEAD
        n_dist, n_shared = (heads - SHARED) // n_dev, SHARED // 2
        shared_at = n_dev * n_dist
        rows = batch * local_len
        tokens = n_dev * rows
        rank = lax.axis_index('sp')
        parity = lax.rem(rank, SLOTS)
        pair = rank + 1 - 2 * parity
        core = parity.reshape(1).astype(jnp.int32)
        gather = functools.partial(lax.all_gather, axis_name='sp')
        gather_core = functools.partial(lax.all_gather, axis_name='sp', axis_index_groups=same_core)
        to_partner = functools.partial(lax.ppermute, axis_name='sp', perm=partners)

        def token_rows(arr, dev):
            split = arr.reshape(arr.shape[:-2] + (2, n_dev, rows // 2, arr.shape[-1]))
            return lax.dynamic_index_in_dim(split, dev, axis=split.ndim - 3, keepdims=False).reshape(arr.shape[:-2] + (rows, arr.shape[-1]))

        def places(head):
            return lambda par: [((2 * c + par) * n_dist + head) * WIDTH for c in range(n_chip)]

        def shared_places(par):
            return [(shared_at + par * n_shared + i) * WIDTH for i in range(n_shared)]

        def wo_tile(t, par):
            spread = t - n_shared
            return jnp.where(t < n_shared, shared_at + par * n_shared + t, (2 * (spread // n_dist) + par) * n_dist + lax.rem(spread, n_dist))

        halves = range(2)
        x_flat, gain = hidden_in.reshape(rows, hidden), ln_gamma.reshape(1, hidden)
        n_own = [normalize(half, x_flat, gain, ln_beta.reshape(1, hidden)) for half in halves]
        dy_own = [grad_out[part(half, per_half)] for half in halves]
        n_own[1], *dy_own = together(n_own[1], *dy_own)
        n_a, n_b, dy_a, dy_b = [gather(send.reshape(per_half, local_len, hidden)) for send in n_own + dy_own]
        cos, sin = rope_tables(prefix_len, n_dev * local_len)
        prefix = [prefix_len[part(half, per_half)] for half in halves]
        starts = jnp.stack([rank * n_dist, shared_at + parity * n_shared, rank, pair]).astype(jnp.int32)
        bias = jnp.concatenate([
            lax.dynamic_slice_in_dim(b_qkv, starts[0] * WIDTH, n_dist * WIDTH),
            lax.dynamic_slice_in_dim(b_qkv, starts[1] * WIDTH, n_shared * WIDTH)]).astype(F32).reshape(1, -1)
        grad_bo = jnp.sum(grad_out.astype(F32), axis=(0, 1))
        n_chip_rows, dy_chip_rows = [
            jnp.stack([own, to_partner(own)]).reshape(CORES, batch, local_len, hidden) for own in (jnp.concatenate(n_own), grad_out.reshape(rows, hidden))]
        qkv_own = project_qkv(starts, n_dist, n_shared, n_chip_rows, w_qkv, bias, cos, sin)
        d_ctx_own = context_grad(starts, n_dist + n_shared, dy_chip_rows, w_o, n_dev)
        n_a, grad_bo, *d_ctx_own = together(n_a, grad_bo, *d_ctx_own)

        ctx_d = ctx_r = None
        qkv, lses = [], []
        for half in halves:
            if half:
                n_b, ctx_r = together(n_b, ctx_r)
            qd, kd, vd, qr, kr, vr = project_qkv(
                starts, n_dist, n_shared, n_b if half else n_a, w_qkv, bias, cos, sin, half, qkv_own[part(half, QKV_IN)])
            ctx_d, lse_d = attention_forward(half, prefix[half], qd, kd, vd, n_dev, ctx_d)
            qr, ctx_d = together(qr, ctx_d)
            ctx_r, lse_r = attention_forward(half, prefix[half], qr, kr, vr, n_dev, ctx_r)
            qkv.append((qd, kd, vd, qr, kr, vr))
            lses.append((lse_d, lse_r))
        ctx_par = gather_core(ctx_d.reshape(tokens, n_dist * HEAD))

        dy_a, ctx_r = together(dy_a, ctx_r)
        g_d = g_r = None
        sum_d, sum_r = [], []
        for half in halves:
            if half:
                dy_b, g_r = together(dy_b, g_r)
            qd, kd, vd, qr, kr, vr = qkv[half]
            d_ctx, = context_grad(starts, n_dist + n_shared, dy_b if half else dy_a, w_o, n_dev, d_ctx_own[half])
            g_d, sums = attention_backward(half, n_shared, prefix[half], qd, kd, vd, ctx_d, d_ctx, lses[half][0], cos, sin, g_d)
            sum_d.append(sums)
            qr, g_d = together(qr, g_d)
            g_r, sums = attention_backward(half, 0, prefix[half], qr, kr, vr, ctx_r, d_ctx, lses[half][1], cos, sin, g_r, CORES)
            sum_r.append(sums)
        g_d = g_d.reshape(n_dist, tokens, WIDTH)
        g_r = g_r.reshape(n_shared, tokens, WIDTH)
        g_par = [gather_core(g_d[head]) for head in range(n_dist)]
        sums = [jnp.sum(jnp.concatenate(part, axis=1), axis=(1, 2)).reshape(-1) for part in (sum_d, sum_r)]

        n_a, n_b, dy_a, dy_b = [part.reshape(tokens // 2, hidden) for part in (n_a, n_b, dy_a, dy_b)]
        ctx_r = ctx_r.reshape(tokens, n_shared * HEAD)
        r_recv, shared_recv = to_partner(token_rows(g_r, pair)), to_partner(token_rows(ctx_r, pair))
        ctx_r, g_r = together(ctx_r, g_r)
        grad_wo, wo_block = weight_grad_o(
            core, ctx_r[None], dy_a, dy_b, lambda c, par: (shared_at + par * n_shared) * HEAD, lambda c: Z, hidden // 2, ())
        r_recv, shared_recv, wo_block, n_a = together(r_recv, shared_recv, wo_block, n_a)
        grad_wqkv, block = weight_grad_qkv(core, shared_places, n_a, n_b, g_r, None)
        ctx_recv = to_partner(token_rows(ctx_par, pair))
        ctx_par, ctx_recv, block = together(ctx_par, ctx_recv, block)
        recv_r = to_partner(block)
        grad_wo, wo_block = weight_grad_o(
            core, ctx_par, dy_a, dy_b, lambda c, par: (2 * c + par) * (n_dist * HEAD), lambda c: (n_shared + c * n_dist) * HEAD,
            hidden // 2, (grad_wo, wo_block))
        ctx_tok = jnp.concatenate([token_rows(ctx_par, rank), ctx_recv])
        ctx_tok, wo_block, recv_r = together(ctx_tok, wo_block, recv_r)
        wo_recv = to_partner(wo_block)
        shared_tok = jnp.stack([token_rows(ctx_r, rank), shared_recv])
        hidden_out = project_out(core, ctx_tok, shared_tok, w_o, n_own, b_o)
        n_a, hidden_out, g_par[0] = together(n_a, hidden_out, g_par[0])

        def columns(table):
            at = [np.array([h * WIDTH for h in table(par)] + [1 - par, 0], np.int32) for par in range(2)]
            last = (np.arange(at[0].size) == at[0].size - 1).astype(np.int32)
            return jnp.asarray(at[0]) + parity.astype(jnp.int32) * jnp.asarray(at[1] - at[0]) + rank.astype(jnp.int32) * jnp.asarray(last)

        def spread_grad(head, whole, **extra):
            whole, block, *rest = weight_grad_qkv(core, places(head), n_a, n_b, g_par[head], whole, **extra)
            tok = to_partner(token_rows(g_par[head], pair))
            tok, block = together(tok, block)
            return whole, tok, to_partner(block), rest

        grad_wqkv, tok_0, recv_0, _ = spread_grad(0, grad_wqkv, recv=recv_r, old_places_of=shared_places)
        g_par[1], grad_wqkv = together(g_par[1], grad_wqkv)
        grad_wqkv, tok_1, recv_1, (grad_wo,) = spread_grad(1, grad_wqkv, wo=(wo_recv, grad_wo, wo_tile))
        cols = columns(lambda mine: [shared_at + par * n_shared + i for par in (mine, 1 - mine) for i in range(n_shared)] + [
            (2 * c + par) * n_dist + head for par in (mine, 1 - mine) for c in range(n_chip) for head in (0, 1)])
        runs = [(src, i) for src in (0, 1) for i in range(n_shared)] + [(src, c) for pair in ((2, 3), (4, 5)) for c in range(n_chip) for src in pair]
        d_norm, grad_wqkv = normed_grad(
            cols, runs, [g_r, r_recv, g_par[0], g_par[1], tok_0, tok_1], w_qkv, grad_out.reshape(rows, hidden), (recv_0, places(0), grad_wqkv))
        n_a, d_norm, g_par[2] = together(n_a, d_norm, g_par[2])
        grad_wqkv, tok_2, recv_2, _ = spread_grad(2, grad_wqkv, recv=recv_1, old_places_of=places(1))
        cols = columns(lambda mine: [(2 * c + par) * n_dist + 2 for c in range(n_chip) for par in (mine, 1 - mine)])
        grad_in, norm_sums = normed_grad(
            cols, [(src, c) for c in range(n_chip) for src in range(2)], [g_par[2], tok_2], w_qkv, d_norm, norm=(x_flat, gain))
        small = gather(jnp.concatenate(sums + [norm_sums.reshape(-1), grad_bo]))
        recv_2, small = together(recv_2, small)
        grad_wqkv = paste_columns(core, places(2), recv_2, grad_wqkv)
        spread, shared = small[:, :n_dist * WIDTH], small[:2, n_dist * WIDTH:(n_dist + n_shared) * WIDTH]
        grad_bqkv = jnp.concatenate([spread.reshape(-1), shared.reshape(-1)])
        grad_gamma, grad_beta, grad_bo = jnp.sum(small[:, (n_dist + n_shared) * WIDTH:], axis=0).reshape(3, hidden)
        shape = (batch, local_len, hidden)
        return (hidden_out.reshape(shape), grad_in.reshape(shape), grad_gamma, grad_beta, grad_wqkv, grad_bqkv, grad_wo, grad_bo)

    return jax.shard_map(device_step, mesh=mesh, in_specs=in_specs, out_specs=out_specs, check_vma=False)
```

```python
import functools
import math
import jax
import jax.numpy as jnp
import numpy as np
from jax import lax
from jax.experimental import pallas as pl
from jax.experimental.pallas import tpu as pltpu
from jax.sharding import PartitionSpec as P

HEAD = 128
QUARTER = 32
ALPHA = math.sqrt(56.0)
LN_EPS = 1e-5
ROT_BASE = 10000.0
SCALE = 1.0 / math.sqrt(HEAD)
LOG2E = math.log2(math.e)
MASK_FILL = -1e30
BLK = 256
VMEM_BIG = pltpu.CompilerParams(vmem_limit_bytes=62 << 20)
SHARED = 8
Z = 0
SLOTS = CORES = 2
WIDTH = 3 * HEAD
F32 = jnp.float32
BF16 = jnp.bfloat16


def dot(lhs, rhs, lhs_dim, rhs_dim):
    return lax.dot_general(lhs, rhs, (((lhs_dim,), (rhs_dim,)), ((), ())), preferred_element_type=F32)


def dot_nn(lhs, rhs):
    return dot(lhs, rhs, 1, 0)


def dot_nt(lhs, rhs):
    return dot(lhs, rhs, 1, 1)


def dot_tn(lhs, rhs):
    return dot(lhs, rhs, 0, 0)


def matmul_cost(rows, depth, cols, extra=0):
    return pl.CostEstimate(
        flops=2 * rows * depth * cols, bytes_accessed=2 * (rows * depth + depth * cols + rows * cols) + extra, transcendentals=0)


def attention_cost(n_head, batch, seq, products):
    pairs = n_head * batch * seq * seq
    return pl.CostEstimate(flops=2 * products * pairs * HEAD, bytes_accessed=8 * products * n_head * batch * seq * HEAD, transcendentals=pairs)


def run(index, size):
    return pl.ds(pl.multiple_of(index * size, size), size)


def part(index, size):
    return slice(index * size, (index + 1) * size)


def rope_tables(prefix_len, seq):
    tok = jnp.arange(seq, dtype=jnp.int32)[None, :]
    pre = prefix_len[:, None]
    inside = tok < pre
    pos = jnp.where(inside, tok, pre - 1)
    blk = jnp.where(inside, 0, tok - pre + 1)
    inv_freq = ROT_BASE ** (-jnp.arange(QUARTER, dtype=F32) / QUARTER)
    angles = jnp.stack([pos, blk], axis=-1).astype(F32)[..., None] * inv_freq
    cos, sin = jnp.cos(angles), jnp.sin(angles)
    shape = pos.shape + (HEAD,)
    return (jnp.stack([cos, cos], axis=-2).reshape(shape), jnp.stack([-sin, sin], axis=-2).reshape(shape))


def turn(x, cos, sin):
    lane = lax.broadcasted_iota(jnp.int32, x.shape, 1)
    other = jnp.where(lane % (2 * QUARTER) < QUARTER, pltpu.roll(x, HEAD - QUARTER, 1), pltpu.roll(x, QUARTER, 1))
    return x * cos + other * sin


def dma_sems(*shape):
    return pltpu.SemaphoreType.DMA(shape)


def dma_sems(*shape):
    return pltpu.SemaphoreType.DMA(shape)


def start_all(copies):
    for copy in copies:
        copy.start()


def wait_all(copies):
    for copy in copies:
        copy.wait()


ANY = pl.BlockSpec(memory_space=pl.ANY)
PIECES = 4
QKV_IN = 6


NORM_ROWS = 32


def centred(x):
    x = x.astype(F32)
    x = x - jnp.mean(x, axis=-1, keepdims=True)
    return x, lax.rsqrt(jnp.mean(x * x, axis=-1, keepdims=True) + LN_EPS)


def norm_kernel(x_ref, gain_ref, shift_ref, out_ref):
    gain, shift = gain_ref[...].astype(F32), shift_ref[...].astype(F32)

    @pl.loop(0, x_ref.shape[0] // NORM_ROWS)
    def _(i):
        rows = run(i, NORM_ROWS)
        x, inv = centred(x_ref[rows])
        out_ref[rows] = (x * inv * gain + shift).astype(BF16)


def normalize(half, x, gain, shift):
    rows, hidden = x.shape
    block = rows // 4
    vec = pl.BlockSpec((1, hidden), lambda i: (Z, Z))
    return pl.pallas_call(
        norm_kernel,
        grid=(2,),
        in_specs=[pl.BlockSpec((block, hidden), lambda i: (2 * half + i, Z)), vec, vec],
        out_specs=pl.BlockSpec((block, hidden), lambda i: (i, Z)),
        out_shape=jax.ShapeDtypeStruct((2 * block, hidden), BF16),
        compiler_params=VMEM_BIG,
        name='norm',
    )(x, gain, shift)


def qkv_kernel(n_dist, n_tile, n_in, start_ref, *rest):
    n_refs, (w_ref, b_ref, cos_ref, sin_ref, *outs), (w_buf, acc, sems) = rest[:n_in], rest[n_in:-3], rest[-3:]
    first, later = n_refs[:(n_in + 1) // CORES], n_refs[n_in // CORES:]
    _, rows, cols = acc.shape
    hidden = w_ref.shape[0]
    dist = n_dist * WIDTH
    step, last = pl.program_id(Z), pl.num_programs(Z) - 1
    slot = lax.rem(step, SLOTS)
    piece = hidden // PIECES
    tile = first[0].shape[-2]

    def tokens(refs, span):
        width = piece if span else hidden
        return jnp.concatenate([ref[:, :, :, span or slice(None)].reshape(-1, width) for ref in refs])

    def loads(i):
        span = run(i, piece)
        for kind, (at, width) in enumerate(((0, dist), (dist, cols - dist))):
            col = pl.multiple_of(start_ref[kind] * WIDTH, HEAD)
            yield pltpu.make_async_copy(w_ref.at[span, pl.ds(col, width)], w_buf.at[span, pl.ds(at, width)], sems.at[i, kind])

    def finish():
        for i in range(rows // tile):
            group, batch, at, table = n_tile(i)
            cos, sin = cos_ref[table, part(at, tile)], sin_ref[table, part(at, tile)]
            for h in range(cols // WIDTH):
                kind, head = (0, h) if h < n_dist else (1, h - n_dist)
                refs = outs[part(CORES * group + kind, 3)]
                pre = [acc[1 - slot, part(i, tile), part(3 * h + j, HEAD)] + b_ref[:, part(3 * h + j, HEAD)] for j in range(3)]
                for ref, val in zip(refs, (turn(pre[0], cos, sin), turn(pre[1], cos, sin), pre[2])):
                    ref[head, batch, part(at, tile)] = val.astype(BF16)

    @pl.when(step == Z)
    def _():
        for i in range(PIECES):
            start_all(loads(i))
        acc[slot] = jnp.zeros((rows, cols), F32)

        @pl.loop(0, PIECES)
        def _(i):
            wait_all(loads(i))
            span = run(i, piece)
            acc[slot] += dot_nn(tokens(first, span), w_buf[span])

    @pl.when(jnp.logical_and(step > 0, step < last))
    def _():
        finish()
        acc[slot] = dot_nn(tokens(later, None), w_buf[...])

    pl.when(step == last)(finish)


def project_qkv(starts, n_dist, n_shared, n_rows, w_qkv, bias, cos, sin, half=None, earlier=None):
    _, per_half, local_len, hidden = n_rows[0].shape
    _, seq, _ = cos.shape
    cols = (n_dist + n_shared) * WIDTH
    own = earlier is None
    batch = per_half * CORES if own else per_half
    steps = CORES if own else seq // local_len // CORES - 1
    n_chip = seq // local_len // CORES
    width = local_len if own else CORES * local_len

    def place(step, at):
        return at[CORES + step] if own else lax.rem(at[CORES] // CORES + 1 + step, n_chip)

    def ahead(step, at):
        return place(jnp.minimum(step, steps - 1), at)

    def behind(step, at):
        return place(jnp.maximum(step - 1, 0), at)

    shapes = [jax.ShapeDtypeStruct((n_head, per_half, seq, HEAD), BF16) for n_head in (n_dist, n_shared) for _ in range(3)]
    shapes = shapes * CORES if own else shapes
    tab_spec = pl.BlockSpec((batch, width, HEAD), lambda step, at: (Z if own else half, behind(step, at), Z))
    arrays = [] if own else list(earlier)

    def own_tile(i):
        return i // per_half, i % per_half, 0, i

    def other_tile(i):
        return 0, i % per_half, i // per_half, i % per_half

    return pl.pallas_call(
        functools.partial(without, len(arrays), len(n_rows) + 5, functools.partial(qkv_kernel, n_dist, own_tile if own else other_tile, len(n_rows))),
        grid_spec=pltpu.PrefetchScalarGridSpec(
            num_scalar_prefetch=1,
            grid=(steps + 1,),
            in_specs=[
                *[pl.BlockSpec((1 if own else CORES, per_half, local_len, hidden), lambda step, at: (Z if own else ahead(step, at), Z, Z, Z))] * len(n_rows),
                ANY,
                pl.BlockSpec((1, cols), lambda step, at: (Z, Z)),
                tab_spec, tab_spec,
            ] + [ANY] * len(arrays),
            out_specs=[pl.BlockSpec(shape.shape[:CORES] + (width, HEAD), lambda step, at: (Z, Z, behind(step, at), Z)) for shape in shapes],
            scratch_shapes=[
                pltpu.VMEM((hidden, cols), BF16), pltpu.VMEM((SLOTS, CORES * CORES * local_len, cols), F32), dma_sems(PIECES, SLOTS)],
        ),
        out_shape=shapes,
        input_output_aliases={QKV_IN + i: i for i in range(len(arrays))},
        compiler_params=VMEM_BIG,
        cost_estimate=matmul_cost(steps * CORES * batch * local_len, hidden, cols),
        name='qkv',
    )(starts, *n_rows, w_qkv, bias, cos, sin, *arrays)


def without(count, start, kernel, *refs):
    kernel(*refs[:start], *refs[start + count:])


def forward_kernel(pre_ref, q_ref, k_ref, v_ref, *rest):
    ctx_ref, lse_ref = rest[-2:]
    n_head, _, seq, _ = q_ref.shape
    local_len = ctx_ref.shape[3]
    per = BLK // local_len
    prefix = pre_ref[pl.program_id(1)]

    def block(r, n_key):
        query = lax.broadcasted_iota(jnp.int32, (1, BLK), 1) + r * BLK
        last = jnp.maximum(query, prefix - 1) - (n_key - 1) * BLK
        scores = []
        for h in range(n_head):
            q_blk = q_ref[h, 0, part(r, BLK)]
            parts = [dot_nt(k_ref[h, 0, part(c, BLK)], q_blk) * (SCALE * LOG2E) for c in range(n_key)]
            key = lax.broadcasted_iota(jnp.int32, (BLK, BLK), 0)
            parts[-1] = jnp.where(key <= last, parts[-1], MASK_FILL)
            scores.append(parts)
        for h, parts in enumerate(scores):
            top = functools.reduce(jnp.maximum, [jnp.max(p, axis=0, keepdims=True) for p in parts])
            parts = [jnp.exp2(p - top) for p in parts]
            total = functools.reduce(jnp.add, [jnp.sum(p, axis=0, keepdims=True) for p in parts])
            inv = 1.0 / total
            probs = jnp.concatenate([(p * inv).astype(BF16) for p in parts], axis=0)
            ctx_t = dot_tn(v_ref[h, 0, :n_key * BLK], probs)
            ctx = ctx_t.T.astype(BF16).reshape(per, local_len, HEAD)
            ctx_ref[0, part(r, per), 0, :, part(h, HEAD)] = ctx
            lse_ref[h, 0, :, part(r, BLK)] = top + jnp.log2(total)

    n_blk = seq // BLK
    for r in range(n_blk):
        for n_key in range(r + 1, n_blk + 1):
            low = (n_key - 1) * BLK
            cond = prefix <= n_key * BLK if n_key == r + 1 else prefix > low
            if n_key < n_blk and n_key > r + 1:
                cond = jnp.logical_and(cond, prefix <= n_key * BLK)
            if n_key == n_blk and n_key == r + 1:
                block(r, n_key)
            else:
                pl.when(cond)(functools.partial(block, r, n_key))


def attention_forward(half, prefix_half, q, k, v, n_dev, ctx):
    own, batch, seq, _ = q.shape
    local_len = seq // n_dev
    group = own
    qkv_spec = pl.BlockSpec((group, 1, seq, HEAD), lambda h, b, pre: (h, b, Z, Z))
    earlier = [] if ctx is None else [ctx]
    return pl.pallas_call(
        forward_kernel,
        grid_spec=pltpu.PrefetchScalarGridSpec(
            num_scalar_prefetch=1,
            grid=(own // group, batch),
            in_specs=[qkv_spec] * 3 + [ANY] * len(earlier),
            out_specs=[
                pl.BlockSpec((1, n_dev, 1, local_len, group * HEAD), lambda h, b, pre: (half, Z, b, Z, h)),
                pl.BlockSpec((group, 1, 1, seq), lambda h, b, pre: (h, b, Z, Z)),
            ],
        ),
        out_shape=[
            jax.ShapeDtypeStruct((2, n_dev, batch, local_len, own * HEAD), BF16),
            jax.ShapeDtypeStruct((own, batch, 1, seq), F32),
        ],
        input_output_aliases={4: 0} if earlier else {},
        compiler_params=VMEM_BIG,
        cost_estimate=attention_cost(own, batch, seq, 2),
        name='attn_fwd',
    )(prefix_half, q, k, v, *earlier)


def d_ctx_kernel(n_in, start_ref, *rest):
    dy_refs, (w_ref, *outs), (w_buf, sems) = rest[:n_in], rest[n_in:-2], rest[-2:]
    step, hidden = pl.program_id(Z), w_ref.shape[1]
    widths = [outs[0].shape[-1], outs[1].shape[-1]]

    def loads():
        for kind, (at, width) in enumerate(zip((0, widths[0]), widths)):
            row = pl.multiple_of(start_ref[kind] * HEAD, HEAD)
            yield pltpu.make_async_copy(w_ref.at[pl.ds(row, width)], w_buf.at[pl.ds(at, width)], sems.at[kind])

    @pl.when(step == Z)
    def _():
        start_all(loads())
        wait_all(loads())

    def multiply(dy_ref):
        res = dot_nt(dy_ref[...].reshape(-1, hidden), w_buf[...]).astype(BF16)
        rows = CORES * res.shape[0] // len(outs)
        for i, out_ref in enumerate(outs):
            cols = slice(widths[0], None) if i % CORES else slice(widths[0])
            out_ref[...] = res[part(i // CORES, rows), cols].reshape(out_ref.shape)

    if n_in > 1:
        for i, dy_ref in enumerate(dy_refs):
            pl.when(step == i)(functools.partial(multiply, dy_ref))
    else:
        multiply(dy_refs[0])


def context_grad(starts, n_dist, n_shared, dy_rows, w_o, n_dev, earlier=()):
    _, batch, local_len, hidden = dy_rows[0].shape
    own = not earlier
    n_chip = n_dev // CORES
    per_half, devs = (batch // CORES, 1) if own else (batch, CORES)

    def block(step, at):
        return (at[CORES + step] if own else lax.rem(at[CORES] // CORES + 1 + step, n_chip), Z, Z, Z)

    cols = [n_dist * HEAD, n_shared * HEAD]
    outs = cols * (CORES if own else 1)
    n_in = len(dy_rows)
    return pl.pallas_call(
        functools.partial(without, len(earlier), n_in + 2, functools.partial(d_ctx_kernel, n_in)),
        grid_spec=pltpu.PrefetchScalarGridSpec(
            num_scalar_prefetch=1,
            grid=(CORES if own else n_chip - 1,),
            in_specs=[pl.BlockSpec((devs, batch, local_len, hidden), (lambda step, at: (Z, Z, Z, Z)) if own else block)] * n_in + [ANY] * (1 + len(earlier)),
            out_specs=[pl.BlockSpec((devs, per_half, local_len, width), block) for width in outs],
            scratch_shapes=[pltpu.VMEM((sum(cols), hidden), BF16), dma_sems(CORES)],
        ),
        out_shape=[jax.ShapeDtypeStruct((n_dev, per_half, local_len, width), BF16) for width in outs],
        input_output_aliases={3 + i: i for i in range(len(earlier))},
        compiler_params=VMEM_BIG,
        cost_estimate=matmul_cost(n_dev * batch * local_len, hidden, sum(cols)),
        name='dctx',
    )(starts, *dy_rows, w_o, *earlier)


def backward_kernel(pre_ref, q_ref, k_ref, v_ref, ctx_ref, dctx_ref, lse_ref, cos_ref, sin_ref, *rest):
    sum_ref, dq_acc, dk_acc, dv_acc = rest[-4:]
    n_head, _, seq, _ = q_ref.shape
    g_refs = rest[-4 - n_head:-4]
    _, n_dev, _, local_len, _ = g_refs[0].shape
    n_blk = seq // BLK
    prefix = pre_ref[pl.program_id(Z)]
    d_ctx, delta = [], []
    for h in range(n_head):
        lanes = part(h, HEAD)
        grad = dctx_ref[:, :, :, lanes].reshape(seq, HEAD)
        prod = grad.astype(F32) * ctx_ref[0, :, :, :, lanes].reshape(seq, HEAD).astype(F32)
        d_ctx.append(grad)
        delta.append(jnp.sum(prod.T, axis=0, keepdims=True))

    def block(c, first):
        span = part(c, BLK)
        start = first * BLK
        products = []
        for h in range(n_head):
            s_t = dot_nt(k_ref[h, 0, span], q_ref[h, 0, start:])
            dp_t = dot_nt(v_ref[h, 0, span], d_ctx[h][start:])
            products.append((s_t, dp_t))
        for h, (s_t, dp_t) in enumerate(products):
            probs, d_scores = [], []
            for r in range(first, n_blk):
                cols, here = part(r, BLK), part(r - first, BLK)
                piece = s_t[:, here] * (SCALE * LOG2E)
                if r <= c:
                    key = lax.broadcasted_iota(jnp.int32, (BLK, BLK), 0)
                    query = lax.broadcasted_iota(jnp.int32, (1, BLK), 1) + r * BLK
                    piece = jnp.where(key <= jnp.maximum(query, prefix - 1) - c * BLK, piece, MASK_FILL)
                p = jnp.exp2(piece - lse_ref[h, 0, :, cols])
                probs.append(p.astype(BF16))
                d_scores.append((p * (dp_t[:, here] - delta[h][:, cols]) * SCALE).astype(BF16))
            probs = jnp.concatenate(probs, axis=1)
            d_scores = jnp.concatenate(d_scores, axis=1)
            dv_acc[h, span] = dot_nn(probs, d_ctx[h][start:])
            dk_acc[h, span] = dot_nn(d_scores, q_ref[h, 0, start:])
            dq_part = dot_tn(k_ref[h, 0, span], d_scores)
            if c:
                dq_acc[h, :, start:] += dq_part
            else:
                dq_acc[h] = dq_part

    block(0, 0)
    for c in range(1, n_blk):
        pl.when(prefix > c * BLK)(functools.partial(block, c, 0))
        pl.when(prefix <= c * BLK)(functools.partial(block, c, c))

    cos, sin = cos_ref[Z], sin_ref[Z]
    for h in range(n_head):
        g_q = turn(dq_acc[h].T.astype(BF16).astype(F32), cos, -sin)
        g_k = turn(dk_acc[h].astype(BF16).astype(F32), cos, -sin)
        g_v = dv_acc[h].astype(BF16).astype(F32)
        for i, g in enumerate((g_q, g_k, g_v)):
            lanes = part(i, HEAD)
            g_refs[h][0, :, 0, :, lanes] = g.astype(BF16).reshape(n_dev, local_len, HEAD)
            sum_ref[h, 0, :, lanes] = jnp.sum(g, axis=0, keepdims=True)


def attention_backward(half, first, group, prefix_half, q, k, v, ctx, d_ctx, lse, cos, sin, earlier):
    _, batch, seq, _ = q.shape
    _, n_dev, _, local_len, _ = ctx.shape
    at = first // group
    qkv_spec = pl.BlockSpec((group, 1, seq, HEAD), lambda b, pre: (at, b, Z, Z))
    tab_spec = pl.BlockSpec((1, seq, HEAD), lambda b, pre: (half * batch + b, Z, Z))
    stat = functools.partial(pltpu.VMEM, dtype=F32)
    return pl.pallas_call(
        backward_kernel,
        grid_spec=pltpu.PrefetchScalarGridSpec(
            num_scalar_prefetch=1,
            grid=(batch,),
            in_specs=[qkv_spec] * 3 + [
                pl.BlockSpec((1, n_dev, 1, local_len, group * HEAD), lambda b, pre: (half, Z, b, Z, at)),
                pl.BlockSpec((n_dev, 1, local_len, group * HEAD), lambda b, pre: (Z, b, Z, at)),
                pl.BlockSpec((group, 1, 1, seq), lambda b, pre: (at, b, Z, Z)), tab_spec, tab_spec] + [ANY] * len(earlier),
            out_specs=[pl.BlockSpec((1, n_dev, 1, local_len, WIDTH), lambda b, pre: (half, Z, b, Z, Z))] * group + [
                pl.BlockSpec((group, 1, 1, WIDTH), lambda b, pre: (Z, b, Z, Z))],
            scratch_shapes=[stat((group, HEAD, seq)), stat((group, seq, HEAD)), stat((group, seq, HEAD))],
        ),
        out_shape=[jax.ShapeDtypeStruct((2, n_dev, batch, local_len, WIDTH), BF16)] * group + [
            jax.ShapeDtypeStruct((group, batch, 1, WIDTH), F32)],
        input_output_aliases={9 + i: i for i in range(len(earlier))},
        compiler_params=VMEM_BIG,
        cost_estimate=attention_cost(group, batch, seq, 5),
        name='attn_bwd',
    )(prefix_half, q, k, v, ctx, d_ctx, lse, cos, sin, *earlier)


def wo_grad_kernel(row_of, block_row_of, core_ref, ctx_ref, dya_ref, dyb_ref, *rest):
    out_ref, copy_ref, rhs, buf, rhs_sems, sems = rest[-6:]
    n, c = pl.program_id(Z), pl.program_id(1)
    n_col, n_grp = pl.num_programs(Z), pl.num_programs(1)
    step = n * n_grp + c
    slot, n_slot = lax.rem(step, SLOTS), lax.rem(n, SLOTS)
    _, rows, wide = buf.shape
    half = dya_ref.shape[0]
    core = core_ref[Z]

    def loads(n_at, at):
        for i, ref in enumerate((dya_ref, dyb_ref)):
            yield pltpu.make_async_copy(ref.at[:, run(n_at, wide)], rhs.at[at, run(i, half)], rhs_sems.at[at, i])

    def stores(at_step, at):
        n_at, c_at = at_step // n_grp, lax.rem(at_step, n_grp)
        for i, (ref, row) in enumerate(((out_ref, row_of(c_at, core)), (copy_ref, block_row_of(c_at)))):
            yield pltpu.make_async_copy(buf.at[at], ref.at[pl.ds(pl.multiple_of(row, HEAD), rows), run(n_at, wide)], sems.at[at, i])

    @pl.when(step == Z)
    def _():
        start_all(loads(0, 0))

    @pl.when(c == Z)
    def _():
        @pl.when(n + 1 < n_col)
        def _():
            start_all(loads(n + 1, 1 - n_slot))

        wait_all(loads(n, n_slot))

    @pl.when(step >= 2)
    def _():
        wait_all(stores(step - 2, slot))

    buf[slot] = dot_tn(ctx_ref[Z], rhs[n_slot])
    start_all(stores(step, slot))

    @pl.when(step == n_col * n_grp - 1)
    def _():
        wait_all(stores(step - 1, 1 - slot))
        wait_all(stores(step, slot))


def weight_grad_o(core, ctx_par, dy_a, dy_b, row_of, block_row_of, block_rows, earlier):
    n_grp, tokens, cols = ctx_par.shape
    hidden = dy_a.shape[1]
    wide = hidden // 4
    return pl.pallas_call(
        functools.partial(wo_grad_kernel, row_of, block_row_of),
        grid_spec=pltpu.PrefetchScalarGridSpec(
            num_scalar_prefetch=1,
            grid=(hidden // wide, n_grp),
            in_specs=[pl.BlockSpec((1, tokens, cols), lambda n, c, core: (c, Z, Z)), ANY, ANY] + [ANY] * len(earlier),
            out_specs=[ANY, ANY],
            scratch_shapes=[pltpu.VMEM((SLOTS, tokens, wide), BF16), pltpu.VMEM((SLOTS, cols, wide), F32), dma_sems(SLOTS, SLOTS), dma_sems(SLOTS, SLOTS)],
        ),
        out_shape=[jax.ShapeDtypeStruct((hidden, hidden), F32), jax.ShapeDtypeStruct((block_rows, hidden), F32)],
        input_output_aliases={4: 0, 5: 1} if earlier else {},
        compiler_params=VMEM_BIG,
        cost_estimate=matmul_cost(n_grp * cols, tokens, hidden, 8 * hidden * n_grp * cols),
        name='wo_grad',
    )(core, ctx_par, dy_a, dy_b, *earlier)


def column_copies(src, out_ref, sem_of, row, places):
    rows, width = src.shape[0], src.shape[1] // len(places)
    for i, col in enumerate(places):
        yield pltpu.make_async_copy(
            src.at[:, run(i, width)],
            out_ref.at[pl.ds(pl.multiple_of(row, BLK), rows), pl.ds(pl.multiple_of(col, HEAD), width)],
            sem_of(i))


def wqkv_grad_kernel(places_of, old_places_of, wo_tile, n_src, core_ref, na_ref, nb_ref, *rest):
    srcs, rest = rest[:n_src], list(rest[n_src:])
    groups = [ref.at[c] for ref in srcs for c in range(ref.shape[0])]
    recv_ref = rest.pop(0) if old_places_of else None
    wo_recv_ref = rest.pop(0) if wo_tile else None
    n_buf, rhs, buf, n_sems, g_sems, out_sems, copy_sems, paste_sems, wo_sems, tok_sems = rest[-10:]
    outs = rest[:-10][-4 if wo_tile else -3:]
    out_ref, copy_ref, tok_ref = outs[:3]
    m = pl.program_id(Z)
    n_m = pl.num_programs(Z)
    core, pair = core_ref[Z], core_ref[1]
    tokens, cols = groups[0].shape
    half, rows = tokens // 2, n_buf.shape[2]
    piece = tokens // PIECES
    slot = lax.rem(m, SLOTS)

    def n_loads(step, at):
        for i, ref in enumerate((na_ref, nb_ref)):
            yield pltpu.make_async_copy(ref.at[:, run(step, rows)], n_buf.at[at, run(i, half)], n_sems.at[at, i])

    def g_loads(i):
        for c, ref in enumerate(groups):
            yield pltpu.make_async_copy(ref.at[run(i, piece)], rhs.at[run(i, piece), run(c, cols)], g_sems.at[i, c])

    def stores(step, at):
        yield from column_copies(buf.at[at], out_ref, lambda i: out_sems.at[at, i], step * rows, places_of(core))
        yield pltpu.make_async_copy(buf.at[at], copy_ref.at[run(step, rows)], copy_sems.at[at])

    def pastes():
        if old_places_of:
            yield from column_copies(recv_ref, out_ref, lambda i: paste_sems.at[i], m * rows, old_places_of(1 - core))
        if wo_tile:
            tiles = wo_recv_ref.shape[0] // HEAD
            for t in range(tiles):
                tile = wo_tile(m * tiles + t, 1 - core)
                yield pltpu.make_async_copy(wo_recv_ref.at[run(t, HEAD)], outs[3].at[run(tile, HEAD)], wo_sems.at[t])

    def token_copies():
        size = tok_ref.shape[0] // 2
        for i in range(2):
            yield pltpu.make_async_copy(rhs.at[pl.ds(pl.multiple_of(i * half + pair * size, BLK), size)], tok_ref.at[run(i, size)], tok_sems.at[i])

    @pl.when(m == Z)
    def _():
        start_all(n_loads(0, 0))
        for i in range(PIECES):
            start_all(g_loads(i))

    @pl.when(m + 1 < n_m)
    def _():
        start_all(n_loads(m + 1, 1 - slot))

    start_all(pastes())

    @pl.when(m >= 2)
    def _():
        wait_all(stores(m - 2, slot))

    wait_all(n_loads(m, slot))

    @pl.when(m == Z)
    def _():
        buf[slot] = jnp.zeros((rows, rhs.shape[1]), F32)

        @pl.loop(0, PIECES)
        def _(i):
            wait_all(g_loads(i))
            buf[slot] += dot_tn(n_buf[slot, run(i, piece)], rhs[run(i, piece)])

        start_all(token_copies())

    @pl.when(m > 0)
    def _():
        buf[slot] = dot_tn(n_buf[slot], rhs[...])

    start_all(stores(m, slot))
    wait_all(pastes())

    @pl.when(m == n_m - 1)
    def _():
        wait_all(stores(m - 1, 1 - slot))
        wait_all(stores(m, slot))
        wait_all(token_copies())


def weight_grad_qkv(core, places_of, n_a, n_b, srcs, whole, recv=None, old_places_of=None, wo=None):
    hidden = n_a.shape[1]
    n_grp, (tokens, cols) = sum(src.shape[0] for src in srcs), srcs[0].shape[1:]
    width = n_grp * cols
    rows = 2 * BLK
    steps = hidden // rows
    args, specs, alias = [core, n_a, n_b, *srcs], [ANY] * (2 + len(srcs)), {}
    outs = [jax.ShapeDtypeStruct((hidden, 3 * hidden), F32), jax.ShapeDtypeStruct((hidden, width), F32), jax.ShapeDtypeStruct((2 * BLK, width), BF16)]
    wo_tile = None
    if recv is not None:
        args.append(recv)
        specs.append(pl.BlockSpec((rows, recv.shape[1]), lambda m, core: (m, Z)))
    if wo is not None:
        wo_recv, wo_whole, wo_tile = wo
        args.append(wo_recv)
        specs.append(pl.BlockSpec((wo_recv.shape[0] // steps, hidden), lambda m, core: (m, Z)))
        outs.append(jax.ShapeDtypeStruct(wo_whole.shape, F32))
    if whole is not None:
        alias[len(args)] = 0
        args.append(whole)
        specs.append(ANY)
    if wo is not None:
        alias[len(args)] = 3
        args.append(wo_whole)
        specs.append(ANY)
    return pl.pallas_call(
        functools.partial(wqkv_grad_kernel, places_of, old_places_of, wo_tile, len(srcs)),
        grid_spec=pltpu.PrefetchScalarGridSpec(
            num_scalar_prefetch=1,
            grid=(steps,),
            in_specs=specs,
            out_specs=[ANY] * len(outs),
            scratch_shapes=[
                pltpu.VMEM((SLOTS, tokens, rows), BF16),
                pltpu.VMEM((tokens, width), BF16),
                pltpu.VMEM((SLOTS, rows, width), F32),
                dma_sems(SLOTS, SLOTS), dma_sems(PIECES, n_grp), dma_sems(SLOTS, n_grp), dma_sems(SLOTS), dma_sems(n_grp), dma_sems(4), dma_sems(SLOTS),
            ],
        ),
        out_shape=outs,
        input_output_aliases=alias,
        compiler_params=VMEM_BIG,
        cost_estimate=matmul_cost(hidden, tokens, width, 16 * hidden * width),
        name='wqkv_grad',
    )(*args)


def normed_grad_kernel(runs, n_src, final, places_of, cols_ref, *rest):
    srcs, (w_ref, init_ref, *rest) = rest[:n_src], rest[n_src:]
    if final:
        x_ref, gain_ref, dx_ref, sum_ref, acc, w_buf, g_buf, sems, g_sems, init_sem, sum_acc = rest
    else:
        recv_ref, _, acc, whole_ref, w_buf, g_buf, sems, g_sems, paste_sems = rest
    j, steps = pl.program_id(Z), pl.num_programs(Z)
    slot = lax.rem(j, SLOTS)
    rows, width = g_buf.shape[1], g_buf.shape[2] // 2
    other, rank = cols_ref[2 * steps], cols_ref[2 * steps + 1]
    n_paste = 0 if final else w_ref.shape[0] // recv_ref.shape[0]

    def w_loads(step, at):
        for i in range(2):
            col = pl.multiple_of(cols_ref[2 * step + i], HEAD)
            yield pltpu.make_async_copy(w_ref.at[:, pl.ds(col, width)], w_buf.at[at, :, run(i, width)], sems.at[at, i])

    def g_loads(step):
        at = step % 2
        for i, (src, grp) in enumerate(runs[part(step, 2)]):
            ref, dst = srcs[src], g_buf.at[at, :, run(i, width)]
            tokens = ref.shape[-2]
            ref = ref.at[:, run(grp, width)] if tokens == rows else ref.at[grp]
            pairs = [(ref, dst)] if tokens == rows else [
                (ref.at[pl.ds(pl.multiple_of(h * (tokens // 2) + rank * (rows // 2), BLK), rows // 2)], dst.at[run(h, rows // 2)]) for h in range(2)]
            for pair in pairs:
                yield pltpu.make_async_copy(*pair, g_sems.at[at, i])

    def g_waits(at):
        for i in range(2):
            block = g_buf.at[at, :, run(i, width)]
            yield pltpu.make_async_copy(block, block, g_sems.at[at, i])

    def pastes():
        return column_copies(recv_ref, whole_ref, lambda i: paste_sems.at[i], j * recv_ref.shape[0], places_of(other))

    @pl.when(j == Z)
    def _():
        start_all(w_loads(0, 0))
        start_all(g_loads(0))
        if final:
            init = pltpu.make_async_copy(init_ref, acc, init_sem)
            init.start()
            init.wait()
        else:
            acc[...] = init_ref[...].astype(F32) * ALPHA

    @pl.when(j + 1 < steps)
    def _():
        start_all(w_loads(j + 1, 1 - slot))

    for step in range(1, len(runs) // 2):
        @pl.when(j + 1 == step)
        def _():
            start_all(g_loads(step))

    @pl.when(j < n_paste)
    def _():
        start_all([] if final else pastes())

    wait_all(w_loads(j, slot))
    wait_all(g_waits(slot))
    acc[...] += dot_nt(g_buf[slot], w_buf[slot])

    if final:
        @pl.when(j == steps - 1)
        def _():
            sum_acc[...] = jnp.zeros_like(sum_acc)
            gain = gain_ref[...].astype(F32)

            @pl.loop(0, rows // NORM_ROWS)
            def _(i):
                at = run(i, NORM_ROWS)
                d_n = acc[at]
                x, inv = centred(x_ref[at])
                x = x * inv
                d_x = d_n * gain
                mean = jnp.mean(d_x, axis=-1, keepdims=True)
                slope = jnp.mean(d_x * x, axis=-1, keepdims=True)
                dx_ref[at] = (inv * (d_x - mean - x * slope)).astype(BF16)
                for kind, term in enumerate((d_n * x, d_n)):
                    sum_acc[kind] += jnp.sum(term.reshape((-1,) + sum_acc.shape[1:]), axis=0)

            sum_ref[...] = jnp.sum(sum_acc[...], axis=1)

    @pl.when(j < n_paste)
    def _():
        wait_all([] if final else pastes())


def normed_grad(cols, runs, srcs, w_qkv, init, paste=None, norm=None):
    rows, hidden = init.shape
    steps, width = len(runs) // 2, 2 * WIDTH
    flat = pl.BlockSpec((rows, hidden), lambda j, cols: (Z, Z))
    args = [cols, *srcs, w_qkv, init]
    specs = [ANY] * (len(srcs) + 1) + [ANY if norm else flat]
    scratch = [pltpu.VMEM((SLOTS, hidden, width), BF16), pltpu.VMEM((SLOTS, rows, width), BF16), dma_sems(SLOTS, SLOTS), dma_sems(SLOTS, SLOTS)]
    alias, places_of = {}, None
    if norm:
        args += list(norm)
        specs += [flat, pl.BlockSpec((1, hidden), lambda j, cols: (Z, Z))]
        outs = [jax.ShapeDtypeStruct((rows, hidden), BF16), jax.ShapeDtypeStruct((2, hidden), F32)]
        out_specs = [flat, pl.BlockSpec((2, hidden), lambda j, cols: (Z, Z))]
        scratch = [pltpu.VMEM((rows, hidden), F32)] + scratch + [pltpu.SemaphoreType.DMA, pltpu.VMEM((2, 8, hidden), F32)]
    else:
        recv, places_of, whole = paste
        n_paste = 8
        alias = {len(args) + 1: 1}
        args += [recv, whole]
        specs += [pl.BlockSpec((hidden // n_paste, recv.shape[1]), lambda j, cols: (jnp.minimum(j, n_paste - 1), Z)), ANY]
        outs = [jax.ShapeDtypeStruct((rows, hidden), F32), jax.ShapeDtypeStruct(whole.shape, F32)]
        out_specs = [flat, ANY]
        scratch.append(dma_sems(8))
    return pl.pallas_call(
        functools.partial(normed_grad_kernel, runs, len(srcs), norm is not None, places_of),
        grid_spec=pltpu.PrefetchScalarGridSpec(
            num_scalar_prefetch=1,
            grid=(steps,),
            in_specs=specs,
            out_specs=out_specs,
            scratch_shapes=scratch,
        ),
        out_shape=outs,
        input_output_aliases=alias,
        compiler_params=VMEM_BIG,
        cost_estimate=matmul_cost(rows, steps * width, hidden),
        name='dn',
    )(*args)


def paste_kernel(places_of, core_ref, recv_ref, _, out_ref, sems):
    row = pl.program_id(Z) * recv_ref.shape[0]
    copies = list(column_copies(recv_ref, out_ref, lambda i: sems.at[i], row, places_of(1 - core_ref[Z])))
    start_all(copies)
    wait_all(copies)


def paste_columns(core, places_of, recv, whole):
    hidden, block = recv.shape
    rows = 2 * BLK
    return pl.pallas_call(
        functools.partial(paste_kernel, places_of),
        grid_spec=pltpu.PrefetchScalarGridSpec(
            num_scalar_prefetch=1,
            grid=(hidden // rows,),
            in_specs=[pl.BlockSpec((rows, block), lambda m, core: (m, Z)), ANY],
            out_specs=ANY,
            scratch_shapes=[dma_sems(8)],
        ),
        out_shape=jax.ShapeDtypeStruct(whole.shape, F32),
        input_output_aliases={2: 0},
        compiler_params=VMEM_BIG,
        name='paste',
    )(core, recv, whole)


def output_kernel(n_dist, core_ref, ctx_ref, shared_ref, w_ref, w_shared_ref, na_ref, nb_ref, b_ref, out_ref, acc):
    j = pl.program_id(Z)

    @pl.when(j == Z)
    def _():
        acc[...] = dot_nn(ctx_ref[Z], w_ref[...])

    @pl.when(jnp.logical_and(j > 0, j < n_dist))
    def _():
        acc[...] += dot_nn(ctx_ref[Z], w_ref[...])

    @pl.when(j >= n_dist)
    def _():
        acc[...] += dot_nn(shared_ref[Z], w_shared_ref[...])

    @pl.when(j == pl.num_programs(Z) - 1)
    def _():
        for half, n_ref in enumerate((na_ref, nb_ref)):
            rows = part(half, n_ref.shape[0])
            out_ref[rows] = (ALPHA * n_ref[...].astype(F32) + (acc[rows] + b_ref[...].astype(F32))).astype(BF16)


def project_out(core, ctx_tok, shared_tok, w_o, n_halves, b_o):
    n_dev, rows, cols = ctx_tok.shape
    n_core, _, shared = shared_tok.shape
    hidden = w_o.shape[1]
    base = n_dev * cols // shared

    def dist_index(j, core):
        at = jnp.minimum(j, n_dev - 1)
        return jnp.where(at < n_dev // 2, 2 * at + core[Z], 2 * (at - n_dev // 2) + 1 - core[Z])

    def shared_index(j, core):
        return jnp.where(j <= n_dev, core[Z], 1 - core[Z])

    whole, half = [pl.BlockSpec((size, hidden), lambda j, core: (Z, Z)) for size in (rows, rows // 2)]
    return pl.pallas_call(
        functools.partial(output_kernel, n_dev),
        grid_spec=pltpu.PrefetchScalarGridSpec(
            num_scalar_prefetch=1,
            grid=(n_dev + n_core,),
            in_specs=[
                pl.BlockSpec((1, rows, cols), lambda j, core: (jnp.minimum(j, n_dev - 1), Z, Z)),
                pl.BlockSpec((1, rows, shared), lambda j, core: (jnp.maximum(j - n_dev, Z), Z, Z)),
                pl.BlockSpec((cols, hidden), lambda j, core: (dist_index(j, core), Z)),
                pl.BlockSpec((shared, hidden), lambda j, core: (base + shared_index(j, core), Z)),
                half, half,
                pl.BlockSpec((1, hidden), lambda j, core: (Z, Z)),
            ],
            out_specs=whole,
            scratch_shapes=[pltpu.VMEM((rows, hidden), F32)],
        ),
        out_shape=jax.ShapeDtypeStruct((rows, hidden), BF16),
        compiler_params=VMEM_BIG,
        cost_estimate=matmul_cost(rows, hidden, hidden),
        name='out_proj',
    )(core, ctx_tok, shared_tok, w_o, w_o, *n_halves, b_o.reshape(1, -1))


def together(*values):
    return lax.optimization_barrier(values)


def solution(mesh):
    n_dev = mesh.shape['sp']
    tok_spec = P('dp', 'sp', None)
    pos_spec = P('dp', 'sp')
    in_specs = (tok_spec, pos_spec, pos_spec, P('dp'), P(), P(), P(), P(), P(), P(), tok_spec)
    out_specs = (tok_spec, tok_spec, P('dp'), P('dp'), P('dp', None), P('dp'), P('dp', None), P('dp'))
    same_core = [list(range(core, n_dev, 2)) for core in range(2)]
    partners = [(dev, dev ^ 1) for dev in range(n_dev)]
    n_chip = n_dev // 2

    def device_step(hidden_in, pos_ids, block_pos, prefix_len, ln_gamma, ln_beta, w_qkv, b_qkv, w_o, b_o, grad_out):
        batch, local_len, hidden = hidden_in.shape
        per_half = batch // 2
        heads = hidden // HEAD
        n_dist, n_shared = (heads - SHARED) // n_dev, SHARED // 2
        shared_at = n_dev * n_dist
        rows = batch * local_len
        tokens = n_dev * rows
        rank = lax.axis_index('sp')
        parity = lax.rem(rank, SLOTS)
        pair = rank + 1 - 2 * parity
        core = jnp.stack([parity, pair]).astype(jnp.int32)
        gather = functools.partial(lax.all_gather, axis_name='sp')
        gather_core = functools.partial(lax.all_gather, axis_name='sp', axis_index_groups=same_core)
        to_partner = functools.partial(lax.ppermute, axis_name='sp', perm=partners)

        def token_rows(arr, dev):
            split = arr.reshape(arr.shape[:-2] + (2, n_dev, rows // 2, arr.shape[-1]))
            return lax.dynamic_index_in_dim(split, dev, axis=split.ndim - 3, keepdims=False).reshape(arr.shape[:-2] + (rows, arr.shape[-1]))

        def places(head):
            return lambda par: [((2 * c + par) * n_dist + head) * WIDTH for c in range(n_chip)]

        def shared_places(par):
            return [(shared_at + par * n_shared + i) * WIDTH for i in range(n_shared)]

        def wo_tile(t, par):
            spread = t - n_shared
            return jnp.where(t < n_shared, shared_at + par * n_shared + t, (2 * (spread // n_dist) + par) * n_dist + lax.rem(spread, n_dist))

        halves = range(2)
        x_flat, gain = hidden_in.reshape(rows, hidden), ln_gamma.reshape(1, hidden)
        n_own = [normalize(half, x_flat, gain, ln_beta.reshape(1, hidden)) for half in halves]
        dy_own = [grad_out[part(half, per_half)] for half in halves]
        n_own[1], *dy_own = together(n_own[1], *dy_own)
        n_own = [own.reshape(per_half, local_len, hidden) for own in n_own]
        n_a, n_b, dy_a, dy_b = [gather(send) for send in n_own + dy_own]
        cos, sin = rope_tables(prefix_len, n_dev * local_len)
        prefix = [prefix_len[part(half, per_half)] for half in halves]
        starts = jnp.stack([rank * n_dist, shared_at + parity * n_shared, rank, pair]).astype(jnp.int32)
        bias = jnp.concatenate([
            lax.dynamic_slice_in_dim(b_qkv, starts[0] * WIDTH, n_dist * WIDTH),
            lax.dynamic_slice_in_dim(b_qkv, starts[1] * WIDTH, n_shared * WIDTH)]).astype(F32).reshape(1, -1)
        grad_bo = jnp.sum(grad_out.astype(F32), axis=(0, 1))
        n_chip_rows = [own[None] for own in n_own + [to_partner(own) for own in n_own]]
        qkv_own = project_qkv(starts, n_dist, n_shared, n_chip_rows, w_qkv, bias, cos, sin)
        d_ctx_own = context_grad(starts, n_dist, n_shared, [own[None] for own in (grad_out, to_partner(grad_out))], w_o, n_dev)
        n_a, grad_bo, *d_ctx_own = together(n_a, grad_bo, *d_ctx_own)

        ctx_d = ctx_r = None
        qkv, lses = [], []
        for half in halves:
            if half:
                n_b, ctx_r = together(n_b, ctx_r)
            qd, kd, vd, qr, kr, vr = project_qkv(
                starts, n_dist, n_shared, [n_b if half else n_a], w_qkv, bias, cos, sin, half, qkv_own[part(half, QKV_IN)])
            ctx_d, lse_d = attention_forward(half, prefix[half], qd, kd, vd, n_dev, ctx_d)
            qr, ctx_d = together(qr, ctx_d)
            ctx_r, lse_r = attention_forward(half, prefix[half], qr, kr, vr, n_dev, ctx_r)
            qkv.append((qd, kd, vd, qr, kr, vr))
            lses.append((lse_d, lse_r))
        ctx_par = gather_core(ctx_d.reshape(tokens, n_dist * HEAD))

        dy_a, ctx_r = together(dy_a, ctx_r)
        g_d, g_r = [], []
        sums = []
        for half in halves:
            if half:
                dy_b, *g_r = together(dy_b, *g_r)
            qd, kd, vd, qr, kr, vr = qkv[half]
            d_ctx, d_ctx_r = context_grad(starts, n_dist, n_shared, [dy_b if half else dy_a], w_o, n_dev, d_ctx_own[part(half, CORES)])
            *g_d, sum_d = attention_backward(half, 0, n_dist, prefix[half], qd, kd, vd, ctx_d, d_ctx, lses[half][0], cos, sin, g_d)
            qr, *g_d = together(qr, *g_d)
            new, sum_r = [], [sum_d]
            for first in range(0, n_shared, CORES):
                *g_pair, sum_pair = attention_backward(
                    half, first, CORES, prefix[half], qr, kr, vr, ctx_r, d_ctx_r, lses[half][1], cos, sin, g_r[part(first // CORES, CORES)])
                new += g_pair
                sum_r.append(sum_pair)
            g_r = new
            sums.append(jnp.sum(jnp.concatenate(sum_r), axis=(1, 2)).reshape(-1))
        g_par = [gather_core(g.reshape(tokens, WIDTH)) for g in g_d]
        g_r = [g.reshape(1, tokens, WIDTH) for g in g_r]

        n_a, n_b, dy_a, dy_b = [part.reshape(tokens // 2, hidden) for part in (n_a, n_b, dy_a, dy_b)]
        ctx_r = ctx_r.reshape(tokens, n_shared * HEAD)
        shared_recv = to_partner(token_rows(ctx_r, pair))
        ctx_r, *g_r = together(ctx_r, *g_r)
        grad_wo, wo_block = weight_grad_o(
            core, ctx_r[None], dy_a, dy_b, lambda c, par: (shared_at + par * n_shared) * HEAD, lambda c: 0, hidden // 2, ())
        shared_recv, wo_block, n_a = together(shared_recv, wo_block, n_a)
        grad_wqkv, block, r_send = weight_grad_qkv(core, shared_places, n_a, n_b, g_r, None)
        r_recv, ctx_recv = to_partner(r_send), to_partner(token_rows(ctx_par, pair))
        ctx_par, block = together(ctx_par, block)
        recv_r = to_partner(block)
        grad_wo, wo_block = weight_grad_o(
            core, ctx_par, dy_a, dy_b, lambda c, par: (2 * c + par) * (n_dist * HEAD), lambda c: (n_shared + c * n_dist) * HEAD,
            hidden // 2, (grad_wo, wo_block))
        ctx_tok = jnp.concatenate([token_rows(ctx_par, rank), ctx_recv])
        ctx_tok, wo_block, recv_r = together(ctx_tok, wo_block, recv_r)
        wo_recv = to_partner(wo_block)
        shared_tok = jnp.stack([token_rows(ctx_r, rank), shared_recv])
        hidden_out = project_out(core, ctx_tok, shared_tok, w_o, [own.reshape(-1, hidden) for own in n_own], b_o)
        n_a, hidden_out, g_par[0] = together(n_a, hidden_out, g_par[0])

        def columns(table):
            at = [np.array([h * WIDTH for h in table(par)] + [1 - par, 0], np.int32) for par in range(2)]
            last = (np.arange(at[0].size) == at[0].size - 1).astype(np.int32)
            return jnp.asarray(at[0]) + parity.astype(jnp.int32) * jnp.asarray(at[1] - at[0]) + rank.astype(jnp.int32) * jnp.asarray(last)

        def spread_grad(head, whole, **extra):
            whole, block, tok, *rest = weight_grad_qkv(core, places(head), n_a, n_b, [g_par[head]], whole, **extra)
            tok = to_partner(tok)
            if head:
                tok, block = together(tok, block)
            return whole, tok, to_partner(block), rest

        grad_wqkv, tok_0, recv_0, _ = spread_grad(0, grad_wqkv, recv=recv_r, old_places_of=shared_places)
        g_par[1], grad_wqkv = together(g_par[1], grad_wqkv)
        grad_wqkv, tok_1, recv_1, (grad_wo,) = spread_grad(1, grad_wqkv, wo=(wo_recv, grad_wo, wo_tile))
        cols = columns(lambda mine: [shared_at + par * n_shared + i for par in (mine, 1 - mine) for i in range(n_shared)] + [
            (2 * c + par) * n_dist + head for par in (mine, 1 - mine) for c in range(n_chip) for head in (0, 1)])
        runs = [(i, 0) for i in range(n_shared)] + [(n_shared, i) for i in range(n_shared)]
        runs += [(n_shared + 1 + CORES * side + head, c) for side in range(CORES) for c in range(n_chip) for head in (0, 1)]
        d_norm, grad_wqkv = normed_grad(
            cols, runs, [*g_r, r_recv, g_par[0], g_par[1], tok_0, tok_1], w_qkv, grad_out.reshape(rows, hidden), (recv_0, places(0), grad_wqkv))
        n_a, d_norm, g_par[2] = together(n_a, d_norm, g_par[2])
        grad_wqkv, tok_2, recv_2, _ = spread_grad(2, grad_wqkv, recv=recv_1, old_places_of=places(1))
        cols = columns(lambda mine: [(2 * c + par) * n_dist + 2 for c in range(n_chip) for par in (mine, 1 - mine)])
        grad_in, norm_sums = normed_grad(
            cols, [(src, c) for c in range(n_chip) for src in range(2)], [g_par[2], tok_2], w_qkv, d_norm, norm=(x_flat, gain))
        small = gather(jnp.concatenate([sums[0] + sums[1]] + [norm_sums.reshape(-1), grad_bo]))
        recv_2, small = together(recv_2, small)
        grad_wqkv = paste_columns(core, places(2), recv_2, grad_wqkv)
        spread, shared = small[:, :n_dist * WIDTH], small[:2, n_dist * WIDTH:(n_dist + n_shared) * WIDTH]
        grad_bqkv = jnp.concatenate([spread.reshape(-1), shared.reshape(-1)])
        grad_gamma, grad_beta, grad_bo = jnp.sum(small[:, (n_dist + n_shared) * WIDTH:], axis=0).reshape(3, hidden)
        shape = (batch, local_len, hidden)
        return (hidden_out.reshape(shape), grad_in.reshape(shape), grad_gamma, grad_beta, grad_wqkv, grad_bqkv, grad_wo, grad_bo)

    return jax.shard_map(device_step, mesh=mesh, in_specs=in_specs, out_specs=out_specs, check_vma=False)
```

```python
import functools
import math
import jax
import jax.numpy as jnp
import numpy as np
from jax import lax
from jax.experimental import pallas as pl
from jax.experimental.pallas import tpu as pltpu
from jax.sharding import PartitionSpec as P

HEAD = 128
QUARTER = 32
ALPHA = math.sqrt(56.0)
LN_EPS = 1e-5
ROT_BASE = 10000.0
SCALE = 1.0 / math.sqrt(HEAD)
LOG2E = math.log2(math.e)
MASK_FILL = -1e30
BLK = 256
VMEM_BIG = pltpu.CompilerParams(vmem_limit_bytes=62 << 20)
SHARED = 8
Z = 0
SLOTS = CORES = 2
WIDTH = 3 * HEAD
F32 = jnp.float32
BF16 = jnp.bfloat16


def dot(lhs, rhs, lhs_dim, rhs_dim):
    return lax.dot_general(lhs, rhs, (((lhs_dim,), (rhs_dim,)), ((), ())), preferred_element_type=F32)


def dot_nn(lhs, rhs):
    return dot(lhs, rhs, 1, 0)


def dot_nt(lhs, rhs):
    return dot(lhs, rhs, 1, 1)


def dot_tn(lhs, rhs):
    return dot(lhs, rhs, 0, 0)


def matmul_cost(rows, depth, cols, extra=0):
    return pl.CostEstimate(
        flops=2 * rows * depth * cols, bytes_accessed=2 * (rows * depth + depth * cols + rows * cols) + extra, transcendentals=0)


def attention_cost(n_head, batch, seq, products):
    pairs = n_head * batch * seq * seq
    return pl.CostEstimate(flops=2 * products * pairs * HEAD, bytes_accessed=8 * products * n_head * batch * seq * HEAD, transcendentals=pairs)


def run(index, size):
    return pl.ds(pl.multiple_of(index * size, size), size)


def part(index, size):
    return slice(index * size, (index + 1) * size)


def rope_tables(prefix_len, seq):
    tok = jnp.arange(seq, dtype=jnp.int32)[None, :]
    pre = prefix_len[:, None]
    inside = tok < pre
    pos = jnp.where(inside, tok, pre - 1)
    blk = jnp.where(inside, 0, tok - pre + 1)
    inv_freq = ROT_BASE ** (-jnp.arange(QUARTER, dtype=F32) / QUARTER)
    angles = jnp.stack([pos, blk], axis=-1).astype(F32)[..., None] * inv_freq
    cos, sin = jnp.cos(angles), jnp.sin(angles)
    shape = pos.shape + (HEAD,)
    return (jnp.stack([cos, cos], axis=-2).reshape(shape), jnp.stack([-sin, sin], axis=-2).reshape(shape))


def turn(x, cos, sin):
    lane = lax.broadcasted_iota(jnp.int32, x.shape, 1)
    other = jnp.where(lane % (2 * QUARTER) < QUARTER, pltpu.roll(x, HEAD - QUARTER, 1), pltpu.roll(x, QUARTER, 1))
    return x * cos + other * sin


def dma_sems(*shape):
    return pltpu.SemaphoreType.DMA(shape)


def dma_sems(*shape):
    return pltpu.SemaphoreType.DMA(shape)


def start_all(copies):
    for copy in copies:
        copy.start()


def wait_all(copies):
    for copy in copies:
        copy.wait()


ANY = pl.BlockSpec(memory_space=pl.ANY)
PIECES = 4
QKV_IN = 6


NORM_ROWS = 32


def centred(x):
    x = x.astype(F32)
    x = x - jnp.mean(x, axis=-1, keepdims=True)
    return x, lax.rsqrt(jnp.mean(x * x, axis=-1, keepdims=True) + LN_EPS)


def norm_kernel(x_ref, gain_ref, shift_ref, out_ref):
    gain, shift = gain_ref[...].astype(F32), shift_ref[...].astype(F32)

    @pl.loop(0, x_ref.shape[0] // NORM_ROWS)
    def _(i):
        rows = run(i, NORM_ROWS)
        x, inv = centred(x_ref[rows])
        out_ref[rows] = (x * inv * gain + shift).astype(BF16)


def normalize(half, x, gain, shift):
    rows, hidden = x.shape
    block = rows // 4
    vec = pl.BlockSpec((1, hidden), lambda i: (Z, Z))
    return pl.pallas_call(
        norm_kernel,
        grid=(2,),
        in_specs=[pl.BlockSpec((block, hidden), lambda i: (2 * half + i, Z)), vec, vec],
        out_specs=pl.BlockSpec((block, hidden), lambda i: (i, Z)),
        out_shape=jax.ShapeDtypeStruct((2 * block, hidden), BF16),
        compiler_params=VMEM_BIG,
        name='norm',
    )(x, gain, shift)


def qkv_kernel(n_dist, n_tile, n_in, start_ref, *rest):
    n_refs, (w_ref, b_ref, cos_ref, sin_ref, *outs), (w_buf, acc, sems) = rest[:n_in], rest[n_in:-3], rest[-3:]
    first, later = n_refs[:(n_in + 1) // CORES], n_refs[n_in // CORES:]
    _, rows, cols = acc.shape
    hidden = w_ref.shape[0]
    dist = n_dist * WIDTH
    step, last = pl.program_id(Z), pl.num_programs(Z) - 1
    slot = lax.rem(step, SLOTS)
    piece = hidden // PIECES
    tile = first[0].shape[-2]

    def loads(i):
        span = run(i, piece)
        for kind, (at, width) in enumerate(((0, dist), (dist, cols - dist))):
            col = pl.multiple_of(start_ref[kind] * WIDTH, HEAD)
            yield pltpu.make_async_copy(w_ref.at[span, pl.ds(col, width)], w_buf.at[span, pl.ds(at, width)], sems.at[i, kind])

    def finish():
        for i in range(rows // tile):
            group, batch, at, table = n_tile(i)
            cos, sin = cos_ref[table, part(at, tile)], sin_ref[table, part(at, tile)]
            for h in range(cols // WIDTH):
                kind, head = (0, h) if h < n_dist else (1, h - n_dist)
                refs = outs[part(CORES * group + kind, 3)]
                pre = [acc[1 - slot, part(i, tile), part(3 * h + j, HEAD)] + b_ref[:, part(3 * h + j, HEAD)] for j in range(3)]
                for ref, val in zip(refs, (turn(pre[0], cos, sin), turn(pre[1], cos, sin), pre[2])):
                    ref[head, batch, part(at, tile)] = val.astype(BF16)

    @pl.when(step == Z)
    def _():
        for i in range(PIECES):
            start_all(loads(i))
        acc[slot] = jnp.zeros((rows, cols), F32)

        @pl.loop(0, PIECES)
        def _(i):
            wait_all(loads(i))
            span = run(i, piece)
            for i, ref in enumerate(first):
                acc[slot, part(i, rows // len(first))] += dot_nn(ref[:, :, :, span].reshape(-1, piece), w_buf[span])

    @pl.when(jnp.logical_and(step > 0, step < last))
    def _():
        finish()
        for i, ref in enumerate(later):
            acc[slot, part(i, rows // len(later))] = dot_nn(ref[...].reshape(-1, hidden), w_buf[...])

    pl.when(step == last)(finish)


def project_qkv(starts, n_dist, n_shared, n_rows, w_qkv, bias, cos, sin, half=None, earlier=None):
    _, per_half, local_len, hidden = n_rows[0].shape
    _, seq, _ = cos.shape
    cols = (n_dist + n_shared) * WIDTH
    own = earlier is None
    batch = per_half * CORES if own else per_half
    steps = CORES if own else seq // local_len // CORES - 1
    n_chip = seq // local_len // CORES
    width = local_len if own else CORES * local_len

    def place(step, at):
        return at[CORES + step] if own else lax.rem(at[CORES] // CORES + 1 + step, n_chip)

    def ahead(step, at):
        return place(jnp.minimum(step, steps - 1), at)

    def behind(step, at):
        return place(jnp.maximum(step - 1, 0), at)

    shapes = [jax.ShapeDtypeStruct((n_head, per_half, seq, HEAD), BF16) for n_head in (n_dist, n_shared) for _ in range(3)]
    shapes = shapes * CORES if own else shapes
    tab_spec = pl.BlockSpec((batch, width, HEAD), lambda step, at: (Z if own else half, behind(step, at), Z))
    arrays = [] if own else list(earlier)

    def own_tile(i):
        return i // per_half, i % per_half, 0, i

    def other_tile(i):
        return 0, i % per_half, i // per_half, i % per_half

    return pl.pallas_call(
        functools.partial(without, len(arrays), len(n_rows) + 5, functools.partial(qkv_kernel, n_dist, own_tile if own else other_tile, len(n_rows))),
        grid_spec=pltpu.PrefetchScalarGridSpec(
            num_scalar_prefetch=1,
            grid=(steps + 1,),
            in_specs=[
                *[pl.BlockSpec((1 if own else CORES, per_half, local_len, hidden), lambda step, at: (Z if own else ahead(step, at), Z, Z, Z))] * len(n_rows),
                ANY,
                pl.BlockSpec((1, cols), lambda step, at: (Z, Z)),
                tab_spec, tab_spec,
            ] + [ANY] * len(arrays),
            out_specs=[pl.BlockSpec(shape.shape[:CORES] + (width, HEAD), lambda step, at: (Z, Z, behind(step, at), Z)) for shape in shapes],
            scratch_shapes=[
                pltpu.VMEM((hidden, cols), BF16), pltpu.VMEM((SLOTS, CORES * CORES * local_len, cols), F32), dma_sems(PIECES, SLOTS)],
        ),
        out_shape=shapes,
        input_output_aliases={QKV_IN + i: i for i in range(len(arrays))},
        compiler_params=VMEM_BIG,
        cost_estimate=matmul_cost(steps * CORES * batch * local_len, hidden, cols),
        name='qkv',
    )(starts, *n_rows, w_qkv, bias, cos, sin, *arrays)


def without(count, start, kernel, *refs):
    kernel(*refs[:start], *refs[start + count:])


def forward_kernel(pre_ref, q_ref, k_ref, v_ref, *rest):
    ctx_ref, lse_ref = rest[-2:]
    n_head, _, seq, _ = q_ref.shape
    local_len = ctx_ref.shape[3]
    per = BLK // local_len
    prefix = pre_ref[pl.program_id(1)]

    def block(r, n_key):
        query = lax.broadcasted_iota(jnp.int32, (1, BLK), 1) + r * BLK
        last = jnp.maximum(query, prefix - 1) - (n_key - 1) * BLK
        scores = []
        for h in range(n_head):
            q_blk = q_ref[h, 0, part(r, BLK)]
            parts = [dot_nt(k_ref[h, 0, part(c, BLK)], q_blk) * (SCALE * LOG2E) for c in range(n_key)]
            key = lax.broadcasted_iota(jnp.int32, (BLK, BLK), 0)
            parts[-1] = jnp.where(key <= last, parts[-1], MASK_FILL)
            scores.append(parts)
        for h, parts in enumerate(scores):
            top = functools.reduce(jnp.maximum, [jnp.max(p, axis=0, keepdims=True) for p in parts])
            parts = [jnp.exp2(p - top) for p in parts]
            total = functools.reduce(jnp.add, [jnp.sum(p, axis=0, keepdims=True) for p in parts])
            inv = 1.0 / total
            probs = jnp.concatenate([(p * inv).astype(BF16) for p in parts], axis=0)
            ctx_t = dot_tn(v_ref[h, 0, :n_key * BLK], probs)
            ctx = ctx_t.T.astype(BF16).reshape(per, local_len, HEAD)
            ctx_ref[0, part(r, per), 0, :, part(h, HEAD)] = ctx
            lse_ref[h, 0, :, part(r, BLK)] = top + jnp.log2(total)

    n_blk = seq // BLK
    for r in range(n_blk):
        for n_key in range(r + 1, n_blk + 1):
            low = (n_key - 1) * BLK
            cond = prefix <= n_key * BLK if n_key == r + 1 else prefix > low
            if n_key < n_blk and n_key > r + 1:
                cond = jnp.logical_and(cond, prefix <= n_key * BLK)
            if n_key == n_blk and n_key == r + 1:
                block(r, n_key)
            else:
                pl.when(cond)(functools.partial(block, r, n_key))


def attention_forward(half, prefix_half, q, k, v, n_dev, ctx):
    own, batch, seq, _ = q.shape
    local_len = seq // n_dev
    group = own
    qkv_spec = pl.BlockSpec((group, 1, seq, HEAD), lambda h, b, pre: (h, b, Z, Z))
    earlier = [] if ctx is None else [ctx]
    return pl.pallas_call(
        forward_kernel,
        grid_spec=pltpu.PrefetchScalarGridSpec(
            num_scalar_prefetch=1,
            grid=(own // group, batch),
            in_specs=[qkv_spec] * 3 + [ANY] * len(earlier),
            out_specs=[
                pl.BlockSpec((1, n_dev, 1, local_len, group * HEAD), lambda h, b, pre: (half, Z, b, Z, h)),
                pl.BlockSpec((group, 1, 1, seq), lambda h, b, pre: (h, b, Z, Z)),
            ],
        ),
        out_shape=[
            jax.ShapeDtypeStruct((2, n_dev, batch, local_len, own * HEAD), BF16),
            jax.ShapeDtypeStruct((own, batch, 1, seq), F32),
        ],
        input_output_aliases={4: 0} if earlier else {},
        compiler_params=VMEM_BIG,
        cost_estimate=attention_cost(own, batch, seq, 2),
        name='attn_fwd',
    )(prefix_half, q, k, v, *earlier)


def d_ctx_kernel(n_in, start_ref, *rest):
    dy_refs, (w_ref, *outs), (w_buf, sems) = rest[:n_in], rest[n_in:-2], rest[-2:]
    step, hidden = pl.program_id(Z), w_ref.shape[1]
    widths = [outs[0].shape[-1], outs[1].shape[-1]]

    def loads():
        for kind, (at, width) in enumerate(zip((0, widths[0]), widths)):
            row = pl.multiple_of(start_ref[kind] * HEAD, HEAD)
            yield pltpu.make_async_copy(w_ref.at[pl.ds(row, width)], w_buf.at[pl.ds(at, width)], sems.at[kind])

    @pl.when(step == Z)
    def _():
        start_all(loads())
        wait_all(loads())

    def multiply(dy_ref):
        res = dot_nt(dy_ref[...].reshape(-1, hidden), w_buf[...]).astype(BF16)
        rows = CORES * res.shape[0] // len(outs)
        for i, out_ref in enumerate(outs):
            cols = slice(widths[0], None) if i % CORES else slice(widths[0])
            out_ref[...] = res[part(i // CORES, rows), cols].reshape(out_ref.shape)

    if n_in > 1:
        for i, dy_ref in enumerate(dy_refs):
            pl.when(step == i)(functools.partial(multiply, dy_ref))
    else:
        multiply(dy_refs[0])


def context_grad(starts, n_dist, n_shared, dy_rows, w_o, n_dev, earlier=()):
    _, batch, local_len, hidden = dy_rows[0].shape
    own = not earlier
    n_chip = n_dev // CORES
    per_half, devs = (batch // CORES, 1) if own else (batch, CORES)

    def block(step, at):
        return (at[CORES + step] if own else lax.rem(at[CORES] // CORES + 1 + step, n_chip), Z, Z, Z)

    cols = [n_dist * HEAD, n_shared * HEAD]
    outs = cols * (CORES if own else 1)
    n_in = len(dy_rows)
    return pl.pallas_call(
        functools.partial(without, len(earlier), n_in + 2, functools.partial(d_ctx_kernel, n_in)),
        grid_spec=pltpu.PrefetchScalarGridSpec(
            num_scalar_prefetch=1,
            grid=(CORES if own else n_chip - 1,),
            in_specs=[pl.BlockSpec((devs, batch, local_len, hidden), (lambda step, at: (Z, Z, Z, Z)) if own else block)] * n_in + [ANY] * (1 + len(earlier)),
            out_specs=[pl.BlockSpec((devs, per_half, local_len, width), block) for width in outs],
            scratch_shapes=[pltpu.VMEM((sum(cols), hidden), BF16), dma_sems(CORES)],
        ),
        out_shape=[jax.ShapeDtypeStruct((n_dev, per_half, local_len, width), BF16) for width in outs],
        input_output_aliases={3 + i: i for i in range(len(earlier))},
        compiler_params=VMEM_BIG,
        cost_estimate=matmul_cost(n_dev * batch * local_len, hidden, sum(cols)),
        name='dctx',
    )(starts, *dy_rows, w_o, *earlier)


def backward_kernel(pre_ref, q_ref, k_ref, v_ref, ctx_ref, dctx_ref, lse_ref, cos_ref, sin_ref, *rest):
    sum_ref, dq_acc, dk_acc, dv_acc = rest[-4:]
    n_head, _, seq, _ = q_ref.shape
    g_refs = rest[-4 - n_head:-4]
    _, n_dev, _, local_len, _ = g_refs[0].shape
    n_blk = seq // BLK
    prefix = pre_ref[pl.program_id(Z)]
    d_ctx, delta = [], []
    for h in range(n_head):
        lanes = part(h, HEAD)
        grad = dctx_ref[:, :, :, lanes].reshape(seq, HEAD)
        prod = grad.astype(F32) * ctx_ref[0, :, :, :, lanes].reshape(seq, HEAD).astype(F32)
        d_ctx.append(grad)
        delta.append(jnp.sum(prod.T, axis=0, keepdims=True))

    def block(c, first):
        span = part(c, BLK)
        start = first * BLK
        products = []
        for h in range(n_head):
            s_t = dot_nt(k_ref[h, 0, span], q_ref[h, 0, start:])
            dp_t = dot_nt(v_ref[h, 0, span], d_ctx[h][start:])
            products.append((s_t, dp_t))
        for h, (s_t, dp_t) in enumerate(products):
            probs, d_scores = [], []
            for r in range(first, n_blk):
                cols, here = part(r, BLK), part(r - first, BLK)
                piece = s_t[:, here] * (SCALE * LOG2E)
                if r <= c:
                    key = lax.broadcasted_iota(jnp.int32, (BLK, BLK), 0)
                    query = lax.broadcasted_iota(jnp.int32, (1, BLK), 1) + r * BLK
                    piece = jnp.where(key <= jnp.maximum(query, prefix - 1) - c * BLK, piece, MASK_FILL)
                p = jnp.exp2(piece - lse_ref[h, 0, :, cols])
                probs.append(p.astype(BF16))
                d_scores.append((p * (dp_t[:, here] - delta[h][:, cols]) * SCALE).astype(BF16))
            probs = jnp.concatenate(probs, axis=1)
            d_scores = jnp.concatenate(d_scores, axis=1)
            dv_acc[h, span] = dot_nn(probs, d_ctx[h][start:])
            dk_acc[h, span] = dot_nn(d_scores, q_ref[h, 0, start:])
            dq_part = dot_tn(k_ref[h, 0, span], d_scores)
            if c:
                dq_acc[h, :, start:] += dq_part
            else:
                dq_acc[h] = dq_part

    block(0, 0)
    for c in range(1, n_blk):
        pl.when(prefix > c * BLK)(functools.partial(block, c, 0))
        pl.when(prefix <= c * BLK)(functools.partial(block, c, c))

    cos, sin = cos_ref[Z], sin_ref[Z]
    for h in range(n_head):
        g_q = turn(dq_acc[h].T.astype(BF16).astype(F32), cos, -sin)
        g_k = turn(dk_acc[h].astype(BF16).astype(F32), cos, -sin)
        g_v = dv_acc[h].astype(BF16).astype(F32)
        for i, g in enumerate((g_q, g_k, g_v)):
            lanes = part(i, HEAD)
            g_refs[h][0, :, 0, :, lanes] = g.astype(BF16).reshape(n_dev, local_len, HEAD)
            sum_ref[h, 0, :, lanes] = jnp.sum(g, axis=0, keepdims=True)


def attention_backward(half, group, prefix_half, q, k, v, ctx, d_ctx, lse, cos, sin, earlier):
    _, batch, seq, _ = q.shape
    _, n_dev, _, local_len, _ = ctx.shape
    qkv_spec = pl.BlockSpec((group, 1, seq, HEAD), lambda b, pre: (Z, b, Z, Z))
    tab_spec = pl.BlockSpec((1, seq, HEAD), lambda b, pre: (half * batch + b, Z, Z))
    stat = functools.partial(pltpu.VMEM, dtype=F32)
    return pl.pallas_call(
        backward_kernel,
        grid_spec=pltpu.PrefetchScalarGridSpec(
            num_scalar_prefetch=1,
            grid=(batch,),
            in_specs=[qkv_spec] * 3 + [
                pl.BlockSpec((1, n_dev, 1, local_len, group * HEAD), lambda b, pre: (half, Z, b, Z, Z)),
                pl.BlockSpec((n_dev, 1, local_len, group * HEAD), lambda b, pre: (Z, b, Z, Z)),
                pl.BlockSpec((group, 1, 1, seq), lambda b, pre: (Z, b, Z, Z)), tab_spec, tab_spec] + [ANY] * len(earlier),
            out_specs=[pl.BlockSpec((1, n_dev, 1, local_len, WIDTH), lambda b, pre: (half, Z, b, Z, Z))] * group + [
                pl.BlockSpec((group, 1, 1, WIDTH), lambda b, pre: (Z, b, Z, Z))],
            scratch_shapes=[stat((group, HEAD, seq)), stat((group, seq, HEAD)), stat((group, seq, HEAD))],
        ),
        out_shape=[jax.ShapeDtypeStruct((2, n_dev, batch, local_len, WIDTH), BF16)] * group + [
            jax.ShapeDtypeStruct((group, batch, 1, WIDTH), F32)],
        input_output_aliases={9 + i: i for i in range(len(earlier))},
        compiler_params=VMEM_BIG,
        cost_estimate=attention_cost(group, batch, seq, 5),
        name='attn_bwd',
    )(prefix_half, q, k, v, ctx, d_ctx, lse, cos, sin, *earlier)


def wo_grad_kernel(row_of, block_row_of, core_ref, ctx_ref, dya_ref, dyb_ref, *rest):
    out_ref, copy_ref, rhs, buf, rhs_sems, sems = rest[-6:]
    n, c = pl.program_id(Z), pl.program_id(1)
    n_col, n_grp = pl.num_programs(Z), pl.num_programs(1)
    step = n * n_grp + c
    slot, n_slot = lax.rem(step, SLOTS), lax.rem(n, SLOTS)
    _, rows, wide = buf.shape
    half = dya_ref.shape[0]
    core = core_ref[Z]

    def loads(n_at, at):
        for i, ref in enumerate((dya_ref, dyb_ref)):
            yield pltpu.make_async_copy(ref.at[:, run(n_at, wide)], rhs.at[at, run(i, half)], rhs_sems.at[at, i])

    def stores(at_step, at):
        n_at, c_at = at_step // n_grp, lax.rem(at_step, n_grp)
        for i, (ref, row) in enumerate(((out_ref, row_of(c_at, core)), (copy_ref, block_row_of(c_at)))):
            yield pltpu.make_async_copy(buf.at[at], ref.at[pl.ds(pl.multiple_of(row, HEAD), rows), run(n_at, wide)], sems.at[at, i])

    @pl.when(step == Z)
    def _():
        start_all(loads(0, 0))

    @pl.when(c == Z)
    def _():
        @pl.when(n + 1 < n_col)
        def _():
            start_all(loads(n + 1, 1 - n_slot))

        wait_all(loads(n, n_slot))

    @pl.when(step >= 2)
    def _():
        wait_all(stores(step - 2, slot))

    buf[slot] = dot_tn(ctx_ref[Z], rhs[n_slot])
    start_all(stores(step, slot))

    @pl.when(step == n_col * n_grp - 1)
    def _():
        wait_all(stores(step - 1, 1 - slot))
        wait_all(stores(step, slot))


def weight_grad_o(core, ctx_par, dy_a, dy_b, row_of, block_row_of, block_rows, earlier):
    n_grp, tokens, cols = ctx_par.shape
    hidden = dy_a.shape[1]
    wide = hidden // 4
    return pl.pallas_call(
        functools.partial(wo_grad_kernel, row_of, block_row_of),
        grid_spec=pltpu.PrefetchScalarGridSpec(
            num_scalar_prefetch=1,
            grid=(hidden // wide, n_grp),
            in_specs=[pl.BlockSpec((1, tokens, cols), lambda n, c, core: (c, Z, Z)), ANY, ANY] + [ANY] * len(earlier),
            out_specs=[ANY, ANY],
            scratch_shapes=[pltpu.VMEM((SLOTS, tokens, wide), BF16), pltpu.VMEM((SLOTS, cols, wide), F32), dma_sems(SLOTS, SLOTS), dma_sems(SLOTS, SLOTS)],
        ),
        out_shape=[jax.ShapeDtypeStruct((hidden, hidden), F32), jax.ShapeDtypeStruct((block_rows, hidden), F32)],
        input_output_aliases={4: 0, 5: 1} if earlier else {},
        compiler_params=VMEM_BIG,
        cost_estimate=matmul_cost(n_grp * cols, tokens, hidden, 8 * hidden * n_grp * cols),
        name='wo_grad',
    )(core, ctx_par, dy_a, dy_b, *earlier)


def column_copies(src, out_ref, sem_of, row, places):
    rows, width = src.shape[0], src.shape[1] // len(places)
    for i, col in enumerate(places):
        yield pltpu.make_async_copy(
            src.at[:, run(i, width)],
            out_ref.at[pl.ds(pl.multiple_of(row, BLK), rows), pl.ds(pl.multiple_of(col, HEAD), width)],
            sem_of(i))


def wqkv_grad_kernel(places_of, old_places, wo_tile, n_src, core_ref, na_ref, nb_ref, *rest):
    srcs, rest = rest[:n_src], list(rest[n_src:])
    groups = [ref.at[c] for ref in srcs for c in range(ref.shape[0])]
    recv_refs = [rest.pop(0) for _ in old_places]
    wo_recv_ref = rest.pop(0) if wo_tile else None
    n_buf, rhs, buf, n_sems, g_sems, out_sems, copy_sems, paste_sems, wo_sems, tok_sems = rest[-10:]
    outs = rest[:-10][-4 if wo_tile else -3:]
    out_ref, copy_ref, tok_ref = outs[:3]
    m = pl.program_id(Z)
    n_m = pl.num_programs(Z)
    core, pair = core_ref[Z], core_ref[1]
    tokens, cols = groups[0].shape
    half, rows = tokens // 2, n_buf.shape[2]
    piece = tokens // PIECES
    slot = lax.rem(m, SLOTS)

    def n_loads(step, at):
        for i, ref in enumerate((na_ref, nb_ref)):
            yield pltpu.make_async_copy(ref.at[:, run(step, rows)], n_buf.at[at, run(i, half)], n_sems.at[at, i])

    def g_loads(i):
        for c, ref in enumerate(groups):
            yield pltpu.make_async_copy(ref.at[run(i, piece)], rhs.at[run(i, piece), run(c, cols)], g_sems.at[i, c])

    def stores(step, at):
        yield from column_copies(buf.at[at], out_ref, lambda i: out_sems.at[at, i], step * rows, places_of(core))
        yield pltpu.make_async_copy(buf.at[at], copy_ref.at[run(step, rows)], copy_sems.at[at])

    def pastes():
        for at, (recv_ref, old_places_of) in enumerate(zip(recv_refs, old_places)):
            yield from column_copies(recv_ref, out_ref, lambda i: paste_sems.at[at, i], m * rows, old_places_of(1 - core))
        if wo_tile:
            tiles = wo_recv_ref.shape[0] // HEAD
            for t in range(tiles):
                tile = wo_tile(m * tiles + t, 1 - core)
                yield pltpu.make_async_copy(wo_recv_ref.at[run(t, HEAD)], outs[3].at[run(tile, HEAD)], wo_sems.at[t])

    def token_copies():
        size = tok_ref.shape[0] // 2
        for i in range(2):
            yield pltpu.make_async_copy(rhs.at[pl.ds(pl.multiple_of(i * half + pair * size, BLK), size)], tok_ref.at[run(i, size)], tok_sems.at[i])

    @pl.when(m == Z)
    def _():
        start_all(n_loads(0, 0))
        for i in range(PIECES):
            start_all(g_loads(i))

    @pl.when(m + 1 < n_m)
    def _():
        start_all(n_loads(m + 1, 1 - slot))

    start_all(pastes())

    @pl.when(m >= 2)
    def _():
        wait_all(stores(m - 2, slot))

    wait_all(n_loads(m, slot))

    @pl.when(m == Z)
    def _():
        buf[slot] = jnp.zeros((rows, rhs.shape[1]), F32)

        @pl.loop(0, PIECES)
        def _(i):
            wait_all(g_loads(i))
            buf[slot] += dot_tn(n_buf[slot, run(i, piece)], rhs[run(i, piece)])

        start_all(token_copies())

    @pl.when(m > 0)
    def _():
        buf[slot] = dot_tn(n_buf[slot], rhs[...])

    start_all(stores(m, slot))
    wait_all(pastes())

    @pl.when(m == n_m - 1)
    def _():
        wait_all(stores(m - 1, 1 - slot))
        wait_all(stores(m, slot))
        wait_all(token_copies())


def weight_grad_qkv(core, places_of, n_a, n_b, srcs, whole, pastes=(), wo=None):
    hidden = n_a.shape[1]
    n_grp, (tokens, cols) = sum(src.shape[0] for src in srcs), srcs[0].shape[1:]
    width = n_grp * cols
    rows = 2 * BLK
    steps = hidden // rows
    args, specs, alias = [core, n_a, n_b, *srcs], [ANY] * (2 + len(srcs)), {}
    outs = [jax.ShapeDtypeStruct((hidden, 3 * hidden), F32), jax.ShapeDtypeStruct((hidden, width), F32), jax.ShapeDtypeStruct((2 * BLK, width), BF16)]
    wo_tile = None
    for recv, _ in pastes:
        args.append(recv)
        specs.append(pl.BlockSpec((rows, width), lambda m, core: (m, Z)))
    if wo is not None:
        wo_recv, wo_whole, wo_tile = wo
        args.append(wo_recv)
        specs.append(pl.BlockSpec((wo_recv.shape[0] // steps, hidden), lambda m, core: (m, Z)))
        outs.append(jax.ShapeDtypeStruct(wo_whole.shape, F32))
    if whole is not None:
        alias[len(args)] = 0
        args.append(whole)
        specs.append(ANY)
    if wo is not None:
        alias[len(args)] = 3
        args.append(wo_whole)
        specs.append(ANY)
    return pl.pallas_call(
        functools.partial(wqkv_grad_kernel, places_of, [old for _, old in pastes], wo_tile, len(srcs)),
        grid_spec=pltpu.PrefetchScalarGridSpec(
            num_scalar_prefetch=1,
            grid=(steps,),
            in_specs=specs,
            out_specs=[ANY] * len(outs),
            scratch_shapes=[
                pltpu.VMEM((SLOTS, tokens, rows), BF16),
                pltpu.VMEM((tokens, width), BF16),
                pltpu.VMEM((SLOTS, rows, width), F32),
                dma_sems(SLOTS, SLOTS), dma_sems(PIECES, n_grp), dma_sems(SLOTS, n_grp), dma_sems(SLOTS), dma_sems(SLOTS, n_grp), dma_sems(4), dma_sems(SLOTS),
            ],
        ),
        out_shape=outs,
        input_output_aliases=alias,
        compiler_params=VMEM_BIG,
        cost_estimate=matmul_cost(hidden, tokens, width, 16 * hidden * width),
        name='wqkv_grad',
    )(*args)


def normed_grad_kernel(runs, n_src, final, cols_ref, *rest):
    srcs, (w_ref, init_ref, *rest) = rest[:n_src], rest[n_src:]
    if final:
        x_ref, gain_ref, dx_ref, sum_ref, acc, w_buf, g_buf, sems, g_sems, init_sem, sum_acc = rest
    else:
        acc, w_buf, g_buf, sems, g_sems = rest
    j, steps = pl.program_id(Z), pl.num_programs(Z)
    slot = lax.rem(j, SLOTS)
    rows, width = g_buf.shape[1], g_buf.shape[2] // 2
    rank = cols_ref[2 * steps]

    def w_loads(step, at):
        for i in range(2):
            col = pl.multiple_of(cols_ref[2 * step + i], HEAD)
            yield pltpu.make_async_copy(w_ref.at[:, pl.ds(col, width)], w_buf.at[at, :, run(i, width)], sems.at[at, i])

    def g_loads(step):
        at = step % 2
        for i, (src, grp) in enumerate(runs[part(step, 2)]):
            ref, dst = srcs[src], g_buf.at[at, :, run(i, width)]
            tokens = ref.shape[-2]
            ref = ref.at[:, run(grp, width)] if tokens == rows else ref.at[grp]
            pairs = [(ref, dst)] if tokens == rows else [
                (ref.at[pl.ds(pl.multiple_of(h * (tokens // 2) + rank * (rows // 2), BLK), rows // 2)], dst.at[run(h, rows // 2)]) for h in range(2)]
            for pair in pairs:
                yield pltpu.make_async_copy(*pair, g_sems.at[at, i])

    def g_waits(at):
        for i in range(2):
            block = g_buf.at[at, :, run(i, width)]
            yield pltpu.make_async_copy(block, block, g_sems.at[at, i])

    @pl.when(j == Z)
    def _():
        start_all(w_loads(0, 0))
        start_all(g_loads(0))
        if final:
            init = pltpu.make_async_copy(init_ref, acc, init_sem)
            init.start()
            init.wait()
        else:
            acc[...] = init_ref[...].astype(F32) * ALPHA

    @pl.when(j + 1 < steps)
    def _():
        start_all(w_loads(j + 1, 1 - slot))

    for step in range(1, len(runs) // 2):
        @pl.when(j + 1 == step)
        def _():
            start_all(g_loads(step))

    wait_all(w_loads(j, slot))
    wait_all(g_waits(slot))
    acc[...] += dot_nt(g_buf[slot], w_buf[slot])

    if final:
        @pl.when(j == steps - 1)
        def _():
            sum_acc[...] = jnp.zeros_like(sum_acc)
            gain = gain_ref[...].astype(F32)

            @pl.loop(0, rows // NORM_ROWS)
            def _(i):
                at = run(i, NORM_ROWS)
                d_n = acc[at]
                x, inv = centred(x_ref[at])
                x = x * inv
                d_x = d_n * gain
                mean = jnp.mean(d_x, axis=-1, keepdims=True)
                slope = jnp.mean(d_x * x, axis=-1, keepdims=True)
                dx_ref[at] = (inv * (d_x - mean - x * slope)).astype(BF16)
                for kind, term in enumerate((d_n * x, d_n)):
                    sum_acc[kind] += jnp.sum(term.reshape((-1,) + sum_acc.shape[1:]), axis=0)

            sum_ref[...] = jnp.sum(sum_acc[...], axis=1)


def normed_grad(cols, runs, srcs, w_qkv, init, norm=None):
    rows, hidden = init.shape
    steps, width = len(runs) // 2, 2 * WIDTH
    flat = pl.BlockSpec((rows, hidden), lambda j, cols: (Z, Z))
    args = [cols, *srcs, w_qkv, init]
    specs = [ANY] * (len(srcs) + 1) + [ANY if norm else flat]
    scratch = [pltpu.VMEM((SLOTS, hidden, width), BF16), pltpu.VMEM((SLOTS, rows, width), BF16), dma_sems(SLOTS, SLOTS), dma_sems(SLOTS, SLOTS)]
    if norm:
        args += list(norm)
        specs += [flat, pl.BlockSpec((1, hidden), lambda j, cols: (Z, Z))]
        outs = [jax.ShapeDtypeStruct((rows, hidden), BF16), jax.ShapeDtypeStruct((2, hidden), F32)]
        out_specs = [flat, pl.BlockSpec((2, hidden), lambda j, cols: (Z, Z))]
        scratch = [pltpu.VMEM((rows, hidden), F32)] + scratch + [pltpu.SemaphoreType.DMA, pltpu.VMEM((2, 8, hidden), F32)]
    else:
        outs, out_specs = [jax.ShapeDtypeStruct((rows, hidden), F32)], [flat]
    return pl.pallas_call(
        functools.partial(normed_grad_kernel, runs, len(srcs), norm is not None),
        grid_spec=pltpu.PrefetchScalarGridSpec(
            num_scalar_prefetch=1,
            grid=(steps,),
            in_specs=specs,
            out_specs=out_specs,
            scratch_shapes=scratch,
        ),
        out_shape=outs,
        compiler_params=VMEM_BIG,
        cost_estimate=matmul_cost(rows, steps * width, hidden),
        name='dn',
    )(*args)


def paste_kernel(places_of, core_ref, recv_ref, _, out_ref, sems):
    row = pl.program_id(Z) * recv_ref.shape[0]
    copies = list(column_copies(recv_ref, out_ref, lambda i: sems.at[i], row, places_of(1 - core_ref[Z])))
    start_all(copies)
    wait_all(copies)


def paste_columns(core, places_of, recv, whole):
    hidden, block = recv.shape
    rows = 2 * BLK
    return pl.pallas_call(
        functools.partial(paste_kernel, places_of),
        grid_spec=pltpu.PrefetchScalarGridSpec(
            num_scalar_prefetch=1,
            grid=(hidden // rows,),
            in_specs=[pl.BlockSpec((rows, block), lambda m, core: (m, Z)), ANY],
            out_specs=ANY,
            scratch_shapes=[dma_sems(8)],
        ),
        out_shape=jax.ShapeDtypeStruct(whole.shape, F32),
        input_output_aliases={2: 0},
        compiler_params=VMEM_BIG,
        name='paste',
    )(core, recv, whole)


def output_kernel(n_chip, core_ref, mine_ref, theirs_ref, shared_ref, other_ref, w_ref, w_shared_ref, na_ref, nb_ref, b_ref, out_ref, acc):
    j, last = pl.program_id(Z), pl.num_programs(Z) - 1
    rows = acc.shape[0]

    def add(ref, weight_ref):
        acc[...] += dot_nn(ref[...].reshape(rows, -1), weight_ref[...])

    @pl.when(j == Z)
    def _():
        acc[...] = jnp.broadcast_to(b_ref[...].astype(F32), acc.shape)

    pl.when(j < n_chip)(functools.partial(add, mine_ref, w_ref))
    pl.when(jnp.logical_and(j >= n_chip, j < CORES * n_chip))(functools.partial(add, theirs_ref, w_ref))
    pl.when(j == last - 1)(functools.partial(add, shared_ref, w_shared_ref))

    @pl.when(j == last)
    def _():
        add(other_ref, w_shared_ref)
        for half, n_ref in enumerate((na_ref, nb_ref)):
            at = part(half, n_ref.shape[0])
            out_ref[at] = (ALPHA * n_ref[...].astype(F32) + acc[at]).astype(BF16)


def project_out(core, ctx_par, ctx_recv, ctx_shared, shared_recv, w_o, n_halves, b_o):
    n_chip, rows, cols = ctx_recv.shape
    shared = shared_recv.shape[1]
    hidden = w_o.shape[1]
    base = CORES * n_chip * cols // shared
    steps = CORES * n_chip + CORES
    split = (CORES, CORES * n_chip, rows // CORES)

    def dist_index(j, core):
        at = jnp.minimum(j, CORES * n_chip - 1)
        return CORES * lax.rem(at, n_chip) + jnp.where(at < n_chip, core[Z], 1 - core[Z])

    def shared_index(j, core):
        return base + jnp.where(j < steps - 1, core[Z], 1 - core[Z])

    whole, half = [pl.BlockSpec((size, hidden), lambda j, core: (Z, Z)) for size in (rows, rows // CORES)]
    return pl.pallas_call(
        functools.partial(output_kernel, n_chip),
        grid_spec=pltpu.PrefetchScalarGridSpec(
            num_scalar_prefetch=1,
            grid=(steps,),
            in_specs=[
                pl.BlockSpec((1, CORES, 1, rows // CORES, cols), lambda j, core: (jnp.minimum(j, n_chip - 1), Z, core[CORES], Z, Z)),
                pl.BlockSpec((1, rows, cols), lambda j, core: (jnp.clip(j - n_chip, 0, n_chip - 1), Z, Z)),
                pl.BlockSpec((CORES, 1, rows // CORES, shared), lambda j, core: (Z, core[CORES], Z, Z)),
                pl.BlockSpec((rows, shared), lambda j, core: (Z, Z)),
                pl.BlockSpec((cols, hidden), lambda j, core: (dist_index(j, core), Z)),
                pl.BlockSpec((shared, hidden), lambda j, core: (shared_index(j, core), Z)),
                half, half,
                pl.BlockSpec((1, hidden), lambda j, core: (Z, Z)),
            ],
            out_specs=whole,
            scratch_shapes=[pltpu.VMEM((rows, hidden), F32)],
        ),
        out_shape=jax.ShapeDtypeStruct((rows, hidden), BF16),
        compiler_params=VMEM_BIG,
        cost_estimate=matmul_cost(rows, hidden, hidden),
        name='out_proj',
    )(core, ctx_par.reshape(n_chip, *split, cols), ctx_recv, ctx_shared.reshape(*split, shared), shared_recv, w_o, w_o, *n_halves, b_o)


def together(*values):
    return lax.optimization_barrier(values)


def solution(mesh):
    n_dev = mesh.shape['sp']
    tok_spec = P('dp', 'sp', None)
    pos_spec = P('dp', 'sp')
    in_specs = (tok_spec, pos_spec, pos_spec, P('dp'), P(), P(), P(), P(), P(), P(), tok_spec)
    out_specs = (tok_spec, tok_spec, P('dp'), P('dp'), P('dp', None), P('dp'), P('dp', None), P('dp'))
    same_core = [list(range(core, n_dev, 2)) for core in range(2)]
    partners = [(dev, dev ^ 1) for dev in range(n_dev)]
    n_chip = n_dev // 2

    def device_step(hidden_in, pos_ids, block_pos, prefix_len, ln_gamma, ln_beta, w_qkv, b_qkv, w_o, b_o, grad_out):
        batch, local_len, hidden = hidden_in.shape
        per_half = batch // 2
        heads = hidden // HEAD
        n_dist, n_shared = (heads - SHARED) // n_dev, SHARED // 2
        shared_at = n_dev * n_dist
        rows = batch * local_len
        tokens = n_dev * rows
        rank = lax.axis_index('sp')
        parity = lax.rem(rank, SLOTS)
        pair = rank + 1 - 2 * parity
        core = jnp.stack([parity, pair, rank]).astype(jnp.int32)
        gather = functools.partial(lax.all_gather, axis_name='sp')
        gather_core = functools.partial(lax.all_gather, axis_name='sp', axis_index_groups=same_core)
        to_partner = functools.partial(lax.ppermute, axis_name='sp', perm=partners)

        def token_rows(arr, dev):
            split = arr.reshape(arr.shape[:-2] + (2, n_dev, rows // 2, arr.shape[-1]))
            return lax.dynamic_index_in_dim(split, dev, axis=split.ndim - 3, keepdims=False).reshape(arr.shape[:-2] + (rows, arr.shape[-1]))

        def places(head):
            return lambda par: [((2 * c + par) * n_dist + head) * WIDTH for c in range(n_chip)]

        def shared_places(par):
            return [(shared_at + par * n_shared + i) * WIDTH for i in range(n_shared)]

        def wo_tile(t, par):
            spread = t - n_shared
            return jnp.where(t < n_shared, shared_at + par * n_shared + t, (2 * (spread // n_dist) + par) * n_dist + lax.rem(spread, n_dist))

        halves = range(2)
        x_flat, gain = hidden_in.reshape(rows, hidden), ln_gamma.reshape(1, hidden)
        n_own = [normalize(half, x_flat, gain, ln_beta.reshape(1, hidden)) for half in halves]
        dy_own = [grad_out[part(half, per_half)] for half in halves]
        n_own[1], *dy_own = together(n_own[1], *dy_own)
        n_own = [own.reshape(per_half, local_len, hidden) for own in n_own]
        n_a, n_b, dy_a, dy_b = [gather(send) for send in n_own + dy_own]
        cos, sin = rope_tables(prefix_len, n_dev * local_len)
        prefix = [prefix_len[part(half, per_half)] for half in halves]
        starts = jnp.stack([rank * n_dist, shared_at + parity * n_shared, rank, pair]).astype(jnp.int32)
        bias = jnp.concatenate([
            lax.dynamic_slice_in_dim(b_qkv, starts[0] * WIDTH, n_dist * WIDTH),
            lax.dynamic_slice_in_dim(b_qkv, starts[1] * WIDTH, n_shared * WIDTH)]).astype(F32).reshape(1, -1)
        grad_bo = jnp.sum(grad_out.astype(F32), axis=(0, 1))
        n_chip_rows = [own[None] for own in n_own + [to_partner(own) for own in n_own]]
        qkv_own = project_qkv(starts, n_dist, n_shared, n_chip_rows, w_qkv, bias, cos, sin)
        d_ctx_own = context_grad(starts, n_dist, n_shared, [own[None] for own in (grad_out, to_partner(grad_out))], w_o, n_dev)
        n_a, grad_bo, *d_ctx_own = together(n_a, grad_bo, *d_ctx_own)

        ctx_d = ctx_r = None
        qkv, lses = [], []
        for half in halves:
            if half:
                n_b, ctx_r = together(n_b, ctx_r)
            qd, kd, vd, qr, kr, vr = project_qkv(
                starts, n_dist, n_shared, [n_b if half else n_a], w_qkv, bias, cos, sin, half, qkv_own[part(half, QKV_IN)])
            ctx_d, lse_d = attention_forward(half, prefix[half], qd, kd, vd, n_dev, ctx_d)
            qr, ctx_d = together(qr, ctx_d)
            ctx_r, lse_r = attention_forward(half, prefix[half], qr, kr, vr, n_dev, ctx_r)
            qkv.append((qd, kd, vd, qr, kr, vr))
            lses.append((lse_d, lse_r))
        ctx_par = gather_core(ctx_d.reshape(tokens, n_dist * HEAD))

        dy_a, ctx_r = together(dy_a, ctx_r)
        g_d, g_r = [], []
        sums = []
        for half in halves:
            if half:
                dy_b, *g_r = together(dy_b, *g_r)
            qd, kd, vd, qr, kr, vr = qkv[half]
            d_ctx, d_ctx_r = context_grad(starts, n_dist, n_shared, [dy_b if half else dy_a], w_o, n_dev, d_ctx_own[part(half, CORES)])
            *g_d, sum_d = attention_backward(half, n_dist, prefix[half], qd, kd, vd, ctx_d, d_ctx, lses[half][0], cos, sin, g_d)
            qr, *g_d = together(qr, *g_d)
            *g_r, sum_r = attention_backward(half, n_shared, prefix[half], qr, kr, vr, ctx_r, d_ctx_r, lses[half][1], cos, sin, g_r)
            sums.append(jnp.sum(jnp.concatenate([sum_d, sum_r]), axis=(1, 2)).reshape(-1))
        g_par = [gather_core(g.reshape(tokens, WIDTH)) for g in g_d]
        g_r = [g.reshape(1, tokens, WIDTH) for g in g_r]

        n_a, n_b, dy_a, dy_b = [part.reshape(tokens // 2, hidden) for part in (n_a, n_b, dy_a, dy_b)]
        ctx_r = ctx_r.reshape(tokens, n_shared * HEAD)
        shared_recv = to_partner(token_rows(ctx_r, pair))
        ctx_r, *g_r = together(ctx_r, *g_r)
        grad_wo, wo_block = weight_grad_o(
            core, ctx_r[None], dy_a, dy_b, lambda c, par: (shared_at + par * n_shared) * HEAD, lambda c: 0, hidden // 2, ())
        shared_recv, wo_block, n_a = together(shared_recv, wo_block, n_a)
        grad_wqkv, block, r_send = weight_grad_qkv(core, shared_places, n_a, n_b, g_r, None)
        r_recv, ctx_recv = to_partner(r_send), to_partner(token_rows(ctx_par, pair))
        ctx_par, block = together(ctx_par, block)
        recv_r = to_partner(block)
        grad_wo, wo_block = weight_grad_o(
            core, ctx_par, dy_a, dy_b, lambda c, par: (2 * c + par) * (n_dist * HEAD), lambda c: (n_shared + c * n_dist) * HEAD,
            hidden // 2, (grad_wo, wo_block))
        ctx_recv, wo_block, recv_r, r_recv = together(ctx_recv, wo_block, recv_r, r_recv)
        wo_recv = to_partner(wo_block)
        hidden_out = project_out(
            core, ctx_par, ctx_recv, ctx_r, shared_recv, w_o, [own.reshape(-1, hidden) for own in n_own], b_o.reshape(1, hidden))
        n_a, hidden_out, g_par[0] = together(n_a, hidden_out, g_par[0])

        def columns(table):
            at = [np.array([h * WIDTH for h in table(par)] + [0], np.int32) for par in range(2)]
            last = (np.arange(at[0].size) == at[0].size - 1).astype(np.int32)
            return jnp.asarray(at[0]) + parity.astype(jnp.int32) * jnp.asarray(at[1] - at[0]) + rank.astype(jnp.int32) * jnp.asarray(last)

        def spread_grad(head, whole, **extra):
            whole, block, tok, *rest = weight_grad_qkv(core, places(head), n_a, n_b, [g_par[head]], whole, **extra)
            tok = to_partner(tok)
            if head:
                tok, block = together(tok, block)
            return whole, tok, to_partner(block), rest

        grad_wqkv, tok_0, recv_0, _ = spread_grad(0, grad_wqkv, pastes=[(recv_r, shared_places)])
        g_par[1], grad_wqkv = together(g_par[1], grad_wqkv)
        wo_recv, tok_0 = together(wo_recv, tok_0)
        grad_wqkv, tok_1, recv_1, (grad_wo,) = spread_grad(1, grad_wqkv, wo=(wo_recv, grad_wo, wo_tile))
        cols = columns(lambda mine: [shared_at + par * n_shared + i for par in (mine, 1 - mine) for i in range(n_shared)] + [
            (2 * c + par) * n_dist + head for par in (mine, 1 - mine) for c in range(n_chip) for head in (0, 1)])
        runs = [(i, 0) for i in range(n_shared)] + [(n_shared, i) for i in range(n_shared)]
        runs += [(n_shared + 1 + CORES * side + head, c) for side in range(CORES) for c in range(n_chip) for head in (0, 1)]
        tok_1, recv_0 = together(tok_1, recv_0)
        d_norm, = normed_grad(cols, runs, [*g_r, r_recv, g_par[0], g_par[1], tok_0, tok_1], w_qkv, grad_out.reshape(rows, hidden))
        n_a, d_norm, g_par[2] = together(n_a, d_norm, g_par[2])
        grad_wqkv, tok_2, recv_2, _ = spread_grad(2, grad_wqkv, pastes=[(recv_0, places(0)), (recv_1, places(1))])
        cols = columns(lambda mine: [(2 * c + par) * n_dist + 2 for c in range(n_chip) for par in (mine, 1 - mine)])
        grad_in, norm_sums = normed_grad(
            cols, [(src, c) for c in range(n_chip) for src in range(2)], [g_par[2], tok_2], w_qkv, d_norm, norm=(x_flat, gain))
        small = gather(jnp.concatenate([sums[0] + sums[1]] + [norm_sums.reshape(-1), grad_bo]))
        recv_2, small = together(recv_2, small)
        grad_wqkv = paste_columns(core, places(2), recv_2, grad_wqkv)
        spread, shared = small[:, :n_dist * WIDTH], small[:2, n_dist * WIDTH:(n_dist + n_shared) * WIDTH]
        grad_bqkv = jnp.concatenate([spread.reshape(-1), shared.reshape(-1)])
        grad_gamma, grad_beta, grad_bo = jnp.sum(small[:, (n_dist + n_shared) * WIDTH:], axis=0).reshape(3, hidden)
        shape = (batch, local_len, hidden)
        return (hidden_out.reshape(shape), grad_in.reshape(shape), grad_gamma, grad_beta, grad_wqkv, grad_bqkv, grad_wo, grad_bo)

    return jax.shard_map(device_step, mesh=mesh, in_specs=in_specs, out_specs=out_specs, check_vma=False)
```

```python
import functools
import math
import jax
import jax.numpy as jnp
import numpy as np
from jax import lax
from jax.experimental import pallas as pl
from jax.experimental.pallas import tpu as pltpu
from jax.sharding import PartitionSpec as P

HEAD = 128
QUARTER = 32
ALPHA = math.sqrt(56.0)
LN_EPS = 1e-5
ROT_BASE = 10000.0
SCALE = 1.0 / math.sqrt(HEAD)
LOG2E = math.log2(math.e)
MASK_FILL = -1e30
BLK = 256
VMEM_BIG = pltpu.CompilerParams(vmem_limit_bytes=62 << 20)
SHARED = 8
Z = 0
SLOTS = CORES = 2
WIDTH = 3 * HEAD
F32 = jnp.float32
BF16 = jnp.bfloat16


def dot(lhs, rhs, lhs_dim, rhs_dim):
    return lax.dot_general(lhs, rhs, (((lhs_dim,), (rhs_dim,)), ((), ())), preferred_element_type=F32)


def dot_nn(lhs, rhs):
    return dot(lhs, rhs, 1, 0)


def dot_nt(lhs, rhs):
    return dot(lhs, rhs, 1, 1)


def dot_tn(lhs, rhs):
    return dot(lhs, rhs, 0, 0)


def matmul_cost(rows, depth, cols, extra=0):
    return pl.CostEstimate(
        flops=2 * rows * depth * cols, bytes_accessed=2 * (rows * depth + depth * cols + rows * cols) + extra, transcendentals=0)


def attention_cost(n_head, batch, seq, products):
    pairs = n_head * batch * seq * seq
    return pl.CostEstimate(flops=2 * products * pairs * HEAD, bytes_accessed=8 * products * n_head * batch * seq * HEAD, transcendentals=pairs)


def run(index, size):
    return pl.ds(pl.multiple_of(index * size, size), size)


def part(index, size):
    return slice(index * size, (index + 1) * size)


def rope_tables(prefix_len, seq):
    tok = jnp.arange(seq, dtype=jnp.int32)[None, :]
    pre = prefix_len[:, None]
    inside = tok < pre
    pos = jnp.where(inside, tok, pre - 1)
    blk = jnp.where(inside, 0, tok - pre + 1)
    inv_freq = ROT_BASE ** (-jnp.arange(QUARTER, dtype=F32) / QUARTER)
    angles = jnp.stack([pos, blk], axis=-1).astype(F32)[..., None] * inv_freq
    cos, sin = jnp.cos(angles), jnp.sin(angles)
    shape = pos.shape + (HEAD,)
    return (jnp.stack([cos, cos], axis=-2).reshape(shape), jnp.stack([-sin, sin], axis=-2).reshape(shape))


def turn(x, cos, sin):
    lane = lax.broadcasted_iota(jnp.int32, x.shape, 1)
    other = jnp.where(lane % (2 * QUARTER) < QUARTER, pltpu.roll(x, HEAD - QUARTER, 1), pltpu.roll(x, QUARTER, 1))
    return x * cos + other * sin


def dma_sems(*shape):
    return pltpu.SemaphoreType.DMA(shape)


def dma_sems(*shape):
    return pltpu.SemaphoreType.DMA(shape)


def start_all(copies):
    for copy in copies:
        copy.start()


def wait_all(copies):
    for copy in copies:
        copy.wait()


ANY = pl.BlockSpec(memory_space=pl.ANY)
PIECES = 4
WIDE_GATHER = 1 << 15
QKV_IN = 6


NORM_ROWS = 32


def centred(x):
    x = x.astype(F32)
    x = x - jnp.mean(x, axis=-1, keepdims=True)
    return x, lax.rsqrt(jnp.mean(x * x, axis=-1, keepdims=True) + LN_EPS)


def norm_kernel(x_ref, gain_ref, shift_ref, out_ref):
    gain, shift = gain_ref[...].astype(F32), shift_ref[...].astype(F32)

    @pl.loop(0, x_ref.shape[0] // NORM_ROWS)
    def _(i):
        rows = run(i, NORM_ROWS)
        x, inv = centred(x_ref[rows])
        out_ref[rows] = (x * inv * gain + shift).astype(BF16)


def normalize(half, x, gain, shift):
    rows, hidden = x.shape
    block = rows // 4
    vec = pl.BlockSpec((1, hidden), lambda i: (Z, Z))
    return pl.pallas_call(
        norm_kernel,
        grid=(2,),
        in_specs=[pl.BlockSpec((block, hidden), lambda i: (2 * half + i, Z)), vec, vec],
        out_specs=pl.BlockSpec((block, hidden), lambda i: (i, Z)),
        out_shape=jax.ShapeDtypeStruct((2 * block, hidden), BF16),
        compiler_params=VMEM_BIG,
        name='norm',
    )(x, gain, shift)


def qkv_kernel(n_dist, n_tile, n_in, start_ref, *rest):
    n_refs, (w_ref, b_ref, cos_ref, sin_ref, *outs), (w_buf, acc, sems) = rest[:n_in], rest[n_in:-3], rest[-3:]
    first, later = n_refs[:(n_in + 1) // CORES], n_refs[n_in // CORES:]
    _, rows, cols = acc.shape
    hidden = w_ref.shape[0]
    dist = n_dist * WIDTH
    step, last = pl.program_id(Z), pl.num_programs(Z) - 1
    slot = lax.rem(step, SLOTS)
    piece = hidden // PIECES
    tile = first[0].shape[-2]

    def loads(i):
        span = run(i, piece)
        for kind, (at, width) in enumerate(((0, dist), (dist, cols - dist))):
            col = pl.multiple_of(start_ref[kind] * WIDTH, HEAD)
            yield pltpu.make_async_copy(w_ref.at[span, pl.ds(col, width)], w_buf.at[span, pl.ds(at, width)], sems.at[i, kind])

    def finish():
        for i in range(rows // tile):
            group, batch, at, table = n_tile(i)
            cos, sin = cos_ref[table, part(at, tile)], sin_ref[table, part(at, tile)]
            for h in range(cols // WIDTH):
                kind, head = (0, h) if h < n_dist else (1, h - n_dist)
                refs = outs[part(CORES * group + kind, 3)]
                pre = [acc[1 - slot, part(i, tile), part(3 * h + j, HEAD)] + b_ref[:, part(3 * h + j, HEAD)] for j in range(3)]
                for ref, val in zip(refs, (turn(pre[0], cos, sin), turn(pre[1], cos, sin), pre[2])):
                    ref[head, batch, part(at, tile)] = val.astype(BF16)

    @pl.when(step == Z)
    def _():
        for i in range(PIECES):
            start_all(loads(i))
        acc[slot] = jnp.zeros((rows, cols), F32)

        @pl.loop(0, PIECES)
        def _(i):
            wait_all(loads(i))
            span = run(i, piece)
            for i, ref in enumerate(first):
                acc[slot, part(i, rows // len(first))] += dot_nn(ref[:, :, :, span].reshape(-1, piece), w_buf[span])

    @pl.when(jnp.logical_and(step > 0, step < last))
    def _():
        finish()
        for i, ref in enumerate(later):
            acc[slot, part(i, rows // len(later))] = dot_nn(ref[...].reshape(-1, hidden), w_buf[...])

    pl.when(step == last)(finish)


def project_qkv(starts, n_dist, n_shared, n_rows, w_qkv, bias, cos, sin, half=None, earlier=None):
    _, per_half, local_len, hidden = n_rows[0].shape
    _, seq, _ = cos.shape
    cols = (n_dist + n_shared) * WIDTH
    own = earlier is None
    batch = per_half * CORES if own else per_half
    steps = CORES if own else seq // local_len // CORES - 1
    n_chip = seq // local_len // CORES
    width = local_len if own else CORES * local_len

    def place(step, at):
        return at[CORES + step] if own else lax.rem(at[CORES] // CORES + 1 + step, n_chip)

    def ahead(step, at):
        return place(jnp.minimum(step, steps - 1), at)

    def behind(step, at):
        return place(jnp.maximum(step - 1, 0), at)

    shapes = [jax.ShapeDtypeStruct((n_head, per_half, seq, HEAD), BF16) for n_head in (n_dist, n_shared) for _ in range(3)]
    shapes = shapes * CORES if own else shapes
    tab_spec = pl.BlockSpec((batch, width, HEAD), lambda step, at: (Z if own else half, behind(step, at), Z))
    arrays = [] if own else list(earlier)

    def own_tile(i):
        return i // per_half, i % per_half, 0, i

    def other_tile(i):
        return 0, i % per_half, i // per_half, i % per_half

    return pl.pallas_call(
        functools.partial(without, len(arrays), len(n_rows) + 5, functools.partial(qkv_kernel, n_dist, own_tile if own else other_tile, len(n_rows))),
        grid_spec=pltpu.PrefetchScalarGridSpec(
            num_scalar_prefetch=1,
            grid=(steps + 1,),
            in_specs=[
                *[pl.BlockSpec((1 if own else CORES, per_half, local_len, hidden), lambda step, at: (Z if own else ahead(step, at), Z, Z, Z))] * len(n_rows),
                ANY,
                pl.BlockSpec((1, cols), lambda step, at: (Z, Z)),
                tab_spec, tab_spec,
            ] + [ANY] * len(arrays),
            out_specs=[pl.BlockSpec(shape.shape[:CORES] + (width, HEAD), lambda step, at: (Z, Z, behind(step, at), Z)) for shape in shapes],
            scratch_shapes=[
                pltpu.VMEM((hidden, cols), BF16), pltpu.VMEM((SLOTS, CORES * CORES * local_len, cols), F32), dma_sems(PIECES, SLOTS)],
        ),
        out_shape=shapes,
        input_output_aliases={QKV_IN + i: i for i in range(len(arrays))},
        compiler_params=VMEM_BIG,
        cost_estimate=matmul_cost(steps * CORES * batch * local_len, hidden, cols),
        name='qkv',
    )(starts, *n_rows, w_qkv, bias, cos, sin, *arrays)


def without(count, start, kernel, *refs):
    kernel(*refs[:start], *refs[start + count:])


def forward_kernel(pre_ref, q_ref, k_ref, v_ref, *rest):
    ctx_ref, lse_ref = rest[-2:]
    n_head, _, seq, _ = q_ref.shape
    local_len = ctx_ref.shape[3]
    per = BLK // local_len
    prefix = pre_ref[pl.program_id(1)]

    def block(r, n_key):
        query = lax.broadcasted_iota(jnp.int32, (1, BLK), 1) + r * BLK
        last = jnp.maximum(query, prefix - 1) - (n_key - 1) * BLK
        scores = []
        for h in range(n_head):
            q_blk = q_ref[h, 0, part(r, BLK)]
            parts = [dot_nt(k_ref[h, 0, part(c, BLK)], q_blk) * (SCALE * LOG2E) for c in range(n_key)]
            key = lax.broadcasted_iota(jnp.int32, (BLK, BLK), 0)
            parts[-1] = jnp.where(key <= last, parts[-1], MASK_FILL)
            scores.append(parts)
        for h, parts in enumerate(scores):
            top = functools.reduce(jnp.maximum, [jnp.max(p, axis=0, keepdims=True) for p in parts])
            parts = [jnp.exp2(p - top) for p in parts]
            total = functools.reduce(jnp.add, [jnp.sum(p, axis=0, keepdims=True) for p in parts])
            inv = 1.0 / total
            probs = jnp.concatenate([(p * inv).astype(BF16) for p in parts], axis=0)
            ctx_t = dot_tn(v_ref[h, 0, :n_key * BLK], probs)
            ctx = ctx_t.T.astype(BF16).reshape(per, local_len, HEAD)
            ctx_ref[0, part(r, per), 0, :, part(h, HEAD)] = ctx
            lse_ref[h, 0, :, part(r, BLK)] = top + jnp.log2(total)

    n_blk = seq // BLK
    for r in range(n_blk):
        for n_key in range(r + 1, n_blk + 1):
            low = (n_key - 1) * BLK
            cond = prefix <= n_key * BLK if n_key == r + 1 else prefix > low
            if n_key < n_blk and n_key > r + 1:
                cond = jnp.logical_and(cond, prefix <= n_key * BLK)
            if n_key == n_blk and n_key == r + 1:
                block(r, n_key)
            else:
                pl.when(cond)(functools.partial(block, r, n_key))


def attention_forward(half, prefix_half, q, k, v, n_dev, ctx):
    own, batch, seq, _ = q.shape
    local_len = seq // n_dev
    group = own
    qkv_spec = pl.BlockSpec((group, 1, seq, HEAD), lambda h, b, pre: (h, b, Z, Z))
    earlier = [] if ctx is None else [ctx]
    return pl.pallas_call(
        forward_kernel,
        grid_spec=pltpu.PrefetchScalarGridSpec(
            num_scalar_prefetch=1,
            grid=(own // group, batch),
            in_specs=[qkv_spec] * 3 + [ANY] * len(earlier),
            out_specs=[
                pl.BlockSpec((1, n_dev, 1, local_len, group * HEAD), lambda h, b, pre: (half, Z, b, Z, h)),
                pl.BlockSpec((group, 1, 1, seq), lambda h, b, pre: (h, b, Z, Z)),
            ],
        ),
        out_shape=[
            jax.ShapeDtypeStruct((2, n_dev, batch, local_len, own * HEAD), BF16),
            jax.ShapeDtypeStruct((own, batch, 1, seq), F32),
        ],
        input_output_aliases={4: 0} if earlier else {},
        compiler_params=VMEM_BIG,
        cost_estimate=attention_cost(own, batch, seq, 2),
        name='attn_fwd',
    )(prefix_half, q, k, v, *earlier)


def d_ctx_kernel(n_in, start_ref, *rest):
    dy_refs, (w_ref, *outs), (w_buf, sems) = rest[:n_in], rest[n_in:-2], rest[-2:]
    step, hidden = pl.program_id(Z), w_ref.shape[1]
    widths = [outs[0].shape[-1], outs[1].shape[-1]]

    def loads():
        for kind, (at, width) in enumerate(zip((0, widths[0]), widths)):
            row = pl.multiple_of(start_ref[kind] * HEAD, HEAD)
            yield pltpu.make_async_copy(w_ref.at[pl.ds(row, width)], w_buf.at[pl.ds(at, width)], sems.at[kind])

    @pl.when(step == Z)
    def _():
        start_all(loads())
        wait_all(loads())

    def multiply(dy_ref):
        res = dot_nt(dy_ref[...].reshape(-1, hidden), w_buf[...]).astype(BF16)
        rows = CORES * res.shape[0] // len(outs)
        for i, out_ref in enumerate(outs):
            cols = slice(widths[0], None) if i % CORES else slice(widths[0])
            out_ref[...] = res[part(i // CORES, rows), cols].reshape(out_ref.shape)

    if n_in > 1:
        for i, dy_ref in enumerate(dy_refs):
            pl.when(step == i)(functools.partial(multiply, dy_ref))
    else:
        multiply(dy_refs[0])


def context_grad(starts, n_dist, n_shared, dy_rows, w_o, n_dev, earlier=()):
    _, batch, local_len, hidden = dy_rows[0].shape
    own = not earlier
    n_chip = n_dev // CORES
    per_half, devs = (batch // CORES, 1) if own else (batch, CORES)

    def block(step, at):
        return (at[CORES + step] if own else lax.rem(at[CORES] // CORES + 1 + step, n_chip), Z, Z, Z)

    cols = [n_dist * HEAD, n_shared * HEAD]
    outs = cols * (CORES if own else 1)
    n_in = len(dy_rows)
    return pl.pallas_call(
        functools.partial(without, len(earlier), n_in + 2, functools.partial(d_ctx_kernel, n_in)),
        grid_spec=pltpu.PrefetchScalarGridSpec(
            num_scalar_prefetch=1,
            grid=(CORES if own else n_chip - 1,),
            in_specs=[pl.BlockSpec((devs, batch, local_len, hidden), (lambda step, at: (Z, Z, Z, Z)) if own else block)] * n_in + [ANY] * (1 + len(earlier)),
            out_specs=[pl.BlockSpec((devs, per_half, local_len, width), block) for width in outs],
            scratch_shapes=[pltpu.VMEM((sum(cols), hidden), BF16), dma_sems(CORES)],
        ),
        out_shape=[jax.ShapeDtypeStruct((n_dev, per_half, local_len, width), BF16) for width in outs],
        input_output_aliases={3 + i: i for i in range(len(earlier))},
        compiler_params=VMEM_BIG,
        cost_estimate=matmul_cost(n_dev * batch * local_len, hidden, sum(cols)),
        name='dctx',
    )(starts, *dy_rows, w_o, *earlier)


def backward_kernel(pre_ref, q_ref, k_ref, v_ref, ctx_ref, dctx_ref, lse_ref, cos_ref, sin_ref, *rest):
    sum_ref, dq_acc, dk_acc, dv_acc = rest[-4:]
    n_head, _, seq, _ = q_ref.shape
    g_refs = rest[-4 - n_head:-4]
    _, n_dev, _, local_len, _ = g_refs[0].shape
    n_blk = seq // BLK
    prefix = pre_ref[pl.program_id(Z)]
    d_ctx, delta = [], []
    for h in range(n_head):
        lanes = part(h, HEAD)
        grad = dctx_ref[:, :, :, lanes].reshape(seq, HEAD)
        prod = grad.astype(F32) * ctx_ref[0, :, :, :, lanes].reshape(seq, HEAD).astype(F32)
        d_ctx.append(grad)
        delta.append(jnp.sum(prod.T, axis=0, keepdims=True))

    def block(c, first):
        span = part(c, BLK)
        start = first * BLK
        products = []
        for h in range(n_head):
            s_t = dot_nt(k_ref[h, 0, span], q_ref[h, 0, start:])
            dp_t = dot_nt(v_ref[h, 0, span], d_ctx[h][start:])
            products.append((s_t, dp_t))
        for h, (s_t, dp_t) in enumerate(products):
            probs, d_scores = [], []
            for r in range(first, n_blk):
                cols, here = part(r, BLK), part(r - first, BLK)
                piece = s_t[:, here] * (SCALE * LOG2E)
                if r <= c:
                    key = lax.broadcasted_iota(jnp.int32, (BLK, BLK), 0)
                    query = lax.broadcasted_iota(jnp.int32, (1, BLK), 1) + r * BLK
                    piece = jnp.where(key <= jnp.maximum(query, prefix - 1) - c * BLK, piece, MASK_FILL)
                p = jnp.exp2(piece - lse_ref[h, 0, :, cols])
                probs.append(p.astype(BF16))
                d_scores.append((p * (dp_t[:, here] - delta[h][:, cols]) * SCALE).astype(BF16))
            probs = jnp.concatenate(probs, axis=1)
            d_scores = jnp.concatenate(d_scores, axis=1)
            dv_acc[h, span] = dot_nn(probs, d_ctx[h][start:])
            dk_acc[h, span] = dot_nn(d_scores, q_ref[h, 0, start:])
            dq_part = dot_tn(k_ref[h, 0, span], d_scores)
            if c:
                dq_acc[h, :, start:] += dq_part
            else:
                dq_acc[h] = dq_part

    block(0, 0)
    for c in range(1, n_blk):
        pl.when(prefix > c * BLK)(functools.partial(block, c, 0))
        pl.when(prefix <= c * BLK)(functools.partial(block, c, c))

    cos, sin = cos_ref[Z], sin_ref[Z]
    for h in range(n_head):
        g_q = turn(dq_acc[h].T.astype(BF16).astype(F32), cos, -sin)
        g_k = turn(dk_acc[h].astype(BF16).astype(F32), cos, -sin)
        g_v = dv_acc[h].astype(BF16).astype(F32)
        for i, g in enumerate((g_q, g_k, g_v)):
            lanes = part(i, HEAD)
            g_refs[h][0, :, 0, :, lanes] = g.astype(BF16).reshape(n_dev, local_len, HEAD)
            sum_ref[h, 0, :, lanes] = jnp.sum(g, axis=0, keepdims=True)


def attention_backward(half, group, prefix_half, q, k, v, ctx, d_ctx, lse, cos, sin, earlier):
    _, batch, seq, _ = q.shape
    _, n_dev, _, local_len, _ = ctx.shape
    qkv_spec = pl.BlockSpec((group, 1, seq, HEAD), lambda b, pre: (Z, b, Z, Z))
    tab_spec = pl.BlockSpec((1, seq, HEAD), lambda b, pre: (half * batch + b, Z, Z))
    stat = functools.partial(pltpu.VMEM, dtype=F32)
    return pl.pallas_call(
        backward_kernel,
        grid_spec=pltpu.PrefetchScalarGridSpec(
            num_scalar_prefetch=1,
            grid=(batch,),
            in_specs=[qkv_spec] * 3 + [
                pl.BlockSpec((1, n_dev, 1, local_len, group * HEAD), lambda b, pre: (half, Z, b, Z, Z)),
                pl.BlockSpec((n_dev, 1, local_len, group * HEAD), lambda b, pre: (Z, b, Z, Z)),
                pl.BlockSpec((group, 1, 1, seq), lambda b, pre: (Z, b, Z, Z)), tab_spec, tab_spec] + [ANY] * len(earlier),
            out_specs=[pl.BlockSpec((1, n_dev, 1, local_len, WIDTH), lambda b, pre: (half, Z, b, Z, Z))] * group + [
                pl.BlockSpec((group, 1, 1, WIDTH), lambda b, pre: (Z, b, Z, Z))],
            scratch_shapes=[stat((group, HEAD, seq)), stat((group, seq, HEAD)), stat((group, seq, HEAD))],
        ),
        out_shape=[jax.ShapeDtypeStruct((2, n_dev, batch, local_len, WIDTH), BF16)] * group + [
            jax.ShapeDtypeStruct((group, batch, 1, WIDTH), F32)],
        input_output_aliases={9 + i: i for i in range(len(earlier))},
        compiler_params=VMEM_BIG,
        cost_estimate=attention_cost(group, batch, seq, 5),
        name='attn_bwd',
    )(prefix_half, q, k, v, ctx, d_ctx, lse, cos, sin, *earlier)


def wo_grad_kernel(row_of, block_row_of, core_ref, ctx_ref, dya_ref, dyb_ref, *rest):
    out_ref, copy_ref, rhs, buf, rhs_sems, sems = rest[-6:]
    n, c = pl.program_id(Z), pl.program_id(1)
    n_col, n_grp = pl.num_programs(Z), pl.num_programs(1)
    step = n * n_grp + c
    slot, n_slot = lax.rem(step, SLOTS), lax.rem(n, SLOTS)
    _, rows, wide = buf.shape
    half = dya_ref.shape[0]
    core = core_ref[Z]

    def loads(n_at, at):
        for i, ref in enumerate((dya_ref, dyb_ref)):
            yield pltpu.make_async_copy(ref.at[:, run(n_at, wide)], rhs.at[at, run(i, half)], rhs_sems.at[at, i])

    def stores(at_step, at):
        n_at, c_at = at_step // n_grp, lax.rem(at_step, n_grp)
        for i, (ref, row) in enumerate(((out_ref, row_of(c_at, core)), (copy_ref, block_row_of(c_at)))):
            yield pltpu.make_async_copy(buf.at[at], ref.at[pl.ds(pl.multiple_of(row, HEAD), rows), run(n_at, wide)], sems.at[at, i])

    @pl.when(step == Z)
    def _():
        start_all(loads(0, 0))

    @pl.when(c == Z)
    def _():
        @pl.when(n + 1 < n_col)
        def _():
            start_all(loads(n + 1, 1 - n_slot))

        wait_all(loads(n, n_slot))

    @pl.when(step >= 2)
    def _():
        wait_all(stores(step - 2, slot))

    buf[slot] = dot_tn(ctx_ref[Z], rhs[n_slot])
    start_all(stores(step, slot))

    @pl.when(step == n_col * n_grp - 1)
    def _():
        wait_all(stores(step - 1, 1 - slot))
        wait_all(stores(step, slot))


def weight_grad_o(core, ctx_par, dy_a, dy_b, row_of, block_row_of, block_rows, earlier):
    n_grp, tokens, cols = ctx_par.shape
    hidden = dy_a.shape[1]
    wide = hidden // 4
    return pl.pallas_call(
        functools.partial(wo_grad_kernel, row_of, block_row_of),
        grid_spec=pltpu.PrefetchScalarGridSpec(
            num_scalar_prefetch=1,
            grid=(hidden // wide, n_grp),
            in_specs=[pl.BlockSpec((1, tokens, cols), lambda n, c, core: (c, Z, Z)), ANY, ANY] + [ANY] * len(earlier),
            out_specs=[ANY, ANY],
            scratch_shapes=[pltpu.VMEM((SLOTS, tokens, wide), BF16), pltpu.VMEM((SLOTS, cols, wide), F32), dma_sems(SLOTS, SLOTS), dma_sems(SLOTS, SLOTS)],
        ),
        out_shape=[jax.ShapeDtypeStruct((hidden, hidden), F32), jax.ShapeDtypeStruct((block_rows, hidden), F32)],
        input_output_aliases={4: 0, 5: 1} if earlier else {},
        compiler_params=VMEM_BIG,
        cost_estimate=matmul_cost(n_grp * cols, tokens, hidden, 8 * hidden * n_grp * cols),
        name='wo_grad',
    )(core, ctx_par, dy_a, dy_b, *earlier)


def column_copies(src, out_ref, sem_of, row, places):
    rows, width = src.shape[0], src.shape[1] // len(places)
    for i, col in enumerate(places):
        yield pltpu.make_async_copy(
            src.at[:, run(i, width)],
            out_ref.at[pl.ds(pl.multiple_of(row, BLK), rows), pl.ds(pl.multiple_of(col, HEAD), width)],
            sem_of(i))


def wqkv_grad_kernel(places_of, old_places, wo_tile, n_src, core_ref, na_ref, nb_ref, *rest):
    srcs, rest = rest[:n_src], list(rest[n_src:])
    groups = [ref.at[c] for ref in srcs for c in range(ref.shape[0])]
    recv_refs = [rest.pop(0) for _ in old_places]
    wo_recv_ref = rest.pop(0) if wo_tile else None
    n_buf, rhs, buf, n_sems, g_sems, out_sems, copy_sems, paste_sems, wo_sems, tok_sems = rest[-10:]
    outs = rest[:-10][-4 if wo_tile else -3:]
    out_ref, copy_ref, tok_ref = outs[:3]
    m = pl.program_id(Z)
    n_m = pl.num_programs(Z)
    core, pair = core_ref[Z], core_ref[1]
    tokens, cols = groups[0].shape
    half, rows = tokens // 2, n_buf.shape[2]
    piece = tokens // PIECES
    slot = lax.rem(m, SLOTS)

    def n_loads(step, at):
        for i, ref in enumerate((na_ref, nb_ref)):
            yield pltpu.make_async_copy(ref.at[:, run(step, rows)], n_buf.at[at, run(i, half)], n_sems.at[at, i])

    def g_loads(i):
        for c, ref in enumerate(groups):
            yield pltpu.make_async_copy(ref.at[run(i, piece)], rhs.at[run(i, piece), run(c, cols)], g_sems.at[i, c])

    def stores(step, at):
        yield from column_copies(buf.at[at], out_ref, lambda i: out_sems.at[at, i], step * rows, places_of(core))
        yield pltpu.make_async_copy(buf.at[at], copy_ref.at[run(step, rows)], copy_sems.at[at])

    def pastes():
        for at, (recv_ref, old_places_of) in enumerate(zip(recv_refs, old_places)):
            yield from column_copies(recv_ref, out_ref, lambda i: paste_sems.at[at, i], m * rows, old_places_of(1 - core))
        if wo_tile:
            tiles = wo_recv_ref.shape[0] // HEAD
            for t in range(tiles):
                tile = wo_tile(m * tiles + t, 1 - core)
                yield pltpu.make_async_copy(wo_recv_ref.at[run(t, HEAD)], outs[3].at[run(tile, HEAD)], wo_sems.at[t])

    def token_copies():
        size = tok_ref.shape[0] // 2
        for i in range(2):
            yield pltpu.make_async_copy(rhs.at[pl.ds(pl.multiple_of(i * half + pair * size, BLK), size)], tok_ref.at[run(i, size)], tok_sems.at[i])

    @pl.when(m == Z)
    def _():
        start_all(n_loads(0, 0))
        for i in range(PIECES):
            start_all(g_loads(i))

    @pl.when(m + 1 < n_m)
    def _():
        start_all(n_loads(m + 1, 1 - slot))

    start_all(pastes())

    @pl.when(m >= 2)
    def _():
        wait_all(stores(m - 2, slot))

    wait_all(n_loads(m, slot))

    @pl.when(m == Z)
    def _():
        buf[slot] = jnp.zeros((rows, rhs.shape[1]), F32)

        @pl.loop(0, PIECES)
        def _(i):
            wait_all(g_loads(i))
            buf[slot] += dot_tn(n_buf[slot, run(i, piece)], rhs[run(i, piece)])

        start_all(token_copies())

    @pl.when(m > 0)
    def _():
        buf[slot] = dot_tn(n_buf[slot], rhs[...])

    start_all(stores(m, slot))
    wait_all(pastes())

    @pl.when(m == n_m - 1)
    def _():
        wait_all(stores(m - 1, 1 - slot))
        wait_all(stores(m, slot))
        wait_all(token_copies())


def weight_grad_qkv(core, places_of, n_a, n_b, srcs, whole, pastes=(), wo=None):
    hidden = n_a.shape[1]
    n_grp, (tokens, cols) = sum(src.shape[0] for src in srcs), srcs[0].shape[1:]
    width = n_grp * cols
    rows = 2 * BLK
    steps = hidden // rows
    args, specs, alias = [core, n_a, n_b, *srcs], [ANY] * (2 + len(srcs)), {}
    outs = [jax.ShapeDtypeStruct((hidden, 3 * hidden), F32), jax.ShapeDtypeStruct((hidden, width), F32), jax.ShapeDtypeStruct((2 * BLK, width), BF16)]
    wo_tile = None
    for recv, _ in pastes:
        args.append(recv)
        specs.append(pl.BlockSpec((rows, width), lambda m, core: (m, Z)))
    if wo is not None:
        wo_recv, wo_whole, wo_tile = wo
        args.append(wo_recv)
        specs.append(pl.BlockSpec((wo_recv.shape[0] // steps, hidden), lambda m, core: (m, Z)))
        outs.append(jax.ShapeDtypeStruct(wo_whole.shape, F32))
    if whole is not None:
        alias[len(args)] = 0
        args.append(whole)
        specs.append(ANY)
    if wo is not None:
        alias[len(args)] = 3
        args.append(wo_whole)
        specs.append(ANY)
    return pl.pallas_call(
        functools.partial(wqkv_grad_kernel, places_of, [old for _, old in pastes], wo_tile, len(srcs)),
        grid_spec=pltpu.PrefetchScalarGridSpec(
            num_scalar_prefetch=1,
            grid=(steps,),
            in_specs=specs,
            out_specs=[ANY] * len(outs),
            scratch_shapes=[
                pltpu.VMEM((SLOTS, tokens, rows), BF16),
                pltpu.VMEM((tokens, width), BF16),
                pltpu.VMEM((SLOTS, rows, width), F32),
                dma_sems(SLOTS, SLOTS), dma_sems(PIECES, n_grp), dma_sems(SLOTS, n_grp), dma_sems(SLOTS), dma_sems(SLOTS, n_grp), dma_sems(4), dma_sems(SLOTS),
            ],
        ),
        out_shape=outs,
        input_output_aliases=alias,
        compiler_params=VMEM_BIG,
        cost_estimate=matmul_cost(hidden, tokens, width, 16 * hidden * width),
        name='wqkv_grad',
    )(*args)


def normed_grad_kernel(runs, n_src, final, more, cols_ref, *rest):
    srcs, (w_ref, init_ref, *rest) = rest[:n_src], rest[n_src:]
    if final:
        x_ref, gain_ref, dx_ref, sum_ref, acc, w_buf, g_buf, sems, g_sems, init_sem, sum_acc = rest
    else:
        acc, w_buf, g_buf, sems, g_sems, init_sem = rest
    j, steps = pl.program_id(Z), pl.num_programs(Z)
    slot = lax.rem(j, SLOTS)
    rows, width = g_buf.shape[1], g_buf.shape[2] // 2
    rank = cols_ref[2 * steps]

    def w_loads(step, at):
        for i in range(2):
            col = pl.multiple_of(cols_ref[2 * step + i], HEAD)
            yield pltpu.make_async_copy(w_ref.at[:, pl.ds(col, width)], w_buf.at[at, :, run(i, width)], sems.at[at, i])

    def g_loads(step):
        at = step % 2
        for i, (src, grp) in enumerate(runs[part(step, 2)]):
            ref, dst = srcs[src], g_buf.at[at, :, run(i, width)]
            tokens = ref.shape[-2]
            ref = ref.at[:, run(grp, width)] if tokens == rows else ref.at[grp]
            pairs = [(ref, dst)] if tokens == rows else [
                (ref.at[pl.ds(pl.multiple_of(h * (tokens // 2) + rank * (rows // 2), BLK), rows // 2)], dst.at[run(h, rows // 2)]) for h in range(2)]
            for pair in pairs:
                yield pltpu.make_async_copy(*pair, g_sems.at[at, i])

    def g_waits(at):
        for i in range(2):
            block = g_buf.at[at, :, run(i, width)]
            yield pltpu.make_async_copy(block, block, g_sems.at[at, i])

    @pl.when(j == Z)
    def _():
        start_all(w_loads(0, 0))
        start_all(g_loads(0))
        if more:
            init = pltpu.make_async_copy(init_ref, acc, init_sem)
            init.start()
            init.wait()
        else:
            acc[...] = init_ref[...].astype(F32) * ALPHA

    @pl.when(j + 1 < steps)
    def _():
        start_all(w_loads(j + 1, 1 - slot))

    for step in range(1, len(runs) // 2):
        @pl.when(j + 1 == step)
        def _():
            start_all(g_loads(step))

    wait_all(w_loads(j, slot))
    wait_all(g_waits(slot))
    acc[...] += dot_nt(g_buf[slot], w_buf[slot])

    if final:
        @pl.when(j == steps - 1)
        def _():
            sum_acc[...] = jnp.zeros_like(sum_acc)
            gain = gain_ref[...].astype(F32)

            @pl.loop(0, rows // NORM_ROWS)
            def _(i):
                at = run(i, NORM_ROWS)
                d_n = acc[at]
                x, inv = centred(x_ref[at])
                x = x * inv
                d_x = d_n * gain
                mean = jnp.mean(d_x, axis=-1, keepdims=True)
                slope = jnp.mean(d_x * x, axis=-1, keepdims=True)
                dx_ref[at] = (inv * (d_x - mean - x * slope)).astype(BF16)
                for kind, term in enumerate((d_n * x, d_n)):
                    sum_acc[kind] += jnp.sum(term.reshape((-1,) + sum_acc.shape[1:]), axis=0)

            sum_ref[...] = jnp.sum(sum_acc[...], axis=1)


def normed_grad(cols, runs, srcs, w_qkv, init, norm=None):
    rows, hidden = init.shape
    steps, width = len(runs) // 2, 2 * WIDTH
    flat = pl.BlockSpec((rows, hidden), lambda j, cols: (Z, Z))
    args = [cols, *srcs, w_qkv, init]
    more = init.dtype == F32
    specs = [ANY] * (len(srcs) + 1) + [ANY if more else flat]
    scratch = [pltpu.VMEM((SLOTS, hidden, width), BF16), pltpu.VMEM((SLOTS, rows, width), BF16), dma_sems(SLOTS, SLOTS), dma_sems(SLOTS, SLOTS), pltpu.SemaphoreType.DMA]
    if norm:
        args += list(norm)
        specs += [flat, pl.BlockSpec((1, hidden), lambda j, cols: (Z, Z))]
        outs = [jax.ShapeDtypeStruct((rows, hidden), BF16), jax.ShapeDtypeStruct((2, hidden), F32)]
        out_specs = [flat, pl.BlockSpec((2, hidden), lambda j, cols: (Z, Z))]
        scratch = [pltpu.VMEM((rows, hidden), F32)] + scratch + [pltpu.VMEM((2, 8, hidden), F32)]
    else:
        outs, out_specs = [jax.ShapeDtypeStruct((rows, hidden), F32)], [flat]
    return pl.pallas_call(
        functools.partial(normed_grad_kernel, runs, len(srcs), norm is not None, more),
        grid_spec=pltpu.PrefetchScalarGridSpec(
            num_scalar_prefetch=1,
            grid=(steps,),
            in_specs=specs,
            out_specs=out_specs,
            scratch_shapes=scratch,
        ),
        out_shape=outs,
        compiler_params=VMEM_BIG,
        cost_estimate=matmul_cost(rows, steps * width, hidden),
        name='dn',
    )(*args)


def paste_kernel(places_of, core_ref, recv_ref, _, out_ref, sems):
    row = pl.program_id(Z) * recv_ref.shape[0]
    copies = list(column_copies(recv_ref, out_ref, lambda i: sems.at[i], row, places_of(1 - core_ref[Z])))
    start_all(copies)
    wait_all(copies)


def paste_columns(core, places_of, recv, whole):
    hidden, block = recv.shape
    rows = 2 * BLK
    return pl.pallas_call(
        functools.partial(paste_kernel, places_of),
        grid_spec=pltpu.PrefetchScalarGridSpec(
            num_scalar_prefetch=1,
            grid=(hidden // rows,),
            in_specs=[pl.BlockSpec((rows, block), lambda m, core: (m, Z)), ANY],
            out_specs=ANY,
            scratch_shapes=[dma_sems(8)],
        ),
        out_shape=jax.ShapeDtypeStruct(whole.shape, F32),
        input_output_aliases={2: 0},
        compiler_params=VMEM_BIG,
        name='paste',
    )(core, recv, whole)


def output_kernel(n_chip, core_ref, mine_ref, theirs_ref, shared_ref, other_ref, w_ref, w_shared_ref, na_ref, nb_ref, b_ref, out_ref, acc):
    j, last = pl.program_id(Z), pl.num_programs(Z) - 1
    rows = acc.shape[0]

    def add(ref, weight_ref):
        acc[...] += dot_nn(ref[...].reshape(rows, -1), weight_ref[...])

    @pl.when(j == Z)
    def _():
        acc[...] = jnp.broadcast_to(b_ref[...].astype(F32), acc.shape)

    pl.when(j < n_chip)(functools.partial(add, mine_ref, w_ref))
    pl.when(jnp.logical_and(j >= n_chip, j < CORES * n_chip))(functools.partial(add, theirs_ref, w_ref))
    pl.when(j == last - 1)(functools.partial(add, shared_ref, w_shared_ref))

    @pl.when(j == last)
    def _():
        add(other_ref, w_shared_ref)
        for half, n_ref in enumerate((na_ref, nb_ref)):
            at = part(half, n_ref.shape[0])
            out_ref[at] = (ALPHA * n_ref[...].astype(F32) + acc[at]).astype(BF16)


def project_out(core, ctx_par, ctx_recv, ctx_shared, shared_recv, w_o, n_halves, b_o):
    n_chip, rows, cols = ctx_recv.shape
    shared = shared_recv.shape[1]
    hidden = w_o.shape[1]
    base = CORES * n_chip * cols // shared
    steps = CORES * n_chip + CORES
    split = (CORES, CORES * n_chip, rows // CORES)

    def dist_index(j, core):
        at = jnp.minimum(j, CORES * n_chip - 1)
        return CORES * lax.rem(at, n_chip) + jnp.where(at < n_chip, core[Z], 1 - core[Z])

    def shared_index(j, core):
        return base + jnp.where(j < steps - 1, core[Z], 1 - core[Z])

    whole, half = [pl.BlockSpec((size, hidden), lambda j, core: (Z, Z)) for size in (rows, rows // CORES)]
    return pl.pallas_call(
        functools.partial(output_kernel, n_chip),
        grid_spec=pltpu.PrefetchScalarGridSpec(
            num_scalar_prefetch=1,
            grid=(steps,),
            in_specs=[
                pl.BlockSpec((1, CORES, 1, rows // CORES, cols), lambda j, core: (jnp.minimum(j, n_chip - 1), Z, core[CORES], Z, Z)),
                pl.BlockSpec((1, rows, cols), lambda j, core: (jnp.clip(j - n_chip, 0, n_chip - 1), Z, Z)),
                pl.BlockSpec((CORES, 1, rows // CORES, shared), lambda j, core: (Z, core[CORES], Z, Z)),
                pl.BlockSpec((rows, shared), lambda j, core: (Z, Z)),
                pl.BlockSpec((cols, hidden), lambda j, core: (dist_index(j, core), Z)),
                pl.BlockSpec((shared, hidden), lambda j, core: (shared_index(j, core), Z)),
                half, half,
                pl.BlockSpec((1, hidden), lambda j, core: (Z, Z)),
            ],
            out_specs=whole,
            scratch_shapes=[pltpu.VMEM((rows, hidden), F32)],
        ),
        out_shape=jax.ShapeDtypeStruct((rows, hidden), BF16),
        compiler_params=VMEM_BIG,
        cost_estimate=matmul_cost(rows, hidden, hidden),
        name='out_proj',
    )(core, ctx_par.reshape(n_chip, *split, cols), ctx_recv, ctx_shared.reshape(*split, shared), shared_recv, w_o, w_o, *n_halves, b_o)


def together(*values):
    return lax.optimization_barrier(values)


def solution(mesh):
    n_dev = mesh.shape['sp']
    tok_spec = P('dp', 'sp', None)
    pos_spec = P('dp', 'sp')
    in_specs = (tok_spec, pos_spec, pos_spec, P('dp'), P(), P(), P(), P(), P(), P(), tok_spec)
    out_specs = (tok_spec, tok_spec, P('dp'), P('dp'), P('dp', None), P('dp'), P('dp', None), P('dp'))
    same_core = [list(range(core, n_dev, 2)) for core in range(2)]
    partners = [(dev, dev ^ 1) for dev in range(n_dev)]
    n_chip = n_dev // 2

    def device_step(hidden_in, pos_ids, block_pos, prefix_len, ln_gamma, ln_beta, w_qkv, b_qkv, w_o, b_o, grad_out):
        batch, local_len, hidden = hidden_in.shape
        per_half = batch // 2
        heads = hidden // HEAD
        n_dist, n_shared = (heads - SHARED) // n_dev, SHARED // 2
        shared_at = n_dev * n_dist
        rows = batch * local_len
        tokens = n_dev * rows
        rank = lax.axis_index('sp')
        parity = lax.rem(rank, SLOTS)
        pair = rank + 1 - 2 * parity
        core = jnp.stack([parity, pair, rank]).astype(jnp.int32)
        gather = functools.partial(lax.all_gather, axis_name='sp')
        gather_core = functools.partial(lax.all_gather, axis_name='sp', axis_index_groups=same_core)
        to_partner = functools.partial(lax.ppermute, axis_name='sp', perm=partners)

        def token_rows(arr, dev):
            split = arr.reshape(arr.shape[:-2] + (2, n_dev, rows // 2, arr.shape[-1]))
            return lax.dynamic_index_in_dim(split, dev, axis=split.ndim - 3, keepdims=False).reshape(arr.shape[:-2] + (rows, arr.shape[-1]))

        def places(head):
            return lambda par: [((2 * c + par) * n_dist + head) * WIDTH for c in range(n_chip)]

        def shared_places(par):
            return [(shared_at + par * n_shared + i) * WIDTH for i in range(n_shared)]

        def wo_tile(t, par):
            spread = t - n_shared
            return jnp.where(t < n_shared, shared_at + par * n_shared + t, (2 * (spread // n_dist) + par) * n_dist + lax.rem(spread, n_dist))

        halves = range(2)
        x_flat, gain = hidden_in.reshape(rows, hidden), ln_gamma.reshape(1, hidden)
        n_own = [normalize(half, x_flat, gain, ln_beta.reshape(1, hidden)) for half in halves]
        dy_own = [grad_out[part(half, per_half)] for half in halves]
        n_own[1], *dy_own = together(n_own[1], *dy_own)
        n_own = [own.reshape(per_half, local_len, hidden) for own in n_own]
        n_a, n_b, dy_a, dy_b = [gather(send) for send in n_own + dy_own]
        cos, sin = rope_tables(prefix_len, n_dev * local_len)
        prefix = [prefix_len[part(half, per_half)] for half in halves]
        starts = jnp.stack([rank * n_dist, shared_at + parity * n_shared, rank, pair]).astype(jnp.int32)
        bias = jnp.concatenate([
            lax.dynamic_slice_in_dim(b_qkv, starts[0] * WIDTH, n_dist * WIDTH),
            lax.dynamic_slice_in_dim(b_qkv, starts[1] * WIDTH, n_shared * WIDTH)]).astype(F32).reshape(1, -1)
        grad_bo = jnp.sum(grad_out.astype(F32), axis=(0, 1))
        n_chip_rows = [own[None] for own in n_own + [to_partner(own) for own in n_own]]
        qkv_own = project_qkv(starts, n_dist, n_shared, n_chip_rows, w_qkv, bias, cos, sin)
        d_ctx_own = context_grad(starts, n_dist, n_shared, [own[None] for own in (grad_out, to_partner(grad_out))], w_o, n_dev)
        n_a, grad_bo, *d_ctx_own = together(n_a, grad_bo, *d_ctx_own)

        ctx_d = ctx_r = None
        qkv, lses = [], []
        for half in halves:
            if half:
                n_b, ctx_r = together(n_b, ctx_r)
            qd, kd, vd, qr, kr, vr = project_qkv(
                starts, n_dist, n_shared, [n_b if half else n_a], w_qkv, bias, cos, sin, half, qkv_own[part(half, QKV_IN)])
            ctx_d, lse_d = attention_forward(half, prefix[half], qd, kd, vd, n_dev, ctx_d)
            qr, ctx_d = together(qr, ctx_d)
            ctx_r, lse_r = attention_forward(half, prefix[half], qr, kr, vr, n_dev, ctx_r)
            qkv.append((qd, kd, vd, qr, kr, vr))
            lses.append((lse_d, lse_r))
        ctx_par = gather_core(ctx_d.reshape(tokens, n_dist * HEAD))

        dy_a, ctx_r = together(dy_a, ctx_r)
        g_d, g_r = [], []
        sums = []
        for half in halves:
            if half:
                dy_b, *g_r = together(dy_b, *g_r)
            qd, kd, vd, qr, kr, vr = qkv[half]
            d_ctx, d_ctx_r = context_grad(starts, n_dist, n_shared, [dy_b if half else dy_a], w_o, n_dev, d_ctx_own[part(half, CORES)])
            *g_d, sum_d = attention_backward(half, n_dist, prefix[half], qd, kd, vd, ctx_d, d_ctx, lses[half][0], cos, sin, g_d)
            qr, *g_d = together(qr, *g_d)
            *g_r, sum_r = attention_backward(half, n_shared, prefix[half], qr, kr, vr, ctx_r, d_ctx_r, lses[half][1], cos, sin, g_r)
            sums.append(jnp.sum(jnp.concatenate([sum_d, sum_r]), axis=(1, 2)).reshape(-1))
        g_par = [gather_core(g.reshape(tokens, WIDTH)) for g in g_d]
        g_r = [g.reshape(1, tokens, WIDTH) for g in g_r]

        n_a, n_b, dy_a, dy_b = [part.reshape(tokens // 2, hidden) for part in (n_a, n_b, dy_a, dy_b)]
        ctx_r = ctx_r.reshape(tokens, n_shared * HEAD)
        shared_recv = to_partner(token_rows(ctx_r, pair))
        ctx_r, *g_r = together(ctx_r, *g_r)
        grad_wo, wo_block = weight_grad_o(
            core, ctx_r[None], dy_a, dy_b, lambda c, par: (shared_at + par * n_shared) * HEAD, lambda c: 0, hidden // 2, ())
        shared_recv, wo_block, n_a = together(shared_recv, wo_block, n_a)
        grad_wqkv, block, r_send = weight_grad_qkv(core, shared_places, n_a, n_b, g_r, None)
        r_recv, ctx_recv = to_partner(r_send), to_partner(token_rows(ctx_par, pair))
        ctx_par, block = together(ctx_par, block)
        recv_r = to_partner(block)
        grad_wo, wo_block = weight_grad_o(
            core, ctx_par, dy_a, dy_b, lambda c, par: (2 * c + par) * (n_dist * HEAD), lambda c: (n_shared + c * n_dist) * HEAD,
            hidden // 2, (grad_wo, wo_block))
        ctx_recv, wo_block, recv_r, r_recv = together(ctx_recv, wo_block, recv_r, r_recv)
        wo_recv = to_partner(wo_block)
        hidden_out = project_out(
            core, ctx_par, ctx_recv, ctx_r, shared_recv, w_o, [own.reshape(-1, hidden) for own in n_own], b_o.reshape(1, hidden))
        n_a, hidden_out, g_par[0] = together(n_a, hidden_out, g_par[0])

        def columns(table):
            at = [np.array([h * WIDTH for h in table(par)] + [0], np.int32) for par in range(2)]
            last = (np.arange(at[0].size) == at[0].size - 1).astype(np.int32)
            return jnp.asarray(at[0]) + parity.astype(jnp.int32) * jnp.asarray(at[1] - at[0]) + rank.astype(jnp.int32) * jnp.asarray(last)

        def spread_grad(head, whole, **extra):
            whole, block, tok, *rest = weight_grad_qkv(core, places(head), n_a, n_b, [g_par[head]], whole, **extra)
            tok = to_partner(tok)
            if head:
                tok, block = together(tok, block)
            return whole, tok, to_partner(block), rest

        grad_wqkv, tok_0, recv_0, _ = spread_grad(0, grad_wqkv, pastes=[(recv_r, shared_places)])
        g_r[0], grad_wqkv = together(g_r[0], grad_wqkv)
        cols = columns(lambda mine: [shared_at + par * n_shared + i for par in (mine, 1 - mine) for i in range(n_shared)])
        runs = [(i, 0) for i in range(n_shared)] + [(n_shared, i) for i in range(n_shared)]
        d_norm, = normed_grad(cols, runs, [*g_r, r_recv], w_qkv, grad_out.reshape(rows, hidden))
        g_par[1], d_norm = together(g_par[1], d_norm)
        wo_recv, tok_0 = together(wo_recv, tok_0)
        grad_wqkv, tok_1, recv_1, (grad_wo,) = spread_grad(1, grad_wqkv, wo=(wo_recv, grad_wo, wo_tile))
        cols = columns(lambda mine: [(2 * c + par) * n_dist + head for par in (mine, 1 - mine) for c in range(n_chip) for head in (0, 1)])
        runs = [(CORES * side + head, c) for side in range(CORES) for c in range(n_chip) for head in (0, 1)]
        tok_1, recv_0 = together(tok_1, recv_0)
        d_norm, = normed_grad(cols, runs, [g_par[0], g_par[1], tok_0, tok_1], w_qkv, d_norm)
        n_a, d_norm, g_par[2] = together(n_a, d_norm, g_par[2])
        grad_wqkv, tok_2, recv_2, _ = spread_grad(2, grad_wqkv, pastes=[(recv_0, places(0)), (recv_1, places(1))])
        cols = columns(lambda mine: [(2 * c + par) * n_dist + 2 for c in range(n_chip) for par in (mine, 1 - mine)])
        grad_in, norm_sums = normed_grad(
            cols, [(src, c) for c in range(n_chip) for src in range(2)], [g_par[2], tok_2], w_qkv, d_norm, norm=(x_flat, gain))
        small = gather(jnp.concatenate([sums[0] + sums[1], norm_sums.reshape(-1), grad_bo, jnp.zeros((WIDE_GATHER,), F32)]))
        grad_wqkv = paste_columns(core, places(2), recv_2, grad_wqkv)
        small, grad_wqkv = together(small, grad_wqkv)
        spread, shared = small[:, :n_dist * WIDTH], small[:2, n_dist * WIDTH:(n_dist + n_shared) * WIDTH]
        grad_bqkv = jnp.concatenate([spread.reshape(-1), shared.reshape(-1)])
        grad_gamma, grad_beta, grad_bo = jnp.sum(small[:, (n_dist + n_shared) * WIDTH:-WIDE_GATHER], axis=0).reshape(3, hidden)
        shape = (batch, local_len, hidden)
        return (hidden_out.reshape(shape), grad_in.reshape(shape), grad_gamma, grad_beta, grad_wqkv, grad_bqkv, grad_wo, grad_bo)

    return jax.shard_map(device_step, mesh=mesh, in_specs=in_specs, out_specs=out_specs, check_vma=False)
```

```python
import functools
import math
import jax
import jax.numpy as jnp
import numpy as np
from jax import lax
from jax.experimental import pallas as pl
from jax.experimental.pallas import tpu as pltpu
from jax.sharding import PartitionSpec as P

HEAD = 128
QUARTER = 32
ALPHA = math.sqrt(56.0)
LN_EPS = 1e-5
ROT_BASE = 10000.0
SCALE = 1.0 / math.sqrt(HEAD)
LOG2E = math.log2(math.e)
MASK_FILL = -1e30
BLK = 256
VMEM_BIG = pltpu.CompilerParams(vmem_limit_bytes=62 << 20)
SHARED = 8
Z = 0
SLOTS = CORES = 2
WIDTH = 3 * HEAD
F32 = jnp.float32
BF16 = jnp.bfloat16


def dot(lhs, rhs, lhs_dim, rhs_dim):
    return lax.dot_general(lhs, rhs, (((lhs_dim,), (rhs_dim,)), ((), ())), preferred_element_type=F32)


def dot_nn(lhs, rhs):
    return dot(lhs, rhs, 1, 0)


def dot_nt(lhs, rhs):
    return dot(lhs, rhs, 1, 1)


def dot_tn(lhs, rhs):
    return dot(lhs, rhs, 0, 0)


def matmul_cost(rows, depth, cols, extra=0):
    return pl.CostEstimate(
        flops=2 * rows * depth * cols, bytes_accessed=2 * (rows * depth + depth * cols + rows * cols) + extra, transcendentals=0)


def attention_cost(n_head, batch, seq, products):
    pairs = n_head * batch * seq * seq
    return pl.CostEstimate(flops=2 * products * pairs * HEAD, bytes_accessed=8 * products * n_head * batch * seq * HEAD, transcendentals=pairs)


def run(index, size):
    return pl.ds(pl.multiple_of(index * size, size), size)


def part(index, size):
    return slice(index * size, (index + 1) * size)


def rope_tables(prefix_len, seq):
    tok = jnp.arange(seq, dtype=jnp.int32)[None, :]
    pre = prefix_len[:, None]
    inside = tok < pre
    pos = jnp.where(inside, tok, pre - 1)
    blk = jnp.where(inside, 0, tok - pre + 1)
    inv_freq = ROT_BASE ** (-jnp.arange(QUARTER, dtype=F32) / QUARTER)
    angles = jnp.stack([pos, blk], axis=-1).astype(F32)[..., None] * inv_freq
    cos, sin = jnp.cos(angles), jnp.sin(angles)
    shape = pos.shape + (HEAD,)
    return (jnp.stack([cos, cos], axis=-2).reshape(shape), jnp.stack([-sin, sin], axis=-2).reshape(shape))


def turn(x, cos, sin):
    lane = lax.broadcasted_iota(jnp.int32, x.shape, 1)
    other = jnp.where(lane % (2 * QUARTER) < QUARTER, pltpu.roll(x, HEAD - QUARTER, 1), pltpu.roll(x, QUARTER, 1))
    return x * cos + other * sin


def dma_sems(*shape):
    return pltpu.SemaphoreType.DMA(shape)


def dma_sems(*shape):
    return pltpu.SemaphoreType.DMA(shape)


def start_all(copies):
    for copy in copies:
        copy.start()


def wait_all(copies):
    for copy in copies:
        copy.wait()


ANY = pl.BlockSpec(memory_space=pl.ANY)
PIECES = 4
QKV_IN = 6


NORM_ROWS = 32


def centred(x):
    x = x.astype(F32)
    x = x - jnp.mean(x, axis=-1, keepdims=True)
    return x, lax.rsqrt(jnp.mean(x * x, axis=-1, keepdims=True) + LN_EPS)


def norm_kernel(x_ref, gain_ref, shift_ref, out_ref):
    gain, shift = gain_ref[...].astype(F32), shift_ref[...].astype(F32)

    @pl.loop(0, x_ref.shape[0] // NORM_ROWS)
    def _(i):
        rows = run(i, NORM_ROWS)
        x, inv = centred(x_ref[rows])
        out_ref[rows] = (x * inv * gain + shift).astype(BF16)


def normalize(half, x, gain, shift):
    rows, hidden = x.shape
    block = rows // 4
    vec = pl.BlockSpec((1, hidden), lambda i: (Z, Z))
    return pl.pallas_call(
        norm_kernel,
        grid=(2,),
        in_specs=[pl.BlockSpec((block, hidden), lambda i: (2 * half + i, Z)), vec, vec],
        out_specs=pl.BlockSpec((block, hidden), lambda i: (i, Z)),
        out_shape=jax.ShapeDtypeStruct((2 * block, hidden), BF16),
        compiler_params=VMEM_BIG,
        name='norm',
    )(x, gain, shift)


def qkv_kernel(n_dist, n_tile, n_in, start_ref, *rest):
    n_refs, (w_ref, b_ref, cos_ref, sin_ref, *outs), (w_buf, acc, sems) = rest[:n_in], rest[n_in:-3], rest[-3:]
    first, later = n_refs[:(n_in + 1) // CORES], n_refs[n_in // CORES:]
    _, rows, cols = acc.shape
    hidden = w_ref.shape[0]
    dist = n_dist * WIDTH
    step, last = pl.program_id(Z), pl.num_programs(Z) - 1
    slot = lax.rem(step, SLOTS)
    piece = hidden // PIECES
    tile = first[0].shape[-2]

    def loads(i):
        span = run(i, piece)
        for kind, (at, width) in enumerate(((0, dist), (dist, cols - dist))):
            col = pl.multiple_of(start_ref[kind] * WIDTH, HEAD)
            yield pltpu.make_async_copy(w_ref.at[span, pl.ds(col, width)], w_buf.at[span, pl.ds(at, width)], sems.at[i, kind])

    def finish():
        for i in range(rows // tile):
            group, batch, at, table = n_tile(i)
            cos, sin = cos_ref[table, part(at, tile)], sin_ref[table, part(at, tile)]
            for h in range(cols // WIDTH):
                kind, head = (0, h) if h < n_dist else (1, h - n_dist)
                refs = outs[part(CORES * group + kind, 3)]
                pre = [acc[1 - slot, part(i, tile), part(3 * h + j, HEAD)] + b_ref[:, part(3 * h + j, HEAD)] for j in range(3)]
                for ref, val in zip(refs, (turn(pre[0], cos, sin), turn(pre[1], cos, sin), pre[2])):
                    ref[head, batch, part(at, tile)] = val.astype(BF16)

    @pl.when(step == Z)
    def _():
        for i in range(PIECES):
            start_all(loads(i))
        acc[slot] = jnp.zeros((rows, cols), F32)

        @pl.loop(0, PIECES)
        def _(i):
            wait_all(loads(i))
            span = run(i, piece)
            for i, ref in enumerate(first):
                acc[slot, part(i, rows // len(first))] += dot_nn(ref[:, :, :, span].reshape(-1, piece), w_buf[span])

    @pl.when(jnp.logical_and(step > 0, step < last))
    def _():
        finish()
        for i, ref in enumerate(later):
            acc[slot, part(i, rows // len(later))] = dot_nn(ref[...].reshape(-1, hidden), w_buf[...])

    pl.when(step == last)(finish)


def project_qkv(starts, n_dist, n_shared, n_rows, w_qkv, bias, cos, sin, half=None, earlier=None):
    _, per_half, local_len, hidden = n_rows[0].shape
    _, seq, _ = cos.shape
    cols = (n_dist + n_shared) * WIDTH
    own = earlier is None
    batch = per_half * CORES if own else per_half
    steps = CORES if own else seq // local_len // CORES - 1
    n_chip = seq // local_len // CORES
    width = local_len if own else CORES * local_len

    def place(step, at):
        return at[CORES + step] if own else lax.rem(at[CORES] // CORES + 1 + step, n_chip)

    def ahead(step, at):
        return place(jnp.minimum(step, steps - 1), at)

    def behind(step, at):
        return place(jnp.maximum(step - 1, 0), at)

    shapes = [jax.ShapeDtypeStruct((n_head, per_half, seq, HEAD), BF16) for n_head in (n_dist, n_shared) for _ in range(3)]
    shapes = shapes * CORES if own else shapes
    tab_spec = pl.BlockSpec((batch, width, HEAD), lambda step, at: (Z if own else half, behind(step, at), Z))
    arrays = [] if own else list(earlier)

    def own_tile(i):
        return i // per_half, i % per_half, 0, i

    def other_tile(i):
        return 0, i % per_half, i // per_half, i % per_half

    return pl.pallas_call(
        functools.partial(without, len(arrays), len(n_rows) + 5, functools.partial(qkv_kernel, n_dist, own_tile if own else other_tile, len(n_rows))),
        grid_spec=pltpu.PrefetchScalarGridSpec(
            num_scalar_prefetch=1,
            grid=(steps + 1,),
            in_specs=[
                *[pl.BlockSpec((1 if own else CORES, per_half, local_len, hidden), lambda step, at: (Z if own else ahead(step, at), Z, Z, Z))] * len(n_rows),
                ANY,
                pl.BlockSpec((1, cols), lambda step, at: (Z, Z)),
                tab_spec, tab_spec,
            ] + [ANY] * len(arrays),
            out_specs=[pl.BlockSpec(shape.shape[:CORES] + (width, HEAD), lambda step, at: (Z, Z, behind(step, at), Z)) for shape in shapes],
            scratch_shapes=[
                pltpu.VMEM((hidden, cols), BF16), pltpu.VMEM((SLOTS, CORES * CORES * local_len, cols), F32), dma_sems(PIECES, SLOTS)],
        ),
        out_shape=shapes,
        input_output_aliases={QKV_IN + i: i for i in range(len(arrays))},
        compiler_params=VMEM_BIG,
        cost_estimate=matmul_cost(steps * CORES * batch * local_len, hidden, cols),
        name='qkv',
    )(starts, *n_rows, w_qkv, bias, cos, sin, *arrays)


def without(count, start, kernel, *refs):
    kernel(*refs[:start], *refs[start + count:])


def forward_kernel(pre_ref, q_ref, k_ref, v_ref, *rest):
    ctx_ref, lse_ref = rest[-2:]
    n_head, _, seq, _ = q_ref.shape
    local_len = ctx_ref.shape[3]
    per = BLK // local_len
    prefix = pre_ref[pl.program_id(1)]

    def block(r, n_key):
        query = lax.broadcasted_iota(jnp.int32, (1, BLK), 1) + r * BLK
        last = jnp.maximum(query, prefix - 1) - (n_key - 1) * BLK
        scores = []
        for h in range(n_head):
            q_blk = q_ref[h, 0, part(r, BLK)]
            parts = [dot_nt(k_ref[h, 0, part(c, BLK)], q_blk) * (SCALE * LOG2E) for c in range(n_key)]
            key = lax.broadcasted_iota(jnp.int32, (BLK, BLK), 0)
            parts[-1] = jnp.where(key <= last, parts[-1], MASK_FILL)
            scores.append(parts)
        for h, parts in enumerate(scores):
            top = functools.reduce(jnp.maximum, [jnp.max(p, axis=0, keepdims=True) for p in parts])
            parts = [jnp.exp2(p - top) for p in parts]
            total = functools.reduce(jnp.add, [jnp.sum(p, axis=0, keepdims=True) for p in parts])
            inv = 1.0 / total
            probs = jnp.concatenate([(p * inv).astype(BF16) for p in parts], axis=0)
            ctx_t = dot_tn(v_ref[h, 0, :n_key * BLK], probs)
            ctx = ctx_t.T.astype(BF16).reshape(per, local_len, HEAD)
            ctx_ref[0, part(r, per), 0, :, part(h, HEAD)] = ctx
            lse_ref[h, 0, :, part(r, BLK)] = top + jnp.log2(total)

    n_blk = seq // BLK
    for r in range(n_blk):
        for n_key in range(r + 1, n_blk + 1):
            low = (n_key - 1) * BLK
            cond = prefix <= n_key * BLK if n_key == r + 1 else prefix > low
            if n_key < n_blk and n_key > r + 1:
                cond = jnp.logical_and(cond, prefix <= n_key * BLK)
            if n_key == n_blk and n_key == r + 1:
                block(r, n_key)
            else:
                pl.when(cond)(functools.partial(block, r, n_key))


def attention_forward(half, prefix_half, q, k, v, n_dev, ctx):
    own, batch, seq, _ = q.shape
    local_len = seq // n_dev
    group = own
    qkv_spec = pl.BlockSpec((group, 1, seq, HEAD), lambda h, b, pre: (h, b, Z, Z))
    earlier = [] if ctx is None else [ctx]
    return pl.pallas_call(
        forward_kernel,
        grid_spec=pltpu.PrefetchScalarGridSpec(
            num_scalar_prefetch=1,
            grid=(own // group, batch),
            in_specs=[qkv_spec] * 3 + [ANY] * len(earlier),
            out_specs=[
                pl.BlockSpec((1, n_dev, 1, local_len, group * HEAD), lambda h, b, pre: (half, Z, b, Z, h)),
                pl.BlockSpec((group, 1, 1, seq), lambda h, b, pre: (h, b, Z, Z)),
            ],
        ),
        out_shape=[
            jax.ShapeDtypeStruct((2, n_dev, batch, local_len, own * HEAD), BF16),
            jax.ShapeDtypeStruct((own, batch, 1, seq), F32),
        ],
        input_output_aliases={4: 0} if earlier else {},
        compiler_params=VMEM_BIG,
        cost_estimate=attention_cost(own, batch, seq, 2),
        name='attn_fwd',
    )(prefix_half, q, k, v, *earlier)


def d_ctx_kernel(n_in, start_ref, *rest):
    dy_refs, (w_ref, *outs), (w_buf, sems) = rest[:n_in], rest[n_in:-2], rest[-2:]
    step, hidden = pl.program_id(Z), w_ref.shape[1]
    widths = [outs[0].shape[-1], outs[1].shape[-1]]

    def loads():
        for kind, (at, width) in enumerate(zip((0, widths[0]), widths)):
            row = pl.multiple_of(start_ref[kind] * HEAD, HEAD)
            yield pltpu.make_async_copy(w_ref.at[pl.ds(row, width)], w_buf.at[pl.ds(at, width)], sems.at[kind])

    @pl.when(step == Z)
    def _():
        start_all(loads())
        wait_all(loads())

    def multiply(dy_ref):
        res = dot_nt(dy_ref[...].reshape(-1, hidden), w_buf[...]).astype(BF16)
        rows = CORES * res.shape[0] // len(outs)
        for i, out_ref in enumerate(outs):
            cols = slice(widths[0], None) if i % CORES else slice(widths[0])
            out_ref[...] = res[part(i // CORES, rows), cols].reshape(out_ref.shape)

    if n_in > 1:
        for i, dy_ref in enumerate(dy_refs):
            pl.when(step == i)(functools.partial(multiply, dy_ref))
    else:
        multiply(dy_refs[0])


def context_grad(starts, n_dist, n_shared, dy_rows, w_o, n_dev, earlier=()):
    _, batch, local_len, hidden = dy_rows[0].shape
    own = not earlier
    n_chip = n_dev // CORES
    per_half, devs = (batch // CORES, 1) if own else (batch, CORES)

    def block(step, at):
        return (at[CORES + step] if own else lax.rem(at[CORES] // CORES + 1 + step, n_chip), Z, Z, Z)

    cols = [n_dist * HEAD, n_shared * HEAD]
    outs = cols * (CORES if own else 1)
    n_in = len(dy_rows)
    return pl.pallas_call(
        functools.partial(without, len(earlier), n_in + 2, functools.partial(d_ctx_kernel, n_in)),
        grid_spec=pltpu.PrefetchScalarGridSpec(
            num_scalar_prefetch=1,
            grid=(CORES if own else n_chip - 1,),
            in_specs=[pl.BlockSpec((devs, batch, local_len, hidden), (lambda step, at: (Z, Z, Z, Z)) if own else block)] * n_in + [ANY] * (1 + len(earlier)),
            out_specs=[pl.BlockSpec((devs, per_half, local_len, width), block) for width in outs],
            scratch_shapes=[pltpu.VMEM((sum(cols), hidden), BF16), dma_sems(CORES)],
        ),
        out_shape=[jax.ShapeDtypeStruct((n_dev, per_half, local_len, width), BF16) for width in outs],
        input_output_aliases={3 + i: i for i in range(len(earlier))},
        compiler_params=VMEM_BIG,
        cost_estimate=matmul_cost(n_dev * batch * local_len, hidden, sum(cols)),
        name='dctx',
    )(starts, *dy_rows, w_o, *earlier)


def backward_kernel(pre_ref, q_ref, k_ref, v_ref, ctx_ref, dctx_ref, lse_ref, cos_ref, sin_ref, *rest):
    sum_ref, dq_acc, dk_acc, dv_acc = rest[-4:]
    n_head, _, seq, _ = q_ref.shape
    g_refs = rest[-4 - n_head:-4]
    _, n_dev, _, local_len, _ = g_refs[0].shape
    n_blk = seq // BLK
    prefix = pre_ref[pl.program_id(Z)]
    d_ctx, delta = [], []
    for h in range(n_head):
        lanes = part(h, HEAD)
        grad = dctx_ref[:, :, :, lanes].reshape(seq, HEAD)
        prod = grad.astype(F32) * ctx_ref[0, :, :, :, lanes].reshape(seq, HEAD).astype(F32)
        d_ctx.append(grad)
        delta.append(jnp.sum(prod.T, axis=0, keepdims=True))

    def block(c, first):
        span = part(c, BLK)
        start = first * BLK
        products = []
        for h in range(n_head):
            s_t = dot_nt(k_ref[h, 0, span], q_ref[h, 0, start:])
            dp_t = dot_nt(v_ref[h, 0, span], d_ctx[h][start:])
            products.append((s_t, dp_t))
        for h, (s_t, dp_t) in enumerate(products):
            probs, d_scores = [], []
            for r in range(first, n_blk):
                cols, here = part(r, BLK), part(r - first, BLK)
                piece = s_t[:, here] * (SCALE * LOG2E)
                if r <= c:
                    key = lax.broadcasted_iota(jnp.int32, (BLK, BLK), 0)
                    query = lax.broadcasted_iota(jnp.int32, (1, BLK), 1) + r * BLK
                    piece = jnp.where(key <= jnp.maximum(query, prefix - 1) - c * BLK, piece, MASK_FILL)
                p = jnp.exp2(piece - lse_ref[h, 0, :, cols])
                probs.append(p.astype(BF16))
                d_scores.append((p * (dp_t[:, here] - delta[h][:, cols]) * SCALE).astype(BF16))
            probs = jnp.concatenate(probs, axis=1)
            d_scores = jnp.concatenate(d_scores, axis=1)
            dv_acc[h, span] = dot_nn(probs, d_ctx[h][start:])
            dk_acc[h, span] = dot_nn(d_scores, q_ref[h, 0, start:])
            dq_part = dot_tn(k_ref[h, 0, span], d_scores)
            if c:
                dq_acc[h, :, start:] += dq_part
            else:
                dq_acc[h] = dq_part

    block(0, 0)
    for c in range(1, n_blk):
        pl.when(prefix > c * BLK)(functools.partial(block, c, 0))
        pl.when(prefix <= c * BLK)(functools.partial(block, c, c))

    cos, sin = cos_ref[Z], sin_ref[Z]
    for h in range(n_head):
        g_q = turn(dq_acc[h].T.astype(BF16).astype(F32), cos, -sin)
        g_k = turn(dk_acc[h].astype(BF16).astype(F32), cos, -sin)
        g_v = dv_acc[h].astype(BF16).astype(F32)
        for i, g in enumerate((g_q, g_k, g_v)):
            lanes = part(i, HEAD)
            g_refs[h][0, :, 0, :, lanes] = g.astype(BF16).reshape(n_dev, local_len, HEAD)
            sum_ref[h, 0, :, lanes] = jnp.sum(g, axis=0, keepdims=True)


def attention_backward(half, group, prefix_half, q, k, v, ctx, d_ctx, lse, cos, sin, earlier):
    _, batch, seq, _ = q.shape
    _, n_dev, _, local_len, _ = ctx.shape
    qkv_spec = pl.BlockSpec((group, 1, seq, HEAD), lambda b, pre: (Z, b, Z, Z))
    tab_spec = pl.BlockSpec((1, seq, HEAD), lambda b, pre: (half * batch + b, Z, Z))
    stat = functools.partial(pltpu.VMEM, dtype=F32)
    return pl.pallas_call(
        backward_kernel,
        grid_spec=pltpu.PrefetchScalarGridSpec(
            num_scalar_prefetch=1,
            grid=(batch,),
            in_specs=[qkv_spec] * 3 + [
                pl.BlockSpec((1, n_dev, 1, local_len, group * HEAD), lambda b, pre: (half, Z, b, Z, Z)),
                pl.BlockSpec((n_dev, 1, local_len, group * HEAD), lambda b, pre: (Z, b, Z, Z)),
                pl.BlockSpec((group, 1, 1, seq), lambda b, pre: (Z, b, Z, Z)), tab_spec, tab_spec] + [ANY] * len(earlier),
            out_specs=[pl.BlockSpec((1, n_dev, 1, local_len, WIDTH), lambda b, pre: (half, Z, b, Z, Z))] * group + [
                pl.BlockSpec((group, 1, 1, WIDTH), lambda b, pre: (Z, b, Z, Z))],
            scratch_shapes=[stat((group, HEAD, seq)), stat((group, seq, HEAD)), stat((group, seq, HEAD))],
        ),
        out_shape=[jax.ShapeDtypeStruct((2, n_dev, batch, local_len, WIDTH), BF16)] * group + [
            jax.ShapeDtypeStruct((group, batch, 1, WIDTH), F32)],
        input_output_aliases={9 + i: i for i in range(len(earlier))},
        compiler_params=VMEM_BIG,
        cost_estimate=attention_cost(group, batch, seq, 5),
        name='attn_bwd',
    )(prefix_half, q, k, v, ctx, d_ctx, lse, cos, sin, *earlier)


def wo_grad_kernel(row_of, block_row_of, core_ref, ctx_ref, dya_ref, dyb_ref, *rest):
    out_ref, copy_ref, rhs, buf, rhs_sems, sems = rest[-6:]
    n, c = pl.program_id(Z), pl.program_id(1)
    n_col, n_grp = pl.num_programs(Z), pl.num_programs(1)
    step = n * n_grp + c
    slot, n_slot = lax.rem(step, SLOTS), lax.rem(n, SLOTS)
    _, rows, wide = buf.shape
    half = dya_ref.shape[0]
    core = core_ref[Z]

    def loads(n_at, at):
        for i, ref in enumerate((dya_ref, dyb_ref)):
            yield pltpu.make_async_copy(ref.at[:, run(n_at, wide)], rhs.at[at, run(i, half)], rhs_sems.at[at, i])

    def stores(at_step, at):
        n_at, c_at = at_step // n_grp, lax.rem(at_step, n_grp)
        for i, (ref, row) in enumerate(((out_ref, row_of(c_at, core)), (copy_ref, block_row_of(c_at)))):
            yield pltpu.make_async_copy(buf.at[at], ref.at[pl.ds(pl.multiple_of(row, HEAD), rows), run(n_at, wide)], sems.at[at, i])

    @pl.when(step == Z)
    def _():
        start_all(loads(0, 0))

    @pl.when(c == Z)
    def _():
        @pl.when(n + 1 < n_col)
        def _():
            start_all(loads(n + 1, 1 - n_slot))

        wait_all(loads(n, n_slot))

    @pl.when(step >= 2)
    def _():
        wait_all(stores(step - 2, slot))

    buf[slot] = dot_tn(ctx_ref[Z], rhs[n_slot])
    start_all(stores(step, slot))

    @pl.when(step == n_col * n_grp - 1)
    def _():
        wait_all(stores(step - 1, 1 - slot))
        wait_all(stores(step, slot))


def weight_grad_o(core, ctx_par, dy_a, dy_b, row_of, block_row_of, block_rows, earlier):
    n_grp, tokens, cols = ctx_par.shape
    hidden = dy_a.shape[1]
    wide = hidden // 4
    return pl.pallas_call(
        functools.partial(wo_grad_kernel, row_of, block_row_of),
        grid_spec=pltpu.PrefetchScalarGridSpec(
            num_scalar_prefetch=1,
            grid=(hidden // wide, n_grp),
            in_specs=[pl.BlockSpec((1, tokens, cols), lambda n, c, core: (c, Z, Z)), ANY, ANY] + [ANY] * len(earlier),
            out_specs=[ANY, ANY],
            scratch_shapes=[pltpu.VMEM((SLOTS, tokens, wide), BF16), pltpu.VMEM((SLOTS, cols, wide), F32), dma_sems(SLOTS, SLOTS), dma_sems(SLOTS, SLOTS)],
        ),
        out_shape=[jax.ShapeDtypeStruct((hidden, hidden), F32), jax.ShapeDtypeStruct((block_rows, hidden), F32)],
        input_output_aliases={4: 0, 5: 1} if earlier else {},
        compiler_params=VMEM_BIG,
        cost_estimate=matmul_cost(n_grp * cols, tokens, hidden, 8 * hidden * n_grp * cols),
        name='wo_grad',
    )(core, ctx_par, dy_a, dy_b, *earlier)


def column_copies(src, out_ref, sem_of, row, places):
    rows, width = src.shape[0], src.shape[1] // len(places)
    for i, col in enumerate(places):
        yield pltpu.make_async_copy(
            src.at[:, run(i, width)],
            out_ref.at[pl.ds(pl.multiple_of(row, BLK), rows), pl.ds(pl.multiple_of(col, HEAD), width)],
            sem_of(i))


def wqkv_grad_kernel(places_of, old_places, wo_tile, n_src, core_ref, na_ref, nb_ref, *rest):
    srcs, rest = rest[:n_src], list(rest[n_src:])
    groups = [ref.at[c] for ref in srcs for c in range(ref.shape[0])]
    recv_refs = [rest.pop(0) for _ in range(len(old_places) + bool(wo_tile))]
    n_buf, rhs, buf, n_sems, g_sems, out_sems, copy_sems, recv_sems, paste_sems, tok_sems, *recv_bufs = rest[-10 - len(recv_refs):]
    outs = rest[:-10 - len(recv_refs)][-4 if wo_tile else -3:]
    out_ref, copy_ref, tok_ref = outs[:3]
    m = pl.program_id(Z)
    n_m = pl.num_programs(Z)
    core, pair = core_ref[Z], core_ref[1]
    tokens, cols = groups[0].shape
    half, rows = tokens // 2, n_buf.shape[2]
    piece = tokens // PIECES
    slot = lax.rem(m, SLOTS)

    def n_loads(step, at):
        for i, ref in enumerate((na_ref, nb_ref)):
            yield pltpu.make_async_copy(ref.at[:, run(step, rows)], n_buf.at[at, run(i, half)], n_sems.at[at, i])

    def g_loads(i):
        for c, ref in enumerate(groups):
            yield pltpu.make_async_copy(ref.at[run(i, piece)], rhs.at[run(i, piece), run(c, cols)], g_sems.at[i, c])

    def stores(step, at):
        yield from column_copies(buf.at[at], out_ref, lambda i: out_sems.at[at, i], step * rows, places_of(core))
        yield pltpu.make_async_copy(buf.at[at], copy_ref.at[run(step, rows)], copy_sems.at[at])

    def recv_loads(step, at):
        for k, (ref, block) in enumerate(zip(recv_refs, recv_bufs)):
            yield pltpu.make_async_copy(ref.at[run(step, block.shape[1])], block.at[at], recv_sems.at[k, at])

    def pastes(step, at):
        for k, old_places_of in enumerate(old_places):
            yield from column_copies(recv_bufs[k].at[at], out_ref, lambda i: paste_sems.at[k, at, i], step * rows, old_places_of(1 - core))
        if wo_tile:
            tiles = recv_bufs[-1].shape[1] // HEAD
            for t in range(tiles):
                tile = wo_tile(step * tiles + t, 1 - core)
                yield pltpu.make_async_copy(recv_bufs[-1].at[at, run(t, HEAD)], outs[3].at[run(tile, HEAD)], paste_sems.at[len(old_places), at, t])

    def token_copies():
        size = tok_ref.shape[0] // 2
        for i in range(2):
            yield pltpu.make_async_copy(rhs.at[pl.ds(pl.multiple_of(i * half + pair * size, BLK), size)], tok_ref.at[run(i, size)], tok_sems.at[i])

    @pl.when(m == Z)
    def _():
        start_all(n_loads(0, 0))
        for i in range(PIECES):
            start_all(g_loads(i))

    @pl.when(m + 1 < n_m)
    def _():
        start_all(n_loads(m + 1, 1 - slot))

    @pl.when(m == 0)
    def _():
        start_all(recv_loads(m, slot))

    @pl.when(m > 0)
    def _():
        wait_all(pastes(m - 1, 1 - slot))

    @pl.when(m + 1 < n_m)
    def _():
        start_all(recv_loads(m + 1, 1 - slot))

    wait_all(recv_loads(m, slot))
    start_all(pastes(m, slot))

    @pl.when(m >= 2)
    def _():
        wait_all(stores(m - 2, slot))

    wait_all(n_loads(m, slot))

    @pl.when(m == Z)
    def _():
        buf[slot] = jnp.zeros((rows, rhs.shape[1]), F32)

        @pl.loop(0, PIECES)
        def _(i):
            wait_all(g_loads(i))
            buf[slot] += dot_tn(n_buf[slot, run(i, piece)], rhs[run(i, piece)])

        start_all(token_copies())

    @pl.when(m > 0)
    def _():
        buf[slot] = dot_tn(n_buf[slot], rhs[...])

    start_all(stores(m, slot))

    @pl.when(m == n_m - 1)
    def _():
        wait_all(stores(m - 1, 1 - slot))
        wait_all(stores(m, slot))
        wait_all(pastes(m, slot))
        wait_all(token_copies())


def weight_grad_qkv(core, places_of, n_a, n_b, srcs, whole, pastes=(), wo=None):
    hidden = n_a.shape[1]
    n_grp, (tokens, cols) = sum(src.shape[0] for src in srcs), srcs[0].shape[1:]
    width = n_grp * cols
    rows = 2 * BLK
    steps = hidden // rows
    args, specs, alias = [core, n_a, n_b, *srcs], [ANY] * (2 + len(srcs)), {}
    outs = [jax.ShapeDtypeStruct((hidden, 3 * hidden), F32), jax.ShapeDtypeStruct((hidden, width), F32), jax.ShapeDtypeStruct((2 * BLK, width), BF16)]
    wo_tile = None
    recvs = [recv for recv, _ in pastes] + ([wo[0]] if wo else [])
    args += recvs
    specs += [ANY] * len(recvs)
    if wo is not None:
        wo_recv, wo_whole, wo_tile = wo
        outs.append(jax.ShapeDtypeStruct(wo_whole.shape, F32))
    if whole is not None:
        alias[len(args)] = 0
        args.append(whole)
        specs.append(ANY)
    if wo is not None:
        alias[len(args)] = 3
        args.append(wo_whole)
        specs.append(ANY)
    return pl.pallas_call(
        functools.partial(wqkv_grad_kernel, places_of, [old for _, old in pastes], wo_tile, len(srcs)),
        grid_spec=pltpu.PrefetchScalarGridSpec(
            num_scalar_prefetch=1,
            grid=(steps,),
            in_specs=specs,
            out_specs=[ANY] * len(outs),
            scratch_shapes=[
                pltpu.VMEM((SLOTS, tokens, rows), BF16),
                pltpu.VMEM((tokens, width), BF16),
                pltpu.VMEM((SLOTS, rows, width), F32),
                dma_sems(SLOTS, SLOTS), dma_sems(PIECES, n_grp), dma_sems(SLOTS, n_grp), dma_sems(SLOTS), dma_sems(SLOTS, SLOTS), dma_sems(SLOTS, SLOTS, n_grp), dma_sems(SLOTS),
                *[pltpu.VMEM((SLOTS, recv.shape[0] // steps, recv.shape[1]), F32) for recv in recvs],
            ],
        ),
        out_shape=outs,
        input_output_aliases=alias,
        compiler_params=VMEM_BIG,
        cost_estimate=matmul_cost(hidden, tokens, width, 16 * hidden * width),
        name='wqkv_grad',
    )(*args)


def normed_grad_kernel(runs, n_src, final, more, cols_ref, *rest):
    srcs, (w_ref, init_ref, *rest) = rest[:n_src], rest[n_src:]
    if final:
        x_ref, gain_ref, dx_ref, sum_ref, acc, w_buf, g_buf, sems, g_sems, init_sem, sum_acc = rest
    else:
        acc, w_buf, g_buf, sems, g_sems, init_sem = rest
    j, steps = pl.program_id(Z), pl.num_programs(Z)
    slot = lax.rem(j, SLOTS)
    rows, width = g_buf.shape[1], g_buf.shape[2] // 2
    rank = cols_ref[2 * steps]

    def w_loads(step, at):
        for i in range(2):
            col = pl.multiple_of(cols_ref[2 * step + i], HEAD)
            yield pltpu.make_async_copy(w_ref.at[:, pl.ds(col, width)], w_buf.at[at, :, run(i, width)], sems.at[at, i])

    def g_loads(step):
        at = step % 2
        for i, (src, grp) in enumerate(runs[part(step, 2)]):
            ref, dst = srcs[src], g_buf.at[at, :, run(i, width)]
            tokens = ref.shape[-2]
            ref = ref.at[:, run(grp, width)] if tokens == rows else ref.at[grp]
            pairs = [(ref, dst)] if tokens == rows else [
                (ref.at[pl.ds(pl.multiple_of(h * (tokens // 2) + rank * (rows // 2), BLK), rows // 2)], dst.at[run(h, rows // 2)]) for h in range(2)]
            for pair in pairs:
                yield pltpu.make_async_copy(*pair, g_sems.at[at, i])

    def g_waits(at):
        for i in range(2):
            block = g_buf.at[at, :, run(i, width)]
            yield pltpu.make_async_copy(block, block, g_sems.at[at, i])

    @pl.when(j == Z)
    def _():
        start_all(w_loads(0, 0))
        start_all(g_loads(0))
        if more:
            init = pltpu.make_async_copy(init_ref, acc, init_sem)
            init.start()
            init.wait()
        else:
            acc[...] = init_ref[...].astype(F32) * ALPHA

    @pl.when(j + 1 < steps)
    def _():
        start_all(w_loads(j + 1, 1 - slot))

    for step in range(1, len(runs) // 2):
        @pl.when(j + 1 == step)
        def _():
            start_all(g_loads(step))

    wait_all(w_loads(j, slot))
    wait_all(g_waits(slot))
    acc[...] += dot_nt(g_buf[slot], w_buf[slot])

    if final:
        @pl.when(j == steps - 1)
        def _():
            sum_acc[...] = jnp.zeros_like(sum_acc)
            gain = gain_ref[...].astype(F32)

            @pl.loop(0, rows // NORM_ROWS)
            def _(i):
                at = run(i, NORM_ROWS)
                d_n = acc[at]
                x, inv = centred(x_ref[at])
                x = x * inv
                d_x = d_n * gain
                mean = jnp.mean(d_x, axis=-1, keepdims=True)
                slope = jnp.mean(d_x * x, axis=-1, keepdims=True)
                dx_ref[at] = (inv * (d_x - mean - x * slope)).astype(BF16)
                for kind, term in enumerate((d_n * x, d_n)):
                    sum_acc[kind] += jnp.sum(term.reshape((-1,) + sum_acc.shape[1:]), axis=0)

            sum_ref[...] = jnp.sum(sum_acc[...], axis=1)


def normed_grad(cols, runs, srcs, w_qkv, init, norm=None):
    rows, hidden = init.shape
    steps, width = len(runs) // 2, 2 * WIDTH
    flat = pl.BlockSpec((rows, hidden), lambda j, cols: (Z, Z))
    args = [cols, *srcs, w_qkv, init]
    more = init.dtype == F32
    specs = [ANY] * (len(srcs) + 1) + [ANY if more else flat]
    scratch = [pltpu.VMEM((SLOTS, hidden, width), BF16), pltpu.VMEM((SLOTS, rows, width), BF16), dma_sems(SLOTS, SLOTS), dma_sems(SLOTS, SLOTS), pltpu.SemaphoreType.DMA]
    if norm:
        args += list(norm)
        specs += [flat, pl.BlockSpec((1, hidden), lambda j, cols: (Z, Z))]
        outs = [jax.ShapeDtypeStruct((rows, hidden), BF16), jax.ShapeDtypeStruct((2, hidden), F32)]
        out_specs = [flat, pl.BlockSpec((2, hidden), lambda j, cols: (Z, Z))]
        scratch = [pltpu.VMEM((rows, hidden), F32)] + scratch + [pltpu.VMEM((2, 8, hidden), F32)]
    else:
        outs, out_specs = [jax.ShapeDtypeStruct((rows, hidden), F32)], [flat]
    return pl.pallas_call(
        functools.partial(normed_grad_kernel, runs, len(srcs), norm is not None, more),
        grid_spec=pltpu.PrefetchScalarGridSpec(
            num_scalar_prefetch=1,
            grid=(steps,),
            in_specs=specs,
            out_specs=out_specs,
            scratch_shapes=scratch,
        ),
        out_shape=outs,
        compiler_params=VMEM_BIG,
        cost_estimate=matmul_cost(rows, steps * width, hidden),
        name='dn',
    )(*args)


def paste_kernel(places_of, core_ref, recv_ref, _, out_ref, sems):
    row = pl.program_id(Z) * recv_ref.shape[0]
    copies = list(column_copies(recv_ref, out_ref, lambda i: sems.at[i], row, places_of(1 - core_ref[Z])))
    start_all(copies)
    wait_all(copies)


def paste_columns(core, places_of, recv, whole):
    hidden, block = recv.shape
    rows = 2 * BLK
    return pl.pallas_call(
        functools.partial(paste_kernel, places_of),
        grid_spec=pltpu.PrefetchScalarGridSpec(
            num_scalar_prefetch=1,
            grid=(hidden // rows,),
            in_specs=[pl.BlockSpec((rows, block), lambda m, core: (m, Z)), ANY],
            out_specs=ANY,
            scratch_shapes=[dma_sems(8)],
        ),
        out_shape=jax.ShapeDtypeStruct(whole.shape, F32),
        input_output_aliases={2: 0},
        compiler_params=VMEM_BIG,
        name='paste',
    )(core, recv, whole)


def output_kernel(n_chip, core_ref, mine_ref, theirs_ref, shared_ref, other_ref, w_ref, w_shared_ref, na_ref, nb_ref, b_ref, out_ref, acc):
    j, last = pl.program_id(Z), pl.num_programs(Z) - 1
    rows = acc.shape[0]

    def add(ref, weight_ref):
        acc[...] += dot_nn(ref[...].reshape(rows, -1), weight_ref[...])

    @pl.when(j == Z)
    def _():
        acc[...] = jnp.broadcast_to(b_ref[...].astype(F32), acc.shape)

    pl.when(j < n_chip)(functools.partial(add, mine_ref, w_ref))
    pl.when(jnp.logical_and(j >= n_chip, j < CORES * n_chip))(functools.partial(add, theirs_ref, w_ref))
    pl.when(j == last - 1)(functools.partial(add, shared_ref, w_shared_ref))

    @pl.when(j == last)
    def _():
        add(other_ref, w_shared_ref)
        for half, n_ref in enumerate((na_ref, nb_ref)):
            at = part(half, n_ref.shape[0])
            out_ref[at] = (ALPHA * n_ref[...].astype(F32) + acc[at]).astype(BF16)


def project_out(core, ctx_par, ctx_recv, ctx_shared, shared_recv, w_o, n_halves, b_o):
    n_chip, rows, cols = ctx_recv.shape
    shared = shared_recv.shape[1]
    hidden = w_o.shape[1]
    base = CORES * n_chip * cols // shared
    steps = CORES * n_chip + CORES
    split = (CORES, CORES * n_chip, rows // CORES)

    def dist_index(j, core):
        at = jnp.minimum(j, CORES * n_chip - 1)
        return CORES * lax.rem(at, n_chip) + jnp.where(at < n_chip, core[Z], 1 - core[Z])

    def shared_index(j, core):
        return base + jnp.where(j < steps - 1, core[Z], 1 - core[Z])

    whole, half = [pl.BlockSpec((size, hidden), lambda j, core: (Z, Z)) for size in (rows, rows // CORES)]
    return pl.pallas_call(
        functools.partial(output_kernel, n_chip),
        grid_spec=pltpu.PrefetchScalarGridSpec(
            num_scalar_prefetch=1,
            grid=(steps,),
            in_specs=[
                pl.BlockSpec((1, CORES, 1, rows // CORES, cols), lambda j, core: (jnp.minimum(j, n_chip - 1), Z, core[CORES], Z, Z)),
                pl.BlockSpec((1, rows, cols), lambda j, core: (jnp.clip(j - n_chip, 0, n_chip - 1), Z, Z)),
                pl.BlockSpec((CORES, 1, rows // CORES, shared), lambda j, core: (Z, core[CORES], Z, Z)),
                pl.BlockSpec((rows, shared), lambda j, core: (Z, Z)),
                pl.BlockSpec((cols, hidden), lambda j, core: (dist_index(j, core), Z)),
                pl.BlockSpec((shared, hidden), lambda j, core: (shared_index(j, core), Z)),
                half, half,
                pl.BlockSpec((1, hidden), lambda j, core: (Z, Z)),
            ],
            out_specs=whole,
            scratch_shapes=[pltpu.VMEM((rows, hidden), F32)],
        ),
        out_shape=jax.ShapeDtypeStruct((rows, hidden), BF16),
        compiler_params=VMEM_BIG,
        cost_estimate=matmul_cost(rows, hidden, hidden),
        name='out_proj',
    )(core, ctx_par.reshape(n_chip, *split, cols), ctx_recv, ctx_shared.reshape(*split, shared), shared_recv, w_o, w_o, *n_halves, b_o)


def together(*values):
    return lax.optimization_barrier(values)


def solution(mesh):
    n_dev = mesh.shape['sp']
    tok_spec = P('dp', 'sp', None)
    pos_spec = P('dp', 'sp')
    in_specs = (tok_spec, pos_spec, pos_spec, P('dp'), P(), P(), P(), P(), P(), P(), tok_spec)
    out_specs = (tok_spec, tok_spec, P('dp'), P('dp'), P('dp', None), P('dp'), P('dp', None), P('dp'))
    same_core = [list(range(core, n_dev, 2)) for core in range(2)]
    partners = [(dev, dev ^ 1) for dev in range(n_dev)]
    n_chip = n_dev // 2

    def device_step(hidden_in, pos_ids, block_pos, prefix_len, ln_gamma, ln_beta, w_qkv, b_qkv, w_o, b_o, grad_out):
        batch, local_len, hidden = hidden_in.shape
        per_half = batch // 2
        heads = hidden // HEAD
        n_dist, n_shared = (heads - SHARED) // n_dev, SHARED // 2
        shared_at = n_dev * n_dist
        rows = batch * local_len
        tokens = n_dev * rows
        rank = lax.axis_index('sp')
        parity = lax.rem(rank, SLOTS)
        pair = rank + 1 - 2 * parity
        core = jnp.stack([parity, pair, rank]).astype(jnp.int32)
        gather = functools.partial(lax.all_gather, axis_name='sp')
        gather_core = functools.partial(lax.all_gather, axis_name='sp', axis_index_groups=same_core)
        to_partner = functools.partial(lax.ppermute, axis_name='sp', perm=partners)

        def token_rows(arr, dev):
            split = arr.reshape(arr.shape[:-2] + (2, n_dev, rows // 2, arr.shape[-1]))
            return lax.dynamic_index_in_dim(split, dev, axis=split.ndim - 3, keepdims=False).reshape(arr.shape[:-2] + (rows, arr.shape[-1]))

        def places(head):
            return lambda par: [((2 * c + par) * n_dist + head) * WIDTH for c in range(n_chip)]

        def shared_places(par):
            return [(shared_at + par * n_shared + i) * WIDTH for i in range(n_shared)]

        def wo_tile(t, par):
            spread = t - n_shared
            return jnp.where(t < n_shared, shared_at + par * n_shared + t, (2 * (spread // n_dist) + par) * n_dist + lax.rem(spread, n_dist))

        halves = range(2)
        x_flat, gain = hidden_in.reshape(rows, hidden), ln_gamma.reshape(1, hidden)
        n_own = [normalize(half, x_flat, gain, ln_beta.reshape(1, hidden)) for half in halves]
        dy_own = [grad_out[part(half, per_half)] for half in halves]
        n_own[1], *dy_own = together(n_own[1], *dy_own)
        n_own = [own.reshape(per_half, local_len, hidden) for own in n_own]
        n_a, n_b, dy_a, dy_b = [gather(send) for send in n_own + dy_own]
        cos, sin = rope_tables(prefix_len, n_dev * local_len)
        prefix = [prefix_len[part(half, per_half)] for half in halves]
        starts = jnp.stack([rank * n_dist, shared_at + parity * n_shared, rank, pair]).astype(jnp.int32)
        bias = jnp.concatenate([
            lax.dynamic_slice_in_dim(b_qkv, starts[0] * WIDTH, n_dist * WIDTH),
            lax.dynamic_slice_in_dim(b_qkv, starts[1] * WIDTH, n_shared * WIDTH)]).astype(F32).reshape(1, -1)
        grad_bo = jnp.sum(grad_out.astype(F32), axis=(0, 1))
        n_chip_rows = [own[None] for own in n_own + [to_partner(own) for own in n_own]]
        qkv_own = project_qkv(starts, n_dist, n_shared, n_chip_rows, w_qkv, bias, cos, sin)
        d_ctx_own = context_grad(starts, n_dist, n_shared, [own[None] for own in (grad_out, to_partner(grad_out))], w_o, n_dev)
        n_a, grad_bo, *d_ctx_own = together(n_a, grad_bo, *d_ctx_own)

        ctx_d = ctx_r = None
        qkv, lses = [], []
        for half in halves:
            if half:
                n_b, ctx_r = together(n_b, ctx_r)
            qd, kd, vd, qr, kr, vr = project_qkv(
                starts, n_dist, n_shared, [n_b if half else n_a], w_qkv, bias, cos, sin, half, qkv_own[part(half, QKV_IN)])
            ctx_d, lse_d = attention_forward(half, prefix[half], qd, kd, vd, n_dev, ctx_d)
            qr, ctx_d = together(qr, ctx_d)
            ctx_r, lse_r = attention_forward(half, prefix[half], qr, kr, vr, n_dev, ctx_r)
            qkv.append((qd, kd, vd, qr, kr, vr))
            lses.append((lse_d, lse_r))
        ctx_par = gather_core(ctx_d.reshape(tokens, n_dist * HEAD))

        dy_a, ctx_r = together(dy_a, ctx_r)
        g_d, g_r = [], []
        sums = []
        for half in halves:
            if half:
                dy_b, *g_r = together(dy_b, *g_r)
            qd, kd, vd, qr, kr, vr = qkv[half]
            d_ctx, d_ctx_r = context_grad(starts, n_dist, n_shared, [dy_b if half else dy_a], w_o, n_dev, d_ctx_own[part(half, CORES)])
            *g_d, sum_d = attention_backward(half, n_dist, prefix[half], qd, kd, vd, ctx_d, d_ctx, lses[half][0], cos, sin, g_d)
            qr, *g_d = together(qr, *g_d)
            *g_r, sum_r = attention_backward(half, n_shared, prefix[half], qr, kr, vr, ctx_r, d_ctx_r, lses[half][1], cos, sin, g_r)
            sums.append(jnp.sum(jnp.concatenate([sum_d, sum_r]), axis=(1, 2)).reshape(-1))
        g_par = [gather_core(g.reshape(tokens, WIDTH)) for g in g_d]
        g_r = [g.reshape(1, tokens, WIDTH) for g in g_r]

        n_a, n_b, dy_a, dy_b = [part.reshape(tokens // 2, hidden) for part in (n_a, n_b, dy_a, dy_b)]
        ctx_r = ctx_r.reshape(tokens, n_shared * HEAD)
        shared_recv = to_partner(token_rows(ctx_r, pair))
        ctx_r, *g_r = together(ctx_r, *g_r)
        grad_wo, wo_block = weight_grad_o(
            core, ctx_r[None], dy_a, dy_b, lambda c, par: (shared_at + par * n_shared) * HEAD, lambda c: 0, hidden // 2, ())
        shared_recv, wo_block, n_a = together(shared_recv, wo_block, n_a)
        grad_wqkv, block, r_send = weight_grad_qkv(core, shared_places, n_a, n_b, g_r, None)
        r_recv, ctx_recv = to_partner(r_send), to_partner(token_rows(ctx_par, pair))
        ctx_par, block = together(ctx_par, block)
        recv_r = to_partner(block)
        grad_wo, wo_block = weight_grad_o(
            core, ctx_par, dy_a, dy_b, lambda c, par: (2 * c + par) * (n_dist * HEAD), lambda c: (n_shared + c * n_dist) * HEAD,
            hidden // 2, (grad_wo, wo_block))
        ctx_recv, wo_block, recv_r, r_recv = together(ctx_recv, wo_block, recv_r, r_recv)
        wo_recv = to_partner(wo_block)
        hidden_out = project_out(
            core, ctx_par, ctx_recv, ctx_r, shared_recv, w_o, [own.reshape(-1, hidden) for own in n_own], b_o.reshape(1, hidden))
        n_a, hidden_out, g_par[0] = together(n_a, hidden_out, g_par[0])

        def columns(table):
            at = [np.array([h * WIDTH for h in table(par)] + [0], np.int32) for par in range(2)]
            last = (np.arange(at[0].size) == at[0].size - 1).astype(np.int32)
            return jnp.asarray(at[0]) + parity.astype(jnp.int32) * jnp.asarray(at[1] - at[0]) + rank.astype(jnp.int32) * jnp.asarray(last)

        def spread_grad(head, whole, **extra):
            whole, block, tok, *rest = weight_grad_qkv(core, places(head), n_a, n_b, [g_par[head]], whole, **extra)
            tok = to_partner(tok)
            if head:
                tok, block = together(tok, block)
            return whole, tok, to_partner(block), rest

        grad_wqkv, tok_0, recv_0, _ = spread_grad(0, grad_wqkv, pastes=[(recv_r, shared_places)])
        g_r[0], grad_wqkv = together(g_r[0], grad_wqkv)
        cols = columns(lambda mine: [shared_at + par * n_shared + i for par in (mine, 1 - mine) for i in range(n_shared)])
        runs = [(i, 0) for i in range(n_shared)] + [(n_shared, i) for i in range(n_shared)]
        d_norm, = normed_grad(cols, runs, [*g_r, r_recv], w_qkv, grad_out.reshape(rows, hidden))
        g_par[1], d_norm = together(g_par[1], d_norm)
        wo_recv, tok_0 = together(wo_recv, tok_0)
        grad_wqkv, tok_1, recv_1, (grad_wo,) = spread_grad(1, grad_wqkv, wo=(wo_recv, grad_wo, wo_tile))
        cols = columns(lambda mine: [(2 * c + par) * n_dist + head for par in (mine, 1 - mine) for c in range(n_chip) for head in (0, 1)])
        runs = [(CORES * side + head, c) for side in range(CORES) for c in range(n_chip) for head in (0, 1)]
        tok_1, recv_0 = together(tok_1, recv_0)
        d_norm, = normed_grad(cols, runs, [g_par[0], g_par[1], tok_0, tok_1], w_qkv, d_norm)
        n_a, d_norm, g_par[2] = together(n_a, d_norm, g_par[2])
        grad_wqkv, tok_2, recv_2, _ = spread_grad(2, grad_wqkv, pastes=[(recv_0, places(0)), (recv_1, places(1))])
        cols = columns(lambda mine: [(2 * c + par) * n_dist + 2 for c in range(n_chip) for par in (mine, 1 - mine)])
        grad_in, norm_sums = normed_grad(
            cols, [(src, c) for c in range(n_chip) for src in range(2)], [g_par[2], tok_2], w_qkv, d_norm, norm=(x_flat, gain))
        small = gather(jnp.concatenate([sums[0] + sums[1], norm_sums.reshape(-1), grad_bo]))
        recv_2, small = together(recv_2, small)
        grad_wqkv = paste_columns(core, places(2), recv_2, grad_wqkv)
        spread, shared = small[:, :n_dist * WIDTH], small[:2, n_dist * WIDTH:(n_dist + n_shared) * WIDTH]
        grad_bqkv = jnp.concatenate([spread.reshape(-1), shared.reshape(-1)])
        grad_gamma, grad_beta, grad_bo = jnp.sum(small[:, (n_dist + n_shared) * WIDTH:], axis=0).reshape(3, hidden)
        shape = (batch, local_len, hidden)
        return (hidden_out.reshape(shape), grad_in.reshape(shape), grad_gamma, grad_beta, grad_wqkv, grad_bqkv, grad_wo, grad_bo)

    return jax.shard_map(device_step, mesh=mesh, in_specs=in_specs, out_specs=out_specs, check_vma=False)
```

```python
import functools
import math
import jax
import jax.numpy as jnp
import numpy as np
from jax import lax
from jax.experimental import pallas as pl
from jax.experimental.pallas import tpu as pltpu
from jax.sharding import PartitionSpec as P

HEAD = 128
QUARTER = 32
ALPHA = math.sqrt(56.0)
LN_EPS = 1e-5
ROT_BASE = 10000.0
SCALE = 1.0 / math.sqrt(HEAD)
LOG2E = math.log2(math.e)
MASK_FILL = -1e30
BLK = 256
VMEM_BIG = pltpu.CompilerParams(vmem_limit_bytes=62 << 20)
SHARED = 8
Z = 0
SLOTS = CORES = 2
WIDTH = 3 * HEAD
F32 = jnp.float32
BF16 = jnp.bfloat16


def dot(lhs, rhs, lhs_dim, rhs_dim):
    return lax.dot_general(lhs, rhs, (((lhs_dim,), (rhs_dim,)), ((), ())), preferred_element_type=F32)


def dot_nn(lhs, rhs):
    return dot(lhs, rhs, 1, 0)


def dot_nt(lhs, rhs):
    return dot(lhs, rhs, 1, 1)


def dot_tn(lhs, rhs):
    return dot(lhs, rhs, 0, 0)


def matmul_cost(rows, depth, cols, extra=0):
    return pl.CostEstimate(
        flops=2 * rows * depth * cols, bytes_accessed=2 * (rows * depth + depth * cols + rows * cols) + extra, transcendentals=0)


def attention_cost(n_head, batch, seq, products):
    pairs = n_head * batch * seq * seq
    return pl.CostEstimate(flops=2 * products * pairs * HEAD, bytes_accessed=8 * products * n_head * batch * seq * HEAD, transcendentals=pairs)


def run(index, size):
    return pl.ds(pl.multiple_of(index * size, size), size)


def part(index, size):
    return slice(index * size, (index + 1) * size)


def rope_tables(prefix_len, seq):
    tok = jnp.arange(seq, dtype=jnp.int32)[None, :]
    pre = prefix_len[:, None]
    inside = tok < pre
    pos = jnp.where(inside, tok, pre - 1)
    blk = jnp.where(inside, 0, tok - pre + 1)
    inv_freq = ROT_BASE ** (-jnp.arange(QUARTER, dtype=F32) / QUARTER)
    angles = jnp.stack([pos, blk], axis=-1).astype(F32)[..., None] * inv_freq
    cos, sin = jnp.cos(angles), jnp.sin(angles)
    shape = pos.shape + (HEAD,)
    return (jnp.stack([cos, cos], axis=-2).reshape(shape), jnp.stack([-sin, sin], axis=-2).reshape(shape))


def turn(x, cos, sin):
    lane = lax.broadcasted_iota(jnp.int32, x.shape, 1)
    other = jnp.where(lane % (2 * QUARTER) < QUARTER, pltpu.roll(x, HEAD - QUARTER, 1), pltpu.roll(x, QUARTER, 1))
    return x * cos + other * sin


def dma_sems(*shape):
    return pltpu.SemaphoreType.DMA(shape)


def dma_sems(*shape):
    return pltpu.SemaphoreType.DMA(shape)


def start_all(copies):
    for copy in copies:
        copy.start()


def wait_all(copies):
    for copy in copies:
        copy.wait()


ANY = pl.BlockSpec(memory_space=pl.ANY)
PIECES = 4
QKV_IN = 6


NORM_ROWS = 32


def centred(x):
    x = x.astype(F32)
    x = x - jnp.mean(x, axis=-1, keepdims=True)
    return x, lax.rsqrt(jnp.mean(x * x, axis=-1, keepdims=True) + LN_EPS)


def norm_kernel(x_ref, affine_ref, out_ref):
    gain, shift = affine_ref[:1].astype(F32), affine_ref[1:].astype(F32)

    @pl.loop(0, x_ref.shape[0] // NORM_ROWS)
    def _(i):
        rows = run(i, NORM_ROWS)
        x, inv = centred(x_ref[rows])
        out_ref[rows] = (x * inv * gain + shift).astype(BF16)


def normalize(half, x, affine):
    rows, hidden = x.shape
    block = rows // 4
    return pl.pallas_call(
        norm_kernel,
        grid=(2,),
        in_specs=[pl.BlockSpec((block, hidden), lambda i: (2 * half + i, Z)), pl.BlockSpec(affine.shape, lambda i: (Z, Z))],
        out_specs=pl.BlockSpec((block, hidden), lambda i: (i, Z)),
        out_shape=jax.ShapeDtypeStruct((2 * block, hidden), BF16),
        compiler_params=VMEM_BIG,
        name='norm',
    )(x, affine)


def qkv_kernel(n_dist, n_tile, n_in, start_ref, *rest):
    n_refs, (w_ref, b_ref, cos_ref, sin_ref, *outs), (w_buf, acc, sems) = rest[:n_in], rest[n_in:-3], rest[-3:]
    first, later = n_refs[:(n_in + 1) // CORES], n_refs[n_in // CORES:]
    _, rows, cols = acc.shape
    hidden = w_ref.shape[0]
    dist = n_dist * WIDTH
    step, last = pl.program_id(Z), pl.num_programs(Z) - 1
    slot = lax.rem(step, SLOTS)
    piece = hidden // PIECES
    tile = first[0].shape[-2]

    def loads(i):
        span = run(i, piece)
        for kind, (at, width) in enumerate(((0, dist), (dist, cols - dist))):
            col = pl.multiple_of(start_ref[kind] * WIDTH, HEAD)
            yield pltpu.make_async_copy(w_ref.at[span, pl.ds(col, width)], w_buf.at[span, pl.ds(at, width)], sems.at[i, kind])

    def finish():
        for i in range(rows // tile):
            group, batch, at, table = n_tile(i)
            cos, sin = cos_ref[table, part(at, tile)], sin_ref[table, part(at, tile)]
            for h in range(cols // WIDTH):
                kind, head = (0, h) if h < n_dist else (1, h - n_dist)
                refs = outs[part(CORES * group + kind, 3)]
                pre = [acc[1 - slot, part(i, tile), part(3 * h + j, HEAD)] + b_ref[:, part(3 * h + j, HEAD)] for j in range(3)]
                for ref, val in zip(refs, (turn(pre[0], cos, sin), turn(pre[1], cos, sin), pre[2])):
                    ref[head, batch, part(at, tile)] = val.astype(BF16)

    @pl.when(step == Z)
    def _():
        for i in range(PIECES):
            start_all(loads(i))
        acc[slot] = jnp.zeros((rows, cols), F32)

        @pl.loop(0, PIECES)
        def _(i):
            wait_all(loads(i))
            span = run(i, piece)
            for i, ref in enumerate(first):
                acc[slot, part(i, rows // len(first))] += dot_nn(ref[:, :, :, span].reshape(-1, piece), w_buf[span])

    @pl.when(jnp.logical_and(step > 0, step < last))
    def _():
        finish()
        for i, ref in enumerate(later):
            acc[slot, part(i, rows // len(later))] = dot_nn(ref[...].reshape(-1, hidden), w_buf[...])

    pl.when(step == last)(finish)


def project_qkv(starts, n_dist, n_shared, n_rows, w_qkv, bias, cos, sin, half=None, earlier=None):
    _, per_half, local_len, hidden = n_rows[0].shape
    _, seq, _ = cos.shape
    cols = (n_dist + n_shared) * WIDTH
    own = earlier is None
    batch = per_half * CORES if own else per_half
    steps = CORES if own else seq // local_len // CORES - 1
    n_chip = seq // local_len // CORES
    width = local_len if own else CORES * local_len

    def place(step, at):
        return at[CORES + step] if own else lax.rem(at[CORES] // CORES + 1 + step, n_chip)

    def ahead(step, at):
        return place(jnp.minimum(step, steps - 1), at)

    def behind(step, at):
        return place(jnp.maximum(step - 1, 0), at)

    shapes = [jax.ShapeDtypeStruct((n_head, per_half, seq, HEAD), BF16) for n_head in (n_dist, n_shared) for _ in range(3)]
    shapes = shapes * CORES if own else shapes
    tab_spec = pl.BlockSpec((batch, width, HEAD), lambda step, at: (Z if own else half, behind(step, at), Z))
    arrays = [] if own else list(earlier)

    def own_tile(i):
        return i // per_half, i % per_half, 0, i

    def other_tile(i):
        return 0, i % per_half, i // per_half, i % per_half

    return pl.pallas_call(
        functools.partial(without, len(arrays), len(n_rows) + 5, functools.partial(qkv_kernel, n_dist, own_tile if own else other_tile, len(n_rows))),
        grid_spec=pltpu.PrefetchScalarGridSpec(
            num_scalar_prefetch=1,
            grid=(steps + 1,),
            in_specs=[
                *[pl.BlockSpec((1 if own else CORES, per_half, local_len, hidden), lambda step, at: (Z if own else ahead(step, at), Z, Z, Z))] * len(n_rows),
                ANY,
                pl.BlockSpec((1, cols), lambda step, at: (Z, Z)),
                tab_spec, tab_spec,
            ] + [ANY] * len(arrays),
            out_specs=[pl.BlockSpec(shape.shape[:CORES] + (width, HEAD), lambda step, at: (Z, Z, behind(step, at), Z)) for shape in shapes],
            scratch_shapes=[
                pltpu.VMEM((hidden, cols), BF16), pltpu.VMEM((SLOTS, CORES * CORES * local_len, cols), F32), dma_sems(PIECES, SLOTS)],
        ),
        out_shape=shapes,
        input_output_aliases={QKV_IN + i: i for i in range(len(arrays))},
        compiler_params=VMEM_BIG,
        cost_estimate=matmul_cost(steps * CORES * batch * local_len, hidden, cols),
        name='qkv',
    )(starts, *n_rows, w_qkv, bias, cos, sin, *arrays)


def without(count, start, kernel, *refs):
    kernel(*refs[:start], *refs[start + count:])


def forward_kernel(pre_ref, q_ref, k_ref, v_ref, *rest):
    ctx_ref, lse_ref = rest[-2:]
    n_head, _, seq, _ = q_ref.shape
    local_len = ctx_ref.shape[3]
    per = BLK // local_len
    prefix = pre_ref[pl.program_id(1)]

    def block(r, n_key):
        query = lax.broadcasted_iota(jnp.int32, (1, BLK), 1) + r * BLK
        last = jnp.maximum(query, prefix - 1) - (n_key - 1) * BLK
        scores = []
        for h in range(n_head):
            q_blk = q_ref[h, 0, part(r, BLK)]
            parts = [dot_nt(k_ref[h, 0, part(c, BLK)], q_blk) * (SCALE * LOG2E) for c in range(n_key)]
            key = lax.broadcasted_iota(jnp.int32, (BLK, BLK), 0)
            parts[-1] = jnp.where(key <= last, parts[-1], MASK_FILL)
            scores.append(parts)
        for h, parts in enumerate(scores):
            top = functools.reduce(jnp.maximum, [jnp.max(p, axis=0, keepdims=True) for p in parts])
            parts = [jnp.exp2(p - top) for p in parts]
            total = functools.reduce(jnp.add, [jnp.sum(p, axis=0, keepdims=True) for p in parts])
            inv = 1.0 / total
            probs = jnp.concatenate([(p * inv).astype(BF16) for p in parts], axis=0)
            ctx_t = dot_tn(v_ref[h, 0, :n_key * BLK], probs)
            ctx = ctx_t.T.astype(BF16).reshape(per, local_len, HEAD)
            ctx_ref[0, part(r, per), 0, :, part(h, HEAD)] = ctx
            lse_ref[h, 0, :, part(r, BLK)] = top + jnp.log2(total)

    n_blk = seq // BLK
    for r in range(n_blk):
        for n_key in range(r + 1, n_blk + 1):
            low = (n_key - 1) * BLK
            cond = prefix <= n_key * BLK if n_key == r + 1 else prefix > low
            if n_key < n_blk and n_key > r + 1:
                cond = jnp.logical_and(cond, prefix <= n_key * BLK)
            if n_key == n_blk and n_key == r + 1:
                block(r, n_key)
            else:
                pl.when(cond)(functools.partial(block, r, n_key))


def attention_forward(half, prefix_half, q, k, v, n_dev, ctx):
    own, batch, seq, _ = q.shape
    local_len = seq // n_dev
    group = own
    qkv_spec = pl.BlockSpec((group, 1, seq, HEAD), lambda h, b, pre: (h, b, Z, Z))
    earlier = [] if ctx is None else [ctx]
    return pl.pallas_call(
        forward_kernel,
        grid_spec=pltpu.PrefetchScalarGridSpec(
            num_scalar_prefetch=1,
            grid=(own // group, batch),
            in_specs=[qkv_spec] * 3 + [ANY] * len(earlier),
            out_specs=[
                pl.BlockSpec((1, n_dev, 1, local_len, group * HEAD), lambda h, b, pre: (half, Z, b, Z, h)),
                pl.BlockSpec((group, 1, 1, seq), lambda h, b, pre: (h, b, Z, Z)),
            ],
        ),
        out_shape=[
            jax.ShapeDtypeStruct((2, n_dev, batch, local_len, own * HEAD), BF16),
            jax.ShapeDtypeStruct((own, batch, 1, seq), F32),
        ],
        input_output_aliases={4: 0} if earlier else {},
        compiler_params=VMEM_BIG,
        cost_estimate=attention_cost(own, batch, seq, 2),
        name='attn_fwd',
    )(prefix_half, q, k, v, *earlier)


def d_ctx_kernel(n_in, start_ref, *rest):
    dy_refs, (w_ref, *outs), (w_buf, sems) = rest[:n_in], rest[n_in:-2], rest[-2:]
    step, hidden = pl.program_id(Z), w_ref.shape[1]
    widths = [outs[0].shape[-1], outs[1].shape[-1]]

    def loads():
        for kind, (at, width) in enumerate(zip((0, widths[0]), widths)):
            row = pl.multiple_of(start_ref[kind] * HEAD, HEAD)
            yield pltpu.make_async_copy(w_ref.at[pl.ds(row, width)], w_buf.at[pl.ds(at, width)], sems.at[kind])

    @pl.when(step == Z)
    def _():
        start_all(loads())
        wait_all(loads())

    def multiply(dy_ref):
        res = dot_nt(dy_ref[...].reshape(-1, hidden), w_buf[...]).astype(BF16)
        rows = CORES * res.shape[0] // len(outs)
        for i, out_ref in enumerate(outs):
            cols = slice(widths[0], None) if i % CORES else slice(widths[0])
            out_ref[...] = res[part(i // CORES, rows), cols].reshape(out_ref.shape)

    if n_in > 1:
        for i, dy_ref in enumerate(dy_refs):
            pl.when(step == i)(functools.partial(multiply, dy_ref))
    else:
        multiply(dy_refs[0])


def context_grad(starts, n_dist, n_shared, dy_rows, w_o, n_dev, earlier=()):
    _, batch, local_len, hidden = dy_rows[0].shape
    own = not earlier
    n_chip = n_dev // CORES
    per_half, devs = (batch // CORES, 1) if own else (batch, CORES)

    def block(step, at):
        return (at[CORES + step] if own else lax.rem(at[CORES] // CORES + 1 + step, n_chip), Z, Z, Z)

    cols = [n_dist * HEAD, n_shared * HEAD]
    outs = cols * (CORES if own else 1)
    n_in = len(dy_rows)
    return pl.pallas_call(
        functools.partial(without, len(earlier), n_in + 2, functools.partial(d_ctx_kernel, n_in)),
        grid_spec=pltpu.PrefetchScalarGridSpec(
            num_scalar_prefetch=1,
            grid=(CORES if own else n_chip - 1,),
            in_specs=[pl.BlockSpec((devs, batch, local_len, hidden), (lambda step, at: (Z, Z, Z, Z)) if own else block)] * n_in + [ANY] * (1 + len(earlier)),
            out_specs=[pl.BlockSpec((devs, per_half, local_len, width), block) for width in outs],
            scratch_shapes=[pltpu.VMEM((sum(cols), hidden), BF16), dma_sems(CORES)],
        ),
        out_shape=[jax.ShapeDtypeStruct((n_dev, per_half, local_len, width), BF16) for width in outs],
        input_output_aliases={3 + i: i for i in range(len(earlier))},
        compiler_params=VMEM_BIG,
        cost_estimate=matmul_cost(n_dev * batch * local_len, hidden, sum(cols)),
        name='dctx',
    )(starts, *dy_rows, w_o, *earlier)


def backward_kernel(pre_ref, q_ref, k_ref, v_ref, ctx_ref, dctx_ref, lse_ref, cos_ref, sin_ref, *rest):
    sum_ref, dq_acc, dk_acc, dv_acc = rest[-4:]
    n_head, _, seq, _ = q_ref.shape
    g_refs = rest[-4 - n_head:-4]
    _, n_dev, _, local_len, _ = g_refs[0].shape
    n_blk = seq // BLK
    prefix = pre_ref[pl.program_id(Z)]
    d_ctx, delta = [], []
    for h in range(n_head):
        lanes = part(h, HEAD)
        grad = dctx_ref[:, :, :, lanes].reshape(seq, HEAD)
        prod = grad.astype(F32) * ctx_ref[0, :, :, :, lanes].reshape(seq, HEAD).astype(F32)
        d_ctx.append(grad)
        delta.append(jnp.sum(prod.T, axis=0, keepdims=True))

    def block(c, first):
        span = part(c, BLK)
        start = first * BLK
        products = []
        for h in range(n_head):
            s_t = dot_nt(k_ref[h, 0, span], q_ref[h, 0, start:])
            dp_t = dot_nt(v_ref[h, 0, span], d_ctx[h][start:])
            products.append((s_t, dp_t))
        for h, (s_t, dp_t) in enumerate(products):
            probs, d_scores = [], []
            for r in range(first, n_blk):
                cols, here = part(r, BLK), part(r - first, BLK)
                piece = s_t[:, here] * (SCALE * LOG2E)
                if r <= c:
                    key = lax.broadcasted_iota(jnp.int32, (BLK, BLK), 0)
                    query = lax.broadcasted_iota(jnp.int32, (1, BLK), 1) + r * BLK
                    piece = jnp.where(key <= jnp.maximum(query, prefix - 1) - c * BLK, piece, MASK_FILL)
                p = jnp.exp2(piece - lse_ref[h, 0, :, cols])
                probs.append(p.astype(BF16))
                d_scores.append((p * (dp_t[:, here] - delta[h][:, cols]) * SCALE).astype(BF16))
            probs = jnp.concatenate(probs, axis=1)
            d_scores = jnp.concatenate(d_scores, axis=1)
            dv_acc[h, span] = dot_nn(probs, d_ctx[h][start:])
            dk_acc[h, span] = dot_nn(d_scores, q_ref[h, 0, start:])
            dq_part = dot_tn(k_ref[h, 0, span], d_scores)
            if c:
                dq_acc[h, :, start:] += dq_part
            else:
                dq_acc[h] = dq_part

    block(0, 0)
    for c in range(1, n_blk):
        pl.when(prefix > c * BLK)(functools.partial(block, c, 0))
        pl.when(prefix <= c * BLK)(functools.partial(block, c, c))

    cos, sin = cos_ref[Z], sin_ref[Z]
    for h in range(n_head):
        g_q = turn(dq_acc[h].T.astype(BF16).astype(F32), cos, -sin)
        g_k = turn(dk_acc[h].astype(BF16).astype(F32), cos, -sin)
        g_v = dv_acc[h].astype(BF16).astype(F32)
        for i, g in enumerate((g_q, g_k, g_v)):
            lanes = part(i, HEAD)
            g_refs[h][0, :, 0, :, lanes] = g.astype(BF16).reshape(n_dev, local_len, HEAD)
            sum_ref[h, 0, :, lanes] = jnp.sum(g, axis=0, keepdims=True)


def attention_backward(half, group, prefix_half, q, k, v, ctx, d_ctx, lse, cos, sin, earlier):
    _, batch, seq, _ = q.shape
    _, n_dev, _, local_len, _ = ctx.shape
    qkv_spec = pl.BlockSpec((group, 1, seq, HEAD), lambda b, pre: (Z, b, Z, Z))
    tab_spec = pl.BlockSpec((1, seq, HEAD), lambda b, pre: (half * batch + b, Z, Z))
    stat = functools.partial(pltpu.VMEM, dtype=F32)
    return pl.pallas_call(
        backward_kernel,
        grid_spec=pltpu.PrefetchScalarGridSpec(
            num_scalar_prefetch=1,
            grid=(batch,),
            in_specs=[qkv_spec] * 3 + [
                pl.BlockSpec((1, n_dev, 1, local_len, group * HEAD), lambda b, pre: (half, Z, b, Z, Z)),
                pl.BlockSpec((n_dev, 1, local_len, group * HEAD), lambda b, pre: (Z, b, Z, Z)),
                pl.BlockSpec((group, 1, 1, seq), lambda b, pre: (Z, b, Z, Z)), tab_spec, tab_spec] + [ANY] * len(earlier),
            out_specs=[pl.BlockSpec((1, n_dev, 1, local_len, WIDTH), lambda b, pre: (half, Z, b, Z, Z))] * group + [
                pl.BlockSpec((group, 1, 1, WIDTH), lambda b, pre: (Z, b, Z, Z))],
            scratch_shapes=[stat((group, HEAD, seq)), stat((group, seq, HEAD)), stat((group, seq, HEAD))],
        ),
        out_shape=[jax.ShapeDtypeStruct((2, n_dev, batch, local_len, WIDTH), BF16)] * group + [
            jax.ShapeDtypeStruct((group, batch, 1, WIDTH), F32)],
        input_output_aliases={9 + i: i for i in range(len(earlier))},
        compiler_params=VMEM_BIG,
        cost_estimate=attention_cost(group, batch, seq, 5),
        name='attn_bwd',
    )(prefix_half, q, k, v, ctx, d_ctx, lse, cos, sin, *earlier)


def wo_grad_kernel(row_of, block_row_of, core_ref, ctx_ref, dya_ref, dyb_ref, *rest):
    out_ref, copy_ref, rhs, buf, rhs_sems, sems = rest[-6:]
    n, c = pl.program_id(Z), pl.program_id(1)
    n_col, n_grp = pl.num_programs(Z), pl.num_programs(1)
    step = n * n_grp + c
    slot, n_slot = lax.rem(step, SLOTS), lax.rem(n, SLOTS)
    _, rows, wide = buf.shape
    half = dya_ref.shape[0]
    core = core_ref[Z]

    piece = half // CORES

    def load(n_at, at, ref, row, i):
        return pltpu.make_async_copy(ref.at[run(row, piece), run(n_at, wide)], rhs.at[at, run(i, piece)], rhs_sems.at[at, i])

    def loads(n_at, at):
        for i in range(PIECES):
            yield load(n_at, at, (dya_ref, dyb_ref)[i // CORES], i % CORES, i)

    def stores(at_step, at):
        n_at, c_at = at_step // n_grp, lax.rem(at_step, n_grp)
        for i, (ref, row) in enumerate(((out_ref, row_of(c_at, core)), (copy_ref, block_row_of(c_at)))):
            yield pltpu.make_async_copy(buf.at[at], ref.at[pl.ds(pl.multiple_of(row, HEAD), rows), run(n_at, wide)], sems.at[at, i])

    @pl.when(step == Z)
    def _():
        start_all(loads(0, 0))

    @pl.when(c == Z)
    def _():
        @pl.when(n + 1 < n_col)
        def _():
            start_all(loads(n + 1, 1 - n_slot))

        @pl.when(step > 0)
        def _():
            wait_all(loads(n, n_slot))

    @pl.when(step >= 2)
    def _():
        wait_all(stores(step - 2, slot))

    @pl.when(step == 0)
    def _():
        buf[slot] = jnp.zeros((rows, wide), F32)

        @pl.loop(0, PIECES)
        def _(i):
            load(0, 0, dya_ref, 0, i).wait()
            buf[slot] += dot_tn(ctx_ref[Z, run(i, piece)], rhs[Z, run(i, piece)])

    @pl.when(step > 0)
    def _():
        buf[slot] = dot_tn(ctx_ref[Z], rhs[n_slot])

    start_all(stores(step, slot))

    @pl.when(step == n_col * n_grp - 1)
    def _():
        wait_all(stores(step - 1, 1 - slot))
        wait_all(stores(step, slot))


def weight_grad_o(core, ctx_par, dy_a, dy_b, row_of, block_row_of, block_rows, earlier):
    n_grp, tokens, cols = ctx_par.shape
    hidden = dy_a.shape[1]
    wide = hidden // 4
    return pl.pallas_call(
        functools.partial(wo_grad_kernel, row_of, block_row_of),
        grid_spec=pltpu.PrefetchScalarGridSpec(
            num_scalar_prefetch=1,
            grid=(hidden // wide, n_grp),
            in_specs=[pl.BlockSpec((1, tokens, cols), lambda n, c, core: (c, Z, Z)), ANY, ANY] + [ANY] * len(earlier),
            out_specs=[ANY, ANY],
            scratch_shapes=[pltpu.VMEM((SLOTS, tokens, wide), BF16), pltpu.VMEM((SLOTS, cols, wide), F32), dma_sems(SLOTS, PIECES), dma_sems(SLOTS, SLOTS)],
        ),
        out_shape=[jax.ShapeDtypeStruct((hidden, hidden), F32), jax.ShapeDtypeStruct((block_rows, hidden), F32)],
        input_output_aliases={4: 0, 5: 1} if earlier else {},
        compiler_params=VMEM_BIG,
        cost_estimate=matmul_cost(n_grp * cols, tokens, hidden, 8 * hidden * n_grp * cols),
        name='wo_grad',
    )(core, ctx_par, dy_a, dy_b, *earlier)


def column_copies(src, out_ref, sem_of, row, places):
    rows, width = src.shape[0], src.shape[1] // len(places)
    for i, col in enumerate(places):
        yield pltpu.make_async_copy(
            src.at[:, run(i, width)],
            out_ref.at[pl.ds(pl.multiple_of(row, BLK), rows), pl.ds(pl.multiple_of(col, HEAD), width)],
            sem_of(i))


def wqkv_grad_kernel(places_of, old_places, wo_tile, n_src, core_ref, na_ref, nb_ref, *rest):
    srcs, rest = rest[:n_src], list(rest[n_src:])
    groups = [ref.at[c] for ref in srcs for c in range(ref.shape[0])]
    recv_refs = [rest.pop(0) for _ in range(len(old_places) + bool(wo_tile))]
    n_buf, rhs, buf, n_sems, g_sems, out_sems, copy_sems, recv_sems, paste_sems, tok_sems, *recv_bufs = rest[-10 - len(recv_refs):]
    outs = rest[:-10 - len(recv_refs)][-4 if wo_tile else -3:]
    out_ref, copy_ref, tok_ref = outs[:3]
    m = pl.program_id(Z)
    n_m = pl.num_programs(Z)
    core, pair = core_ref[Z], core_ref[1]
    tokens, cols = groups[0].shape
    half, rows = tokens // 2, n_buf.shape[2]
    piece = tokens // PIECES
    slot = lax.rem(m, SLOTS)

    def n_loads(step, at):
        for i, ref in enumerate((na_ref, nb_ref)):
            yield pltpu.make_async_copy(ref.at[:, run(step, rows)], n_buf.at[at, run(i, half)], n_sems.at[at, i])

    def g_loads(i):
        for c, ref in enumerate(groups):
            yield pltpu.make_async_copy(ref.at[run(i, piece)], rhs.at[run(i, piece), run(c, cols)], g_sems.at[i, c])

    def stores(step, at):
        yield from column_copies(buf.at[at], out_ref, lambda i: out_sems.at[at, i], step * rows, places_of(core))
        yield pltpu.make_async_copy(buf.at[at], copy_ref.at[run(step, rows)], copy_sems.at[at])

    def recv_loads(step, at):
        for k, (ref, block) in enumerate(zip(recv_refs, recv_bufs)):
            yield pltpu.make_async_copy(ref.at[run(step, block.shape[1])], block.at[at], recv_sems.at[k, at])

    def pastes(step, at):
        for k, old_places_of in enumerate(old_places):
            yield from column_copies(recv_bufs[k].at[at], out_ref, lambda i: paste_sems.at[k, at, i], step * rows, old_places_of(1 - core))
        if wo_tile:
            tiles = recv_bufs[-1].shape[1] // HEAD
            for t in range(tiles):
                tile = wo_tile(step * tiles + t, 1 - core)
                yield pltpu.make_async_copy(recv_bufs[-1].at[at, run(t, HEAD)], outs[3].at[run(tile, HEAD)], paste_sems.at[len(old_places), at, t])

    def token_copies():
        size = tok_ref.shape[0] // 2
        for i in range(2):
            yield pltpu.make_async_copy(rhs.at[pl.ds(pl.multiple_of(i * half + pair * size, BLK), size)], tok_ref.at[run(i, size)], tok_sems.at[i])

    @pl.when(m == Z)
    def _():
        start_all(n_loads(0, 0))
        for i in range(PIECES):
            start_all(g_loads(i))

    @pl.when(m + 1 < n_m)
    def _():
        start_all(n_loads(m + 1, 1 - slot))

    @pl.when(m == 0)
    def _():
        start_all(recv_loads(m, slot))

    @pl.when(m > 0)
    def _():
        wait_all(pastes(m - 1, 1 - slot))

    @pl.when(m + 1 < n_m)
    def _():
        start_all(recv_loads(m + 1, 1 - slot))

    wait_all(recv_loads(m, slot))
    start_all(pastes(m, slot))

    @pl.when(m >= 2)
    def _():
        wait_all(stores(m - 2, slot))

    wait_all(n_loads(m, slot))

    @pl.when(m == Z)
    def _():
        buf[slot] = jnp.zeros((rows, rhs.shape[1]), F32)

        @pl.loop(0, PIECES)
        def _(i):
            wait_all(g_loads(i))
            buf[slot] += dot_tn(n_buf[slot, run(i, piece)], rhs[run(i, piece)])

        start_all(token_copies())

    @pl.when(m > 0)
    def _():
        buf[slot] = dot_tn(n_buf[slot], rhs[...])

    start_all(stores(m, slot))

    @pl.when(m == n_m - 1)
    def _():
        wait_all(stores(m - 1, 1 - slot))
        wait_all(stores(m, slot))
        wait_all(pastes(m, slot))
        wait_all(token_copies())


def weight_grad_qkv(core, places_of, n_a, n_b, srcs, whole, pastes=(), wo=None):
    hidden = n_a.shape[1]
    n_grp, (tokens, cols) = sum(src.shape[0] for src in srcs), srcs[0].shape[1:]
    width = n_grp * cols
    rows = 2 * BLK
    steps = hidden // rows
    args, specs, alias = [core, n_a, n_b, *srcs], [ANY] * (2 + len(srcs)), {}
    outs = [jax.ShapeDtypeStruct((hidden, 3 * hidden), F32), jax.ShapeDtypeStruct((hidden, width), F32), jax.ShapeDtypeStruct((2 * BLK, width), BF16)]
    wo_tile = None
    recvs = [recv for recv, _ in pastes] + ([wo[0]] if wo else [])
    args += recvs
    specs += [ANY] * len(recvs)
    if wo is not None:
        wo_recv, wo_whole, wo_tile = wo
        outs.append(jax.ShapeDtypeStruct(wo_whole.shape, F32))
    if whole is not None:
        alias[len(args)] = 0
        args.append(whole)
        specs.append(ANY)
    if wo is not None:
        alias[len(args)] = 3
        args.append(wo_whole)
        specs.append(ANY)
    return pl.pallas_call(
        functools.partial(wqkv_grad_kernel, places_of, [old for _, old in pastes], wo_tile, len(srcs)),
        grid_spec=pltpu.PrefetchScalarGridSpec(
            num_scalar_prefetch=1,
            grid=(steps,),
            in_specs=specs,
            out_specs=[ANY] * len(outs),
            scratch_shapes=[
                pltpu.VMEM((SLOTS, tokens, rows), BF16),
                pltpu.VMEM((tokens, width), BF16),
                pltpu.VMEM((SLOTS, rows, width), F32),
                dma_sems(SLOTS, SLOTS), dma_sems(PIECES, n_grp), dma_sems(SLOTS, n_grp), dma_sems(SLOTS), dma_sems(SLOTS, SLOTS), dma_sems(SLOTS, SLOTS, n_grp), dma_sems(SLOTS),
                *[pltpu.VMEM((SLOTS, recv.shape[0] // steps, recv.shape[1]), F32) for recv in recvs],
            ],
        ),
        out_shape=outs,
        input_output_aliases=alias,
        compiler_params=VMEM_BIG,
        cost_estimate=matmul_cost(hidden, tokens, width, 16 * hidden * width),
        name='wqkv_grad',
    )(*args)


def normed_grad_kernel(runs, n_src, final, more, cols_ref, *rest):
    srcs, (w_ref, init_ref, *rest) = rest[:n_src], rest[n_src:]
    if final:
        x_ref, affine_ref, dx_ref, sum_ref, acc, w_buf, g_buf, sems, g_sems, init_sem, sum_acc = rest
    else:
        acc, w_buf, g_buf, sems, g_sems, init_sem = rest
    j, steps = pl.program_id(Z), pl.num_programs(Z)
    slot = lax.rem(j, SLOTS)
    rows, width = g_buf.shape[1], g_buf.shape[2] // 2
    rank = cols_ref[2 * steps]

    def w_loads(step, at):
        for i in range(2):
            col = pl.multiple_of(cols_ref[2 * step + i], HEAD)
            yield pltpu.make_async_copy(w_ref.at[:, pl.ds(col, width)], w_buf.at[at, :, run(i, width)], sems.at[at, i])

    def g_loads(step):
        at = step % 2
        for i, (src, grp) in enumerate(runs[part(step, 2)]):
            ref, dst = srcs[src], g_buf.at[at, :, run(i, width)]
            tokens = ref.shape[-2]
            ref = ref.at[:, run(grp, width)] if tokens == rows else ref.at[grp]
            pairs = [(ref, dst)] if tokens == rows else [
                (ref.at[pl.ds(pl.multiple_of(h * (tokens // 2) + rank * (rows // 2), BLK), rows // 2)], dst.at[run(h, rows // 2)]) for h in range(2)]
            for pair in pairs:
                yield pltpu.make_async_copy(*pair, g_sems.at[at, i])

    def g_waits(at):
        for i in range(2):
            block = g_buf.at[at, :, run(i, width)]
            yield pltpu.make_async_copy(block, block, g_sems.at[at, i])

    @pl.when(j == Z)
    def _():
        start_all(w_loads(0, 0))
        start_all(g_loads(0))
        if more:
            init = pltpu.make_async_copy(init_ref, acc, init_sem)
            init.start()
            init.wait()
        else:
            acc[...] = init_ref[...].astype(F32) * ALPHA

    @pl.when(j + 1 < steps)
    def _():
        start_all(w_loads(j + 1, 1 - slot))

    for step in range(1, len(runs) // 2):
        @pl.when(j + 1 == step)
        def _():
            start_all(g_loads(step))

    wait_all(w_loads(j, slot))
    wait_all(g_waits(slot))
    acc[...] += dot_nt(g_buf[slot], w_buf[slot])

    if final:
        @pl.when(j == steps - 1)
        def _():
            sum_acc[...] = jnp.zeros_like(sum_acc)
            gain = affine_ref[:1].astype(F32)

            @pl.loop(0, rows // NORM_ROWS)
            def _(i):
                at = run(i, NORM_ROWS)
                d_n = acc[at]
                x, inv = centred(x_ref[at])
                x = x * inv
                d_x = d_n * gain
                mean = jnp.mean(d_x, axis=-1, keepdims=True)
                slope = jnp.mean(d_x * x, axis=-1, keepdims=True)
                dx_ref[at] = (inv * (d_x - mean - x * slope)).astype(BF16)
                for kind, term in enumerate((d_n * x, d_n)):
                    sum_acc[kind] += jnp.sum(term.reshape((-1,) + sum_acc.shape[1:]), axis=0)

            sum_ref[...] = jnp.sum(sum_acc[...], axis=1)


def normed_grad(cols, runs, srcs, w_qkv, init, norm=None):
    rows, hidden = init.shape
    steps, width = len(runs) // 2, 2 * WIDTH
    flat = pl.BlockSpec((rows, hidden), lambda j, cols: (Z, Z))
    args = [cols, *srcs, w_qkv, init]
    more = init.dtype == F32
    specs = [ANY] * (len(srcs) + 1) + [ANY if more else flat]
    scratch = [pltpu.VMEM((SLOTS, hidden, width), BF16), pltpu.VMEM((SLOTS, rows, width), BF16), dma_sems(SLOTS, SLOTS), dma_sems(SLOTS, SLOTS), pltpu.SemaphoreType.DMA]
    if norm:
        args += list(norm)
        specs += [flat, pl.BlockSpec((2, hidden), lambda j, cols: (Z, Z))]
        outs = [jax.ShapeDtypeStruct((rows, hidden), BF16), jax.ShapeDtypeStruct((2, hidden), F32)]
        out_specs = [flat, pl.BlockSpec((2, hidden), lambda j, cols: (Z, Z))]
        scratch = [pltpu.VMEM((rows, hidden), F32)] + scratch + [pltpu.VMEM((2, 8, hidden), F32)]
    else:
        outs, out_specs = [jax.ShapeDtypeStruct((rows, hidden), F32)], [flat]
    return pl.pallas_call(
        functools.partial(normed_grad_kernel, runs, len(srcs), norm is not None, more),
        grid_spec=pltpu.PrefetchScalarGridSpec(
            num_scalar_prefetch=1,
            grid=(steps,),
            in_specs=specs,
            out_specs=out_specs,
            scratch_shapes=scratch,
        ),
        out_shape=outs,
        compiler_params=VMEM_BIG,
        cost_estimate=matmul_cost(rows, steps * width, hidden),
        name='dn',
    )(*args)


def paste_kernel(places_of, core_ref, recv_ref, _, out_ref, sems):
    row = pl.program_id(Z) * recv_ref.shape[0]
    copies = list(column_copies(recv_ref, out_ref, lambda i: sems.at[i], row, places_of(1 - core_ref[Z])))
    start_all(copies)
    wait_all(copies)


def paste_columns(core, places_of, recv, whole):
    hidden, block = recv.shape
    rows = 2 * BLK
    return pl.pallas_call(
        functools.partial(paste_kernel, places_of),
        grid_spec=pltpu.PrefetchScalarGridSpec(
            num_scalar_prefetch=1,
            grid=(hidden // rows,),
            in_specs=[pl.BlockSpec((rows, block), lambda m, core: (m, Z)), ANY],
            out_specs=ANY,
            scratch_shapes=[dma_sems(8)],
        ),
        out_shape=jax.ShapeDtypeStruct(whole.shape, F32),
        input_output_aliases={2: 0},
        compiler_params=VMEM_BIG,
        name='paste',
    )(core, recv, whole)


def output_kernel(n_chip, core_ref, mine_ref, theirs_ref, shared_ref, other_ref, w_ref, w_shared_ref, na_ref, nb_ref, b_ref, out_ref, acc):
    j, last = pl.program_id(Z), pl.num_programs(Z) - 1
    rows = acc.shape[0]

    def add(ref, weight_ref):
        acc[...] += dot_nn(ref[...].reshape(rows, -1), weight_ref[...])

    @pl.when(j == Z)
    def _():
        acc[...] = jnp.broadcast_to(b_ref[...].astype(F32), acc.shape)

    pl.when(j < n_chip)(functools.partial(add, mine_ref, w_ref))
    pl.when(jnp.logical_and(j >= n_chip, j < CORES * n_chip))(functools.partial(add, theirs_ref, w_ref))
    pl.when(j == last - 1)(functools.partial(add, shared_ref, w_shared_ref))

    @pl.when(j == last)
    def _():
        add(other_ref, w_shared_ref)
        for half, n_ref in enumerate((na_ref, nb_ref)):
            at = part(half, n_ref.shape[0])
            out_ref[at] = (ALPHA * n_ref[...].astype(F32) + acc[at]).astype(BF16)


def project_out(core, ctx_par, ctx_recv, ctx_shared, shared_recv, w_o, n_halves, b_o):
    n_chip, rows, cols = ctx_recv.shape
    shared = shared_recv.shape[1]
    hidden = w_o.shape[1]
    base = CORES * n_chip * cols // shared
    steps = CORES * n_chip + CORES
    split = (CORES, CORES * n_chip, rows // CORES)

    def dist_index(j, core):
        at = jnp.minimum(j, CORES * n_chip - 1)
        return CORES * lax.rem(at, n_chip) + jnp.where(at < n_chip, core[Z], 1 - core[Z])

    def shared_index(j, core):
        return base + jnp.where(j < steps - 1, core[Z], 1 - core[Z])

    whole, half = [pl.BlockSpec((size, hidden), lambda j, core: (Z, Z)) for size in (rows, rows // CORES)]
    return pl.pallas_call(
        functools.partial(output_kernel, n_chip),
        grid_spec=pltpu.PrefetchScalarGridSpec(
            num_scalar_prefetch=1,
            grid=(steps,),
            in_specs=[
                pl.BlockSpec((1, CORES, 1, rows // CORES, cols), lambda j, core: (jnp.minimum(j, n_chip - 1), Z, core[CORES], Z, Z)),
                pl.BlockSpec((1, rows, cols), lambda j, core: (jnp.clip(j - n_chip, 0, n_chip - 1), Z, Z)),
                pl.BlockSpec((CORES, 1, rows // CORES, shared), lambda j, core: (Z, core[CORES], Z, Z)),
                pl.BlockSpec((rows, shared), lambda j, core: (Z, Z)),
                pl.BlockSpec((cols, hidden), lambda j, core: (dist_index(j, core), Z)),
                pl.BlockSpec((shared, hidden), lambda j, core: (shared_index(j, core), Z)),
                half, half,
                pl.BlockSpec((1, hidden), lambda j, core: (Z, Z)),
            ],
            out_specs=whole,
            scratch_shapes=[pltpu.VMEM((rows, hidden), F32)],
        ),
        out_shape=jax.ShapeDtypeStruct((rows, hidden), BF16),
        compiler_params=VMEM_BIG,
        cost_estimate=matmul_cost(rows, hidden, hidden),
        name='out_proj',
    )(core, ctx_par.reshape(n_chip, *split, cols), ctx_recv, ctx_shared.reshape(*split, shared), shared_recv, w_o, w_o, *n_halves, b_o)


def together(*values):
    return lax.optimization_barrier(values)


def solution(mesh):
    n_dev = mesh.shape['sp']
    tok_spec = P('dp', 'sp', None)
    pos_spec = P('dp', 'sp')
    in_specs = (tok_spec, pos_spec, pos_spec, P('dp'), P(), P(), P(), P(), P(), P(), tok_spec)
    out_specs = (tok_spec, tok_spec, P('dp'), P('dp'), P('dp', None), P('dp'), P('dp', None), P('dp'))
    same_core = [list(range(core, n_dev, 2)) for core in range(2)]
    partners = [(dev, dev ^ 1) for dev in range(n_dev)]
    n_chip = n_dev // 2

    def device_step(hidden_in, pos_ids, block_pos, prefix_len, ln_gamma, ln_beta, w_qkv, b_qkv, w_o, b_o, grad_out):
        batch, local_len, hidden = hidden_in.shape
        per_half = batch // 2
        heads = hidden // HEAD
        n_dist, n_shared = (heads - SHARED) // n_dev, SHARED // 2
        shared_at = n_dev * n_dist
        rows = batch * local_len
        tokens = n_dev * rows
        rank = lax.axis_index('sp')
        parity = lax.rem(rank, SLOTS)
        pair = rank + 1 - 2 * parity
        core = jnp.stack([parity, pair, rank]).astype(jnp.int32)
        gather = functools.partial(lax.all_gather, axis_name='sp')
        gather_core = functools.partial(lax.all_gather, axis_name='sp', axis_index_groups=same_core)
        to_partner = functools.partial(lax.ppermute, axis_name='sp', perm=partners)

        def token_rows(arr, dev):
            split = arr.reshape(arr.shape[:-2] + (2, n_dev, rows // 2, arr.shape[-1]))
            return lax.dynamic_index_in_dim(split, dev, axis=split.ndim - 3, keepdims=False).reshape(arr.shape[:-2] + (rows, arr.shape[-1]))

        def places(head):
            return lambda par: [((2 * c + par) * n_dist + head) * WIDTH for c in range(n_chip)]

        def shared_places(par):
            return [(shared_at + par * n_shared + i) * WIDTH for i in range(n_shared)]

        def wo_tile(t, par):
            spread = t - n_shared
            return jnp.where(t < n_shared, shared_at + par * n_shared + t, (2 * (spread // n_dist) + par) * n_dist + lax.rem(spread, n_dist))

        halves = range(2)
        x_flat, affine = hidden_in.reshape(rows, hidden), jnp.stack([ln_gamma, ln_beta])
        n_own = [normalize(half, x_flat, affine) for half in halves]
        dy_own = [grad_out[part(half, per_half)] for half in halves]
        n_own[1], *dy_own = together(n_own[1], *dy_own)
        n_own = [own.reshape(per_half, local_len, hidden) for own in n_own]
        n_a, n_b, dy_a, dy_b = [gather(send) for send in n_own + dy_own]
        cos, sin = rope_tables(prefix_len, n_dev * local_len)
        prefix = [prefix_len[part(half, per_half)] for half in halves]
        starts = jnp.stack([rank * n_dist, shared_at + parity * n_shared, rank, pair]).astype(jnp.int32)
        bias = jnp.concatenate([
            lax.dynamic_slice_in_dim(b_qkv, starts[0] * WIDTH, n_dist * WIDTH),
            lax.dynamic_slice_in_dim(b_qkv, starts[1] * WIDTH, n_shared * WIDTH)]).astype(F32).reshape(1, -1)
        grad_bo = jnp.sum(grad_out.astype(F32), axis=(0, 1))
        n_chip_rows = [own[None] for own in n_own + [to_partner(own) for own in n_own]]
        qkv_own = project_qkv(starts, n_dist, n_shared, n_chip_rows, w_qkv, bias, cos, sin)
        d_ctx_own = context_grad(starts, n_dist, n_shared, [own[None] for own in (grad_out, to_partner(grad_out))], w_o, n_dev)
        n_a, grad_bo, *d_ctx_own = together(n_a, grad_bo, *d_ctx_own)

        ctx_d = ctx_r = None
        qkv, lses = [], []
        for half in halves:
            if half:
                n_b, ctx_r = together(n_b, ctx_r)
            qd, kd, vd, qr, kr, vr = project_qkv(
                starts, n_dist, n_shared, [n_b if half else n_a], w_qkv, bias, cos, sin, half, qkv_own[part(half, QKV_IN)])
            ctx_d, lse_d = attention_forward(half, prefix[half], qd, kd, vd, n_dev, ctx_d)
            qr, ctx_d = together(qr, ctx_d)
            ctx_r, lse_r = attention_forward(half, prefix[half], qr, kr, vr, n_dev, ctx_r)
            qkv.append((qd, kd, vd, qr, kr, vr))
            lses.append((lse_d, lse_r))
        ctx_par = gather_core(ctx_d.reshape(tokens, n_dist * HEAD))

        dy_a, ctx_r = together(dy_a, ctx_r)
        g_d, g_r = [], []
        sums = []
        for half in halves:
            if half:
                dy_b, *g_r = together(dy_b, *g_r)
            qd, kd, vd, qr, kr, vr = qkv[half]
            d_ctx, d_ctx_r = context_grad(starts, n_dist, n_shared, [dy_b if half else dy_a], w_o, n_dev, d_ctx_own[part(half, CORES)])
            *g_d, sum_d = attention_backward(half, n_dist, prefix[half], qd, kd, vd, ctx_d, d_ctx, lses[half][0], cos, sin, g_d)
            qr, *g_d = together(qr, *g_d)
            *g_r, sum_r = attention_backward(half, n_shared, prefix[half], qr, kr, vr, ctx_r, d_ctx_r, lses[half][1], cos, sin, g_r)
            sums.append(jnp.sum(jnp.concatenate([sum_d, sum_r]), axis=(1, 2)).reshape(-1))
        g_par = [gather_core(g.reshape(tokens, WIDTH)) for g in g_d]
        g_r = [g.reshape(1, tokens, WIDTH) for g in g_r]

        n_a, n_b, dy_a, dy_b = [part.reshape(tokens // 2, hidden) for part in (n_a, n_b, dy_a, dy_b)]
        ctx_r = ctx_r.reshape(tokens, n_shared * HEAD)
        shared_recv = to_partner(token_rows(ctx_r, pair))
        ctx_r, *g_r = together(ctx_r, *g_r)
        grad_wo, wo_block = weight_grad_o(
            core, ctx_r[None], dy_a, dy_b, lambda c, par: (shared_at + par * n_shared) * HEAD, lambda c: 0, hidden // 2, ())
        shared_recv, wo_block, n_a = together(shared_recv, wo_block, n_a)
        grad_wqkv, block, r_send = weight_grad_qkv(core, shared_places, n_a, n_b, g_r, None)
        r_recv, ctx_recv = to_partner(r_send), to_partner(token_rows(ctx_par, pair))
        ctx_par, block = together(ctx_par, block)
        recv_r = to_partner(block)
        grad_wo, wo_block = weight_grad_o(
            core, ctx_par, dy_a, dy_b, lambda c, par: (2 * c + par) * (n_dist * HEAD), lambda c: (n_shared + c * n_dist) * HEAD,
            hidden // 2, (grad_wo, wo_block))
        ctx_recv, wo_block, recv_r, r_recv = together(ctx_recv, wo_block, recv_r, r_recv)
        wo_recv = to_partner(wo_block)
        hidden_out = project_out(
            core, ctx_par, ctx_recv, ctx_r, shared_recv, w_o, [own.reshape(-1, hidden) for own in n_own], b_o.reshape(1, hidden))
        n_a, hidden_out, g_par[0] = together(n_a, hidden_out, g_par[0])

        def columns(table):
            at = [np.array([h * WIDTH for h in table(par)] + [0], np.int32) for par in range(2)]
            last = (np.arange(at[0].size) == at[0].size - 1).astype(np.int32)
            return jnp.asarray(at[0]) + parity.astype(jnp.int32) * jnp.asarray(at[1] - at[0]) + rank.astype(jnp.int32) * jnp.asarray(last)

        def spread_grad(head, whole, **extra):
            whole, block, tok, *rest = weight_grad_qkv(core, places(head), n_a, n_b, [g_par[head]], whole, **extra)
            tok = to_partner(tok)
            if head:
                tok, block = together(tok, block)
            return whole, tok, to_partner(block), rest

        grad_wqkv, tok_0, recv_0, _ = spread_grad(0, grad_wqkv, pastes=[(recv_r, shared_places)])
        g_r[0], grad_wqkv = together(g_r[0], grad_wqkv)
        cols = columns(lambda mine: [shared_at + par * n_shared + i for par in (mine, 1 - mine) for i in range(n_shared)])
        runs = [(i, 0) for i in range(n_shared)] + [(n_shared, i) for i in range(n_shared)]
        d_norm, = normed_grad(cols, runs, [*g_r, r_recv], w_qkv, grad_out.reshape(rows, hidden))
        g_par[1], d_norm = together(g_par[1], d_norm)
        wo_recv, tok_0 = together(wo_recv, tok_0)
        grad_wqkv, tok_1, recv_1, (grad_wo,) = spread_grad(1, grad_wqkv, wo=(wo_recv, grad_wo, wo_tile))
        cols = columns(lambda mine: [(2 * c + par) * n_dist + head for par in (mine, 1 - mine) for c in range(n_chip) for head in (0, 1)])
        runs = [(CORES * side + head, c) for side in range(CORES) for c in range(n_chip) for head in (0, 1)]
        tok_1, recv_0 = together(tok_1, recv_0)
        d_norm, = normed_grad(cols, runs, [g_par[0], g_par[1], tok_0, tok_1], w_qkv, d_norm)
        n_a, d_norm, g_par[2] = together(n_a, d_norm, g_par[2])
        grad_wqkv, tok_2, recv_2, _ = spread_grad(2, grad_wqkv, pastes=[(recv_0, places(0)), (recv_1, places(1))])
        cols = columns(lambda mine: [(2 * c + par) * n_dist + 2 for c in range(n_chip) for par in (mine, 1 - mine)])
        grad_in, norm_sums = normed_grad(
            cols, [(src, c) for c in range(n_chip) for src in range(2)], [g_par[2], tok_2], w_qkv, d_norm, norm=(x_flat, affine))
        small = gather(jnp.concatenate([sums[0] + sums[1], norm_sums.reshape(-1), grad_bo]))
        recv_2, small = together(recv_2, small)
        grad_wqkv = paste_columns(core, places(2), recv_2, grad_wqkv)
        spread, shared = small[:, :n_dist * WIDTH], small[:2, n_dist * WIDTH:(n_dist + n_shared) * WIDTH]
        grad_bqkv = jnp.concatenate([spread.reshape(-1), shared.reshape(-1)])
        grad_gamma, grad_beta, grad_bo = jnp.sum(small[:, (n_dist + n_shared) * WIDTH:], axis=0).reshape(3, hidden)
        shape = (batch, local_len, hidden)
        return (hidden_out.reshape(shape), grad_in.reshape(shape), grad_gamma, grad_beta, grad_wqkv, grad_bqkv, grad_wo, grad_bo)

    return jax.shard_map(device_step, mesh=mesh, in_specs=in_specs, out_specs=out_specs, check_vma=False)
```
